32 devices in a mesh: lat: 8 (over z, y), lon: 4 (over x, core).
Axes of the slice: x: 2, y: 2, z: 4, core: 2. Of those that a mesh axis runs over, the one named last changes fastest.
Arguments:
- block_in: bfloat16 [192, 720, 641], P('lat', 'lon'), may hold values from -6 to 6
- noise: bfloat16 [8, 192, 720], P(None, 'lat', 'lon'), may hold values from -6 to 6
- cotangent: bfloat16 [192, 720, 641], P('lat', 'lon'), may hold values from -6 to 6
- band_heights: int32 [8], replicated, may hold values from 1 to 24, 144 in all
- support_lon: int32 [192, 12], P('lat'), may hold values from -2 to 2
- support_vals: float32 [192, 12, 9], P('lat'), may hold values from -4 to 4
- master: float32 [1658880], P(('lat', 'lon')), as said below
- moment_one: float32 [1658880], P(('lat', 'lon')), may hold values from -1.335144e-05 to 1.335144e-05
- moment_two: float32 [1658880], P(('lat', 'lon')), may hold values from 1.808449e-14 to 1.8084491e-13
- average: float32 [1658880], P(('lat', 'lon')), may hold values from -0.75 to 0.75
- step_count: int32 [1], replicated, may hold values from 1 to 20
Outputs:
- block_out: bfloat16 [192, 720, 641], P('lat', 'lon')
- grad_in: float32 [192, 720, 641], P('lat', 'lon')
- grad_flat: float32 [1658880], P(('lat', 'lon'))
- grad_norm: float32 [1], replicated
- new_master: float32 [1658880], P(('lat', 'lon'))
- new_one: float32 [1658880], P(('lat', 'lon'))
- new_two: float32 [1658880], P(('lat', 'lon'))
- new_avg: float32 [1658880], P(('lat', 'lon'))
- copies: bfloat16 [1658880], P(('lat', 'lon'))
The draws below stay inside these ranges and needn't reach their ends.
Inputs may be any that keep to these rules, and one draw needn't show every extreme that they name: `band_heights`: every band has at least one used row and together they hold 144 rows; some band is full. `master`: packed weights.
All inputs are finite; a program needn't handle non-finite values.
Results may differ from the reference program's by a relative error of at most 0.0014.
The reference program's roundings to bfloat16 on the way count: a program that leaves them out, or rounds other values in their place, can miss the bound.
Values may be sent and summed in bfloat16 or wider, within the bound.
A program may use at most 448 MiB of HBM per device.

```python
import math
import jax
import jax.numpy as jnp
import numpy as np
from jax import lax

C = 641
FF = 1282
NOISE = 8
K = 9
S = 12
LON_REACH = 2
ROWS_CAP = 24
HG = 192
WG = 720
HLAT = 144
PFLAT = 1658880
N_LAT = 8


def draw_master(key, part):
    position = jnp.arange(PFLAT)
    baseline = jnp.clip(jax.random.normal(key, (PFLAT,), jnp.float32), -3.0, 3.0)
    bound_one = C * FF
    bound_two = 2 * C * FF
    bound_bias = bound_two + FF
    bound_out = bound_bias + C
    bound_gain = bound_out + C
    bound_disco = bound_gain + K * C
    bound_noise = bound_disco + NOISE * C
    spread_scale = jnp.where(position < bound_one, C ** (-0.5), jnp.where(position < bound_two, FF ** (-0.5), jnp.where(position < bound_out, 0.3, jnp.where(position < bound_gain, 0.25, jnp.where(position < bound_disco, K ** (-0.5), jnp.where(position < bound_noise, NOISE ** (-0.5), 0.02))))))
    drawn = baseline * spread_scale
    drawn = jnp.where((position >= bound_out) & (position < bound_gain), 1.0 + drawn, drawn)
    return drawn.astype(jnp.float32)


def set_ends(values, stream_key, smallest, top_value):
    spot = [jax.random.randint(jax.random.fold_in(stream_key, axis), (), 0, length) for axis, length in enumerate(values.shape)]
    widest = values.shape.index(max(values.shape))
    next_to = spot[:widest] + [(spot[widest] + 1) % values.shape[widest]] + spot[widest + 1:]
    return values.at[tuple(spot)].set(smallest).at[tuple(next_to)].set(top_value)


def level_of(own_key, extent, split, low, top_value):
    loudness, own = 1.0, jax.random.fold_in(own_key, 6)
    for axis_at, shards_of in split:
        steps = jnp.exp(jax.random.uniform(jax.random.fold_in(own, axis_at), (shards_of,), jnp.float32, low / len(split), top_value / len(split)))
        loudness = loudness * jnp.repeat(steps, extent[axis_at] // shards_of).reshape([-1 if axis == axis_at else 1 for axis in range(len(extent))])
    return loudness


def profile(count, total, most, lean):
    weights = [(1 << 20) // math.isqrt(rank ** lean) + 1 for rank in range(2, count + 1)]
    surplus, counts = total - most - (count - 1), [1] * (count - 1)
    while surplus > 0:
        candidates = [i for i in range(count - 1) if counts[i] < most]
        whole, left = sum([weights[i] for i in candidates]), surplus
        for i in candidates:
            addition = min(most - counts[i], max(1, left * weights[i] // whole), surplus)
            counts[i] = counts[i] + addition
            surplus = surplus - addition
    return np.array([most] + counts)


def uneven_parts(rng, number_of, total, most, lean):
    if number_of == 2:
        one = jax.random.randint(rng, (), max(1, total - most), min(most, total - 1) + 1)
        return jnp.stack([one, total - one])
    sizes = jnp.asarray(profile(number_of, total, most, lean), jnp.int32)
    pairs = (number_of - 1) // 2
    source_of, sink = sizes[1:1 + 2 * pairs:2], sizes[2:2 + 2 * pairs:2]
    margin = jnp.minimum(source_of - 1, most - sink)
    shifted = jax.random.randint(jax.random.fold_in(rng, 1), (pairs,), 0, 1 << 20) % (margin + 1)
    sizes = sizes.at[1:1 + 2 * pairs:2].set(source_of - shifted).at[2:2 + 2 * pairs:2].set(sink + shifted)
    return sizes[jax.random.permutation(jax.random.fold_in(rng, 2), number_of)]


def scatter_about(own_key, dims, width, bound, cuts=(), held_as=jnp.bfloat16):
    result = width * jax.random.normal(own_key, dims, jnp.float32)
    if cuts:
        result = result * level_of(own_key, dims, cuts, -0.22, 0.18)
    return jnp.clip(result, -bound, bound).astype(held_as)


def setup_inputs(seed: int = 0) -> dict:
    key_of = jax.random.split(jax.random.key(seed), 12)
    return {
        "block_in": scatter_about(key_of[0], (HG, WG, C), 1.0, 6.0, ((0, 8), (1, 4))),
        "noise": scatter_about(key_of[1], (NOISE, HG, WG), 1.0, 6.0, ((1, 8), (2, 4))),
        "cotangent": scatter_about(key_of[2], (HG, WG, C), 1.0, 6.0, ((0, 8), (1, 4))),
        "band_heights": uneven_parts(key_of[3], N_LAT, HLAT, ROWS_CAP, 1).astype(jnp.int32),
        "support_lon": set_ends(jax.random.randint(key_of[4], (HG, S), -2, 3), jax.random.fold_in(key_of[4], 1), -2, 2).astype(jnp.int32),
        "support_vals": scatter_about(key_of[5], (HG, S, K), 0.3, 4.0, ((0, 8),), jnp.float32),
        "master": draw_master(jax.random.fold_in(key_of[11], 71), 0),
        "moment_one": scatter_about(key_of[7], (PFLAT,), (0.0012 / PFLAT ** 0.5), 1.33514404296875e-05, ((0, 32),), jnp.float32),
        "moment_two": jnp.clip(jnp.exp(math.log(1.8084490881805498e-13) - 2.3025851 * jax.random.uniform(key_of[8], (PFLAT,), jnp.float32) ** level_of(key_of[8], (PFLAT,), ((0, 32),), -0.2, 0.2)), 1.808449054299232e-14, 1.8084490881805498e-13),
        "average": scatter_about(key_of[9], (PFLAT,), 0.05, 0.75, ((0, 32),), jnp.float32),
        "step_count": jax.random.randint(key_of[10], (1,), 1, 21).astype(jnp.int32),
    }


@jax.custom_vjp
def low(v):
    return lax.optimization_barrier(v.astype(jnp.bfloat16)).astype(jnp.float32)

@jax.custom_vjp
def low_back(v):
    return v

def low_keep(v):
    return (low(v), None)

def low_pass(kept, grad):
    return (grad,)

def back_keep(v):
    return (v, None)

def back_low(kept, grad):
    return (low(grad),)
low.defvjp(low_keep, low_pass)
low_back.defvjp(back_keep, back_low)
highest_precision = lax.Precision.HIGHEST

def unpack(flat):
    shapes = ((C, FF), (FF, C), (FF,), (C,), (C,), (K, C), (NOISE, C))
    pieces = []
    offset = 0
    for layout in shapes:
        amount = math.prod(layout)
        pieces.append(flat[offset:offset + amount].reshape(layout))
        offset = offset + amount
    return pieces

def stencil_table(support_vals, support_lon):
    lat_rows = (jnp.arange(S) % 3 - 1)[:, None] == jnp.arange(-1, 2)[None, :]
    lon_rows = support_lon[:, :, None] == jnp.arange(-LON_REACH, LON_REACH + 1)[None, None, :]
    return jnp.einsum('hsk,sl,hsw->hlwk', support_vals.astype(jnp.float32), lat_rows.astype(jnp.float32), lon_rows.astype(jnp.float32), precision=highest_precision)

def reference(block_in, noise, cotangent, band_heights, support_lon, support_vals, master, moment_one, moment_two, average, step_count):
    slot_valid = (jnp.arange(ROWS_CAP)[None, :] < band_heights[:, None]).reshape(-1)
    latitude = jnp.cumsum(slot_valid.astype(jnp.int32)) - 1
    target = jnp.where(slot_valid, latitude, HLAT).astype(jnp.int32)

    def compact(array):
        holder = jnp.zeros((HLAT + 1,) + array.shape[1:], array.dtype)
        return holder.at[target].set(array)[:HLAT]

    def spread(array):
        source = jnp.clip(target, 0, HLAT - 1).astype(jnp.int32)
        picked = array[source]
        return jnp.where(slot_valid[:, None, None], picked, jnp.zeros_like(picked))
    inputs = compact(block_in.astype(jnp.float32))
    upstream = compact(cotangent.astype(jnp.float32))
    forcing = compact(jnp.moveaxis(noise.astype(jnp.float32), 0, 2))
    stencil = stencil_table(compact(support_vals), compact(support_lon))

    def forward(inputs, master):
        w_one, w_two, bias_one, bias_two, gain, w_disco, w_noise = [low(piece) for piece in unpack(master)]
        center = inputs - lax.optimization_barrier(jnp.mean(inputs, -1, keepdims=True))
        variance = lax.optimization_barrier(jnp.mean(center * center, -1, keepdims=True))
        normed = center * lax.rsqrt(variance + 1e-05)
        mixed_in = low(normed * gain)
        padded = jnp.pad(mixed_in, ((1, 1), (0, 0), (0, 0)))
        padded = jnp.concatenate([padded[:, WG - LON_REACH:], padded, padded[:, :LON_REACH]], 1)
        kernel = jnp.einsum('hlwk,kc->hlwc', stencil, w_disco, precision=highest_precision)
        convolved = jnp.einsum('hwn,nc->hwc', forcing, w_noise, precision=highest_precision)
        for lat_tap in range(3):
            for lon_tap in range(2 * LON_REACH + 1):
                convolved = convolved + kernel[:, lat_tap, lon_tap][:, None, :] * padded[lat_tap:lat_tap + HLAT, lon_tap:lon_tap + WG]
        conv_low = low(convolved)
        hidden = low_back(jnp.einsum('hwc,cf->hwf', conv_low, w_one, precision=highest_precision) + bias_one)
        active = low(jax.nn.gelu(hidden, approximate=True))
        branch = jnp.einsum('hwf,fc->hwc', active, w_two, precision=highest_precision) + bias_two
        return inputs + branch
    outputs, pullback = jax.vjp(forward, inputs, master)
    grad_in, grad_flat = pullback(upstream)
    norm_square = jnp.sum(grad_flat * grad_flat)
    grad_norm = jnp.sqrt(norm_square)
    factor = 0.01 / jnp.maximum(grad_norm, 0.01)
    clipped = grad_flat * factor
    new_one = 0.9 * moment_one + 0.1 * clipped
    new_two = 0.999 * moment_two + 0.001 * clipped * clipped
    step_float = step_count[0].astype(jnp.float32)
    fix_one = 1.0 - jnp.power(jnp.float32(0.9), step_float)
    fix_two = 1.0 - jnp.power(jnp.float32(0.999), step_float)
    update = new_one / fix_one / (jnp.sqrt(new_two / fix_two) + 1e-08) + 0.1 * master
    new_master = master - 0.02 * update
    new_avg = 0.9 * average + 0.1 * new_master
    return (spread(outputs).astype(jnp.bfloat16), spread(grad_in), grad_flat, grad_norm.reshape(1), new_master, new_one, new_two, new_avg, new_master.astype(jnp.bfloat16))
```

```python
from functools import partial
import math

import jax
import jax.numpy as jnp
from jax import lax
from jax.experimental import pallas as pl
from jax.experimental.pallas import tpu as pltpu
from jax.sharding import PartitionSpec as P

C = 641
FF = 1282
NOISE = 8
K = 9
S = 12
REACH = 2
LANES = 128
CB = 6
CP = CB * LANES
FB = 11
FP = FB * LANES
TAPS = 15
MESH = pl.DeviceIdType.MESH
HIGHEST = lax.Precision.HIGHEST
F32 = jnp.float32
BF16 = jnp.bfloat16
VMEM_LIMIT = 60 * 1024 * 1024
ROW_TWO = (C * FF) // LANES
LANE_TWO = (C * FF) % LANES
TAIL_ROW = (2 * C * FF) // LANES
OFF_B1 = 2 * C * FF
OFF_B2 = OFF_B1 + FF
OFF_GAIN = OFF_B2 + C
OFF_DISCO = OFF_GAIN + C
OFF_NOISE = OFF_DISCO + K * C
END_FLAT = OFF_NOISE + NOISE * C


def params(**kw):
    return pltpu.CompilerParams(vmem_limit_bytes=VMEM_LIMIT, **kw)


def any_spec():
    return pl.BlockSpec(memory_space=pl.ANY)


def vmem_spec():
    return pl.BlockSpec(memory_space=pltpu.VMEM)


def iota(shape, dim):
    return lax.broadcasted_iota(jnp.int32, shape, dim)


def bit_list(mesh):
    bits = []
    for axis in ("lat", "lon"):
        count = int(math.log2(mesh.shape[axis]))
        assert 1 << count == mesh.shape[axis]
        bits += [(axis, b) for b in reversed(range(count))]
    return bits


def my_bits(bits):
    ids = {"lat": lax.axis_index("lat"), "lon": lax.axis_index("lon")}
    return [(ids[a] >> b) & 1 for a, b in bits]


def partner(axis, bit):
    lat, lon = lax.axis_index("lat"), lax.axis_index("lon")
    if axis == "lat":
        return (lat ^ (1 << bit), lon)
    return (lat, lon ^ (1 << bit))


def stage_orders(mesh):
    bits = bit_list(mesh)
    n = len(bits)
    if (mesh.shape["lat"], mesh.shape["lon"]) == (8, 4):
        return [[0, 1, 2, 3, 4], [0, 1, 3, 2, 4]]
    order = list(range(n))
    return [order, order]


def rotl_rows(v, unit):
    row = iota((8, LANES), 0)
    for b in range(3):
        amount = unit << b
        v = jnp.where((row >> b) & 1 == 1, pltpu.roll(v, LANES - amount, 1), v)
    return v


def row_vector(flat_ref, offset, length):
    blocks = -(-length // LANES)
    row, shift = divmod(offset, LANES)
    near = flat_ref[row : row + blocks, :]
    if shift:
        far = flat_ref[row + 1 : row + 1 + blocks, :]
        lane = iota((blocks, LANES), 1)
        near = pltpu.roll(jnp.where(lane >= shift, near, far), LANES - shift, 1)
    index = iota((blocks, LANES), 0) * LANES + iota((blocks, LANES), 1)
    return jnp.where(index < length, near, 0.0)


def put_row(ref, row, value):
    for q in range(value.shape[0]):
        ref[row : row + 1, q * LANES : (q + 1) * LANES] = value[q : q + 1, :].astype(ref.dtype)


def unpack_weights(flat, w1, w2, wn, wd, small, wnf):
    lane = iota((8, LANES), 1)
    row = iota((8, LANES), 0)

    def half_one(r0, q):
        start = 10 * r0 + q + r0 // 64
        near = flat[pl.ds(start, 8, stride=10), :]
        far = flat[pl.ds(start + 1, 8, stride=10), :]
        s0 = (2 * r0) % LANES
        v = jnp.where(lane >= s0 + 2 * row, near, far)
        v = rotl_rows(pltpu.roll(v, (LANES - s0) % LANES, 1), 2)
        ok = r0 + row < C
        if q == FB - 1:
            ok = ok & (lane < FF - (FB - 1) * LANES)
        return jnp.where(ok, v, 0.0)

    def body_one(a, carry):
        r0 = a * 16
        for q in range(FB):
            v = jnp.concatenate([half_one(r0, q), half_one(r0 + 8, q)], 0)
            w1[pl.ds(pl.multiple_of(r0, 16), 16), q * LANES : (q + 1) * LANES] = v.astype(BF16)
        return carry

    groups = -(-C // 16)
    lax.fori_loop(0, groups, body_one, 0)
    w1[groups * 16 :, :] = jnp.zeros((CP - groups * 16, FP), BF16)

    def half_two(r0, q):
        start = ROW_TWO + 5 * r0 + q + (LANE_TWO + r0) // LANES
        v0 = flat[pl.ds(start, 8, stride=5), :]
        v1 = flat[pl.ds(start + 1, 8, stride=5), :]
        v2 = flat[pl.ds(start + 2, 8, stride=5), :]
        s0 = (LANE_TWO + r0) % LANES
        s = s0 + row
        v = jnp.where(lane >= s, v0, jnp.where(lane >= s - LANES, v1, v2))
        v = rotl_rows(pltpu.roll(v, (LANES - s0) % LANES, 1), 1)
        ok = r0 + row < FF
        if q == CB - 1:
            ok = ok & (lane < C - (CB - 1) * LANES)
        return jnp.where(ok, v, 0.0)

    def body_two(a, carry):
        r0 = a * 16
        for q in range(CB):
            v = jnp.concatenate([half_two(r0, q), half_two(r0 + 8, q)], 0)
            w2[pl.ds(pl.multiple_of(r0, 16), 16), q * LANES : (q + 1) * LANES] = v.astype(BF16)
        return carry

    groups = -(-FF // 16)
    lax.fori_loop(0, groups, body_two, 0)
    w2[groups * 16 :, :] = jnp.zeros((FP - groups * 16, CP), BF16)
    small[...] = jnp.zeros_like(small)
    put_row(small, 0, row_vector(flat, OFF_B1, FF))
    put_row(small, 1, row_vector(flat, OFF_B2, C))
    put_row(small, 2, row_vector(flat, OFF_GAIN, C))
    wd[...] = jnp.zeros_like(wd)
    wnf[...] = jnp.zeros_like(wnf)
    for k in range(K):
        put_row(wd, k, row_vector(flat, OFF_DISCO + k * C, C))
    for k in range(NOISE):
        put_row(wnf, 1 + k, row_vector(flat, OFF_NOISE + k * C, C))
    wn[...] = wnf[...].astype(BF16)


def neighbours():
    lat, lon = lax.axis_index("lat"), lax.axis_index("lon")
    nlat, nlon = lax.axis_size("lat"), lax.axis_size("lon")
    return lat, lon, nlat, nlon, lax.rem(lon + 1, nlon), lax.rem(lon + nlon - 1, nlon)


def halo_copies(cols, rows, corners, colh, rowh, cornh, send, recv):
    lat, lon, nlat, nlon, east, west = neighbours()
    out = []

    def add(src, dst, target, k, sends, gets):
        out.append(
            (
                sends,
                gets,
                pltpu.make_async_remote_copy(
                    src_ref=src,
                    dst_ref=dst,
                    send_sem=send.at[k],
                    recv_sem=recv.at[k],
                    device_id=target,
                    device_id_type=MESH,
                ),
            )
        )

    has_up, has_down = lat > 0, lat < nlat - 1
    up, down = lat - 1, lat + 1
    add(rows.at[0], rowh.at[1], (up, lon), 2, has_up, has_down)
    add(rows.at[1], rowh.at[0], (down, lon), 3, has_down, has_up)
    add(cols.at[0], colh.at[1], (lat, west), 0, None, None)
    add(cols.at[1], colh.at[0], (lat, east), 1, None, None)
    add(corners.at[0, 0], cornh.at[1, 1], (up, west), 4, has_up, has_down)
    add(corners.at[0, 1], cornh.at[1, 0], (up, east), 5, has_up, has_down)
    add(corners.at[1, 0], cornh.at[0, 1], (down, west), 6, has_down, has_up)
    add(corners.at[1, 1], cornh.at[0, 0], (down, east), 7, has_down, has_up)
    return out


def start_halo(copies):
    for sends, _, copy in copies:
        if sends is None:
            copy.start()
        else:
            pl.when(sends)(copy.start)


def wait_halo(copies):
    for sends, gets, copy in copies:
        if sends is None:
            copy.wait()
        else:
            pl.when(sends)(copy.wait_send)
            pl.when(gets)(copy.wait_recv)


def greet(bits, halo):
    barrier = pltpu.get_barrier_semaphore()
    lat, lon, nlat, nlon, east, west = neighbours()

    def hello(target):
        pl.semaphore_signal(barrier, inc=1, device_id=target, device_id_type=MESH)

    count = 0
    for axis, bit in bits:
        hello(partner(axis, bit))
        count += 1
    if halo:
        for target in ((lat, east), (lat, west)):
            hello(target)
            count += 1
        for side, cond in ((lat - 1, lat > 0), (lat + 1, lat < nlat - 1)):

            @pl.when(cond)
            def _(side=side):
                for x in (lon, east, west):
                    hello((side, x))

    if halo:
        count = count + 3 * (lat > 0).astype(jnp.int32) + 3 * (lat < nlat - 1).astype(jnp.int32)
    pl.semaphore_wait(barrier, count)


def gather_kernel(
    mesh, share_ref, cols, rows, corners,
    w1, w2, wn, wd, small, colh, rowh, cornh,
    buf, flat, wnf, send, recv, hsend, hrecv, local_sem,
):
    bits = bit_list(mesh)
    orders = stage_orders(mesh)
    mine = my_bits(bits)
    n = len(bits)
    shard_rows = share_ref.shape[0]
    cut = (shard_rows // 2 + 15) // 16 * 16
    spans = [(0, cut), (cut, shard_rows - cut)]
    own = pltpu.make_async_copy(share_ref, buf.at[tuple(mine)], local_sem)
    own.start()
    greet(bits, True)
    halos = halo_copies(cols, rows, corners, colh, rowh, cornh, hsend, hrecv)

    def copy(colour, k):
        order = orders[colour]
        done = order[:k]
        start, count = spans[colour]
        index = tuple(slice(None) if i in done else mine[i] for i in range(n)) + (
            pl.ds(start, count),
        )
        return pltpu.make_async_remote_copy(
            src_ref=buf.at[index],
            dst_ref=buf.at[index],
            send_sem=send.at[colour, k],
            recv_sem=recv.at[colour, k],
            device_id=partner(*bits[order[k]]),
            device_id_type=MESH,
        )

    own.wait()
    for colour in range(2):
        copy(colour, 0).start()
    start_halo(halos)
    for k in range(n):
        for colour in range(2):
            copy(colour, k).wait()
            if k + 1 < n:
                copy(colour, k + 1).start()
    wait_halo(halos)
    lat, _, nlat, *_ = neighbours()
    for r, cond in ((0, lat == 0), (1, lat == nlat - 1)):

        @pl.when(cond)
        def _(r=r):
            rowh[r] = jnp.zeros(rowh.shape[1:], rowh.dtype)
            for s in range(2):
                cornh[r, s] = jnp.zeros(cornh.shape[2:], cornh.dtype)

    total = 1 << n

    def widen(d, carry):
        index = tuple((d >> (n - 1 - i)) & 1 for i in range(n))
        flat[pl.ds(d * shard_rows, shard_rows), :] = buf[index].astype(F32)
        return carry

    lax.fori_loop(0, total, widen, 0)
    flat[total * shard_rows :, :] = jnp.zeros((flat.shape[0] - total * shard_rows, LANES), F32)
    unpack_weights(flat, w1, w2, wn, wd, small, wnf)


def gather_weights(mesh, share, cols, rows, corners):
    bits = bit_list(mesh)
    n = len(bits)
    shard_rows = share.shape[0]
    total = shard_rows << n
    sd = jax.ShapeDtypeStruct
    return pl.pallas_call(
        partial(gather_kernel, mesh),
        name="gather_weights",
        out_shape=(
            sd((CP, FP), BF16),
            sd((FP, CP), BF16),
            sd((LANES, CP), BF16),
            sd((16, CP), F32),
            sd((8, FP), F32),
            sd(cols.shape, BF16),
            sd(rows.shape, BF16),
            sd(corners.shape, BF16),
        ),
        in_specs=[vmem_spec()] * 4,
        out_specs=(vmem_spec(),) * 8,
        scratch_shapes=[
            pltpu.VMEM((2,) * n + (shard_rows, LANES), BF16),
            pltpu.VMEM((total + 96, LANES), F32),
            pltpu.VMEM((LANES, CP), F32),
            pltpu.SemaphoreType.DMA((2, n)),
            pltpu.SemaphoreType.DMA((2, n)),
            pltpu.SemaphoreType.DMA((8,)),
            pltpu.SemaphoreType.DMA((8,)),
            pltpu.SemaphoreType.DMA,
        ],
        compiler_params=params(collective_id=0, has_side_effects=True),
    )(share, cols, rows, corners)


def norm_parts(x):
    mean = jnp.mean(x, -1, keepdims=True)
    center = x - mean
    var = jnp.mean(center * center, -1, keepdims=True)
    return center, lax.rsqrt(var + 1e-05)


def rounded(v):
    return v.astype(BF16).astype(F32)


def stencil_fwd_kernel(
    chunks, cells, height_ref, x_ref, colh, rowh, cornh, table, wd, gain, aug, wn,
    out_ref, m_scr, k_scr, nt_scr,
):
    step = pl.program_id(0)
    rows = x_ref.shape[1]
    width = chunks * cells
    height = height_ref[0]
    slots = m_scr.shape[2] // (width + 2 * REACH) if m_scr.ndim == 3 else 32
    gvec = gain[2:3, :C]

    def bottom_mix(j, base):
        return base

    def put_cell(column, x, top, low):
        center, inv = norm_parts(x)
        mixed = rounded(center * inv * gvec)
        hrow = iota((rows, C), 0)
        mixed = jnp.where(hrow < height, mixed, jnp.where(hrow == height, low, 0.0))
        for g in range(CB):
            lo, hi = g * LANES, min((g + 1) * LANES, C)
            m_scr[g, column, 1 : rows + 1, : hi - lo] = mixed[:, lo:hi]
            m_scr[g, column, 0:1, : hi - lo] = top[:, lo:hi]
            m_scr[g, column, rows + 1 : rows + 2, : hi - lo] = low[:, lo:hi]

    def halo_mix(v):
        center, inv = norm_parts(v.astype(F32))
        return rounded(center * inv * gvec)

    @pl.when(step == 0)
    def _():
        k_scr[...] = jnp.dot(
            table[...], wd[...], preferred_element_type=F32, precision=HIGHEST
        ).reshape(k_scr.shape)
        lat = lax.axis_index("lat")
        for side in range(2):
            for i in range(REACH):
                column = i if side == 0 else width + REACH + i
                top = halo_mix(cornh[0, side])[i : i + 1]
                low = halo_mix(cornh[1, side])[i : i + 1]
                put_cell(column, colh[side, i].astype(F32), top, low)

    @pl.when(step < chunks)
    def _():
        top = halo_mix(rowh[0, 0])
        low = halo_mix(rowh[0, 1])
        nt_scr[0:cells, :C] = top
        nt_scr[32 : 32 + cells, :C] = low

        def cell(j, carry):
            put_cell(
                step * cells + j + REACH,
                x_ref[j].astype(F32),
                nt_scr[pl.ds(j, 1), :C],
                nt_scr[pl.ds(32 + j, 1), :C],
            )
            return carry

        lax.fori_loop(0, cells, cell, 0)

    @pl.when(step >= chunks)
    def _():
        first = (step - chunks) * cells
        nt_scr[...] = jnp.dot(
            aug[...].reshape(cells * rows, LANES), wn[...], preferred_element_type=F32
        )
        lane = iota((8, LANES), 1)
        for g in range(CB):
            lanes = slice(g * LANES, (g + 1) * LANES)
            for hb in range(rows // 8):
                taps = [k_scr[t, 8 * hb : 8 * hb + 8, lanes] for t in range(TAPS)]

                def cell(j, carry):
                    acc = nt_scr[pl.ds(j * rows + 8 * hb, 8), lanes]
                    for t in range(TAPS):
                        l, w = divmod(t, 5)
                        acc = acc + taps[t] * m_scr[g, first + j + w, 8 * hb + l : 8 * hb + l + 8, :]
                    if g == CB - 1:
                        extra = aug[j, 8 * hb : 8 * hb + 8, :].astype(F32)
                        acc = jnp.where(lane == 0, acc, extra)
                    out_ref[j, 8 * hb : 8 * hb + 8, lanes] = acc.astype(BF16)
                    return carry

                lax.fori_loop(0, cells, cell, 0, unroll=2)


def stencil_fwd(height, x, colh, rowh, cornh, table, wd, small, aug, wn, chunks):
    width, rows, _ = x.shape
    cells = width // chunks
    first = lambda i: jnp.where(i < chunks, i, chunks - 1)
    second = lambda i: jnp.where(i < chunks, 0, i - chunks)
    return pl.pallas_call(
        partial(stencil_fwd_kernel, chunks, cells),
        name="stencil_fwd",
        grid=(2 * chunks,),
        out_shape=jax.ShapeDtypeStruct((width, rows, CP), BF16),
        in_specs=[
            pl.BlockSpec(memory_space=pltpu.SMEM),
            pl.BlockSpec((cells, rows, C), lambda i: (first(i), 0, 0)),
            vmem_spec(),
            pl.BlockSpec((1, 2, cells, C), lambda i: (first(i), 0, 0, 0)),
            vmem_spec(),
            vmem_spec(),
            vmem_spec(),
            vmem_spec(),
            pl.BlockSpec((cells, rows, LANES), lambda i: (second(i), 0, 0)),
            vmem_spec(),
        ],
        out_specs=pl.BlockSpec((cells, rows, CP), lambda i: (second(i), 0, 0)),
        scratch_shapes=[
            pltpu.VMEM((CB, width + 2 * REACH, 32, LANES), F32),
            pltpu.VMEM((TAPS, rows, CP), F32),
            pltpu.VMEM((cells * rows, CP), F32),
        ],
        compiler_params=params(dimension_semantics=("arbitrary",)),
    )(height, x, colh, rowh, cornh, table, wd, small, aug, wn)


def pack_weights(one, two, flat):
    lane = iota((8, LANES), 1)
    row = iota((8, LANES), 0)
    flat[...] = jnp.zeros_like(flat)

    def turned(v, s0, unit):
        return pltpu.roll(pltpu.roll(v, s0, 1), 0, 1, stride=unit, stride_axis=0)

    def one_main(a, carry):
        r0 = pl.multiple_of(a * 8, 8)
        s0 = (2 * r0) % LANES
        keep = lane >= s0 + 2 * row
        before = jnp.zeros((8, LANES), F32)
        for q in range(FB - 1):
            now = turned(one[q, pl.ds(r0, 8), :], s0, 2)
            flat[pl.ds(10 * r0 + q + r0 // 64, 8, stride=10), :] = jnp.where(keep, now, before)
            before = now
        return carry

    def one_rest(a, carry):
        r0 = pl.multiple_of(a * 8, 8)
        s0 = (2 * r0) % LANES
        s = s0 + 2 * row
        before = turned(one[FB - 2, pl.ds(r0, 8), :], s0, 2)
        now = turned(one[FB - 1, pl.ds(r0, 8), :], s0, 2)
        v = jnp.where(lane < s, before, jnp.where(lane < s + FF - (FB - 1) * LANES, now, 0.0))
        at = pl.ds(10 * r0 + FB - 1 + r0 // 64, 8, stride=10)
        flat[at, :] = flat[at, :] + v
        return carry

    lax.fori_loop(0, C // 8, one_main, 0)
    last = C - 1
    assert last % 64 == 0 and C % 8 == 1
    for q in range(FB - 1):
        at = 10 * last + q + last // 64
        flat[at : at + 1, :] = one[q, last : last + 1, :]
    lax.fori_loop(0, C // 8, one_rest, 0)

    groups = -(-(FF + LANE_TWO) // 8)

    def two_rolled(q, a):
        v = turned(two[q, pl.ds(8 * a + 8 - LANE_TWO, 8), :], (8 * a) % LANES, 1)
        r = 8 * a - LANE_TWO + row
        return jnp.where((r >= 0) & (r < FF), v, 0.0)

    def two_base(a):
        return ROW_TWO + 5 * (8 * a - LANE_TWO) + a // 16

    def two_main(a, carry, add=False):
        keep = lane >= (8 * a) % LANES + row
        before = jnp.zeros((8, LANES), F32)
        for q in range(CB - 1):
            now = two_rolled(q, a)
            at = pl.ds(two_base(a) + q, 8, stride=5)
            v = jnp.where(keep, now, before)
            flat[at, :] = flat[at, :] + v if add else v
            before = now
        return carry

    def two_rest(a, carry):
        s = (8 * a) % LANES + row
        before = two_rolled(CB - 2, a)
        now = two_rolled(CB - 1, a)
        v = jnp.where(lane < s, before, jnp.where(lane < s + C - (CB - 1) * LANES, now, 0.0))
        at = pl.ds(two_base(a) + CB - 1, 8, stride=5)
        flat[at, :] = flat[at, :] + v
        return carry

    lax.fori_loop(1, groups, two_main, 0)
    two_main(0, 0, add=True)
    at = 10 * last + FB - 1 + last // 64
    lane1 = iota((1, LANES), 1)
    v = jnp.where(lane1 < FF - (FB - 1) * LANES, one[FB - 1, last : last + 1, :], 0.0)
    flat[at : at + 1, :] = flat[at : at + 1, :] + v
    lax.fori_loop(0, groups, two_rest, 0)


GELU_A = math.sqrt(2.0 / math.pi)
GELU_B = 0.044715
WIDE = 256


def dot(a, b, dims=((1,), (0,))):
    return lax.dot_general(a, b, (dims, ((), ())), preferred_element_type=F32)


def mlp_kernel(
    blocks, height_ref, conv_ref, g_ref, x_ref, w1, w2, small,
    out_ref, gconv_ref, rows_ref, cols_ref, corn_ref, flat_ref, extra_ref,
    one, two, g_scr, conv_t, g_t, branch, gc,
):
    step = pl.program_id(0)
    cells, rows, _ = x_ref.shape
    m = cells * rows
    height = height_ref[0]

    @pl.when(step == 0)
    def _():
        one[...] = jnp.zeros_like(one)
        two[...] = jnp.zeros_like(two)
        g_scr[...] = jnp.zeros_like(g_scr)

    live = (iota((1, rows, 1), 1) < height).astype(F32)
    g_scr[:, :C] = (g_ref[...].astype(F32) * live).reshape(m, C).astype(BF16)
    conv = conv_ref[...].reshape(m, CP)
    conv_t[...] = conv.T[: conv_t.shape[0]]
    branch[...] = jnp.zeros_like(branch)
    gc[...] = jnp.zeros_like(gc)
    rows_one = conv_t.shape[0]

    def chunk(start, wide, tail):
        lanes = pl.ds(start, wide)
        conv_block = conv_ref[...].reshape(m, CP)
        g_block = g_scr[...]
        h = dot(conv_block, w1[:, lanes]) + small[0:1, lanes]
        ga = dot(g_block, w2[lanes, :], ((1,), (1,)))
        h2 = h * h
        t = jnp.tanh(h * (GELU_A + (GELU_A * GELU_B) * h2))
        cdf = 0.5 * t + 0.5
        act = (h * cdf).astype(BF16)
        slope = cdf + h * (0.5 - 0.5 * (t * t)) * (GELU_A + (3 * GELU_A * GELU_B) * h2)
        gh = (ga * slope).astype(BF16)
        if tail:
            act = jnp.where(iota((m, wide), 1) == FF - (FB - 1) * LANES, jnp.ones_like(act), act)
        branch[...] += dot(act, w2[lanes, :])
        gc[...] += dot(gh, w1[:, lanes], ((1,), (1,)))
        r1 = dot(conv_t[...], gh)
        r2 = dot(act, g_block, ((0,), (0,)))
        for i in range(wide // LANES):
            one[start // LANES + i] += r1[:, i * LANES : (i + 1) * LANES]
        for q in range(CB):
            two[q, pl.ds(start + 8, wide), :] += r2[:, q * LANES : (q + 1) * LANES]

    def body(f, carry):
        chunk(pl.multiple_of(f * WIDE, WIDE), WIDE, False)
        return carry

    lax.fori_loop(0, FP // WIDE, body, 0)
    chunk(FP // WIDE * WIDE, FP % WIDE, True)

    out = x_ref[...].astype(F32).reshape(m, C) + branch[:, :C] + small[1:2, :C]
    out_ref[...] = (out.reshape(cells, rows, C) * live).astype(BF16)
    gconv_ref[...] = gc[...].reshape(cells, rows, CP)
    onehot = (iota((1, rows, 1), 1) == height - 1).astype(F32)
    block = gc[...].reshape(cells, rows, CP)
    edges = (block[:, 0, :].astype(BF16), jnp.sum(block * onehot, 1).astype(BF16))
    for r in range(2):
        rows_ref[0, r] = edges[r]
    for side, at, first in ((0, 0, 0), (1, blocks - 1, cells - REACH)):

        @pl.when(step == at)
        def _(side=side, first=first):
            for i in range(REACH):
                base = (first + i) * rows
                cols_ref[side, i] = gc[base : base + rows, :].astype(BF16)
            for r in range(2):
                corn_ref[r, side] = edges[r][first : first + REACH]

    @pl.when(step == blocks - 1)
    def _():
        extra_ref[...] = jnp.zeros_like(extra_ref)
        for q in range(FB):
            extra_ref[0 : NOISE + 1, q * LANES : (q + 1) * LANES] = one[q, C : C + NOISE + 1, :]
        for q in range(CB):
            lanes = slice(q * LANES, (q + 1) * LANES)
            extra_ref[NOISE + 1 : NOISE + 2, lanes] = two[q, FF + 8 : FF + 9, :]
        pack_weights(one, two, flat_ref)


def mlp(height, conv, g, x, w1, w2, small, flat_rows, blocks):
    width, rows, _ = x.shape
    cells = width // blocks
    m = cells * rows
    sd = jax.ShapeDtypeStruct
    block = lambda c: pl.BlockSpec((cells, rows, c), lambda i: (i, 0, 0))
    rows_one = -(-(C + NOISE + 1) // 16) * 16
    flops = 12 * width * rows * C * FF
    return pl.pallas_call(
        partial(mlp_kernel, blocks),
        name="mlp",
        grid=(blocks,),
        out_shape=(
            sd((width, rows, C), BF16),
            sd((width, rows, CP), F32),
            sd((blocks, 2, cells, CP), BF16),
            sd((2, REACH, rows, CP), BF16),
            sd((2, 2, REACH, CP), BF16),
            sd((flat_rows, LANES), F32),
            sd((16, FP), F32),
        ),
        in_specs=[
            pl.BlockSpec(memory_space=pltpu.SMEM),
            block(CP),
            block(C),
            block(C),
            vmem_spec(),
            vmem_spec(),
            vmem_spec(),
        ],
        out_specs=(
            block(C),
            block(CP),
            pl.BlockSpec((1, 2, cells, CP), lambda i: (i, 0, 0, 0)),
            vmem_spec(),
            vmem_spec(),
            vmem_spec(),
            vmem_spec(),
        ),
        scratch_shapes=[
            pltpu.VMEM((FB, rows_one, LANES), F32),
            pltpu.VMEM((CB, FP + 16, LANES), F32),
            pltpu.VMEM((m, CP), BF16),
            pltpu.VMEM((rows_one, m), BF16),
            pltpu.VMEM((8, LANES), BF16),
            pltpu.VMEM((m, CP), F32),
            pltpu.VMEM((m, CP), F32),
        ],
        compiler_params=params(dimension_semantics=("arbitrary",)),
        cost_estimate=pl.CostEstimate(flops=flops, bytes_accessed=50_000_000, transcendentals=0),
    )(height, conv, g, x, w1, w2, small)


def exchange_kernel(cols, rows, corners, colh, rowh, cornh, send, recv):
    greet([], True)
    halos = halo_copies(cols, rows, corners, colh, rowh, cornh, send, recv)
    start_halo(halos)
    wait_halo(halos)
    lat, _, nlat, *_ = neighbours()
    for r, cond in ((0, lat == 0), (1, lat == nlat - 1)):

        @pl.when(cond)
        def _(r=r):
            rowh[r] = jnp.zeros(rowh.shape[1:], rowh.dtype)
            for s in range(2):
                cornh[r, s] = jnp.zeros(cornh.shape[2:], cornh.dtype)


def exchange(cols, rows, corners):
    sd = jax.ShapeDtypeStruct
    return pl.pallas_call(
        exchange_kernel,
        name="exchange_edges",
        out_shape=(sd(cols.shape, BF16), sd(rows.shape, BF16), sd(corners.shape, BF16)),
        in_specs=[vmem_spec()] * 3,
        out_specs=(vmem_spec(),) * 3,
        scratch_shapes=[pltpu.SemaphoreType.DMA((8,)), pltpu.SemaphoreType.DMA((8,))],
        compiler_params=params(collective_id=1, has_side_effects=True),
    )(cols, rows, corners)


def scatter_kernel(mesh, flat, out_ref, buf, *rest):
    bits = bit_list(mesh)
    n = len(bits)
    recvs, (send, recv) = rest[:n], rest[n:]
    orders = [order[::-1] for order in stage_orders(mesh)]
    mine = my_bits(bits)
    shard_rows = out_ref.shape[0]
    cut = (shard_rows // 2 + 7) // 8 * 8
    spans = [(0, cut), (cut, shard_rows - cut)]

    def shard_index(d):
        return tuple((d >> (n - 1 - i)) & 1 for i in range(n))

    def fill(d, carry):
        buf[shard_index(d)] = flat[pl.ds(d * shard_rows, shard_rows), :]
        return carry

    lax.fori_loop(0, 1 << n, fill, 0)
    greet(bits, False)

    def copy(colour, k):
        order = orders[colour]
        done, now = order[:k], order[k]
        start, count = spans[colour]
        index = tuple(
            1 - mine[i] if i == now else mine[i] if i in done else slice(None) for i in range(n)
        )
        at = pl.ds(start, count)
        return pltpu.make_async_remote_copy(
            src_ref=buf.at[index + (at,)],
            dst_ref=recvs[k].at[(slice(None),) * (n - 1 - k) + (at,)],
            send_sem=send.at[colour, k],
            recv_sem=recv.at[colour, k],
            device_id=partner(*bits[now]),
            device_id_type=MESH,
        )

    def accumulate(colour, k):
        order = orders[colour]
        start, count = spans[colour]
        free = [i for i in range(n) if i not in order[: k + 1]]

        def add(d, carry):
            sub = tuple((d >> (len(free) - 1 - i)) & 1 for i in range(len(free)))
            index = tuple(sub[free.index(i)] if i in free else mine[i] for i in range(n))
            at = pl.ds(start, count)
            buf[index + (at,)] = buf[index + (at,)] + recvs[k][sub + (at,)]
            return carry

        lax.fori_loop(0, 1 << len(free), add, 0)

    for colour in range(2):
        copy(colour, 0).start()
    for k in range(n):
        for colour in range(2):
            copy(colour, k).wait()
            accumulate(colour, k)
            if k + 1 < n:
                copy(colour, k + 1).start()
    out_ref[...] = buf[tuple(mine)]


def scatter(mesh, flat, shard_rows):
    n = len(bit_list(mesh))
    return pl.pallas_call(
        partial(scatter_kernel, mesh),
        name="reduce_scatter",
        out_shape=jax.ShapeDtypeStruct((shard_rows, LANES), F32),
        in_specs=[vmem_spec()],
        out_specs=vmem_spec(),
        scratch_shapes=[pltpu.VMEM((2,) * n + (shard_rows, LANES), F32)]
        + [pltpu.VMEM((2,) * (n - 1 - k) + (shard_rows, LANES), F32) for k in range(n)]
        + [pltpu.SemaphoreType.DMA((2, n)), pltpu.SemaphoreType.DMA((2, n))],
        compiler_params=params(collective_id=2, has_side_effects=True),
    )(flat)


def add_vector(tail, offset, value):
    row, shift = divmod(offset - TAIL_ROW * LANES, LANES)
    blocks = value.shape[0]
    lane = iota((blocks + 1, LANES), 1)
    zero = jnp.zeros((1, LANES), F32)
    here = pltpu.roll(jnp.concatenate([value, zero], 0), shift, 1) if shift else jnp.concatenate([value, zero], 0)
    back = jnp.concatenate([zero, here[:blocks]], 0)
    at = slice(row, row + blocks + 1)
    tail[at, :] = tail[at, :] + jnp.where(lane >= shift, here, back if shift else here)


def as_blocks(value, length):
    blocks = -(-length // LANES)
    v = jnp.concatenate([value[:, q * LANES : (q + 1) * LANES] for q in range(blocks)], 0)
    index = iota((blocks, LANES), 0) * LANES + iota((blocks, LANES), 1)
    return jnp.where(index < length, v, 0.0)


def stencil_bwd_kernel(
    chunks, cells, height_ref, x_ref, g_ref, gconv_ref, colh, rowh, cornh, table, wd, gain, extra, w1,
    out_ref, tail_ref, g_scr, m_scr, k_scr, e_scr, gg_scr, row_scr,
):
    step = pl.program_id(0)
    rows = x_ref.shape[1]
    width = chunks * cells
    height = height_ref[0]
    gvec = gain[2:3, :C]

    def put_column(column, v, top, low):
        hrow = iota((rows, CP), 0)
        v = jnp.where(hrow == height, low, v)
        for q in range(CB):
            lanes = slice(q * LANES, (q + 1) * LANES)
            g_scr[q, column, 1 : rows + 1, :] = v[:, lanes]
            g_scr[q, column, 0:1, :] = top[:, lanes]
            g_scr[q, column, rows + 1 : rows + 2, :] = low[:, lanes]

    @pl.when(step == 0)
    def _():
        k_scr[...] = jnp.dot(
            table[...], wd[...], preferred_element_type=F32, precision=HIGHEST
        ).reshape(k_scr.shape)
        e_scr[...] = jnp.zeros_like(e_scr)
        gg_scr[...] = jnp.zeros_like(gg_scr)
        for q in range(CB - 1, CB):
            m_scr[q] = jnp.zeros(m_scr.shape[1:], F32)
        for side in range(2):
            for i in range(REACH):
                column = i if side == 0 else width + REACH + i
                put_column(
                    column,
                    colh[side, i].astype(F32),
                    cornh[0, side].astype(F32)[i : i + 1],
                    cornh[1, side].astype(F32)[i : i + 1],
                )

    @pl.when(step < chunks)
    def _():
        row_scr[0:cells, :] = rowh[0, 0].astype(F32)
        row_scr[32 : 32 + cells, :] = rowh[0, 1].astype(F32)

        def cell(j, carry):
            put_column(
                step * cells + j + REACH,
                gconv_ref[j],
                row_scr[pl.ds(j, 1), :],
                row_scr[pl.ds(32 + j, 1), :],
            )
            center, inv = norm_parts(x_ref[j].astype(F32))
            mixed = rounded(center * inv * gvec)
            mixed = jnp.where(iota((rows, C), 0) < height, mixed, 0.0)
            for q in range(CB):
                lo, hi = q * LANES, min((q + 1) * LANES, C)
                m_scr[q, step * cells + j, :, : hi - lo] = mixed[:, lo:hi]
            return carry

        lax.fori_loop(0, cells, cell, 0)

    @pl.when(step == chunks)
    def _():
        for q in range(CB):
            lanes = slice(q * LANES, (q + 1) * LANES)
            for hb in range(rows // 8):
                at = slice(8 * hb, 8 * hb + 8)
                taps = [k_scr[t, at, lanes] for t in range(TAPS)]

                def cell(j, sums):
                    mx = m_scr[q, j, at, :]
                    sums = list(sums)
                    gm = jnp.zeros((8, LANES), F32)
                    for t in range(TAPS):
                        l, w = divmod(t, 5)
                        v = g_scr[q, j + 2 * REACH - w, 8 * hb + 2 - l : 8 * hb + 10 - l, :]
                        gm = gm + taps[t] * v
                        sums[t] = sums[t] + mx * v
                    m_scr[q, j, at, :] = gm
                    return tuple(sums)

                zero = jnp.zeros((8, LANES), F32)
                sums = lax.fori_loop(0, width, cell, (zero,) * TAPS)
                for t in range(TAPS):
                    e_scr[t, at, lanes] = sums[t]

    @pl.when(step > chunks)
    def _():
        first = (step - chunks - 1) * cells
        live = iota((rows, C), 0) < height

        def cell(j, total):
            center, inv = norm_parts(x_ref[j].astype(F32))
            normed = center * inv
            gm = jnp.concatenate([m_scr[q, first + j] for q in range(CB)], 1)[:, :C]
            gm = jnp.where(live, gm, 0.0)
            total = total + gm * normed
            v = gm * gvec
            mean = jnp.mean(v, -1, keepdims=True)
            mean_n = jnp.mean(v * normed, -1, keepdims=True)
            up = jnp.where(live, g_ref[j].astype(F32), 0.0)
            out_ref[j] = inv * (v - mean - normed * mean_n) + up
            return total

        gg_scr[:, :C] = lax.fori_loop(0, cells, cell, gg_scr[:, :C])

    @pl.when(step == 2 * chunks)
    def _():
        tail_ref[...] = jnp.zeros_like(tail_ref)
        add_vector(tail_ref, OFF_B1, as_blocks(extra[NOISE : NOISE + 1, :], FF))
        add_vector(tail_ref, OFF_B2, as_blocks(extra[NOISE + 1 : NOISE + 2, :], C))
        add_vector(tail_ref, OFF_GAIN, as_blocks(jnp.sum(gg_scr[...], 0, keepdims=True), C))
        disco = lax.dot_general(
            table[...], e_scr[...].reshape(TAPS * rows, CP), (((0,), (0,)), ((), ())),
            preferred_element_type=F32, precision=HIGHEST,
        )
        for k in range(K):
            add_vector(tail_ref, OFF_DISCO + k * C, as_blocks(disco[k : k + 1, :], C))
        ng = extra[0:NOISE, :]
        hi = ng.astype(BF16)
        mid = (ng - hi.astype(F32)).astype(BF16)
        lo = (ng - hi.astype(F32) - mid.astype(F32)).astype(BF16)
        parts = [dot(p, w1[...], ((1,), (1,))) for p in (hi, mid, lo)]
        gn = parts[0] + parts[1] + parts[2]
        for k in range(NOISE):
            add_vector(tail_ref, OFF_NOISE + k * C, as_blocks(gn[k : k + 1, :], C))


def stencil_bwd(height, x, g, gconv, colh, rowh, cornh, table, wd, small, extra, w1, tail_rows, chunks):
    width, rows, _ = x.shape
    cells = width // chunks
    first = lambda i: jnp.where(i < chunks, i, chunks - 1)
    third = lambda i: jnp.where(i <= chunks, 0, i - chunks - 1)
    both = lambda i: jnp.where(i < chunks, i, third(i))
    sd = jax.ShapeDtypeStruct
    return pl.pallas_call(
        partial(stencil_bwd_kernel, chunks, cells),
        name="stencil_bwd",
        grid=(2 * chunks + 1,),
        out_shape=(sd((width, rows, C), F32), sd((tail_rows, LANES), F32)),
        in_specs=[
            pl.BlockSpec(memory_space=pltpu.SMEM),
            pl.BlockSpec((cells, rows, C), lambda i: (both(i), 0, 0)),
            pl.BlockSpec((cells, rows, C), lambda i: (third(i), 0, 0)),
            pl.BlockSpec((cells, rows, CP), lambda i: (first(i), 0, 0)),
            vmem_spec(),
            pl.BlockSpec((1, 2, cells, CP), lambda i: (first(i), 0, 0, 0)),
        ]
        + [vmem_spec()] * 6,
        out_specs=(
            pl.BlockSpec((cells, rows, C), lambda i: (third(i), 0, 0)),
            vmem_spec(),
        ),
        scratch_shapes=[
            pltpu.VMEM((CB, width + 2 * REACH, 32, LANES), F32),
            pltpu.VMEM((CB, width, rows, LANES), F32),
            pltpu.VMEM((TAPS, rows, CP), F32),
            pltpu.VMEM((TAPS, rows, CP), F32),
            pltpu.VMEM((rows, CP), F32),
            pltpu.VMEM((64, CP), F32),
        ],
        compiler_params=params(dimension_semantics=("arbitrary",)),
    )(height, x, g, gconv, colh, rowh, cornh, table, wd, small, extra, w1)


def tail_kernel(mesh, part_ref, tail_ref, grad_ref, scale_ref, got, msg, full, place, send, recv):
    nlat, nlon = mesh.shape["lat"], mesh.shape["lon"]
    n = nlat * nlon
    lat, lon = lax.axis_index("lat"), lax.axis_index("lon")
    me = lat * nlon + lon
    piece = tail_ref.shape[1]
    shard_rows = part_ref.shape[0]
    barrier = pltpu.get_barrier_semaphore()

    def others(body):
        def step(i, carry):
            body(lax.rem(me + i, n))
            return carry

        lax.fori_loop(1, n, step, 0)

    def hello(d):
        pl.semaphore_signal(
            barrier, inc=1, device_id=(d // nlon, lax.rem(d, nlon)), device_id_type=MESH
        )

    others(hello)
    pl.semaphore_wait(barrier, n - 1)

    def scatter_piece(d):
        pltpu.make_async_remote_copy(
            src_ref=tail_ref.at[d],
            dst_ref=got.at[me],
            send_sem=send.at[0],
            recv_sem=recv.at[0],
            device_id=(d // nlon, lax.rem(d, nlon)),
            device_id_type=MESH,
        ).start()

    def wait_all(buffer, k):
        pltpu.make_async_remote_copy(
            src_ref=buffer.at[pl.ds(0, n - 1)],
            dst_ref=buffer.at[pl.ds(0, n - 1)],
            send_sem=send.at[k],
            recv_sem=recv.at[k],
            device_id=(lat, lon),
            device_id_type=MESH,
        ).wait()

    others(scatter_piece)
    got[me] = tail_ref[me]
    square = jnp.sum(part_ref[...] * part_ref[...])
    wait_all(got, 0)

    total = lax.fori_loop(
        1, n, lambda i, acc: acc + got[lax.rem(i, n)], got[0]
    )
    square = square + jnp.sum(total * total)
    msg[0:piece, :] = total
    msg[piece : piece + 1, :] = jnp.broadcast_to(square, (1, LANES))

    def share(d):
        pltpu.make_async_remote_copy(
            src_ref=msg,
            dst_ref=full.at[me],
            send_sem=send.at[1],
            recv_sem=recv.at[1],
            device_id=(d // nlon, lax.rem(d, nlon)),
            device_id_type=MESH,
        ).start()

    others(share)
    full[me] = msg[...]
    place[...] = jnp.zeros_like(place)
    wait_all(full, 1)

    def take(d, acc):
        place[pl.ds(shard_rows + d * piece, piece), :] = full[d, 0:piece, :]
        return acc + full[d, piece : piece + 1, :]

    squares = lax.fori_loop(0, n, take, jnp.zeros((1, LANES), F32))
    start = jnp.clip(me * shard_rows - TAIL_ROW + shard_rows, 0, shard_rows + n * piece)
    grad_ref[...] = part_ref[...] + place[pl.ds(start, shard_rows), :]
    scale_ref[...] = jnp.broadcast_to(jnp.sqrt(squares), scale_ref.shape)


def finish(mesh, part, tail):
    n, piece, _ = tail.shape
    shard_rows = part.shape[0]
    sd = jax.ShapeDtypeStruct
    return pl.pallas_call(
        partial(tail_kernel, mesh),
        name="small_gradients",
        out_shape=(sd(part.shape, F32), sd((8, LANES), F32)),
        in_specs=[vmem_spec()] * 2,
        out_specs=(vmem_spec(),) * 2,
        scratch_shapes=[
            pltpu.VMEM((n, piece, LANES), F32),
            pltpu.VMEM((piece + 1, LANES), F32),
            pltpu.VMEM((n, piece + 1, LANES), F32),
            pltpu.VMEM((2 * shard_rows + n * piece + 8, LANES), F32),
            pltpu.SemaphoreType.DMA((2,)),
            pltpu.SemaphoreType.DMA((2,)),
        ],
        compiler_params=params(collective_id=3, has_side_effects=True),
    )(part, tail)


def stencil_table(support_vals, support_lon):
    rows = support_vals.shape[0]
    vals = support_vals.reshape(rows, S // 3, 3, K)
    offsets = jnp.arange(-REACH, REACH + 1)
    hit = support_lon.reshape(rows, S // 3, 3)[:, :, :, None] == offsets
    picked = jnp.where(hit[:, :, :, :, None], vals[:, :, :, None, :], 0.0)
    return jnp.transpose(jnp.sum(picked, 1), (1, 2, 0, 3))


def neighbour_rows(table, height):
    count = lax.axis_size("lat")
    up = [(i, i + 1) for i in range(count - 1)]
    last = lax.dynamic_index_in_dim(table, height - 1, 2, keepdims=True)
    above = lax.ppermute(last, "lat", up)
    below = lax.ppermute(table[:, :, :1], "lat", [(j, i) for i, j in up])
    ext = jnp.concatenate([above, table, jnp.zeros_like(above)], 2)
    ext = jnp.where(jnp.arange(ext.shape[2])[None, None, :, None] == height + 1, below, ext)
    rows = table.shape[2]
    return jnp.stack([ext[l, :, 2 - l : 2 - l + rows] for l in range(3)])


def flat_table(table):
    t = table.reshape(-1, K)
    return jnp.pad(t, ((0, 0), (0, 16 - K)))


def local(
    mesh, block_in, noise, cotangent, band_heights, support_lon, support_vals,
    master, moment_one, moment_two, average, step_count,
):
    rows, width, _ = block_in.shape
    devices = mesh.shape["lat"] * mesh.shape["lon"]
    shard = master.shape[0]
    shard_rows = shard // LANES
    assert shard_rows * LANES == shard
    flat_rows = shard_rows * devices
    chunks = 6
    cells = width // chunks
    height = lax.dynamic_slice_in_dim(band_heights, lax.axis_index("lat"), 1, 0)
    x = jnp.transpose(block_in, (1, 0, 2))
    g = jnp.transpose(cotangent, (1, 0, 2))

    share = master.astype(BF16).reshape(shard_rows, LANES)
    edge = jnp.stack([x[:, 0], lax.dynamic_index_in_dim(x, height[0] - 1, 1, keepdims=False)])
    cols = jnp.stack([x[:REACH], x[width - REACH :]])
    corners = jnp.stack([edge[:, :REACH], edge[:, width - REACH :]], 1)
    edge = jnp.transpose(edge.reshape(2, chunks, cells, C), (0, 1, 2, 3))
    w1, w2, wn, wd, small, colh, rowh, cornh = gather_weights(mesh, share, cols, edge, corners)
    rowh = jnp.transpose(rowh, (1, 0, 2, 3))

    table = stencil_table(support_vals, support_lon)
    aug = jnp.concatenate(
        [
            jnp.zeros((width, rows, 1), BF16),
            jnp.transpose(noise, (2, 1, 0)),
            jnp.ones((width, rows, 1), BF16),
            jnp.zeros((width, rows, LANES - NOISE - 2), BF16),
        ],
        2,
    )
    conv = stencil_fwd(height, x, colh, rowh, cornh, flat_table(table), wd, small, aug, wn, chunks)
    out, gconv, grow, gcol, gcorn, flat, extra = mlp(
        height, conv, g, x, w1, w2, small, flat_rows, chunks
    )
    gcolh, growh, gcornh = exchange(gcol, jnp.transpose(grow, (1, 0, 2, 3)), gcorn)
    growh = jnp.transpose(growh, (1, 0, 2, 3))
    part = scatter(mesh, flat, shard_rows)
    piece = -(-(flat_rows - TAIL_ROW) // devices)
    grad_in, tail = stencil_bwd(
        height, x, g, gconv, gcolh, growh, gcornh,
        flat_table(neighbour_rows(table, height[0])), wd, small, extra, w1, devices * piece, chunks,
    )
    grad, norm = finish(mesh, part, tail.reshape(devices, piece, LANES))
    grad_part = grad.reshape(shard)
    grad_norm = norm[0, :1]
    factor = 0.01 / jnp.maximum(grad_norm, 0.01)
    clipped = grad_part * factor
    new_one = 0.9 * moment_one + 0.1 * clipped
    new_two = 0.999 * moment_two + 0.001 * clipped * clipped
    step_float = step_count[0].astype(F32)
    fix_one = 1.0 - jnp.power(jnp.float32(0.9), step_float)
    fix_two = 1.0 - jnp.power(jnp.float32(0.999), step_float)
    update = new_one / fix_one / (jnp.sqrt(new_two / fix_two) + 1e-08) + 0.1 * master
    new_master = master - 0.02 * update
    new_avg = 0.9 * average + 0.1 * new_master
    return (
        jnp.transpose(out, (1, 0, 2)),
        jnp.transpose(grad_in, (1, 0, 2)),
        grad_part,
        grad_norm,
        new_master,
        new_one,
        new_two,
        new_avg,
        new_master.astype(BF16),
    )


def solution(mesh):
    flat = P(("lat", "lon"))
    field = P("lat", "lon", None)
    return jax.shard_map(
        partial(local, mesh),
        mesh=mesh,
        in_specs=(
            field, P(None, "lat", "lon"), field, P(), P("lat", None), P("lat", None, None),
            flat, flat, flat, flat, P(),
        ),
        out_specs=(field, field, flat, P(), flat, flat, flat, flat, flat),
        check_vma=False,
    )
```

```python
from functools import partial
import math

import jax
import jax.numpy as jnp
from jax import lax
from jax.experimental import pallas as pl
from jax.experimental.pallas import tpu as pltpu
from jax.sharding import PartitionSpec as P

C = 641
FF = 1282
NOISE = 8
K = 9
S = 12
REACH = 2
LANES = 128
CB = 6
CP = CB * LANES
FB = 11
FP = FB * LANES
TAPS = 15
MESH = pl.DeviceIdType.MESH
HIGHEST = lax.Precision.HIGHEST
F32 = jnp.float32
BF16 = jnp.bfloat16
VMEM_LIMIT = 60 * 1024 * 1024
SLOTS = 28
REUSE = 10
ROW_TWO = (C * FF) // LANES
LANE_TWO = (C * FF) % LANES
TAIL_ROW = (2 * C * FF) // LANES
OFF_B1 = 2 * C * FF
OFF_B2 = OFF_B1 + FF
OFF_GAIN = OFF_B2 + C
OFF_DISCO = OFF_GAIN + C
OFF_NOISE = OFF_DISCO + K * C
END_FLAT = OFF_NOISE + NOISE * C


def params(**kw):
    return pltpu.CompilerParams(vmem_limit_bytes=VMEM_LIMIT, **kw)


def any_spec():
    return pl.BlockSpec(memory_space=pl.ANY)


def vmem_spec():
    return pl.BlockSpec(memory_space=pltpu.VMEM)


def iota(shape, dim):
    return lax.broadcasted_iota(jnp.int32, shape, dim)


def bit_list(mesh):
    bits = []
    for axis in ("lat", "lon"):
        count = int(math.log2(mesh.shape[axis]))
        assert 1 << count == mesh.shape[axis]
        bits += [(axis, b) for b in reversed(range(count))]
    return bits


def my_bits(bits):
    ids = {"lat": lax.axis_index("lat"), "lon": lax.axis_index("lon")}
    return [(ids[a] >> b) & 1 for a, b in bits]


def partner(axis, bit):
    lat, lon = lax.axis_index("lat"), lax.axis_index("lon")
    if axis == "lat":
        return (lat ^ (1 << bit), lon)
    return (lat, lon ^ (1 << bit))


def stage_orders(mesh):
    bits = bit_list(mesh)
    n = len(bits)
    if (mesh.shape["lat"], mesh.shape["lon"]) == (8, 4):
        return [[0, 1, 2, 3, 4], [0, 1, 3, 2, 4]]
    order = list(range(n))
    return [order, order]


def rotl_rows(v, first, unit):
    row = iota((8, LANES), 0)
    left = lambda u, n: pltpu.roll(u, (LANES - n) % LANES, 1) if n % LANES else u
    low = [left(v, first + unit * b) for b in range(4)]
    odd = (row & 1) == 1
    v = jnp.where((row & 2) == 2, jnp.where(odd, low[3], low[2]), jnp.where(odd, low[1], low[0]))
    return jnp.where((row & 4) == 4, left(v, 4 * unit), v)


def row_vector(flat_ref, offset, length):
    blocks = -(-length // LANES)
    row, shift = divmod(offset, LANES)
    near = flat_ref[row : row + blocks, :]
    if shift:
        far = flat_ref[row + 1 : row + 1 + blocks, :]
        lane = iota((blocks, LANES), 1)
        near = pltpu.roll(jnp.where(lane >= shift, near, far), LANES - shift, 1)
    index = iota((blocks, LANES), 0) * LANES + iota((blocks, LANES), 1)
    return jnp.where(index < length, near, 0.0)


def put_row(ref, row, value):
    for q in range(value.shape[0]):
        ref[row : row + 1, q * LANES : (q + 1) * LANES] = value[q : q + 1, :].astype(ref.dtype)


def unpack_weights(flat, w1, w2, wn, wd, small, wnf):
    lane = iota((8, LANES), 1)
    row = iota((8, LANES), 0)

    def rows_one(base, first):
        near = [flat[pl.ds(base + q, 8, stride=10), :] for q in range(FB + 1)]
        out = [
            rotl_rows(jnp.where(lane >= first + 2 * row, near[q], near[q + 1]), first, 2)
            for q in range(FB)
        ]
        out[-1] = jnp.where(lane < FF - (FB - 1) * LANES, out[-1], 0.0)
        return out

    def body_one(b, carry):
        for k in range(0, 8, 2):
            pair = [rows_one(641 * b + 80 * (k + h), 16 * (k + h)) for h in range(2)]
            at = pl.ds(pl.multiple_of(64 * b + 8 * k, 16), 16)
            for q in range(FB):
                v = jnp.concatenate([pair[0][q], pair[1][q]], 0)
                w1[at, q * LANES : (q + 1) * LANES] = v.astype(BF16)
        return carry

    last = C - 1
    lax.fori_loop(0, last // 64, body_one, 0)
    zero = jnp.zeros((8, LANES), F32)
    for q, v in enumerate(rows_one(641 * (last // 64), 0)):
        v = jnp.concatenate([jnp.where(row == 0, v, 0.0), zero], 0)
        w1[last : last + 16, q * LANES : (q + 1) * LANES] = v.astype(BF16)
    w1[last + 16 :, :] = jnp.zeros((CP - last - 16, FP), BF16)

    def rows_two(base, first):
        count = CB + 2 if first + 7 >= LANES else CB + 1
        near = [flat[pl.ds(base + q, 8, stride=5), :] for q in range(count)]
        out = []
        for q in range(CB):
            v = jnp.where(lane >= first + row, near[q], near[q + 1])
            if first + 7 >= LANES:
                v = jnp.where(lane < first + row - LANES, near[q + 2], v)
            out.append(rotl_rows(v, first, 1))
        out[-1] = jnp.where(lane < C - (CB - 1) * LANES, out[-1], 0.0)
        return out

    def body_two(b, carry):
        for k in range(0, 16, 2):
            pair = [
                rows_two(ROW_TWO + 641 * b + 40 * (k + h), LANE_TWO + 8 * (k + h))
                for h in range(2)
            ]
            at = pl.ds(pl.multiple_of(128 * b + 8 * k, 16), 16)
            for q in range(CB):
                v = jnp.concatenate([pair[0][q], pair[1][q]], 0)
                w2[at, q * LANES : (q + 1) * LANES] = v.astype(BF16)
        return carry

    full = FF // LANES
    lax.fori_loop(0, full, body_two, 0)
    for q, v in enumerate(rows_two(ROW_TWO + 641 * full, LANE_TWO)):
        v = jnp.concatenate([jnp.where(row < FF - full * LANES, v, 0.0), zero], 0)
        w2[full * LANES : full * LANES + 16, q * LANES : (q + 1) * LANES] = v.astype(BF16)
    w2[full * LANES + 16 :, :] = jnp.zeros((FP - full * LANES - 16, CP), BF16)
    small[...] = jnp.zeros_like(small)
    put_row(small, 0, row_vector(flat, OFF_B1, FF))
    put_row(small, 1, row_vector(flat, OFF_B2, C))
    put_row(small, 2, row_vector(flat, OFF_GAIN, C))
    wd[...] = jnp.zeros_like(wd)
    wnf[...] = jnp.zeros_like(wnf)
    for k in range(K):
        put_row(wd, k, row_vector(flat, OFF_DISCO + k * C, C))
    for k in range(NOISE):
        put_row(wnf, 1 + k, row_vector(flat, OFF_NOISE + k * C, C))
    wn[...] = wnf[...].astype(BF16)


def neighbours():
    lat, lon = lax.axis_index("lat"), lax.axis_index("lon")
    nlat, nlon = lax.axis_size("lat"), lax.axis_size("lon")
    return lat, lon, nlat, nlon, lax.rem(lon + 1, nlon), lax.rem(lon + nlon - 1, nlon)


def halo_copies(cols, rows, corners, colh, rowh, cornh, send, recv, trow=None, trowh=None):
    lat, lon, nlat, nlon, east, west = neighbours()
    out = []

    def add(src, dst, target, k, sends, gets):
        out.append(
            (
                sends,
                gets,
                pltpu.make_async_remote_copy(
                    src_ref=src,
                    dst_ref=dst,
                    send_sem=send.at[k],
                    recv_sem=recv.at[k],
                    device_id=target,
                    device_id_type=MESH,
                ),
            )
        )

    has_up, has_down = lat > 0, lat < nlat - 1
    up, down = lat - 1, lat + 1
    add(rows.at[:, 0], rowh.at[:, 1], (up, lon), 2, has_up, has_down)
    add(rows.at[:, 1], rowh.at[:, 0], (down, lon), 3, has_down, has_up)
    add(cols.at[0], colh.at[1], (lat, west), 0, None, None)
    add(cols.at[1], colh.at[0], (lat, east), 1, None, None)
    add(corners.at[0, 0], cornh.at[1, 1], (up, west), 4, has_up, has_down)
    add(corners.at[0, 1], cornh.at[1, 0], (up, east), 5, has_up, has_down)
    add(corners.at[1, 0], cornh.at[0, 1], (down, west), 6, has_down, has_up)
    add(corners.at[1, 1], cornh.at[0, 0], (down, east), 7, has_down, has_up)
    if trow is not None:
        add(trow.at[0], trowh.at[1], (up, lon), 8, has_up, has_down)
        add(trow.at[1], trowh.at[0], (down, lon), 9, has_down, has_up)
    return out


def start_halo(copies):
    for sends, _, copy in copies:
        if sends is None:
            copy.start()
        else:
            pl.when(sends)(copy.start)


def wait_halo(copies):
    for sends, gets, copy in copies:
        if sends is None:
            copy.wait()
        else:
            pl.when(sends)(copy.wait_send)
            pl.when(gets)(copy.wait_recv)


def greet(bits, halo):
    barrier = pltpu.get_barrier_semaphore()
    lat, lon, nlat, nlon, east, west = neighbours()

    def hello(target):
        pl.semaphore_signal(barrier, inc=1, device_id=target, device_id_type=MESH)

    count = 0
    for axis, bit in bits:
        hello(partner(axis, bit))
        count += 1
    if halo:
        for target in ((lat, east), (lat, west)):
            hello(target)
            count += 1
        for side, cond in ((lat - 1, lat > 0), (lat + 1, lat < nlat - 1)):

            @pl.when(cond)
            def _(side=side):
                for x in (lon, east, west):
                    hello((side, x))

    if halo:
        count = count + 3 * (lat > 0).astype(jnp.int32) + 3 * (lat < nlat - 1).astype(jnp.int32)
    pl.semaphore_wait(barrier, count)


def gather_kernel(
    mesh, share_ref, cols, rows, corners, trow,
    w1, w2, wn, wd, small, colh, rowh, cornh, trowh,
    buf, flat, wnf, send, recv, hsend, hrecv, local_sem,
):
    bits = bit_list(mesh)
    orders = stage_orders(mesh)
    mine = my_bits(bits)
    n = len(bits)
    shard_rows = share_ref.shape[0]
    cut = (shard_rows // 2 + 15) // 16 * 16
    spans = [(0, cut), (cut, shard_rows - cut)]
    own = pltpu.make_async_copy(share_ref, buf.at[tuple(mine)], local_sem)
    own.start()
    greet(bits, True)
    halos = halo_copies(cols, rows, corners, colh, rowh, cornh, hsend, hrecv, trow, trowh)

    def copy(colour, k):
        order = orders[colour]
        done = order[:k]
        start, count = spans[colour]
        index = tuple(slice(None) if i in done else mine[i] for i in range(n)) + (
            pl.ds(start, count),
        )
        return pltpu.make_async_remote_copy(
            src_ref=buf.at[index],
            dst_ref=buf.at[index],
            send_sem=send.at[colour, k],
            recv_sem=recv.at[colour, k],
            device_id=partner(*bits[order[k]]),
            device_id_type=MESH,
        )

    own.wait()
    for colour in range(2):
        copy(colour, 0).start()
    start_halo(halos)
    for k in range(n):
        for colour in range(2):
            copy(colour, k).wait()
            if k + 1 < n:
                copy(colour, k + 1).start()
    wait_halo(halos)
    lat, _, nlat, *_ = neighbours()
    for r, cond in ((0, lat == 0), (1, lat == nlat - 1)):

        @pl.when(cond)
        def _(r=r):
            for i in range(rowh.shape[0]):
                rowh[i, r] = jnp.zeros(rowh.shape[2:], rowh.dtype)
            trowh[r] = jnp.zeros(trowh.shape[1:], F32)
            for s in range(2):
                cornh[r, s] = jnp.zeros(cornh.shape[2:], cornh.dtype)

    total = 1 << n

    def widen(d, carry):
        index = tuple((d >> (n - 1 - i)) & 1 for i in range(n))
        flat[pl.ds(d * shard_rows, shard_rows), :] = buf[index].astype(F32)
        return carry

    lax.fori_loop(0, total, widen, 0)
    flat[total * shard_rows :, :] = jnp.zeros((flat.shape[0] - total * shard_rows, LANES), F32)
    unpack_weights(flat, w1, w2, wn, wd, small, wnf)


def gather_weights(mesh, share, cols, rows, corners, trow):
    bits = bit_list(mesh)
    n = len(bits)
    shard_rows = share.shape[0]
    total = shard_rows << n
    sd = jax.ShapeDtypeStruct
    return pl.pallas_call(
        partial(gather_kernel, mesh),
        name="gather_weights",
        out_shape=(
            sd((CP, FP), BF16),
            sd((FP, CP), BF16),
            sd((LANES, CP), BF16),
            sd((16, CP), F32),
            sd((8, FP), F32),
            sd(cols.shape, BF16),
            sd(rows.shape, BF16),
            sd(corners.shape, BF16),
            sd(trow.shape, F32),
        ),
        in_specs=[vmem_spec()] * 5,
        out_specs=(vmem_spec(),) * 9,
        scratch_shapes=[
            pltpu.VMEM((2,) * n + (shard_rows, LANES), BF16),
            pltpu.VMEM((total + 96, LANES), F32),
            pltpu.VMEM((LANES, CP), F32),
            pltpu.SemaphoreType.DMA((2, n)),
            pltpu.SemaphoreType.DMA((2, n)),
            pltpu.SemaphoreType.DMA((10,)),
            pltpu.SemaphoreType.DMA((10,)),
            pltpu.SemaphoreType.DMA,
        ],
        compiler_params=params(collective_id=0, has_side_effects=True),
    )(share, cols, rows, corners, trow)


def norm_parts(x):
    mean = jnp.mean(x, -1, keepdims=True)
    center = x - mean
    var = jnp.mean(center * center, -1, keepdims=True)
    return center, lax.rsqrt(var + 1e-05)


def rounded(v):
    return v.astype(BF16).astype(F32)


def stencil_fwd_kernel(
    chunks, cells, height_ref, x_ref, colh, rowh, cornh, table, wd, gain, aug, wn,
    out_ref, mix_ref, mean_ref, inv_ref, m_scr, k_scr, nt_scr,
):
    step = pl.program_id(0)
    rows = x_ref.shape[1]
    width = chunks * cells
    height = height_ref[0]
    gvec = gain[2:3, :C]

    def put_cell(column, x, top, low, j=None):
        mean = jnp.mean(x, -1, keepdims=True)
        center = x - mean
        inv = lax.rsqrt(jnp.mean(center * center, -1, keepdims=True) + 1e-05)
        mixed = rounded(center * inv * gvec)
        hrow = iota((rows, C), 0)
        if j is not None:
            mean_ref[j] = jnp.broadcast_to(mean, (rows, LANES))
            inv_ref[j] = jnp.broadcast_to(inv, (rows, LANES))
            mix_ref[j, :, :C] = jnp.where(hrow < height, mixed, 0.0).astype(BF16)
        mixed = jnp.where(hrow < height, mixed, jnp.where(hrow == height, low, 0.0))
        at = column * SLOTS
        for g in range(CB):
            lo, hi = g * LANES, min((g + 1) * LANES, C)
            m_scr[g, pl.ds(at + 1, rows), : hi - lo] = mixed[:, lo:hi]
            m_scr[g, pl.ds(at, 1), : hi - lo] = top[:, lo:hi]
            m_scr[g, pl.ds(at + rows + 1, 1), : hi - lo] = low[:, lo:hi]

    def halo_mix(v):
        center, inv = norm_parts(v.astype(F32))
        return rounded(center * inv * gvec)

    @pl.when(step == 0)
    def _():
        k_scr[...] = jnp.dot(
            table[...], wd[...], preferred_element_type=F32, precision=HIGHEST
        ).reshape(k_scr.shape)
        for side in range(2):
            for i in range(REACH):
                column = i if side == 0 else width + REACH + i
                top = halo_mix(cornh[0, side])[i : i + 1]
                low = halo_mix(cornh[1, side])[i : i + 1]
                put_cell(column, colh[side, i].astype(F32), top, low)

    @pl.when(step < chunks)
    def _():
        nt_scr[0:cells, :C] = halo_mix(rowh[0, 0])
        nt_scr[32 : 32 + cells, :C] = halo_mix(rowh[0, 1])
        lanes = slice((CB - 1) * LANES, CB * LANES)
        mix_ref[:, :, lanes] = jnp.zeros((cells, rows, LANES), BF16)

        def cell(j, carry):
            put_cell(
                step * cells + j + REACH,
                x_ref[j].astype(F32),
                nt_scr[pl.ds(j, 1), :C],
                nt_scr[pl.ds(32 + j, 1), :C],
                j,
            )
            return carry

        lax.fori_loop(0, cells, cell, 0, unroll=3)

    @pl.when(step >= chunks)
    def _():
        first = (step - chunks) * cells
        nt_scr[...] = jnp.dot(
            aug[...].reshape(cells * rows, LANES), wn[...], preferred_element_type=F32
        )
        lane = iota((8, LANES), 1)
        for g in range(CB):
            lanes = slice(g * LANES, (g + 1) * LANES)
            for hb in range(rows // 8):
                at = slice(8 * hb, 8 * hb + 8)

                def cell(i, carry):
                    j = i * REUSE
                    acc = [nt_scr[pl.ds((j + u) * rows + 8 * hb, 8), lanes] for u in range(REUSE)]
                    for l in range(3):
                        near = [
                            m_scr[g, pl.ds((first + j + u) * SLOTS + 8 * hb + l, 8), :]
                            for u in range(REUSE + 2 * REACH)
                        ]
                        for w in range(5):
                            tap = k_scr[5 * l + w, at, lanes]
                            acc = [a + tap * near[u + w] for u, a in enumerate(acc)]
                    for u in range(REUSE):
                        v = acc[u]
                        if g == CB - 1:
                            v = jnp.where(lane == 0, v, aug[j + u, at, :].astype(F32))
                        out_ref[j + u, at, lanes] = v.astype(BF16)
                    return carry

                lax.fori_loop(0, cells // REUSE, cell, 0)


def stencil_fwd(height, x, colh, rowh, cornh, table, wd, small, aug, wn, chunks):
    width, rows, _ = x.shape
    cells = width // chunks
    assert cells % REUSE == 0
    first = lambda i: jnp.where(i < chunks, i, chunks - 1)
    second = lambda i: jnp.where(i < chunks, 0, i - chunks)
    sd = jax.ShapeDtypeStruct
    by_first = lambda c: pl.BlockSpec((cells, rows, c), lambda i: (first(i), 0, 0))
    by_second = lambda c: pl.BlockSpec((cells, rows, c), lambda i: (second(i), 0, 0))
    return pl.pallas_call(
        partial(stencil_fwd_kernel, chunks, cells),
        name="stencil_fwd",
        grid=(2 * chunks,),
        out_shape=(
            sd((width, rows, CP), BF16),
            sd((width, rows, CP), BF16),
            sd((width, rows, LANES), F32),
            sd((width, rows, LANES), F32),
        ),
        in_specs=[
            pl.BlockSpec(memory_space=pltpu.SMEM),
            by_first(C),
            vmem_spec(),
            pl.BlockSpec((1, 2, cells, C), lambda i: (first(i), 0, 0, 0)),
            vmem_spec(),
            vmem_spec(),
            vmem_spec(),
            vmem_spec(),
            by_second(LANES),
            vmem_spec(),
        ],
        out_specs=(by_second(CP), by_first(CP), by_first(LANES), by_first(LANES)),
        scratch_shapes=[
            pltpu.VMEM((CB, (width + 2 * REACH) * SLOTS, LANES), F32),
            pltpu.VMEM((TAPS, rows, CP), F32),
            pltpu.VMEM((cells * rows, CP), F32),
        ],
        compiler_params=params(dimension_semantics=("arbitrary",)),
    )(height, x, colh, rowh, cornh, table, wd, small, aug, wn)


def pack_weights(one, two, flat):
    lane = iota((8, LANES), 1)
    row = iota((8, LANES), 0)
    flat[...] = jnp.zeros_like(flat)

    def turned(v, first, unit):
        return pltpu.roll(v, first, 1, stride=unit, stride_axis=0)

    def main(ref, at, first, unit, out, base, step, count):
        keep = lane >= first + unit * row
        before = jnp.zeros((8, LANES), F32)
        for q in range(count):
            now = turned(ref[q, at, :], first, unit)
            flat[pl.ds(base + q, 8, stride=step), :] = jnp.where(keep, now, before)
            before = now

    def rest(ref, at, first, unit, count, width, mask=None):
        s = first + unit * row
        before = turned(ref[count - 1, at, :], first, unit)
        now = turned(ref[count, at, :], first, unit)
        v = jnp.where(lane < s, before, jnp.where(lane < s + width, now, 0.0))
        return v if mask is None else jnp.where(mask, v, 0.0)

    shift = 8 - LANE_TWO
    base_two = ROW_TWO - 5 * LANE_TWO
    full = FF // LANES
    extra = C - (CB - 1) * LANES

    def two_main(b, carry):
        for k in range(16):
            at = pl.ds(128 * b + 8 * k + shift, 8)
            main(two, at, 8 * k, 1, flat, base_two + 641 * b + 40 * k, 5, CB - 1)
        return carry

    lax.fori_loop(0, full, two_main, 0)
    end = slice(128 * full + shift, 128 * full + shift + 8)
    mask = row < FF - full * LANES + LANE_TWO
    before = jnp.zeros((8, LANES), F32)
    for q in range(CB - 1):
        now = jnp.where(mask, turned(two[q, end, :], 0, 1), 0.0)
        at = pl.ds(base_two + 641 * full + q, 8, stride=5)
        flat[at, :] = jnp.where(lane >= row, now, before)
        before = now

    def one_main(b, carry):
        for k in range(8):
            at = pl.ds(pl.multiple_of(64 * b + 8 * k, 8), 8)
            main(one, at, 16 * k, 2, flat, 641 * b + 80 * k, 10, FB - 1)
        return carry

    last = C - 1
    assert last % 64 == 0
    lax.fori_loop(0, last // 64, one_main, 0)
    row_last = 641 * (last // 64)
    for q in range(FB - 1):
        flat[row_last + q : row_last + q + 1, :] = one[q, last : last + 1, :]

    def add_all(places, values):
        olds = [flat[at, :] for at in places]
        for at, old, v in zip(places, olds, values):
            flat[at, :] = old + v

    def one_rest(b, carry):
        values = [
            rest(one, pl.ds(pl.multiple_of(64 * b + 8 * k, 8), 8), 16 * k, 2, FB - 1, FF - (FB - 1) * LANES)
            for k in range(8)
        ]
        add_all([pl.ds(641 * b + 80 * k + FB - 1, 8, stride=10) for k in range(8)], values)
        return carry

    lax.fori_loop(0, last // 64, one_rest, 0)
    lane1 = iota((1, LANES), 1)
    v = jnp.where(lane1 < FF - (FB - 1) * LANES, one[FB - 1, last : last + 1, :], 0.0)
    add_all([slice(row_last + FB - 1, row_last + FB)], [v])

    def two_rest(b, carry):
        values = [
            rest(two, pl.ds(128 * b + 8 * k + shift, 8), 8 * k, 1, CB - 1, extra) for k in range(16)
        ]
        places = [pl.ds(base_two + 641 * b + 40 * k + CB - 1, 8, stride=5) for k in range(16)]
        add_all(places, values)
        return carry

    lax.fori_loop(0, full, two_rest, 0)
    add_all(
        [pl.ds(base_two + 641 * full + CB - 1, 8, stride=5)],
        [rest(two, end, 0, 1, CB - 1, extra, mask)],
    )


GELU_A = math.sqrt(2.0 / math.pi)
GELU_B = 0.044715
WIDE = 256


def dot(a, b, dims=((1,), (0,))):
    return lax.dot_general(a, b, (dims, ((), ())), preferred_element_type=F32)


def mlp_kernel(
    blocks, height_ref, conv_ref, g_ref, x_ref, w1, w2, small,
    out_ref, gconv_ref, rows_ref, cols_ref, corn_ref, flat_ref, extra_ref,
    one, two, g_scr, conv_t, act, gh,
):
    step = pl.program_id(0)
    cells, rows, _ = x_ref.shape
    m = cells * rows
    height = height_ref[0]

    @pl.when(step == 0)
    def _():
        one[...] = jnp.zeros_like(one)
        two[...] = jnp.zeros_like(two)
        g_scr[...] = jnp.zeros_like(g_scr)

    live = (iota((1, rows, 1), 1) < height).astype(F32)
    g_scr[:, :C] = (g_ref[...].astype(F32) * live).reshape(m, C).astype(BF16)
    rows_one = conv_t.shape[0]

    def hidden(start, wide, tail):
        lanes = pl.ds(start, wide)
        h = dot(conv_ref[...].reshape(m, CP), w1[:, lanes]) + small[0:1, lanes]
        ga = dot(g_scr[...], w2[lanes, :], ((1,), (1,)))
        h2 = h * h
        t = jnp.tanh(h * (GELU_A + (GELU_A * GELU_B) * h2))
        cdf = 0.5 * t + 0.5
        value = (h * cdf).astype(BF16)
        slope = cdf + h * (0.5 - 0.5 * (t * t)) * (GELU_A + (3 * GELU_A * GELU_B) * h2)
        if tail:
            ones = iota((m, wide), 1) == FF - (FB - 1) * LANES
            value = jnp.where(ones, jnp.ones_like(value), value)
        act[:, lanes] = value
        gh[:, lanes] = (ga * slope).astype(BF16)

    def turn(i, count):
        part = conv_ref[:, :, pl.ds(i * LANES, LANES)].reshape(m, LANES)
        conv_t[pl.ds(i * LANES, count), :] = part.T[:count]

    def first(f, carry):
        turn(pl.multiple_of(f, 1), LANES)
        hidden(pl.multiple_of(f * WIDE, WIDE), WIDE, False)
        return carry

    lax.fori_loop(0, FP // WIDE, first, 0)
    assert FP // WIDE == CB - 1
    turn(CB - 1, rows_one - (CB - 1) * LANES)
    hidden(FP // WIDE * WIDE, FP % WIDE, True)

    for n in range(CP // WIDE):
        lanes = slice(n * WIDE, (n + 1) * WIDE)
        end = min((n + 1) * WIDE, C)
        part = slice(n * WIDE, end)
        branch = dot(act[...], w2[:, lanes])[:, : end - n * WIDE]
        v = x_ref[:, :, part].astype(F32).reshape(m, -1) + branch + small[1:2, part]
        out_ref[:, :, part] = (v.reshape(cells, rows, -1) * live).astype(BF16)
        gc = dot(gh[...], w1[lanes, :], ((1,), (1,)))
        gconv_ref[:, :, lanes] = gc.reshape(cells, rows, WIDE)

    def weights(start, wide):
        lanes = pl.ds(start, wide)
        r1 = dot(conv_t[...], gh[:, lanes])
        r2 = dot(act[:, lanes], g_scr[...], ((0,), (0,)))
        for i in range(wide // LANES):
            one[start // LANES + i] += r1[:, i * LANES : (i + 1) * LANES]
        for q in range(CB):
            two[q, pl.ds(start + 8, wide), :] += r2[:, q * LANES : (q + 1) * LANES]

    def third(f, carry):
        weights(pl.multiple_of(f * WIDE, WIDE), WIDE)
        return carry

    lax.fori_loop(0, FP // WIDE, third, 0)
    weights(FP // WIDE * WIDE, FP % WIDE)

    onehot = (iota((1, rows, 1), 1) == height - 1).astype(F32)
    block = gconv_ref[...]
    edges = (block[:, 0, :].astype(BF16), jnp.sum(block * onehot, 1).astype(BF16))
    for r in range(2):
        rows_ref[0, r] = edges[r]
    for side, at, first in ((0, 0, 0), (1, blocks - 1, cells - REACH)):

        @pl.when(step == at)
        def _(side=side, first=first):
            for i in range(REACH):
                cols_ref[side, i] = gconv_ref[first + i].astype(BF16)
            for r in range(2):
                corn_ref[r, side] = edges[r][first : first + REACH]

    @pl.when(step == blocks - 1)
    def _():
        extra_ref[...] = jnp.zeros_like(extra_ref)
        for q in range(FB):
            extra_ref[0 : NOISE + 1, q * LANES : (q + 1) * LANES] = one[q, C : C + NOISE + 1, :]
        for q in range(CB):
            lanes = slice(q * LANES, (q + 1) * LANES)
            extra_ref[NOISE + 1 : NOISE + 2, lanes] = two[q, FF + 8 : FF + 9, :]
        pack_weights(one, two, flat_ref)


def mlp(height, conv, g, x, w1, w2, small, flat_rows, blocks):
    width, rows, _ = x.shape
    cells = width // blocks
    m = cells * rows
    sd = jax.ShapeDtypeStruct
    block = lambda c: pl.BlockSpec((cells, rows, c), lambda i: (i, 0, 0))
    rows_one = -(-(C + NOISE + 1) // 16) * 16
    flops = 12 * width * rows * C * FF
    return pl.pallas_call(
        partial(mlp_kernel, blocks),
        name="mlp",
        grid=(blocks,),
        out_shape=(
            sd((width, rows, C), BF16),
            sd((width, rows, CP), F32),
            sd((blocks, 2, cells, CP), BF16),
            sd((2, REACH, rows, CP), BF16),
            sd((2, 2, REACH, CP), BF16),
            sd((flat_rows, LANES), F32),
            sd((16, FP), F32),
        ),
        in_specs=[
            pl.BlockSpec(memory_space=pltpu.SMEM),
            block(CP),
            block(C),
            block(C),
            vmem_spec(),
            vmem_spec(),
            vmem_spec(),
        ],
        out_specs=(
            block(C),
            block(CP),
            pl.BlockSpec((1, 2, cells, CP), lambda i: (i, 0, 0, 0)),
            vmem_spec(),
            vmem_spec(),
            vmem_spec(),
            vmem_spec(),
        ),
        scratch_shapes=[
            pltpu.VMEM((FB, rows_one, LANES), F32),
            pltpu.VMEM((CB, FP + 16, LANES), F32),
            pltpu.VMEM((m, CP), BF16),
            pltpu.VMEM((rows_one, m), BF16),
            pltpu.VMEM((m, FP), BF16),
            pltpu.VMEM((m, FP), BF16),
        ],
        compiler_params=params(dimension_semantics=("arbitrary",)),
        cost_estimate=pl.CostEstimate(flops=flops, bytes_accessed=50_000_000, transcendentals=0),
    )(height, conv, g, x, w1, w2, small)


def exchange_kernel(cols, rows, corners, colh, rowh, cornh, send, recv):
    greet([], True)
    halos = halo_copies(cols, rows, corners, colh, rowh, cornh, send, recv)
    start_halo(halos)
    wait_halo(halos)
    lat, _, nlat, *_ = neighbours()
    for r, cond in ((0, lat == 0), (1, lat == nlat - 1)):

        @pl.when(cond)
        def _(r=r):
            for i in range(rowh.shape[0]):
                rowh[i, r] = jnp.zeros(rowh.shape[2:], rowh.dtype)
            for s in range(2):
                cornh[r, s] = jnp.zeros(cornh.shape[2:], cornh.dtype)


def exchange(cols, rows, corners):
    sd = jax.ShapeDtypeStruct
    return pl.pallas_call(
        exchange_kernel,
        name="exchange_edges",
        out_shape=(sd(cols.shape, BF16), sd(rows.shape, BF16), sd(corners.shape, BF16)),
        in_specs=[vmem_spec()] * 3,
        out_specs=(vmem_spec(),) * 3,
        scratch_shapes=[pltpu.SemaphoreType.DMA((8,)), pltpu.SemaphoreType.DMA((8,))],
        compiler_params=params(collective_id=1, has_side_effects=True),
    )(cols, rows, corners)


def scatter_kernel(mesh, flat, out_ref, buf, *rest):
    bits = bit_list(mesh)
    n = len(bits)
    recvs, (send, recv) = rest[:n], rest[n:]
    orders = [order[::-1] for order in stage_orders(mesh)]
    mine = my_bits(bits)
    shard_rows = out_ref.shape[0]
    cut = (shard_rows // 2 + 7) // 8 * 8
    spans = [(0, cut), (cut, shard_rows - cut)]

    def shard_index(d):
        return tuple((d >> (n - 1 - i)) & 1 for i in range(n))

    def fill(d, carry):
        buf[shard_index(d)] = flat[pl.ds(d * shard_rows, shard_rows), :]
        return carry

    lax.fori_loop(0, 1 << n, fill, 0)
    greet(bits, False)

    def copy(colour, k):
        order = orders[colour]
        done, now = order[:k], order[k]
        start, count = spans[colour]
        index = tuple(
            1 - mine[i] if i == now else mine[i] if i in done else slice(None) for i in range(n)
        )
        at = pl.ds(start, count)
        return pltpu.make_async_remote_copy(
            src_ref=buf.at[index + (at,)],
            dst_ref=recvs[k].at[(slice(None),) * (n - 1 - k) + (at,)],
            send_sem=send.at[colour, k],
            recv_sem=recv.at[colour, k],
            device_id=partner(*bits[now]),
            device_id_type=MESH,
        )

    def accumulate(colour, k):
        order = orders[colour]
        start, count = spans[colour]
        free = [i for i in range(n) if i not in order[: k + 1]]

        def add(d, carry):
            sub = tuple((d >> (len(free) - 1 - i)) & 1 for i in range(len(free)))
            index = tuple(sub[free.index(i)] if i in free else mine[i] for i in range(n))
            at = pl.ds(start, count)
            buf[index + (at,)] = buf[index + (at,)] + recvs[k][sub + (at,)]
            return carry

        lax.fori_loop(0, 1 << len(free), add, 0)

    for colour in range(2):
        copy(colour, 0).start()
    for k in range(n):
        for colour in range(2):
            copy(colour, k).wait()
            accumulate(colour, k)
            if k + 1 < n:
                copy(colour, k + 1).start()
    out_ref[...] = buf[tuple(mine)]


def scatter(mesh, flat, shard_rows):
    n = len(bit_list(mesh))
    return pl.pallas_call(
        partial(scatter_kernel, mesh),
        name="reduce_scatter",
        out_shape=jax.ShapeDtypeStruct((shard_rows, LANES), F32),
        in_specs=[vmem_spec()],
        out_specs=vmem_spec(),
        scratch_shapes=[pltpu.VMEM((2,) * n + (shard_rows, LANES), F32)]
        + [pltpu.VMEM((2,) * (n - 1 - k) + (shard_rows, LANES), F32) for k in range(n)]
        + [pltpu.SemaphoreType.DMA((2, n)), pltpu.SemaphoreType.DMA((2, n))],
        compiler_params=params(collective_id=2, has_side_effects=True),
    )(flat)


def add_vector(tail, offset, value):
    row, shift = divmod(offset - TAIL_ROW * LANES, LANES)
    blocks = value.shape[0]
    lane = iota((blocks + 1, LANES), 1)
    zero = jnp.zeros((1, LANES), F32)
    here = pltpu.roll(jnp.concatenate([value, zero], 0), shift, 1) if shift else jnp.concatenate([value, zero], 0)
    back = jnp.concatenate([zero, here[:blocks]], 0)
    at = slice(row, row + blocks + 1)
    tail[at, :] = tail[at, :] + jnp.where(lane >= shift, here, back if shift else here)


def as_blocks(value, length):
    blocks = -(-length // LANES)
    v = jnp.concatenate([value[:, q * LANES : (q + 1) * LANES] for q in range(blocks)], 0)
    index = iota((blocks, LANES), 0) * LANES + iota((blocks, LANES), 1)
    return jnp.where(index < length, v, 0.0)


def stencil_bwd_kernel(
    chunks, cells, height_ref, x_ref, mix_ref, mean_ref, inv_ref, g_ref, gconv_ref,
    colh, rowh, cornh, table, trowh, wd, gain, extra, w1,
    out_ref, tail_ref, g_scr, m_scr, k_scr, t_scr, e_scr, gg_scr, row_scr,
):
    step = pl.program_id(0)
    rows = x_ref.shape[1]
    width = chunks * cells
    height = height_ref[0]
    gvec = gain[2:3, :C]

    def put_column(column, v, top, low):
        v = jnp.where(iota((rows, CP), 0) == height, low, v)
        at = column * SLOTS
        for q in range(CB):
            lanes = slice(q * LANES, (q + 1) * LANES)
            g_scr[q, pl.ds(at + 1, rows), :] = v[:, lanes]
            g_scr[q, pl.ds(at, 1), :] = top[:, lanes]
            g_scr[q, pl.ds(at + rows + 1, 1), :] = low[:, lanes]

    @pl.when(step == 0)
    def _():
        hrow = iota((rows, 16), 0)
        for t in range(TAPS):
            l = t // 5
            own = table[t * rows : (t + 1) * rows, :]
            if l == 0:
                own = jnp.concatenate([own[1:], own[:1]], 0)
                own = jnp.where(hrow == height - 1, trowh[1, t : t + 1, :], own)
            if l == 2:
                own = jnp.concatenate([trowh[0, t : t + 1, :], own[: rows - 1]], 0)
            t_scr[t * rows : (t + 1) * rows, :] = own
        k_scr[...] = jnp.dot(
            t_scr[...], wd[...], preferred_element_type=F32, precision=HIGHEST
        ).reshape(k_scr.shape)
        e_scr[...] = jnp.zeros_like(e_scr)
        gg_scr[...] = jnp.zeros_like(gg_scr)
        for side in range(2):
            for i in range(REACH):
                column = i if side == 0 else width + REACH + i
                put_column(
                    column,
                    colh[side, i].astype(F32),
                    cornh[0, side].astype(F32)[i : i + 1],
                    cornh[1, side].astype(F32)[i : i + 1],
                )

    @pl.when(step < chunks)
    def _():
        row_scr[0:cells, :] = rowh[0, 0].astype(F32)
        row_scr[32 : 32 + cells, :] = rowh[0, 1].astype(F32)

        def cell(j, carry):
            put_column(
                step * cells + j + REACH,
                gconv_ref[j],
                row_scr[pl.ds(j, 1), :],
                row_scr[pl.ds(32 + j, 1), :],
            )
            mixed = mix_ref[j].astype(F32)
            for q in range(CB):
                m_scr[q, step * cells + j] = mixed[:, q * LANES : (q + 1) * LANES]
            return carry

        lax.fori_loop(0, cells, cell, 0, unroll=2)

    @pl.when(step == chunks)
    def _():
        for q in range(CB):
            lanes = slice(q * LANES, (q + 1) * LANES)
            for hb in range(rows // 8):
                at = slice(8 * hb, 8 * hb + 8)

                def cell(i, carry):
                    j = i * REUSE
                    mixed = [m_scr[q, j + u, at, :] for u in range(REUSE)]
                    total = [None] * REUSE
                    for l in range(3):
                        near = [
                            g_scr[q, pl.ds((j + u) * SLOTS + 8 * hb + 2 - l, 8), :]
                            for u in range(REUSE + 2 * REACH)
                        ]
                        for w in range(5):
                            t = 5 * l + w
                            tap = k_scr[t, at, lanes]
                            views = near[2 * REACH - w : 2 * REACH - w + REUSE]
                            terms = [tap * v for v in views]
                            total = [a if b is None else a + b for a, b in zip(terms, total)]
                            sums = [m * v for m, v in zip(mixed, views)]
                            while len(sums) > 1:
                                sums = [
                                    sums[k] + sums[k + 1] if k + 1 < len(sums) else sums[k]
                                    for k in range(0, len(sums), 2)
                                ]
                            e_scr[t, at, lanes] = e_scr[t, at, lanes] + sums[0]
                    for u in range(REUSE):
                        m_scr[q, j + u, at, :] = total[u]
                    return carry

                lax.fori_loop(0, width // REUSE, cell, 0)

    @pl.when(step > chunks)
    def _():
        first = (step - chunks - 1) * cells
        live = iota((rows, C), 0) < height

        def cell(j, total):
            inv = inv_ref[j][:, :1]
            normed = (x_ref[j].astype(F32) - mean_ref[j][:, :1]) * inv
            gm = jnp.concatenate([m_scr[q, first + j] for q in range(CB)], 1)[:, :C]
            gm = jnp.where(live, gm, 0.0)
            total = total + gm * normed
            v = gm * gvec
            mean = jnp.mean(v, -1, keepdims=True)
            mean_n = jnp.mean(v * normed, -1, keepdims=True)
            up = jnp.where(live, g_ref[j].astype(F32), 0.0)
            out_ref[j] = inv * (v - mean - normed * mean_n) + up
            return total

        gg_scr[:, :C] = lax.fori_loop(0, cells, cell, gg_scr[:, :C], unroll=2)

    @pl.when(step == 2 * chunks)
    def _():
        tail_ref[...] = jnp.zeros_like(tail_ref)
        add_vector(tail_ref, OFF_B1, as_blocks(extra[NOISE : NOISE + 1, :], FF))
        add_vector(tail_ref, OFF_B2, as_blocks(extra[NOISE + 1 : NOISE + 2, :], C))
        add_vector(tail_ref, OFF_GAIN, as_blocks(jnp.sum(gg_scr[...], 0, keepdims=True), C))
        disco = lax.dot_general(
            t_scr[...], e_scr[...].reshape(TAPS * rows, CP), (((0,), (0,)), ((), ())),
            preferred_element_type=F32, precision=HIGHEST,
        )
        for k in range(K):
            add_vector(tail_ref, OFF_DISCO + k * C, as_blocks(disco[k : k + 1, :], C))
        ng = extra[0:NOISE, :]
        hi = ng.astype(BF16)
        mid = (ng - hi.astype(F32)).astype(BF16)
        lo = (ng - hi.astype(F32) - mid.astype(F32)).astype(BF16)
        parts = [dot(p, w1[...], ((1,), (1,))) for p in (hi, mid, lo)]
        gn = parts[0] + parts[1] + parts[2]
        for k in range(NOISE):
            add_vector(tail_ref, OFF_NOISE + k * C, as_blocks(gn[k : k + 1, :], C))


def stencil_bwd(
    height, x, mixed, mean, inv, g, gconv, colh, rowh, cornh, table, trowh, wd, small, extra, w1,
    tail_rows, chunks,
):
    width, rows, _ = x.shape
    cells = width // chunks
    first = lambda i: jnp.where(i < chunks, i, chunks - 1)
    third = lambda i: jnp.where(i <= chunks, 0, i - chunks - 1)
    sd = jax.ShapeDtypeStruct
    by_first = lambda c: pl.BlockSpec((cells, rows, c), lambda i: (first(i), 0, 0))
    by_third = lambda c: pl.BlockSpec((cells, rows, c), lambda i: (third(i), 0, 0))
    return pl.pallas_call(
        partial(stencil_bwd_kernel, chunks, cells),
        name="stencil_bwd",
        grid=(2 * chunks + 1,),
        out_shape=(sd((width, rows, C), F32), sd((tail_rows, LANES), F32)),
        in_specs=[
            pl.BlockSpec(memory_space=pltpu.SMEM),
            by_third(C),
            by_first(CP),
            by_third(LANES),
            by_third(LANES),
            by_third(C),
            by_first(CP),
            vmem_spec(),
            pl.BlockSpec((1, 2, cells, CP), lambda i: (first(i), 0, 0, 0)),
        ]
        + [vmem_spec()] * 7,
        out_specs=(by_third(C), vmem_spec()),
        scratch_shapes=[
            pltpu.VMEM((CB, (width + 2 * REACH) * SLOTS, LANES), F32),
            pltpu.VMEM((CB, width, rows, LANES), F32),
            pltpu.VMEM((TAPS, rows, CP), F32),
            pltpu.VMEM((TAPS * rows, 16), F32),
            pltpu.VMEM((TAPS, rows, CP), F32),
            pltpu.VMEM((rows, CP), F32),
            pltpu.VMEM((64, CP), F32),
        ],
        compiler_params=params(dimension_semantics=("arbitrary",)),
    )(height, x, mixed, mean, inv, g, gconv, colh, rowh, cornh, table, trowh, wd, small, extra, w1)


def tail_kernel(mesh, part_ref, tail_ref, grad_ref, scale_ref, got, msg, full, place, send, recv):
    nlat, nlon = mesh.shape["lat"], mesh.shape["lon"]
    n = nlat * nlon
    lat, lon = lax.axis_index("lat"), lax.axis_index("lon")
    me = lat * nlon + lon
    piece = tail_ref.shape[1]
    shard_rows = part_ref.shape[0]
    barrier = pltpu.get_barrier_semaphore()

    def others(body):
        def step(i, carry):
            body(lax.rem(me + i, n))
            return carry

        lax.fori_loop(1, n, step, 0)

    def hello(d):
        pl.semaphore_signal(
            barrier, inc=1, device_id=(d // nlon, lax.rem(d, nlon)), device_id_type=MESH
        )

    others(hello)
    pl.semaphore_wait(barrier, n - 1)

    def scatter_piece(d):
        pltpu.make_async_remote_copy(
            src_ref=tail_ref.at[d],
            dst_ref=got.at[me],
            send_sem=send.at[0],
            recv_sem=recv.at[0],
            device_id=(d // nlon, lax.rem(d, nlon)),
            device_id_type=MESH,
        ).start()

    def wait_all(buffer, k):
        pltpu.make_async_remote_copy(
            src_ref=buffer.at[pl.ds(0, n - 1)],
            dst_ref=buffer.at[pl.ds(0, n - 1)],
            send_sem=send.at[k],
            recv_sem=recv.at[k],
            device_id=(lat, lon),
            device_id_type=MESH,
        ).wait()

    others(scatter_piece)
    got[me] = tail_ref[me]
    square = jnp.sum(part_ref[...] * part_ref[...])
    wait_all(got, 0)

    total = lax.fori_loop(
        1, n, lambda i, acc: acc + got[lax.rem(i, n)], got[0]
    )
    square = square + jnp.sum(total * total)
    msg[0:piece, :] = total
    msg[piece : piece + 1, :] = jnp.broadcast_to(square, (1, LANES))

    def share(d):
        pltpu.make_async_remote_copy(
            src_ref=msg,
            dst_ref=full.at[me],
            send_sem=send.at[1],
            recv_sem=recv.at[1],
            device_id=(d // nlon, lax.rem(d, nlon)),
            device_id_type=MESH,
        ).start()

    others(share)
    full[me] = msg[...]
    place[...] = jnp.zeros_like(place)
    wait_all(full, 1)

    def take(d, acc):
        place[pl.ds(shard_rows + d * piece, piece), :] = full[d, 0:piece, :]
        return acc + full[d, piece : piece + 1, :]

    squares = lax.fori_loop(0, n, take, jnp.zeros((1, LANES), F32))
    start = jnp.clip(me * shard_rows - TAIL_ROW + shard_rows, 0, shard_rows + n * piece)
    grad_ref[...] = part_ref[...] + place[pl.ds(start, shard_rows), :]
    scale_ref[...] = jnp.broadcast_to(jnp.sqrt(squares), scale_ref.shape)


def finish(mesh, part, tail):
    n, piece, _ = tail.shape
    shard_rows = part.shape[0]
    sd = jax.ShapeDtypeStruct
    return pl.pallas_call(
        partial(tail_kernel, mesh),
        name="small_gradients",
        out_shape=(sd(part.shape, F32), sd((8, LANES), F32)),
        in_specs=[vmem_spec()] * 2,
        out_specs=(vmem_spec(),) * 2,
        scratch_shapes=[
            pltpu.VMEM((n, piece, LANES), F32),
            pltpu.VMEM((piece + 1, LANES), F32),
            pltpu.VMEM((n, piece + 1, LANES), F32),
            pltpu.VMEM((2 * shard_rows + n * piece + 8, LANES), F32),
            pltpu.SemaphoreType.DMA((2,)),
            pltpu.SemaphoreType.DMA((2,)),
        ],
        compiler_params=params(collective_id=3, has_side_effects=True),
    )(part, tail)


def stencil_table(support_vals, support_lon):
    rows = support_vals.shape[0]
    vals = support_vals.reshape(rows, S // 3, 3, K)
    offsets = jnp.arange(-REACH, REACH + 1)
    hit = support_lon.reshape(rows, S // 3, 3)[:, :, :, None] == offsets
    picked = jnp.where(hit[:, :, :, :, None], vals[:, :, :, None, :], 0.0)
    return jnp.transpose(jnp.sum(picked, 1), (1, 2, 0, 3))


def flat_table(table):
    t = table.reshape(-1, K)
    return jnp.pad(t, ((0, 0), (0, 16 - K)))


def local(
    mesh, block_in, noise, cotangent, band_heights, support_lon, support_vals,
    master, moment_one, moment_two, average, step_count,
):
    rows, width, _ = block_in.shape
    devices = mesh.shape["lat"] * mesh.shape["lon"]
    shard = master.shape[0]
    shard_rows = shard // LANES
    assert shard_rows * LANES == shard
    flat_rows = shard_rows * devices
    chunks = 6
    cells = width // chunks
    height = lax.dynamic_slice_in_dim(band_heights, lax.axis_index("lat"), 1, 0)
    x = jnp.transpose(block_in, (1, 0, 2))
    g = jnp.transpose(cotangent, (1, 0, 2))

    table = flat_table(stencil_table(support_vals, support_lon))
    planes = table.reshape(TAPS, rows, 16)
    trow = jnp.stack([planes[:, 0], lax.dynamic_index_in_dim(planes, height[0] - 1, 1, keepdims=False)])
    trow = jnp.pad(trow, ((0, 0), (0, 1), (0, 0)))
    share = master.astype(BF16).reshape(shard_rows, LANES)
    edge = jnp.stack([x[:, 0], lax.dynamic_index_in_dim(x, height[0] - 1, 1, keepdims=False)], 1)
    cols = jnp.stack([x[:REACH], x[width - REACH :]])
    corners = jnp.stack([edge[:REACH], edge[width - REACH :]], 0)
    corners = jnp.transpose(corners, (2, 0, 1, 3))
    edge = jnp.transpose(edge.reshape(chunks, cells, 2, C), (0, 2, 1, 3))
    w1, w2, wn, wd, small, colh, rowh, cornh, trowh = gather_weights(
        mesh, share, cols, edge, corners, trow
    )
    aug = jnp.concatenate(
        [
            jnp.zeros((width, rows, 1), BF16),
            jnp.transpose(noise, (2, 1, 0)),
            jnp.ones((width, rows, 1), BF16),
            jnp.zeros((width, rows, LANES - NOISE - 2), BF16),
        ],
        2,
    )
    conv, mixed, mean, inv = stencil_fwd(
        height, x, colh, rowh, cornh, table, wd, small, aug, wn, chunks
    )
    out, gconv, grow, gcol, gcorn, flat, extra = mlp(
        height, conv, g, x, w1, w2, small, flat_rows, chunks
    )
    gcolh, growh, gcornh = exchange(gcol, grow, gcorn)
    part = scatter(mesh, flat, shard_rows)
    piece = -(-(flat_rows - TAIL_ROW) // devices)
    grad_in, tail = stencil_bwd(
        height, x, mixed, mean, inv, g, gconv, gcolh, growh, gcornh, table, trowh, wd, small,
        extra, w1, devices * piece, chunks,
    )
    grad, norm = finish(mesh, part, tail.reshape(devices, piece, LANES))
    grad_part = grad.reshape(shard)
    grad_norm = norm[0, :1]
    factor = 0.01 / jnp.maximum(grad_norm, 0.01)
    clipped = grad_part * factor
    new_one = 0.9 * moment_one + 0.1 * clipped
    new_two = 0.999 * moment_two + 0.001 * clipped * clipped
    step_float = step_count[0].astype(F32)
    fix_one = 1.0 - jnp.power(jnp.float32(0.9), step_float)
    fix_two = 1.0 - jnp.power(jnp.float32(0.999), step_float)
    update = new_one / fix_one / (jnp.sqrt(new_two / fix_two) + 1e-08) + 0.1 * master
    new_master = master - 0.02 * update
    new_avg = 0.9 * average + 0.1 * new_master
    return (
        jnp.transpose(out, (1, 0, 2)),
        jnp.transpose(grad_in, (1, 0, 2)),
        grad_part,
        grad_norm,
        new_master,
        new_one,
        new_two,
        new_avg,
        new_master.astype(BF16),
    )


def solution(mesh):
    flat = P(("lat", "lon"))
    field = P("lat", "lon", None)
    return jax.shard_map(
        partial(local, mesh),
        mesh=mesh,
        in_specs=(
            field, P(None, "lat", "lon"), field, P(), P("lat", None), P("lat", None, None),
            flat, flat, flat, flat, P(),
        ),
        out_specs=(field, field, flat, P(), flat, flat, flat, flat, flat),
        check_vma=False,
    )
```

```python
from functools import partial
import math

import jax
import jax.numpy as jnp
from jax import lax
from jax.experimental import pallas as pl
from jax.experimental.pallas import tpu as pltpu
from jax.sharding import PartitionSpec as P

C = 641
FF = 1282
NOISE = 8
K = 9
S = 12
REACH = 2
LANES = 128
CB = 6
CP = CB * LANES
FB = 11
FP = FB * LANES
TAPS = 15
MESH = pl.DeviceIdType.MESH
HIGHEST = lax.Precision.HIGHEST
F32 = jnp.float32
BF16 = jnp.bfloat16
VMEM_LIMIT = 60 * 1024 * 1024
SLOTS = 28
REUSE = 10
ROW_TWO = (C * FF) // LANES
LANE_TWO = (C * FF) % LANES
TAIL_ROW = (2 * C * FF) // LANES
OFF_B1 = 2 * C * FF
OFF_B2 = OFF_B1 + FF
OFF_GAIN = OFF_B2 + C
OFF_DISCO = OFF_GAIN + C
OFF_NOISE = OFF_DISCO + K * C
END_FLAT = OFF_NOISE + NOISE * C


def params(**kw):
    return pltpu.CompilerParams(vmem_limit_bytes=VMEM_LIMIT, **kw)


def any_spec():
    return pl.BlockSpec(memory_space=pl.ANY)


def vmem_spec():
    return pl.BlockSpec(memory_space=pltpu.VMEM)


def iota(shape, dim):
    return lax.broadcasted_iota(jnp.int32, shape, dim)


def bit_list(mesh):
    bits = []
    for axis in ("lat", "lon"):
        count = int(math.log2(mesh.shape[axis]))
        assert 1 << count == mesh.shape[axis]
        bits += [(axis, b) for b in reversed(range(count))]
    return bits


def my_bits(bits):
    ids = {"lat": lax.axis_index("lat"), "lon": lax.axis_index("lon")}
    return [(ids[a] >> b) & 1 for a, b in bits]


def partner(axis, bit):
    lat, lon = lax.axis_index("lat"), lax.axis_index("lon")
    if axis == "lat":
        return (lat ^ (1 << bit), lon)
    return (lat, lon ^ (1 << bit))


def stage_orders(mesh):
    bits = bit_list(mesh)
    n = len(bits)
    if (mesh.shape["lat"], mesh.shape["lon"]) == (8, 4):
        return [[0, 1, 2, 3, 4], [0, 1, 3, 2, 4]]
    order = list(range(n))
    return [order, order]


def scatter_orders(mesh):
    n = len(bit_list(mesh))
    if (mesh.shape["lat"], mesh.shape["lon"]) == (8, 4):
        return [[4, 3, 2, 1, 0], [4, 2, 3, 1, 0], [4, 1, 0, 3, 2]]
    return [list(reversed(range(n)))] * 3


def rotl_rows(v, first, unit):
    index = (iota((8, LANES), 1) + first + unit * iota((8, LANES), 0)) % LANES
    return jnp.take_along_axis(v, index, axis=1)


def row_vector(flat_ref, offset, length):
    blocks = -(-length // LANES)
    row, shift = divmod(offset, LANES)
    near = flat_ref[row : row + blocks, :]
    if shift:
        far = flat_ref[row + 1 : row + 1 + blocks, :]
        lane = iota((blocks, LANES), 1)
        near = pltpu.roll(jnp.where(lane >= shift, near, far), LANES - shift, 1)
    index = iota((blocks, LANES), 0) * LANES + iota((blocks, LANES), 1)
    return jnp.where(index < length, near, 0.0)


def put_row(ref, row, value):
    for q in range(value.shape[0]):
        ref[row : row + 1, q * LANES : (q + 1) * LANES] = value[q : q + 1, :].astype(ref.dtype)


def unpack_weights(flat, w1, w2, wn, wd, small, wnf):
    lane = iota((8, LANES), 1)
    row = iota((8, LANES), 0)

    def rows_one(base, first):
        near = [flat[pl.ds(base + q, 8, stride=10), :] for q in range(FB + 1)]
        out = [
            rotl_rows(jnp.where(lane >= first + 2 * row, near[q], near[q + 1]), first, 2)
            for q in range(FB)
        ]
        out[-1] = jnp.where(lane < FF - (FB - 1) * LANES, out[-1], 0.0)
        return out

    def body_one(b, carry):
        for k in range(0, 8, 2):
            pair = [rows_one(641 * b + 80 * (k + h), 16 * (k + h)) for h in range(2)]
            at = pl.ds(pl.multiple_of(64 * b + 8 * k, 16), 16)
            for q in range(FB):
                v = jnp.concatenate([pair[0][q], pair[1][q]], 0)
                w1[at, q * LANES : (q + 1) * LANES] = v.astype(BF16)
        return carry

    last = C - 1
    lax.fori_loop(0, last // 64, body_one, 0)
    zero = jnp.zeros((8, LANES), F32)
    for q, v in enumerate(rows_one(641 * (last // 64), 0)):
        v = jnp.concatenate([jnp.where(row == 0, v, 0.0), zero], 0)
        w1[last : last + 16, q * LANES : (q + 1) * LANES] = v.astype(BF16)
    w1[last + 16 :, :] = jnp.zeros((CP - last - 16, FP), BF16)

    def rows_two(base, first):
        count = CB + 2 if first + 7 >= LANES else CB + 1
        near = [flat[pl.ds(base + q, 8, stride=5), :] for q in range(count)]
        out = []
        for q in range(CB):
            v = jnp.where(lane >= first + row, near[q], near[q + 1])
            if first + 7 >= LANES:
                v = jnp.where(lane < first + row - LANES, near[q + 2], v)
            out.append(rotl_rows(v, first, 1))
        out[-1] = jnp.where(lane < C - (CB - 1) * LANES, out[-1], 0.0)
        return out

    def body_two(b, carry):
        for k in range(0, 16, 2):
            pair = [
                rows_two(ROW_TWO + 641 * b + 40 * (k + h), LANE_TWO + 8 * (k + h))
                for h in range(2)
            ]
            at = pl.ds(pl.multiple_of(128 * b + 8 * k, 16), 16)
            for q in range(CB):
                v = jnp.concatenate([pair[0][q], pair[1][q]], 0)
                w2[at, q * LANES : (q + 1) * LANES] = v.astype(BF16)
        return carry

    full = FF // LANES
    lax.fori_loop(0, full, body_two, 0)
    for q, v in enumerate(rows_two(ROW_TWO + 641 * full, LANE_TWO)):
        v = jnp.concatenate([jnp.where(row < FF - full * LANES, v, 0.0), zero], 0)
        w2[full * LANES : full * LANES + 16, q * LANES : (q + 1) * LANES] = v.astype(BF16)
    w2[full * LANES + 16 :, :] = jnp.zeros((FP - full * LANES - 16, CP), BF16)
    small[...] = jnp.zeros_like(small)
    put_row(small, 0, row_vector(flat, OFF_B1, FF))
    put_row(small, 1, row_vector(flat, OFF_B2, C))
    put_row(small, 2, row_vector(flat, OFF_GAIN, C))
    wd[...] = jnp.zeros_like(wd)
    wnf[...] = jnp.zeros_like(wnf)
    for k in range(K):
        put_row(wd, k, row_vector(flat, OFF_DISCO + k * C, C))
    for k in range(NOISE):
        put_row(wnf, 1 + k, row_vector(flat, OFF_NOISE + k * C, C))
    wn[...] = wnf[...].astype(BF16)


def neighbours():
    lat, lon = lax.axis_index("lat"), lax.axis_index("lon")
    nlat, nlon = lax.axis_size("lat"), lax.axis_size("lon")
    return lat, lon, nlat, nlon, lax.rem(lon + 1, nlon), lax.rem(lon + nlon - 1, nlon)


def halo_copies(cols, rows, corners, colh, rowh, cornh, send, recv, trow=None, trowh=None):
    lat, lon, nlat, nlon, east, west = neighbours()
    out = []

    def add(src, dst, target, k, sends, gets):
        out.append(
            (
                sends,
                gets,
                pltpu.make_async_remote_copy(
                    src_ref=src,
                    dst_ref=dst,
                    send_sem=send.at[k],
                    recv_sem=recv.at[k],
                    device_id=target,
                    device_id_type=MESH,
                ),
            )
        )

    has_up, has_down = lat > 0, lat < nlat - 1
    up, down = lat - 1, lat + 1
    add(rows.at[:, 0], rowh.at[:, 1], (up, lon), 2, has_up, has_down)
    add(rows.at[:, 1], rowh.at[:, 0], (down, lon), 3, has_down, has_up)
    add(cols.at[0], colh.at[1], (lat, west), 0, None, None)
    add(cols.at[1], colh.at[0], (lat, east), 1, None, None)
    add(corners.at[0, 0], cornh.at[1, 1], (up, west), 4, has_up, has_down)
    add(corners.at[0, 1], cornh.at[1, 0], (up, east), 5, has_up, has_down)
    add(corners.at[1, 0], cornh.at[0, 1], (down, west), 6, has_down, has_up)
    add(corners.at[1, 1], cornh.at[0, 0], (down, east), 7, has_down, has_up)
    if trow is not None:
        add(trow.at[0], trowh.at[1], (up, lon), 8, has_up, has_down)
        add(trow.at[1], trowh.at[0], (down, lon), 9, has_down, has_up)
    return out


def start_halo(copies):
    for sends, _, copy in copies:
        if sends is None:
            copy.start()
        else:
            pl.when(sends)(copy.start)


def wait_halo(copies):
    for sends, gets, copy in copies:
        if sends is None:
            copy.wait()
        else:
            pl.when(sends)(copy.wait_send)
            pl.when(gets)(copy.wait_recv)


def greet(bits, halo):
    barrier = pltpu.get_barrier_semaphore()
    lat, lon, nlat, nlon, east, west = neighbours()

    def hello(target):
        pl.semaphore_signal(barrier, inc=1, device_id=target, device_id_type=MESH)

    count = 0
    for axis, bit in bits:
        hello(partner(axis, bit))
        count += 1
    if halo:
        for target in ((lat, east), (lat, west)):
            hello(target)
            count += 1
        for side, cond in ((lat - 1, lat > 0), (lat + 1, lat < nlat - 1)):

            @pl.when(cond)
            def _(side=side):
                for x in (lon, east, west):
                    hello((side, x))

    if halo:
        count = count + 3 * (lat > 0).astype(jnp.int32) + 3 * (lat < nlat - 1).astype(jnp.int32)
    pl.semaphore_wait(barrier, count)


def gather_kernel(
    mesh, share_ref, cols, rows, corners, trow,
    w1, w2, wn, wd, small, colh, rowh, cornh, trowh,
    buf, flat, wnf, send, recv, hsend, hrecv, local_sem,
):
    bits = bit_list(mesh)
    orders = stage_orders(mesh)
    mine = my_bits(bits)
    n = len(bits)
    shard_rows = share_ref.shape[0]
    cut = (shard_rows // 2 + 15) // 16 * 16
    spans = [(0, cut), (cut, shard_rows - cut)]
    own = pltpu.make_async_copy(share_ref, buf.at[tuple(mine)], local_sem)
    own.start()
    greet(bits, True)
    halos = halo_copies(cols, rows, corners, colh, rowh, cornh, hsend, hrecv, trow, trowh)

    def copy(colour, k):
        order = orders[colour]
        done = order[:k]
        start, count = spans[colour]
        index = tuple(slice(None) if i in done else mine[i] for i in range(n)) + (
            pl.ds(start, count),
        )
        return pltpu.make_async_remote_copy(
            src_ref=buf.at[index],
            dst_ref=buf.at[index],
            send_sem=send.at[colour, k],
            recv_sem=recv.at[colour, k],
            device_id=partner(*bits[order[k]]),
            device_id_type=MESH,
        )

    own.wait()
    for colour in range(2):
        copy(colour, 0).start()
    start_halo(halos)
    for k in range(n):
        for colour in range(2):
            copy(colour, k).wait()
            if k + 1 < n:
                copy(colour, k + 1).start()
    wait_halo(halos)
    lat, _, nlat, *_ = neighbours()
    for r, cond in ((0, lat == 0), (1, lat == nlat - 1)):

        @pl.when(cond)
        def _(r=r):
            for i in range(rowh.shape[0]):
                rowh[i, r] = jnp.zeros(rowh.shape[2:], rowh.dtype)
            trowh[r] = jnp.zeros(trowh.shape[1:], F32)
            for s in range(2):
                cornh[r, s] = jnp.zeros(cornh.shape[2:], cornh.dtype)

    total = 1 << n

    def widen(d, carry):
        index = tuple((d >> (n - 1 - i)) & 1 for i in range(n))
        flat[pl.ds(d * shard_rows, shard_rows), :] = buf[index].astype(F32)
        return carry

    lax.fori_loop(0, total, widen, 0)
    flat[total * shard_rows :, :] = jnp.zeros((flat.shape[0] - total * shard_rows, LANES), F32)
    unpack_weights(flat, w1, w2, wn, wd, small, wnf)


def gather_weights(mesh, share, cols, rows, corners, trow):
    bits = bit_list(mesh)
    n = len(bits)
    shard_rows = share.shape[0]
    total = shard_rows << n
    sd = jax.ShapeDtypeStruct
    return pl.pallas_call(
        partial(gather_kernel, mesh),
        name="gather_weights",
        out_shape=(
            sd((CP, FP), BF16),
            sd((FP, CP), BF16),
            sd((LANES, CP), BF16),
            sd((16, CP), F32),
            sd((8, FP), F32),
            sd(cols.shape, BF16),
            sd(rows.shape, BF16),
            sd(corners.shape, BF16),
            sd(trow.shape, F32),
        ),
        in_specs=[vmem_spec()] * 5,
        out_specs=(vmem_spec(),) * 9,
        scratch_shapes=[
            pltpu.VMEM((2,) * n + (shard_rows, LANES), BF16),
            pltpu.VMEM((total + 96, LANES), F32),
            pltpu.VMEM((LANES, CP), F32),
            pltpu.SemaphoreType.DMA((2, n)),
            pltpu.SemaphoreType.DMA((2, n)),
            pltpu.SemaphoreType.DMA((10,)),
            pltpu.SemaphoreType.DMA((10,)),
            pltpu.SemaphoreType.DMA,
        ],
        compiler_params=params(collective_id=0, has_side_effects=True),
    )(share, cols, rows, corners, trow)


def norm_parts(x):
    mean = jnp.mean(x, -1, keepdims=True)
    center = x - mean
    var = jnp.mean(center * center, -1, keepdims=True)
    return center, lax.rsqrt(var + 1e-05)


def rounded(v):
    return v.astype(BF16).astype(F32)


def stencil_fwd_kernel(
    chunks, cells, height_ref, x_ref, colh, rowh, cornh, table, wd, gain, aug, wn,
    out_ref, mix_ref, mean_ref, inv_ref, m_scr, k_scr, nt_scr,
):
    step = pl.program_id(0)
    rows = x_ref.shape[1]
    width = chunks * cells
    height = height_ref[0]
    gvec = gain[2:3, :C]

    def put_cell(column, x, top, low, j=None):
        mean = jnp.mean(x, -1, keepdims=True)
        center = x - mean
        inv = lax.rsqrt(jnp.mean(center * center, -1, keepdims=True) + 1e-05)
        mixed = rounded(center * inv * gvec)
        hrow = iota((rows, C), 0)
        if j is not None:
            mean_ref[j] = jnp.broadcast_to(mean, (rows, LANES))
            inv_ref[j] = jnp.broadcast_to(inv, (rows, LANES))
            mix_ref[j, :, :C] = jnp.where(hrow < height, mixed, 0.0).astype(BF16)
        mixed = jnp.where(hrow < height, mixed, jnp.where(hrow == height, low, 0.0))
        at = column * SLOTS
        for g in range(CB):
            lo, hi = g * LANES, min((g + 1) * LANES, C)
            m_scr[g, pl.ds(at + 1, rows), : hi - lo] = mixed[:, lo:hi]
            m_scr[g, pl.ds(at, 1), : hi - lo] = top[:, lo:hi]
            m_scr[g, pl.ds(at + rows + 1, 1), : hi - lo] = low[:, lo:hi]

    def halo_mix(v):
        center, inv = norm_parts(v.astype(F32))
        return rounded(center * inv * gvec)

    @pl.when(step == 0)
    def _():
        k_scr[...] = jnp.dot(
            table[...], wd[...], preferred_element_type=F32, precision=HIGHEST
        ).reshape(k_scr.shape)
        for side in range(2):
            for i in range(REACH):
                column = i if side == 0 else width + REACH + i
                top = halo_mix(cornh[0, side])[i : i + 1]
                low = halo_mix(cornh[1, side])[i : i + 1]
                put_cell(column, colh[side, i].astype(F32), top, low)

    @pl.when(step < chunks)
    def _():
        nt_scr[0:cells, :C] = halo_mix(rowh[0, 0])
        nt_scr[32 : 32 + cells, :C] = halo_mix(rowh[0, 1])
        lanes = slice((CB - 1) * LANES, CB * LANES)
        mix_ref[:, :, lanes] = jnp.zeros((cells, rows, LANES), BF16)

        def cell(j, carry):
            put_cell(
                step * cells + j + REACH,
                x_ref[j].astype(F32),
                nt_scr[pl.ds(j, 1), :C],
                nt_scr[pl.ds(32 + j, 1), :C],
                j,
            )
            return carry

        lax.fori_loop(0, cells, cell, 0, unroll=3)

    @pl.when(step >= chunks)
    def _():
        first = (step - chunks) * cells
        nt_scr[...] = jnp.dot(
            aug[...].reshape(cells * rows, LANES), wn[...], preferred_element_type=F32
        )
        lane = iota((8, LANES), 1)
        for g in range(CB):
            lanes = slice(g * LANES, (g + 1) * LANES)
            for hb in range(rows // 8):
                at = slice(8 * hb, 8 * hb + 8)

                def cell(i, carry):
                    j = i * REUSE
                    acc = [nt_scr[pl.ds((j + u) * rows + 8 * hb, 8), lanes] for u in range(REUSE)]
                    for l in range(3):
                        near = [
                            m_scr[g, pl.ds((first + j + u) * SLOTS + 8 * hb + l, 8), :]
                            for u in range(REUSE + 2 * REACH)
                        ]
                        for w in range(5):
                            tap = k_scr[5 * l + w, at, lanes]
                            acc = [a + tap * near[u + w] for u, a in enumerate(acc)]
                    for u in range(REUSE):
                        v = acc[u]
                        if g == CB - 1:
                            v = jnp.where(lane == 0, v, aug[j + u, at, :].astype(F32))
                        out_ref[j + u, at, lanes] = v.astype(BF16)
                    return carry

                lax.fori_loop(0, cells // REUSE, cell, 0)


def stencil_fwd(height, x, colh, rowh, cornh, table, wd, small, aug, wn, chunks):
    width, rows, _ = x.shape
    cells = width // chunks
    assert cells % REUSE == 0
    first = lambda i: jnp.where(i < chunks, i, chunks - 1)
    second = lambda i: jnp.where(i < chunks, 0, i - chunks)
    sd = jax.ShapeDtypeStruct
    by_first = lambda c: pl.BlockSpec((cells, rows, c), lambda i: (first(i), 0, 0))
    by_second = lambda c: pl.BlockSpec((cells, rows, c), lambda i: (second(i), 0, 0))
    return pl.pallas_call(
        partial(stencil_fwd_kernel, chunks, cells),
        name="stencil_fwd",
        grid=(2 * chunks,),
        out_shape=(
            sd((width, rows, CP), BF16),
            sd((width, rows, CP), BF16),
            sd((width, rows, LANES), F32),
            sd((width, rows, LANES), F32),
        ),
        in_specs=[
            pl.BlockSpec(memory_space=pltpu.SMEM),
            by_first(C),
            vmem_spec(),
            pl.BlockSpec((1, 2, cells, C), lambda i: (first(i), 0, 0, 0)),
            vmem_spec(),
            vmem_spec(),
            vmem_spec(),
            vmem_spec(),
            by_second(LANES),
            vmem_spec(),
        ],
        out_specs=(by_second(CP), by_first(CP), by_first(LANES), by_first(LANES)),
        scratch_shapes=[
            pltpu.VMEM((CB, (width + 2 * REACH) * SLOTS, LANES), F32),
            pltpu.VMEM((TAPS, rows, CP), F32),
            pltpu.VMEM((cells * rows, CP), F32),
        ],
        compiler_params=params(dimension_semantics=("arbitrary",)),
    )(height, x, colh, rowh, cornh, table, wd, small, aug, wn)


def pack_weights(one, two, flat):
    lane = iota((8, LANES), 1)
    row = iota((8, LANES), 0)
    flat[...] = jnp.zeros_like(flat)

    def turned(v, first, unit):
        return pltpu.roll(v, first, 1, stride=unit, stride_axis=0)

    def main(ref, at, first, unit, out, base, step, count):
        keep = lane >= first + unit * row
        before = jnp.zeros((8, LANES), F32)
        for q in range(count):
            now = turned(ref[q, at, :], first, unit)
            flat[pl.ds(base + q, 8, stride=step), :] = jnp.where(keep, now, before)
            before = now

    def rest(ref, at, first, unit, count, width, mask=None):
        s = first + unit * row
        before = turned(ref[count - 1, at, :], first, unit)
        now = turned(ref[count, at, :], first, unit)
        v = jnp.where(lane < s, before, jnp.where(lane < s + width, now, 0.0))
        return v if mask is None else jnp.where(mask, v, 0.0)

    shift = 8 - LANE_TWO
    base_two = ROW_TWO - 5 * LANE_TWO
    full = FF // LANES
    extra = C - (CB - 1) * LANES

    def two_main(b, carry):
        for k in range(16):
            at = pl.ds(128 * b + 8 * k + shift, 8)
            main(two, at, 8 * k, 1, flat, base_two + 641 * b + 40 * k, 5, CB - 1)
        return carry

    lax.fori_loop(0, full, two_main, 0)
    end = slice(128 * full + shift, 128 * full + shift + 8)
    mask = row < FF - full * LANES + LANE_TWO
    before = jnp.zeros((8, LANES), F32)
    for q in range(CB - 1):
        now = jnp.where(mask, turned(two[q, end, :], 0, 1), 0.0)
        at = pl.ds(base_two + 641 * full + q, 8, stride=5)
        flat[at, :] = jnp.where(lane >= row, now, before)
        before = now

    def one_main(b, carry):
        for k in range(8):
            at = pl.ds(pl.multiple_of(64 * b + 8 * k, 8), 8)
            main(one, at, 16 * k, 2, flat, 641 * b + 80 * k, 10, FB - 1)
        return carry

    last = C - 1
    assert last % 64 == 0
    lax.fori_loop(0, last // 64, one_main, 0)
    row_last = 641 * (last // 64)
    for q in range(FB - 1):
        flat[row_last + q : row_last + q + 1, :] = one[q, last : last + 1, :]

    def add_all(places, values):
        olds = [flat[at, :] for at in places]
        for at, old, v in zip(places, olds, values):
            flat[at, :] = old + v

    def one_rest(b, carry):
        values = [
            rest(one, pl.ds(pl.multiple_of(64 * b + 8 * k, 8), 8), 16 * k, 2, FB - 1, FF - (FB - 1) * LANES)
            for k in range(8)
        ]
        add_all([pl.ds(641 * b + 80 * k + FB - 1, 8, stride=10) for k in range(8)], values)
        return carry

    lax.fori_loop(0, last // 64, one_rest, 0)
    lane1 = iota((1, LANES), 1)
    v = jnp.where(lane1 < FF - (FB - 1) * LANES, one[FB - 1, last : last + 1, :], 0.0)
    add_all([slice(row_last + FB - 1, row_last + FB)], [v])

    def two_rest(b, carry):
        values = [
            rest(two, pl.ds(128 * b + 8 * k + shift, 8), 8 * k, 1, CB - 1, extra) for k in range(16)
        ]
        places = [pl.ds(base_two + 641 * b + 40 * k + CB - 1, 8, stride=5) for k in range(16)]
        add_all(places, values)
        return carry

    lax.fori_loop(0, full, two_rest, 0)
    add_all(
        [pl.ds(base_two + 641 * full + CB - 1, 8, stride=5)],
        [rest(two, end, 0, 1, CB - 1, extra, mask)],
    )


GELU_A = math.sqrt(2.0 / math.pi)
GELU_B = 0.044715
WIDE = 256


def dot(a, b, dims=((1,), (0,))):
    return lax.dot_general(a, b, (dims, ((), ())), preferred_element_type=F32)


def mlp_kernel(
    blocks, height_ref, conv_ref, g_ref, x_ref, w1, w2, small,
    out_ref, gconv_ref, rows_ref, cols_ref, corn_ref, shards_ref, extra_ref,
    one, two, g_scr, conv_t, act, gh, flat,
):
    step = pl.program_id(0)
    cells, rows, _ = x_ref.shape
    m = cells * rows
    height = height_ref[0]

    @pl.when(step == 0)
    def _():
        one[...] = jnp.zeros_like(one)
        two[...] = jnp.zeros_like(two)
        g_scr[...] = jnp.zeros_like(g_scr)

    live = (iota((1, rows, 1), 1) < height).astype(F32)
    g_scr[:, :C] = (g_ref[...].astype(F32) * live).reshape(m, C).astype(BF16)
    rows_one = conv_t.shape[0]

    def hidden(start, wide, tail):
        lanes = pl.ds(start, wide)
        h = dot(conv_ref[...].reshape(m, CP), w1[:, lanes]) + small[0:1, lanes]
        ga = dot(g_scr[...], w2[lanes, :], ((1,), (1,)))
        h2 = h * h
        t = jnp.tanh(h * (GELU_A + (GELU_A * GELU_B) * h2))
        cdf = 0.5 * t + 0.5
        value = (h * cdf).astype(BF16)
        slope = cdf + h * (0.5 - 0.5 * (t * t)) * (GELU_A + (3 * GELU_A * GELU_B) * h2)
        if tail:
            ones = iota((m, wide), 1) == FF - (FB - 1) * LANES
            value = jnp.where(ones, jnp.ones_like(value), value)
        act[:, lanes] = value
        gh[:, lanes] = (ga * slope).astype(BF16)

    def turn(i, count):
        part = conv_ref[:, :, pl.ds(i * LANES, LANES)].reshape(m, LANES)
        conv_t[pl.ds(i * LANES, count), :] = part.T[:count]

    def first(f, carry):
        turn(pl.multiple_of(f, 1), LANES)
        hidden(pl.multiple_of(f * WIDE, WIDE), WIDE, False)
        return carry

    lax.fori_loop(0, FP // WIDE, first, 0)
    assert FP // WIDE == CB - 1
    turn(CB - 1, rows_one - (CB - 1) * LANES)
    hidden(FP // WIDE * WIDE, FP % WIDE, True)

    for n in range(CP // WIDE):
        lanes = slice(n * WIDE, (n + 1) * WIDE)
        end = min((n + 1) * WIDE, C)
        part = slice(n * WIDE, end)
        branch = dot(act[...], w2[:, lanes])[:, : end - n * WIDE]
        v = x_ref[:, :, part].astype(F32).reshape(m, -1) + branch + small[1:2, part]
        out_ref[:, :, part] = (v.reshape(cells, rows, -1) * live).astype(BF16)
        gc = dot(gh[...], w1[lanes, :], ((1,), (1,)))
        gconv_ref[:, :, lanes] = gc.reshape(cells, rows, WIDE)

    def weights(start, wide):
        lanes = pl.ds(start, wide)
        r1 = dot(conv_t[...], gh[:, lanes])
        r2 = dot(act[:, lanes], g_scr[...], ((0,), (0,)))
        for i in range(wide // LANES):
            one[start // LANES + i] += r1[:, i * LANES : (i + 1) * LANES]
        for q in range(CB):
            two[q, pl.ds(start + 8, wide), :] += r2[:, q * LANES : (q + 1) * LANES]

    def third(f, carry):
        weights(pl.multiple_of(f * WIDE, WIDE), WIDE)
        return carry

    lax.fori_loop(0, FP // WIDE, third, 0)
    weights(FP // WIDE * WIDE, FP % WIDE)

    onehot = (iota((1, rows, 1), 1) == height - 1).astype(F32)
    block = gconv_ref[...]
    edges = (block[:, 0, :].astype(BF16), jnp.sum(block * onehot, 1).astype(BF16))
    for r in range(2):
        rows_ref[0, r] = edges[r]
    for side, at, first in ((0, 0, 0), (1, blocks - 1, cells - REACH)):

        @pl.when(step == at)
        def _(side=side, first=first):
            for i in range(REACH):
                cols_ref[side, i] = gconv_ref[first + i].astype(BF16)
            for r in range(2):
                corn_ref[r, side] = edges[r][first : first + REACH]

    @pl.when(step == blocks - 1)
    def _():
        extra_ref[...] = jnp.zeros_like(extra_ref)
        for q in range(FB):
            extra_ref[0 : NOISE + 1, q * LANES : (q + 1) * LANES] = one[q, C : C + NOISE + 1, :]
        for q in range(CB):
            lanes = slice(q * LANES, (q + 1) * LANES)
            extra_ref[NOISE + 1 : NOISE + 2, lanes] = two[q, FF + 8 : FF + 9, :]
        pack_weights(one, two, flat)
        bits = len(shards_ref.shape) - 2
        shard_rows = shards_ref.shape[-2]

        def store(d, carry):
            index = tuple((d >> (bits - 1 - i)) & 1 for i in range(bits))
            shards_ref[index] = flat[pl.ds(d * shard_rows, shard_rows), :]
            return carry

        lax.fori_loop(0, 1 << bits, store, 0)


def mlp(height, conv, g, x, w1, w2, small, shards, blocks):
    width, rows, _ = x.shape
    cells = width // blocks
    m = cells * rows
    sd = jax.ShapeDtypeStruct
    block = lambda c: pl.BlockSpec((cells, rows, c), lambda i: (i, 0, 0))
    rows_one = -(-(C + NOISE + 1) // 16) * 16
    flops = 12 * width * rows * C * FF
    return pl.pallas_call(
        partial(mlp_kernel, blocks),
        name="mlp",
        grid=(blocks,),
        out_shape=(
            sd((width, rows, C), BF16),
            sd((width, rows, CP), F32),
            sd((blocks, 2, cells, CP), BF16),
            sd((2, REACH, rows, CP), BF16),
            sd((2, 2, REACH, CP), BF16),
            sd(shards, F32),
            sd((16, FP), F32),
        ),
        in_specs=[
            pl.BlockSpec(memory_space=pltpu.SMEM),
            block(CP),
            block(C),
            block(C),
            vmem_spec(),
            vmem_spec(),
            vmem_spec(),
        ],
        out_specs=(
            block(C),
            block(CP),
            pl.BlockSpec((1, 2, cells, CP), lambda i: (i, 0, 0, 0)),
            vmem_spec(),
            vmem_spec(),
            vmem_spec(),
            vmem_spec(),
        ),
        scratch_shapes=[
            pltpu.VMEM((FB, rows_one, LANES), F32),
            pltpu.VMEM((CB, FP + 16, LANES), F32),
            pltpu.VMEM((m, CP), BF16),
            pltpu.VMEM((rows_one, m), BF16),
            pltpu.VMEM((m, FP), BF16),
            pltpu.VMEM((m, FP), BF16),
            pltpu.VMEM((math.prod(shards[:-1]), LANES), F32),
        ],
        compiler_params=params(dimension_semantics=("arbitrary",)),
        cost_estimate=pl.CostEstimate(flops=flops, bytes_accessed=50_000_000, transcendentals=0),
    )(height, conv, g, x, w1, w2, small)


def add_vector(tail, offset, value):
    row, shift = divmod(offset - TAIL_ROW * LANES, LANES)
    blocks = value.shape[0]
    lane = iota((blocks + 1, LANES), 1)
    zero = jnp.zeros((1, LANES), F32)
    here = pltpu.roll(jnp.concatenate([value, zero], 0), shift, 1) if shift else jnp.concatenate([value, zero], 0)
    back = jnp.concatenate([zero, here[:blocks]], 0)
    at = slice(row, row + blocks + 1)
    tail[at, :] = tail[at, :] + jnp.where(lane >= shift, here, back if shift else here)


def as_blocks(value, length):
    blocks = -(-length // LANES)
    v = jnp.concatenate([value[:, q * LANES : (q + 1) * LANES] for q in range(blocks)], 0)
    index = iota((blocks, LANES), 0) * LANES + iota((blocks, LANES), 1)
    return jnp.where(index < length, v, 0.0)


class Scatter:
    def __init__(self, mesh, shards, buf, recvs, send, recv):
        self.bits = bit_list(mesh)
        self.n = len(self.bits)
        self.orders = scatter_orders(mesh)
        self.first = self.orders[0][0]
        assert all(order[0] == self.first for order in self.orders)
        self.mine = my_bits(self.bits)
        self.shards, self.buf, self.recvs = shards, buf, recvs
        self.send, self.recv = send, recv
        rows = shards.shape[-2]
        one, two = (int(rows * f) // 8 * 8 for f in (0.36, 0.71))
        self.spans = [(0, one), (one, two - one), (two, rows - two)]

    def copy(self, colour, k):
        order, mine, n = self.orders[colour], self.mine, self.n
        done, now = order[:k], order[k]
        at = (pl.ds(*self.spans[colour]),)
        index = tuple(
            1 - mine[i] if i == now else mine[i] if i in done else slice(None) for i in range(n)
        )
        if k == 0:
            src = self.shards.at[index + at]
        else:
            src = self.buf.at[tuple(v for i, v in enumerate(index) if i != self.first) + at]
        return pltpu.make_async_remote_copy(
            src_ref=src,
            dst_ref=self.recvs[k].at[(slice(None),) * (n - 1 - k) + at],
            send_sem=self.send.at[colour, k],
            recv_sem=self.recv.at[colour, k],
            device_id=partner(*self.bits[now]),
            device_id_type=MESH,
        )

    def load(self, sem):
        index = tuple(self.mine[i] if i == self.first else slice(None) for i in range(self.n))
        return pltpu.make_async_copy(self.shards.at[index], self.buf, sem)

    def advance(self, colour, k):
        self.copy(colour, k).wait()
        order, n = self.orders[colour], self.n
        free = [i for i in range(n) if i not in order[: k + 1]]
        at = (pl.ds(*self.spans[colour]),)

        def add(d, carry):
            sub = tuple((d >> (len(free) - 1 - i)) & 1 for i in range(len(free)))
            index = tuple(
                sub[free.index(i)] if i in free else self.mine[i]
                for i in range(n)
                if i != self.first
            )
            self.buf[index + at] = self.buf[index + at] + self.recvs[k][sub + at]
            return carry

        lax.fori_loop(0, 1 << len(free), add, 0)
        if k + 1 < n:
            self.copy(colour, k + 1).start()

    def result(self):
        return self.buf[tuple(v for i, v in enumerate(self.mine) if i != self.first)]


def scatter_plan(n):
    if n == 5:
        return {8: [(0, 1), (1, 1), (2, 1)], 13: [(0, 2), (1, 2)], 15: [(2, 2)], 17: [(0, 3), (1, 3), (2, 3)]}
    return {}


def stencil_bwd_kernel(
    mesh, chunks, cells, height_ref, mix_ref, gconv_ref,
    cols, edge, corners, table, trowh, wd, extra, w1, shards,
    tail_ref, part_ref, gm_ref,
    g_scr, m_scr, k_scr, t_scr, e_scr, colh, rowh, cornh, buf, *rest,
):
    n = len(bit_list(mesh))
    recvs, (send, recv, hsend, hrecv, load_sem, out_sem) = rest[:n], rest[n:]
    scatter = Scatter(mesh, shards, buf, recvs, send, recv)
    step = pl.program_id(0)
    rows = mix_ref.shape[1]
    width = chunks * cells
    height = height_ref[0]
    plan = scatter_plan(n)

    @pl.when(step == 0)
    def _():
        scatter.load(load_sem).start()
        greet(scatter.bits, True)
        start_halo(halo_copies(cols, edge, corners, colh, rowh, cornh, hsend, hrecv))
        for colour in range(3):
            scatter.copy(colour, 0).start()
        hrow = iota((rows, 16), 0)
        for t in range(TAPS):
            l = t // 5
            own = table[t * rows : (t + 1) * rows, :]
            if l == 0:
                own = jnp.concatenate([own[1:], own[:1]], 0)
                own = jnp.where(hrow == height - 1, trowh[1, t : t + 1, :], own)
            if l == 2:
                own = jnp.concatenate([trowh[0, t : t + 1, :], own[: rows - 1]], 0)
            t_scr[t * rows : (t + 1) * rows, :] = own
        k_scr[...] = jnp.dot(
            t_scr[...], wd[...], preferred_element_type=F32, precision=HIGHEST
        ).reshape(k_scr.shape)
        e_scr[...] = jnp.zeros_like(e_scr)

    @pl.when(step < chunks)
    def _():
        def cell(j, carry):
            v = gconv_ref[j]
            mixed = mix_ref[j].astype(F32)
            at = (step * cells + j + REACH) * SLOTS
            for q in range(CB):
                lanes = slice(q * LANES, (q + 1) * LANES)
                g_scr[q, pl.ds(at + 1, rows), :] = v[:, lanes]
                m_scr[q, step * cells + j] = mixed[:, lanes]
            return carry

        lax.fori_loop(0, cells, cell, 0, unroll=2)

    @pl.when(step == chunks)
    def _():
        scatter.load(load_sem).wait()
        for colour in range(3):
            scatter.advance(colour, 0)
        wait_halo(halo_copies(cols, edge, corners, colh, rowh, cornh, hsend, hrecv))
        lat, _, nlat, *_ = neighbours()
        keep = ((lat > 0).astype(F32), (lat < nlat - 1).astype(F32))

        def put(column, top, low, fresh=None):
            at = column * SLOTS
            here = iota((rows, LANES), 0) == height
            for q in range(CB):
                lanes = slice(q * LANES, (q + 1) * LANES)
                body = pl.ds(at + 1, rows)
                old = g_scr[q, body, :] if fresh is None else fresh[:, lanes]
                g_scr[q, body, :] = jnp.where(here, low[:, lanes], old)
                g_scr[q, pl.ds(at, 1), :] = top[:, lanes]
                g_scr[q, pl.ds(at + rows + 1, 1), :] = low[:, lanes]

        def beside(ref):
            return [jnp.where(keep[r] > 0, ref(r).astype(F32), 0.0) for r in range(2)]

        for side in range(2):
            top, low = beside(lambda r: cornh[r, side])
            for i in range(REACH):
                column = i if side == 0 else width + REACH + i
                put(column, top[i : i + 1], low[i : i + 1], colh[side, i].astype(F32))

        def strip(c, carry):
            tops, lows = beside(lambda r: rowh[c, r])
            for i in range(cells):
                put(c * cells + i + REACH, tops[i : i + 1], lows[i : i + 1])
            return carry

        lax.fori_loop(0, chunks, strip, 0)
        for q in range(CB):
            lanes = slice(q * LANES, (q + 1) * LANES)
            for hb in range(rows // 8):
                at = slice(8 * hb, 8 * hb + 8)

                def cell(i, carry):
                    j = i * REUSE
                    mixed = [m_scr[q, j + u, at, :] for u in range(REUSE)]
                    total = [None] * REUSE
                    for l in range(3):
                        near = [
                            g_scr[q, pl.ds((j + u) * SLOTS + 8 * hb + 2 - l, 8), :]
                            for u in range(REUSE + 2 * REACH)
                        ]
                        for w in range(5):
                            t = 5 * l + w
                            tap = k_scr[t, at, lanes]
                            views = near[2 * REACH - w : 2 * REACH - w + REUSE]
                            terms = [tap * v for v in views]
                            total = [a if b is None else a + b for a, b in zip(terms, total)]
                            sums = [m * v for m, v in zip(mixed, views)]
                            while len(sums) > 1:
                                sums = [
                                    sums[k] + sums[k + 1] if k + 1 < len(sums) else sums[k]
                                    for k in range(0, len(sums), 2)
                                ]
                            e_scr[t, at, lanes] = e_scr[t, at, lanes] + sums[0]
                    for u in range(REUSE):
                        m_scr[q, j + u, at, :] = total[u]
                    return carry

                lax.fori_loop(0, width // REUSE, cell, 0)
                for colour, k in plan.get(q * (rows // 8) + hb, []):
                    scatter.advance(colour, k)
            pltpu.make_async_copy(m_scr.at[q], gm_ref.at[q], out_sem.at[q]).start()

        tail_ref[...] = jnp.zeros_like(tail_ref)
        add_vector(tail_ref, OFF_B1, as_blocks(extra[NOISE : NOISE + 1, :], FF))
        add_vector(tail_ref, OFF_B2, as_blocks(extra[NOISE + 1 : NOISE + 2, :], C))
        disco = lax.dot_general(
            t_scr[...], e_scr[...].reshape(TAPS * rows, CP), (((0,), (0,)), ((), ())),
            preferred_element_type=F32, precision=HIGHEST,
        )
        for k in range(K):
            add_vector(tail_ref, OFF_DISCO + k * C, as_blocks(disco[k : k + 1, :], C))
        ng = extra[0:NOISE, :]
        hi = ng.astype(BF16)
        mid = (ng - hi.astype(F32)).astype(BF16)
        lo = (ng - hi.astype(F32) - mid.astype(F32)).astype(BF16)
        parts = [dot(p, w1[...], ((1,), (1,))) for p in (hi, mid, lo)]
        gn = parts[0] + parts[1] + parts[2]
        for k in range(NOISE):
            add_vector(tail_ref, OFF_NOISE + k * C, as_blocks(gn[k : k + 1, :], C))
        taken = {e for events in plan.values() for e in events}
        for k in range(1, n):
            for colour in range(3):
                if (colour, k) not in taken:
                    scatter.advance(colour, k)
        part_ref[...] = scatter.result()
        for q in range(CB):
            pltpu.make_async_copy(m_scr.at[q], gm_ref.at[q], out_sem.at[q]).wait()


def stencil_bwd(
    mesh, height, mixed, gconv, cols, edge, corners, table, trowh, wd, extra, w1, shards,
    tail_rows, chunks,
):
    width, rows, _ = mixed.shape
    cells = width // chunks
    shard_rows = shards.shape[-2]
    n = len(bit_list(mesh))
    first = lambda i: jnp.where(i < chunks, i, chunks - 1)
    sd = jax.ShapeDtypeStruct
    by_first = lambda c: pl.BlockSpec((cells, rows, c), lambda i: (first(i), 0, 0))
    return pl.pallas_call(
        partial(stencil_bwd_kernel, mesh, chunks, cells),
        name="stencil_bwd",
        grid=(chunks + 1,),
        out_shape=(
            sd((tail_rows, LANES), F32),
            sd((shard_rows, LANES), F32),
            sd((CB, width, rows, LANES), F32),
        ),
        in_specs=[pl.BlockSpec(memory_space=pltpu.SMEM), by_first(CP), by_first(CP)]
        + [vmem_spec()] * 8
        + [any_spec()],
        out_specs=(vmem_spec(), vmem_spec(), any_spec()),
        scratch_shapes=[
            pltpu.VMEM((CB, (width + 2 * REACH) * SLOTS, LANES), F32),
            pltpu.VMEM((CB, width, rows, LANES), F32),
            pltpu.VMEM((TAPS, rows, CP), F32),
            pltpu.VMEM((TAPS * rows, 16), F32),
            pltpu.VMEM((TAPS, rows, CP), F32),
            pltpu.VMEM(cols.shape, BF16),
            pltpu.VMEM(edge.shape, BF16),
            pltpu.VMEM(corners.shape, BF16),
            pltpu.VMEM((2,) * (n - 1) + (shard_rows, LANES), F32),
        ]
        + [pltpu.VMEM((2,) * (n - 1 - k) + (shard_rows, LANES), F32) for k in range(n)]
        + [
            pltpu.SemaphoreType.DMA((3, n)),
            pltpu.SemaphoreType.DMA((3, n)),
            pltpu.SemaphoreType.DMA((8,)),
            pltpu.SemaphoreType.DMA((8,)),
            pltpu.SemaphoreType.DMA,
            pltpu.SemaphoreType.DMA((CB,)),
        ],
        compiler_params=params(
            dimension_semantics=("arbitrary",), collective_id=1, has_side_effects=True
        ),
    )(height, mixed, gconv, cols, edge, corners, table, trowh, wd, extra, w1, shards)


def norm_bwd_kernel(
    height_ref, gm_ref, x_ref, mean_ref, inv_ref, g_ref, gain, tail_in, out_ref, tail_ref, gg_scr
):
    step = pl.program_id(0)
    cells, rows, _ = x_ref.shape
    gvec = gain[2:3, :C]
    live = iota((rows, C), 0) < height_ref[0]

    @pl.when(step == 0)
    def _():
        gg_scr[...] = jnp.zeros_like(gg_scr)

    def cell(j, total):
        inv = inv_ref[j][:, :1]
        normed = (x_ref[j].astype(F32) - mean_ref[j][:, :1]) * inv
        gm = jnp.concatenate([gm_ref[q, j] for q in range(CB)], 1)[:, :C]
        gm = jnp.where(live, gm, 0.0)
        total = total + gm * normed
        v = gm * gvec
        mean = jnp.mean(v, -1, keepdims=True)
        mean_n = jnp.mean(v * normed, -1, keepdims=True)
        up = jnp.where(live, g_ref[j].astype(F32), 0.0)
        out_ref[j] = inv * (v - mean - normed * mean_n) + up
        return total

    gg_scr[:, :C] = lax.fori_loop(0, cells, cell, gg_scr[:, :C], unroll=2)

    @pl.when(step == pl.num_programs(0) - 1)
    def _():
        tail_ref[...] = tail_in[...]
        add_vector(tail_ref, OFF_GAIN, as_blocks(jnp.sum(gg_scr[...], 0, keepdims=True), C))


def norm_bwd(height, gm, x, mean, inv, g, small, tail, chunks):
    width, rows, _ = x.shape
    cells = width // chunks
    sd = jax.ShapeDtypeStruct
    block = lambda c: pl.BlockSpec((cells, rows, c), lambda i: (i, 0, 0))
    return pl.pallas_call(
        norm_bwd_kernel,
        name="norm_bwd",
        grid=(chunks,),
        out_shape=(sd((width, rows, C), F32), sd(tail.shape, F32)),
        in_specs=[
            pl.BlockSpec(memory_space=pltpu.SMEM),
            pl.BlockSpec((CB, cells, rows, LANES), lambda i: (0, i, 0, 0)),
            block(C),
            block(LANES),
            block(LANES),
            block(C),
            vmem_spec(),
            vmem_spec(),
        ],
        out_specs=(block(C), vmem_spec()),
        scratch_shapes=[pltpu.VMEM((rows, CP), F32)],
        compiler_params=params(dimension_semantics=("arbitrary",)),
    )(height, gm, x, mean, inv, g, small, tail)


def tail_kernel(mesh, part_ref, tail_ref, grad_ref, scale_ref, got, msg, full, place, send, recv):
    nlat, nlon = mesh.shape["lat"], mesh.shape["lon"]
    n = nlat * nlon
    lat, lon = lax.axis_index("lat"), lax.axis_index("lon")
    me = lat * nlon + lon
    piece = tail_ref.shape[1]
    shard_rows = part_ref.shape[0]
    barrier = pltpu.get_barrier_semaphore()

    def others(body):
        def step(i, carry):
            body(lax.rem(me + i, n))
            return carry

        lax.fori_loop(1, n, step, 0)

    def hello(d):
        pl.semaphore_signal(
            barrier, inc=1, device_id=(d // nlon, lax.rem(d, nlon)), device_id_type=MESH
        )

    others(hello)
    pl.semaphore_wait(barrier, n - 1)

    def scatter_piece(d):
        pltpu.make_async_remote_copy(
            src_ref=tail_ref.at[d],
            dst_ref=got.at[me],
            send_sem=send.at[0],
            recv_sem=recv.at[0],
            device_id=(d // nlon, lax.rem(d, nlon)),
            device_id_type=MESH,
        ).start()

    def wait_all(buffer, k):
        pltpu.make_async_remote_copy(
            src_ref=buffer.at[pl.ds(0, n - 1)],
            dst_ref=buffer.at[pl.ds(0, n - 1)],
            send_sem=send.at[k],
            recv_sem=recv.at[k],
            device_id=(lat, lon),
            device_id_type=MESH,
        ).wait()

    others(scatter_piece)
    got[me] = tail_ref[me]
    square = jnp.sum(part_ref[...] * part_ref[...])
    wait_all(got, 0)

    total = lax.fori_loop(
        1, n, lambda i, acc: acc + got[lax.rem(i, n)], got[0]
    )
    square = square + jnp.sum(total * total)
    msg[0:piece, :] = total
    msg[piece : piece + 1, :] = jnp.broadcast_to(square, (1, LANES))

    def share(d):
        pltpu.make_async_remote_copy(
            src_ref=msg,
            dst_ref=full.at[me],
            send_sem=send.at[1],
            recv_sem=recv.at[1],
            device_id=(d // nlon, lax.rem(d, nlon)),
            device_id_type=MESH,
        ).start()

    others(share)
    full[me] = msg[...]
    place[...] = jnp.zeros_like(place)
    wait_all(full, 1)

    def take(d, acc):
        place[pl.ds(shard_rows + d * piece, piece), :] = full[d, 0:piece, :]
        return acc + full[d, piece : piece + 1, :]

    squares = lax.fori_loop(0, n, take, jnp.zeros((1, LANES), F32))
    start = jnp.clip(me * shard_rows - TAIL_ROW + shard_rows, 0, shard_rows + n * piece)
    grad_ref[...] = part_ref[...] + place[pl.ds(start, shard_rows), :]
    scale_ref[...] = jnp.broadcast_to(jnp.sqrt(squares), scale_ref.shape)


def finish(mesh, part, tail):
    n, piece, _ = tail.shape
    shard_rows = part.shape[0]
    sd = jax.ShapeDtypeStruct
    return pl.pallas_call(
        partial(tail_kernel, mesh),
        name="small_gradients",
        out_shape=(sd(part.shape, F32), sd((8, LANES), F32)),
        in_specs=[vmem_spec()] * 2,
        out_specs=(vmem_spec(),) * 2,
        scratch_shapes=[
            pltpu.VMEM((n, piece, LANES), F32),
            pltpu.VMEM((piece + 1, LANES), F32),
            pltpu.VMEM((n, piece + 1, LANES), F32),
            pltpu.VMEM((2 * shard_rows + n * piece + 8, LANES), F32),
            pltpu.SemaphoreType.DMA((2,)),
            pltpu.SemaphoreType.DMA((2,)),
        ],
        compiler_params=params(collective_id=3, has_side_effects=True),
    )(part, tail)


def stencil_table(support_vals, support_lon):
    rows = support_vals.shape[0]
    vals = support_vals.reshape(rows, S // 3, 3, K)
    offsets = jnp.arange(-REACH, REACH + 1)
    hit = support_lon.reshape(rows, S // 3, 3)[:, :, :, None] == offsets
    picked = jnp.where(hit[:, :, :, :, None], vals[:, :, :, None, :], 0.0)
    return jnp.transpose(jnp.sum(picked, 1), (1, 2, 0, 3))


def flat_table(table):
    t = table.reshape(-1, K)
    return jnp.pad(t, ((0, 0), (0, 16 - K)))


def local(
    mesh, block_in, noise, cotangent, band_heights, support_lon, support_vals,
    master, moment_one, moment_two, average, step_count,
):
    rows, width, _ = block_in.shape
    devices = mesh.shape["lat"] * mesh.shape["lon"]
    shard = master.shape[0]
    shard_rows = shard // LANES
    assert shard_rows * LANES == shard
    flat_rows = shard_rows * devices
    chunks = 6
    cells = width // chunks
    height = lax.dynamic_slice_in_dim(band_heights, lax.axis_index("lat"), 1, 0)
    x = jnp.transpose(block_in, (1, 0, 2))
    g = jnp.transpose(cotangent, (1, 0, 2))

    table = flat_table(stencil_table(support_vals, support_lon))
    planes = table.reshape(TAPS, rows, 16)
    trow = jnp.stack([planes[:, 0], lax.dynamic_index_in_dim(planes, height[0] - 1, 1, keepdims=False)])
    trow = jnp.pad(trow, ((0, 0), (0, 1), (0, 0)))
    share = master.astype(BF16).reshape(shard_rows, LANES)
    edge = jnp.stack([x[:, 0], lax.dynamic_index_in_dim(x, height[0] - 1, 1, keepdims=False)], 1)
    cols = jnp.stack([x[:REACH], x[width - REACH :]])
    corners = jnp.stack([edge[:REACH], edge[width - REACH :]], 0)
    corners = jnp.transpose(corners, (2, 0, 1, 3))
    edge = jnp.transpose(edge.reshape(chunks, cells, 2, C), (0, 2, 1, 3))
    w1, w2, wn, wd, small, colh, rowh, cornh, trowh = gather_weights(
        mesh, share, cols, edge, corners, trow
    )
    aug = jnp.concatenate(
        [
            jnp.zeros((width, rows, 1), BF16),
            jnp.transpose(noise, (2, 1, 0)),
            jnp.ones((width, rows, 1), BF16),
            jnp.zeros((width, rows, LANES - NOISE - 2), BF16),
        ],
        2,
    )
    conv, mixed, mean, inv = stencil_fwd(
        height, x, colh, rowh, cornh, table, wd, small, aug, wn, chunks
    )
    shards = (2,) * len(bit_list(mesh)) + (shard_rows, LANES)
    out, gconv, grow, gcol, gcorn, packed, extra = mlp(
        height, conv, g, x, w1, w2, small, shards, chunks
    )
    piece = -(-(flat_rows - TAIL_ROW) // devices)
    tail, part, gm = stencil_bwd(
        mesh, height, mixed, gconv, gcol, grow, gcorn, table, trowh, wd, extra, w1, packed,
        devices * piece, chunks,
    )
    grad_in, tail = norm_bwd(height, gm, x, mean, inv, g, small, tail, chunks)
    grad, norm = finish(mesh, part, tail.reshape(devices, piece, LANES))
    grad_part = grad.reshape(shard)
    grad_norm = norm[0, :1]
    factor = 0.01 / jnp.maximum(grad_norm, 0.01)
    clipped = grad_part * factor
    new_one = 0.9 * moment_one + 0.1 * clipped
    new_two = 0.999 * moment_two + 0.001 * clipped * clipped
    step_float = step_count[0].astype(F32)
    fix_one = 1.0 - jnp.power(jnp.float32(0.9), step_float)
    fix_two = 1.0 - jnp.power(jnp.float32(0.999), step_float)
    update = new_one / fix_one / (jnp.sqrt(new_two / fix_two) + 1e-08) + 0.1 * master
    new_master = master - 0.02 * update
    new_avg = 0.9 * average + 0.1 * new_master
    return (
        jnp.transpose(out, (1, 0, 2)),
        jnp.transpose(grad_in, (1, 0, 2)),
        grad_part,
        grad_norm,
        new_master,
        new_one,
        new_two,
        new_avg,
        new_master.astype(BF16),
    )


def solution(mesh):
    flat = P(("lat", "lon"))
    field = P("lat", "lon", None)
    return jax.shard_map(
        partial(local, mesh),
        mesh=mesh,
        in_specs=(
            field, P(None, "lat", "lon"), field, P(), P("lat", None), P("lat", None, None),
            flat, flat, flat, flat, P(),
        ),
        out_specs=(field, field, flat, P(), flat, flat, flat, flat, flat),
        check_vma=False,
    )
```

```python
from functools import partial
import math

import jax
import jax.numpy as jnp
from jax import lax
from jax.experimental import pallas as pl
from jax.experimental.pallas import tpu as pltpu
from jax.sharding import PartitionSpec as P

C = 641
FF = 1282
NOISE = 8
K = 9
S = 12
REACH = 2
LANES = 128
CB = 6
CP = CB * LANES
FB = 11
FP = FB * LANES
TAPS = 15
MESH = pl.DeviceIdType.MESH
HIGHEST = lax.Precision.HIGHEST
F32 = jnp.float32
BF16 = jnp.bfloat16
VMEM_LIMIT = 60 * 1024 * 1024
SLOTS = 28
REUSE = 10
ROW_TWO = (C * FF) // LANES
LANE_TWO = (C * FF) % LANES
TAIL_ROW = (2 * C * FF) // LANES
OFF_B1 = 2 * C * FF
OFF_B2 = OFF_B1 + FF
OFF_GAIN = OFF_B2 + C
OFF_DISCO = OFF_GAIN + C
OFF_NOISE = OFF_DISCO + K * C
END_FLAT = OFF_NOISE + NOISE * C


def params(**kw):
    return pltpu.CompilerParams(vmem_limit_bytes=VMEM_LIMIT, **kw)


def any_spec():
    return pl.BlockSpec(memory_space=pl.ANY)


def vmem_spec():
    return pl.BlockSpec(memory_space=pltpu.VMEM)


def iota(shape, dim):
    return lax.broadcasted_iota(jnp.int32, shape, dim)


def bit_list(mesh):
    bits = []
    for axis in ("lat", "lon"):
        count = int(math.log2(mesh.shape[axis]))
        assert 1 << count == mesh.shape[axis]
        bits += [(axis, b) for b in reversed(range(count))]
    return bits


def my_bits(bits):
    ids = {"lat": lax.axis_index("lat"), "lon": lax.axis_index("lon")}
    return [(ids[a] >> b) & 1 for a, b in bits]


def partner(axis, bit):
    lat, lon = lax.axis_index("lat"), lax.axis_index("lon")
    if axis == "lat":
        return (lat ^ (1 << bit), lon)
    return (lat, lon ^ (1 << bit))


def stage_orders(mesh):
    bits = bit_list(mesh)
    n = len(bits)
    if (mesh.shape["lat"], mesh.shape["lon"]) == (8, 4):
        return [[0, 1, 2, 3, 4], [0, 1, 3, 2, 4]]
    order = list(range(n))
    return [order, order]


def scatter_orders(mesh):
    n = len(bit_list(mesh))
    if (mesh.shape["lat"], mesh.shape["lon"]) == (8, 4):
        return [[4, 3, 2, 1, 0], [4, 2, 3, 1, 0], [4, 1, 0, 3, 2]]
    return [list(reversed(range(n)))] * 3


def rotl_rows(v, first, unit):
    index = (iota((8, LANES), 1) + first + unit * iota((8, LANES), 0)) % LANES
    return jnp.take_along_axis(v, index, axis=1)


def row_vector(flat_ref, offset, length):
    blocks = -(-length // LANES)
    row, shift = divmod(offset, LANES)
    near = flat_ref[row : row + blocks, :]
    if shift:
        far = flat_ref[row + 1 : row + 1 + blocks, :]
        lane = iota((blocks, LANES), 1)
        near = pltpu.roll(jnp.where(lane >= shift, near, far), LANES - shift, 1)
    index = iota((blocks, LANES), 0) * LANES + iota((blocks, LANES), 1)
    return jnp.where(index < length, near, 0.0)


def put_row(ref, row, value):
    for q in range(value.shape[0]):
        ref[row : row + 1, q * LANES : (q + 1) * LANES] = value[q : q + 1, :].astype(ref.dtype)


def unpack_weights(flat, w1, w2):
    lane = iota((8, LANES), 1)
    row = iota((8, LANES), 0)

    def rows_one(base, first):
        near = [flat[pl.ds(base + q, 8, stride=10), :] for q in range(FB + 1)]
        out = [
            rotl_rows(jnp.where(lane >= first + 2 * row, near[q], near[q + 1]), first, 2)
            for q in range(FB)
        ]
        out[-1] = jnp.where(lane < FF - (FB - 1) * LANES, out[-1], 0.0)
        return out

    def body_one(b, carry):
        for k in range(0, 8, 2):
            pair = [rows_one(641 * b + 80 * (k + h), 16 * (k + h)) for h in range(2)]
            at = pl.ds(pl.multiple_of(64 * b + 8 * k, 16), 16)
            for q in range(FB):
                v = jnp.concatenate([pair[0][q], pair[1][q]], 0)
                w1[at, q * LANES : (q + 1) * LANES] = v.astype(BF16)
        return carry

    last = C - 1
    lax.fori_loop(0, last // 64, body_one, 0)
    zero = jnp.zeros((8, LANES), F32)
    for q, v in enumerate(rows_one(641 * (last // 64), 0)):
        v = jnp.concatenate([jnp.where(row == 0, v, 0.0), zero], 0)
        w1[last : last + 16, q * LANES : (q + 1) * LANES] = v.astype(BF16)
    w1[last + 16 :, :] = jnp.zeros((CP - last - 16, FP), BF16)

    def rows_two(base, first):
        count = CB + 2 if first + 7 >= LANES else CB + 1
        near = [flat[pl.ds(base + q, 8, stride=5), :] for q in range(count)]
        out = []
        for q in range(CB):
            v = jnp.where(lane >= first + row, near[q], near[q + 1])
            if first + 7 >= LANES:
                v = jnp.where(lane < first + row - LANES, near[q + 2], v)
            out.append(rotl_rows(v, first, 1))
        out[-1] = jnp.where(lane < C - (CB - 1) * LANES, out[-1], 0.0)
        return out

    def body_two(b, carry):
        for k in range(0, 16, 2):
            pair = [
                rows_two(ROW_TWO + 641 * b + 40 * (k + h), LANE_TWO + 8 * (k + h))
                for h in range(2)
            ]
            at = pl.ds(pl.multiple_of(128 * b + 8 * k, 16), 16)
            for q in range(CB):
                v = jnp.concatenate([pair[0][q], pair[1][q]], 0)
                w2[at, q * LANES : (q + 1) * LANES] = v.astype(BF16)
        return carry

    full = FF // LANES
    lax.fori_loop(0, full, body_two, 0)
    for q, v in enumerate(rows_two(ROW_TWO + 641 * full, LANE_TWO)):
        v = jnp.concatenate([jnp.where(row < FF - full * LANES, v, 0.0), zero], 0)
        w2[full * LANES : full * LANES + 16, q * LANES : (q + 1) * LANES] = v.astype(BF16)
    w2[full * LANES + 16 :, :] = jnp.zeros((FP - full * LANES - 16, CP), BF16)


def unpack_small(flat, base, wn, wd, small, wnf):
    vector = lambda offset, length: row_vector(flat, offset - base * LANES, length)
    small[...] = jnp.zeros_like(small)
    put_row(small, 0, vector(OFF_B1, FF))
    put_row(small, 1, vector(OFF_B2, C))
    put_row(small, 2, vector(OFF_GAIN, C))
    wd[...] = jnp.zeros_like(wd)
    wnf[...] = jnp.zeros_like(wnf)
    for k in range(K):
        put_row(wd, k, vector(OFF_DISCO + k * C, C))
    for k in range(NOISE):
        put_row(wnf, 1 + k, vector(OFF_NOISE + k * C, C))
    wn[...] = wnf[...].astype(BF16)


def neighbours():
    lat, lon = lax.axis_index("lat"), lax.axis_index("lon")
    nlat, nlon = lax.axis_size("lat"), lax.axis_size("lon")
    return lat, lon, nlat, nlon, lax.rem(lon + 1, nlon), lax.rem(lon + nlon - 1, nlon)


def halo_copies(cols, rows, corners, colh, rowh, cornh, send, recv, trow=None, trowh=None):
    lat, lon, nlat, nlon, east, west = neighbours()
    out = []

    def add(src, dst, target, k, sends, gets):
        out.append(
            (
                sends,
                gets,
                pltpu.make_async_remote_copy(
                    src_ref=src,
                    dst_ref=dst,
                    send_sem=send.at[k],
                    recv_sem=recv.at[k],
                    device_id=target,
                    device_id_type=MESH,
                ),
            )
        )

    has_up, has_down = lat > 0, lat < nlat - 1
    up, down = lat - 1, lat + 1
    add(rows.at[:, 0], rowh.at[:, 1], (up, lon), 2, has_up, has_down)
    add(rows.at[:, 1], rowh.at[:, 0], (down, lon), 3, has_down, has_up)
    add(cols.at[0], colh.at[1], (lat, west), 0, None, None)
    add(cols.at[1], colh.at[0], (lat, east), 1, None, None)
    add(corners.at[0, 0], cornh.at[1, 1], (up, west), 4, has_up, has_down)
    add(corners.at[0, 1], cornh.at[1, 0], (up, east), 5, has_up, has_down)
    add(corners.at[1, 0], cornh.at[0, 1], (down, west), 6, has_down, has_up)
    add(corners.at[1, 1], cornh.at[0, 0], (down, east), 7, has_down, has_up)
    if trow is not None:
        add(trow.at[0], trowh.at[1], (up, lon), 8, has_up, has_down)
        add(trow.at[1], trowh.at[0], (down, lon), 9, has_down, has_up)
    return out


def start_halo(copies):
    for sends, _, copy in copies:
        if sends is None:
            copy.start()
        else:
            pl.when(sends)(copy.start)


def wait_halo(copies):
    for sends, gets, copy in copies:
        if sends is None:
            copy.wait()
        else:
            pl.when(sends)(copy.wait_send)
            pl.when(gets)(copy.wait_recv)


def greet(bits, halo):
    barrier = pltpu.get_barrier_semaphore()
    lat, lon, nlat, nlon, east, west = neighbours()

    def hello(target):
        pl.semaphore_signal(barrier, inc=1, device_id=target, device_id_type=MESH)

    count = 0
    for axis, bit in bits:
        hello(partner(axis, bit))
        count += 1
    if halo:
        for target in ((lat, east), (lat, west)):
            hello(target)
            count += 1
        for side, cond in ((lat - 1, lat > 0), (lat + 1, lat < nlat - 1)):

            @pl.when(cond)
            def _(side=side):
                for x in (lon, east, west):
                    hello((side, x))

    if halo:
        count = count + 3 * (lat > 0).astype(jnp.int32) + 3 * (lat < nlat - 1).astype(jnp.int32)
    pl.semaphore_wait(barrier, count)


class Gather:
    def __init__(self, mesh, share, buf, early, send, recv, bsend, brecv):
        self.bits = bit_list(mesh)
        self.n = len(self.bits)
        self.orders = stage_orders(mesh)
        self.mine = my_bits(self.bits)
        self.share, self.buf, self.early = share, buf, early
        self.send, self.recv, self.bsend, self.brecv = send, recv, bsend, brecv
        rows = share.shape[0]
        cut = (rows // 2 + 15) // 16 * 16
        self.spans = [(0, cut), (cut, rows - cut)]
        self.roots, self.start = early_shards(1 << self.n, rows)

    def own(self, sem):
        return pltpu.make_async_copy(self.share, self.buf.at[tuple(self.mine)], sem)

    def copy(self, colour, k):
        order = self.orders[colour]
        index = tuple(
            slice(None) if i in order[:k] else self.mine[i] for i in range(self.n)
        ) + (pl.ds(*self.spans[colour]),)
        return pltpu.make_async_remote_copy(
            src_ref=self.buf.at[index],
            dst_ref=self.buf.at[index],
            send_sem=self.send.at[colour, k],
            recv_sem=self.recv.at[colour, k],
            device_id=partner(*self.bits[order[k]]),
            device_id_type=MESH,
        )

    def advance(self, k):
        for colour in range(2):
            self.copy(colour, k).wait()
            if k + 1 < self.n:
                self.copy(colour, k + 1).start()

    def same(self, root, indices):
        cond = True
        for i in indices:
            cond = jnp.logical_and(cond, self.mine[i] == ((root >> (self.n - 1 - i)) & 1))
        return cond

    def early_own(self, sem):
        for r, root in enumerate(self.roots):

            @pl.when(self.same(root, range(self.n)))
            def _(r=r):
                rows = self.share.shape[0] - self.start
                copy = pltpu.make_async_copy(
                    self.share.at[pl.ds(self.start, rows)], self.early.at[r], sem
                )
                copy.start()
                copy.wait()

    def early_copies(self, k):
        order = self.orders[0]
        for r, root in enumerate(self.roots):
            sends = self.same(root, order[k:])
            now = order[k]
            other = self.mine[now] != ((root >> (self.n - 1 - now)) & 1)
            gets = jnp.logical_and(other, self.same(root, order[k + 1 :]))
            yield sends, gets, pltpu.make_async_remote_copy(
                src_ref=self.early.at[r],
                dst_ref=self.early.at[r],
                send_sem=self.bsend.at[r, k],
                recv_sem=self.brecv.at[r, k],
                device_id=partner(*self.bits[now]),
                device_id_type=MESH,
            )

    def early_start(self, k):
        for sends, _, copy in self.early_copies(k):
            pl.when(sends)(copy.start)

    def early_wait(self, k):
        for sends, gets, copy in self.early_copies(k):
            pl.when(sends)(copy.wait_send)
            pl.when(gets)(copy.wait_recv)


def early_shards(devices, shard_rows):
    roots = list(range(TAIL_ROW // shard_rows, (END_FLAT - 1) // LANES // shard_rows + 1))
    start = (TAIL_ROW - roots[0] * shard_rows) // 16 * 16 if len(roots) == 1 else 0
    return roots, start


def gather_plan(n):
    if n == 5:
        return {0: (0, -1), 1: (1, -1), 2: (2, 8), 3: (4, 14)}
    return {}


def norm_parts(x):
    mean = jnp.mean(x, -1, keepdims=True)
    center = x - mean
    var = jnp.mean(center * center, -1, keepdims=True)
    return center, lax.rsqrt(var + 1e-05)


def rounded(v):
    return v.astype(BF16).astype(F32)


def stencil_fwd_kernel(
    mesh, chunks, cells, height_ref, x_ref, share, cols, edge, corners, trow, table, aug,
    out_ref, mean_ref, inv_ref, mix_hbm, w1, w2, wd, small, trowh,
    m_scr, k_scr, nt_scr, mix_scr, wnf, wn, colh, rowh, cornh, trh, buf, early, flat, eflat,
    send, recv, bsend, brecv, hsend, hrecv, own_sem, mix_sem,
):
    gather = Gather(mesh, share, buf, early, send, recv, bsend, brecv)
    n = gather.n
    plan = gather_plan(n)
    step = pl.program_id(0)
    rows = x_ref.shape[1]
    width = chunks * cells
    height = height_ref[0]
    shard_rows = share.shape[0]
    halos = lambda: halo_copies(cols, edge, corners, colh, rowh, cornh, hsend, hrecv, trow, trh)
    mix_copy = lambda: pltpu.make_async_copy(mix_scr, mix_hbm, mix_sem)

    @pl.when(step == 0)
    def _():
        gather.own(own_sem).start()
        gather.early_own(mix_sem)
        gather.own(own_sem).wait()
        greet(gather.bits, True)
        gather.early_start(0)
        for colour in range(2):
            gather.copy(colour, 0).start()
        start_halo(halos())

    for k in range(n):

        @pl.when(step == min(k + 1, chunks))
        def _(k=k):
            gather.early_wait(k)
            if k + 1 < n:
                gather.early_start(k + 1)

    @pl.when(step < chunks)
    def _():
        def cell(j, carry):
            x = x_ref[j].astype(F32)
            mean = jnp.mean(x, -1, keepdims=True)
            center = x - mean
            inv = lax.rsqrt(jnp.mean(center * center, -1, keepdims=True) + 1e-05)
            normed = center * inv
            mean_ref[j] = jnp.broadcast_to(mean, (rows, LANES))
            inv_ref[j] = jnp.broadcast_to(inv, (rows, LANES))
            at = pl.ds((step * cells + j + REACH) * SLOTS + 1, rows)
            for g in range(CB):
                lo, hi = g * LANES, min((g + 1) * LANES, C)
                m_scr[g, at, : hi - lo] = normed[:, lo:hi]
            return carry

        lax.fori_loop(0, cells, cell, 0, unroll=3)

    @pl.when(step == chunks)
    def _():
        if 0 in plan:
            gather.advance(0)
        lat, _, nlat, *_ = neighbours()
        wait_halo(halos())
        keep = (lat > 0, lat < nlat - 1)
        for r in range(2):
            trowh[r] = jnp.where(keep[r], trh[r], 0.0)

        base = gather.roots[0] * shard_rows + gather.start
        count = shard_rows - gather.start
        eflat[...] = jnp.zeros_like(eflat)
        for r in range(len(gather.roots)):
            eflat[r * count : (r + 1) * count, :] = early[r].astype(F32)
        unpack_small(eflat, base, wn, wd, small, wnf)
        k_scr[...] = jnp.dot(
            table[...], wd[...], preferred_element_type=F32, precision=HIGHEST
        ).reshape(k_scr.shape)
        gvec = small[2:3, :C]

        def mix(v):
            center, inv = norm_parts(v.astype(F32))
            return rounded(center * inv * gvec)

        def beside(ref):
            return [jnp.where(keep[r], mix(ref(r)), 0.0) for r in range(2)]

        def put(column, top, low, fresh=None):
            at = column * SLOTS
            hrow = iota((rows, LANES), 0)
            for q in range(CB):
                lo, hi = q * LANES, min((q + 1) * LANES, C)
                body = pl.ds(at + 1, rows)
                wide = slice(0, hi - lo)
                if fresh is None:
                    v = rounded(m_scr[q, body, wide] * gvec[:, lo:hi])
                    v = jnp.where(hrow[:, wide] < height, v, 0.0)
                    mix_scr[column - REACH, :, lo:hi] = v.astype(BF16)
                else:
                    v = jnp.where(hrow[:, wide] < height, fresh[:, lo:hi], 0.0)
                m_scr[q, body, wide] = jnp.where(hrow[:, wide] == height, low[:, lo:hi], v)
                m_scr[q, pl.ds(at, 1), wide] = top[:, lo:hi]
                m_scr[q, pl.ds(at + rows + 1, 1), wide] = low[:, lo:hi]

        lanes = slice((CB - 1) * LANES, CB * LANES)
        mix_scr[:, :, lanes] = jnp.zeros((width, rows, LANES), BF16)
        for side in range(2):
            top, low = beside(lambda r: cornh[r, side])
            for i in range(REACH):
                column = i if side == 0 else width + REACH + i
                put(column, top[i : i + 1], low[i : i + 1], mix(colh[side, i]))

        def strip(c, carry):
            tops, lows = beside(lambda r: rowh[c, r])
            for i in range(cells):
                put(c * cells + i + REACH, tops[i : i + 1], lows[i : i + 1])
            return carry

        lax.fori_loop(0, chunks, strip, 0)
        mix_copy().start()

    for k, (at, loop) in plan.items():
        if k > 0 and loop < 0:

            @pl.when(step == chunks + at)
            def _(k=k):
                gather.advance(k)

    @pl.when(step >= chunks)
    def _():
        first = (step - chunks) * cells
        nt_scr[...] = jnp.dot(
            aug[...].reshape(cells * rows, LANES), wn[...], preferred_element_type=F32
        )
        lane = iota((8, LANES), 1)
        for g in range(CB):
            lanes = slice(g * LANES, (g + 1) * LANES)
            for hb in range(rows // 8):
                at = slice(8 * hb, 8 * hb + 8)

                def cell(i, carry):
                    j = i * REUSE
                    acc = [nt_scr[pl.ds((j + u) * rows + 8 * hb, 8), lanes] for u in range(REUSE)]
                    for l in range(3):
                        near = [
                            m_scr[g, pl.ds((first + j + u) * SLOTS + 8 * hb + l, 8), :]
                            for u in range(REUSE + 2 * REACH)
                        ]
                        for w in range(5):
                            tap = k_scr[5 * l + w, at, lanes]
                            acc = [a + tap * near[u + w] for u, a in enumerate(acc)]
                    for u in range(REUSE):
                        v = acc[u]
                        if g == CB - 1:
                            v = jnp.where(lane == 0, v, aug[j + u, at, :].astype(F32))
                        out_ref[j + u, at, lanes] = v.astype(BF16)
                    return carry

                lax.fori_loop(0, cells // REUSE, cell, 0)
                for k, (past, loop) in plan.items():
                    if loop == g * (rows // 8) + hb:

                        @pl.when(step == chunks + past)
                        def _(k=k):
                            gather.advance(k)

    @pl.when(step == 2 * chunks - 1)
    def _():
        for k in range(n):
            if k not in plan:
                gather.advance(k)
        total = 1 << n

        def widen(d, carry):
            index = tuple((d >> (n - 1 - i)) & 1 for i in range(n))
            flat[pl.ds(d * shard_rows, shard_rows), :] = buf[index].astype(F32)
            return carry

        lax.fori_loop(0, total, widen, 0)
        flat[total * shard_rows :, :] = jnp.zeros((flat.shape[0] - total * shard_rows, LANES), F32)
        unpack_weights(flat, w1, w2)
        mix_copy().wait()


def stencil_fwd(mesh, height, x, share, cols, edge, corners, trow, table, aug, chunks):
    width, rows, _ = x.shape
    cells = width // chunks
    assert cells % REUSE == 0
    n = len(bit_list(mesh))
    shard_rows = share.shape[0]
    total = shard_rows << n
    roots, start = early_shards(1 << n, shard_rows)
    count = shard_rows - start
    first = lambda i: jnp.where(i < chunks, i, chunks - 1)
    second = lambda i: jnp.where(i < chunks, 0, i - chunks)
    sd = jax.ShapeDtypeStruct
    by_first = lambda c: pl.BlockSpec((cells, rows, c), lambda i: (first(i), 0, 0))
    by_second = lambda c: pl.BlockSpec((cells, rows, c), lambda i: (second(i), 0, 0))
    dma = pltpu.SemaphoreType.DMA
    return pl.pallas_call(
        partial(stencil_fwd_kernel, mesh, chunks, cells),
        name="stencil_fwd",
        grid=(2 * chunks,),
        out_shape=(
            sd((width, rows, CP), BF16),
            sd((width, rows, LANES), F32),
            sd((width, rows, LANES), F32),
            sd((width, rows, CP), BF16),
            sd((CP, FP), BF16),
            sd((FP, CP), BF16),
            sd((16, CP), F32),
            sd((8, FP), F32),
            sd(trow.shape, F32),
        ),
        in_specs=[pl.BlockSpec(memory_space=pltpu.SMEM), by_first(C)]
        + [vmem_spec()] * 6
        + [by_second(LANES)],
        out_specs=(by_second(CP), by_first(LANES), by_first(LANES), any_spec())
        + (vmem_spec(),) * 5,
        scratch_shapes=[
            pltpu.VMEM((CB, (width + 2 * REACH) * SLOTS, LANES), F32),
            pltpu.VMEM((TAPS, rows, CP), F32),
            pltpu.VMEM((cells * rows, CP), F32),
            pltpu.VMEM((width, rows, CP), BF16),
            pltpu.VMEM((LANES, CP), F32),
            pltpu.VMEM((LANES, CP), BF16),
            pltpu.VMEM(cols.shape, BF16),
            pltpu.VMEM(edge.shape, BF16),
            pltpu.VMEM(corners.shape, BF16),
            pltpu.VMEM(trow.shape, F32),
            pltpu.VMEM((2,) * n + (shard_rows, LANES), BF16),
            pltpu.VMEM((len(roots), count, LANES), BF16),
            pltpu.VMEM((total + 96, LANES), F32),
            pltpu.VMEM((len(roots) * count + 16, LANES), F32),
            dma((2, n)),
            dma((2, n)),
            dma((len(roots), n)),
            dma((len(roots), n)),
            dma((10,)),
            dma((10,)),
            dma,
            dma,
        ],
        compiler_params=params(
            dimension_semantics=("arbitrary",), collective_id=0, has_side_effects=True
        ),
    )(height, x, share, cols, edge, corners, trow, table, aug)


def pack_weights(one, two, flat):
    lane = iota((8, LANES), 1)
    row = iota((8, LANES), 0)
    flat[...] = jnp.zeros_like(flat)

    def turned(v, first, unit):
        return pltpu.roll(v, first, 1, stride=unit, stride_axis=0)

    def main(ref, at, first, unit, out, base, step, count):
        keep = lane >= first + unit * row
        before = jnp.zeros((8, LANES), F32)
        for q in range(count):
            now = turned(ref[q, at, :], first, unit)
            flat[pl.ds(base + q, 8, stride=step), :] = jnp.where(keep, now, before)
            before = now

    def rest(ref, at, first, unit, count, width, mask=None):
        s = first + unit * row
        before = turned(ref[count - 1, at, :], first, unit)
        now = turned(ref[count, at, :], first, unit)
        v = jnp.where(lane < s, before, jnp.where(lane < s + width, now, 0.0))
        return v if mask is None else jnp.where(mask, v, 0.0)

    shift = 8 - LANE_TWO
    base_two = ROW_TWO - 5 * LANE_TWO
    full = FF // LANES
    extra = C - (CB - 1) * LANES

    def two_main(b, carry):
        for k in range(16):
            at = pl.ds(128 * b + 8 * k + shift, 8)
            main(two, at, 8 * k, 1, flat, base_two + 641 * b + 40 * k, 5, CB - 1)
        return carry

    lax.fori_loop(0, full, two_main, 0)
    end = slice(128 * full + shift, 128 * full + shift + 8)
    mask = row < FF - full * LANES + LANE_TWO
    before = jnp.zeros((8, LANES), F32)
    for q in range(CB - 1):
        now = jnp.where(mask, turned(two[q, end, :], 0, 1), 0.0)
        at = pl.ds(base_two + 641 * full + q, 8, stride=5)
        flat[at, :] = jnp.where(lane >= row, now, before)
        before = now

    def one_main(b, carry):
        for k in range(8):
            at = pl.ds(pl.multiple_of(64 * b + 8 * k, 8), 8)
            main(one, at, 16 * k, 2, flat, 641 * b + 80 * k, 10, FB - 1)
        return carry

    last = C - 1
    assert last % 64 == 0
    lax.fori_loop(0, last // 64, one_main, 0)
    row_last = 641 * (last // 64)
    for q in range(FB - 1):
        flat[row_last + q : row_last + q + 1, :] = one[q, last : last + 1, :]

    def add_all(places, values):
        olds = [flat[at, :] for at in places]
        for at, old, v in zip(places, olds, values):
            flat[at, :] = old + v

    def one_rest(b, carry):
        values = [
            rest(one, pl.ds(pl.multiple_of(64 * b + 8 * k, 8), 8), 16 * k, 2, FB - 1, FF - (FB - 1) * LANES)
            for k in range(8)
        ]
        add_all([pl.ds(641 * b + 80 * k + FB - 1, 8, stride=10) for k in range(8)], values)
        return carry

    lax.fori_loop(0, last // 64, one_rest, 0)
    lane1 = iota((1, LANES), 1)
    v = jnp.where(lane1 < FF - (FB - 1) * LANES, one[FB - 1, last : last + 1, :], 0.0)
    add_all([slice(row_last + FB - 1, row_last + FB)], [v])

    def two_rest(b, carry):
        values = [
            rest(two, pl.ds(128 * b + 8 * k + shift, 8), 8 * k, 1, CB - 1, extra) for k in range(16)
        ]
        places = [pl.ds(base_two + 641 * b + 40 * k + CB - 1, 8, stride=5) for k in range(16)]
        add_all(places, values)
        return carry

    lax.fori_loop(0, full, two_rest, 0)
    add_all(
        [pl.ds(base_two + 641 * full + CB - 1, 8, stride=5)],
        [rest(two, end, 0, 1, CB - 1, extra, mask)],
    )


GELU_A = math.sqrt(2.0 / math.pi)
GELU_B = 0.044715
WIDE = 256


def dot(a, b, dims=((1,), (0,))):
    return lax.dot_general(a, b, (dims, ((), ())), preferred_element_type=F32)


def mlp_kernel(
    blocks, height_ref, conv_ref, g_ref, x_ref, w1, w2, small,
    out_ref, gconv_ref, rows_ref, cols_ref, corn_ref, shards_ref, extra_ref,
    one, two, g_scr, conv_t, act, gh, flat,
):
    step = pl.program_id(0)
    cells, rows, _ = x_ref.shape
    m = cells * rows
    height = height_ref[0]

    @pl.when(step == 0)
    def _():
        one[...] = jnp.zeros_like(one)
        two[...] = jnp.zeros_like(two)
        g_scr[...] = jnp.zeros_like(g_scr)

    live = (iota((1, rows, 1), 1) < height).astype(F32)
    g_scr[:, :C] = (g_ref[...].astype(F32) * live).reshape(m, C).astype(BF16)
    rows_one = conv_t.shape[0]

    def hidden(start, wide, tail):
        lanes = pl.ds(start, wide)
        h = dot(conv_ref[...].reshape(m, CP), w1[:, lanes]) + small[0:1, lanes]
        ga = dot(g_scr[...], w2[lanes, :], ((1,), (1,)))
        h2 = h * h
        t = jnp.tanh(h * (GELU_A + (GELU_A * GELU_B) * h2))
        cdf = 0.5 * t + 0.5
        value = (h * cdf).astype(BF16)
        slope = cdf + h * (0.5 - 0.5 * (t * t)) * (GELU_A + (3 * GELU_A * GELU_B) * h2)
        if tail:
            ones = iota((m, wide), 1) == FF - (FB - 1) * LANES
            value = jnp.where(ones, jnp.ones_like(value), value)
        act[:, lanes] = value
        gh[:, lanes] = (ga * slope).astype(BF16)

    def turn(i, count):
        part = conv_ref[:, :, pl.ds(i * LANES, LANES)].reshape(m, LANES)
        conv_t[pl.ds(i * LANES, count), :] = part.T[:count]

    def first(f, carry):
        turn(pl.multiple_of(f, 1), LANES)
        hidden(pl.multiple_of(f * WIDE, WIDE), WIDE, False)
        return carry

    lax.fori_loop(0, FP // WIDE, first, 0)
    assert FP // WIDE == CB - 1
    turn(CB - 1, rows_one - (CB - 1) * LANES)
    hidden(FP // WIDE * WIDE, FP % WIDE, True)

    for n in range(CP // WIDE):
        lanes = slice(n * WIDE, (n + 1) * WIDE)
        end = min((n + 1) * WIDE, C)
        part = slice(n * WIDE, end)
        branch = dot(act[...], w2[:, lanes])[:, : end - n * WIDE]
        v = x_ref[:, :, part].astype(F32).reshape(m, -1) + branch + small[1:2, part]
        out_ref[:, :, part] = (v.reshape(cells, rows, -1) * live).astype(BF16)
        gc = dot(gh[...], w1[lanes, :], ((1,), (1,)))
        gconv_ref[:, :, lanes] = gc.reshape(cells, rows, WIDE)

    def weights(start, wide):
        lanes = pl.ds(start, wide)
        r1 = dot(conv_t[...], gh[:, lanes])
        r2 = dot(act[:, lanes], g_scr[...], ((0,), (0,)))
        for i in range(wide // LANES):
            one[start // LANES + i] += r1[:, i * LANES : (i + 1) * LANES]
        for q in range(CB):
            two[q, pl.ds(start + 8, wide), :] += r2[:, q * LANES : (q + 1) * LANES]

    def third(f, carry):
        weights(pl.multiple_of(f * WIDE, WIDE), WIDE)
        return carry

    lax.fori_loop(0, FP // WIDE, third, 0)
    weights(FP // WIDE * WIDE, FP % WIDE)

    onehot = (iota((1, rows, 1), 1) == height - 1).astype(F32)
    block = gconv_ref[...]
    edges = (block[:, 0, :].astype(BF16), jnp.sum(block * onehot, 1).astype(BF16))
    for r in range(2):
        rows_ref[0, r] = edges[r]
    for side, at, first in ((0, 0, 0), (1, blocks - 1, cells - REACH)):

        @pl.when(step == at)
        def _(side=side, first=first):
            for i in range(REACH):
                cols_ref[side, i] = gconv_ref[first + i].astype(BF16)
            for r in range(2):
                corn_ref[r, side] = edges[r][first : first + REACH]

    @pl.when(step == blocks - 1)
    def _():
        extra_ref[...] = jnp.zeros_like(extra_ref)
        for q in range(FB):
            extra_ref[0 : NOISE + 1, q * LANES : (q + 1) * LANES] = one[q, C : C + NOISE + 1, :]
        for q in range(CB):
            lanes = slice(q * LANES, (q + 1) * LANES)
            extra_ref[NOISE + 1 : NOISE + 2, lanes] = two[q, FF + 8 : FF + 9, :]
        pack_weights(one, two, flat)
        bits = len(shards_ref.shape) - 2
        shard_rows = shards_ref.shape[-2]

        def store(d, carry):
            index = tuple((d >> (bits - 1 - i)) & 1 for i in range(bits))
            shards_ref[index] = flat[pl.ds(d * shard_rows, shard_rows), :]
            return carry

        lax.fori_loop(0, 1 << bits, store, 0)


def mlp(height, conv, g, x, w1, w2, small, shards, blocks):
    width, rows, _ = x.shape
    cells = width // blocks
    m = cells * rows
    sd = jax.ShapeDtypeStruct
    block = lambda c: pl.BlockSpec((cells, rows, c), lambda i: (i, 0, 0))
    rows_one = -(-(C + NOISE + 1) // 16) * 16
    flops = 12 * width * rows * C * FF
    return pl.pallas_call(
        partial(mlp_kernel, blocks),
        name="mlp",
        grid=(blocks,),
        out_shape=(
            sd((width, rows, C), BF16),
            sd((width, rows, CP), F32),
            sd((blocks, 2, cells, CP), BF16),
            sd((2, REACH, rows, CP), BF16),
            sd((2, 2, REACH, CP), BF16),
            sd(shards, F32),
            sd((16, FP), F32),
        ),
        in_specs=[
            pl.BlockSpec(memory_space=pltpu.SMEM),
            block(CP),
            block(C),
            block(C),
            vmem_spec(),
            vmem_spec(),
            vmem_spec(),
        ],
        out_specs=(
            block(C),
            block(CP),
            pl.BlockSpec((1, 2, cells, CP), lambda i: (i, 0, 0, 0)),
            vmem_spec(),
            vmem_spec(),
            vmem_spec(),
            vmem_spec(),
        ),
        scratch_shapes=[
            pltpu.VMEM((FB, rows_one, LANES), F32),
            pltpu.VMEM((CB, FP + 16, LANES), F32),
            pltpu.VMEM((m, CP), BF16),
            pltpu.VMEM((rows_one, m), BF16),
            pltpu.VMEM((m, FP), BF16),
            pltpu.VMEM((m, FP), BF16),
            pltpu.VMEM((math.prod(shards[:-1]), LANES), F32),
        ],
        compiler_params=params(dimension_semantics=("arbitrary",)),
        cost_estimate=pl.CostEstimate(flops=flops, bytes_accessed=50_000_000, transcendentals=0),
    )(height, conv, g, x, w1, w2, small)


def add_vector(tail, offset, value):
    row, shift = divmod(offset - TAIL_ROW * LANES, LANES)
    blocks = value.shape[0]
    lane = iota((blocks + 1, LANES), 1)
    zero = jnp.zeros((1, LANES), F32)
    here = pltpu.roll(jnp.concatenate([value, zero], 0), shift, 1) if shift else jnp.concatenate([value, zero], 0)
    back = jnp.concatenate([zero, here[:blocks]], 0)
    at = slice(row, row + blocks + 1)
    tail[at, :] = tail[at, :] + jnp.where(lane >= shift, here, back if shift else here)


def as_blocks(value, length):
    blocks = -(-length // LANES)
    v = jnp.concatenate([value[:, q * LANES : (q + 1) * LANES] for q in range(blocks)], 0)
    index = iota((blocks, LANES), 0) * LANES + iota((blocks, LANES), 1)
    return jnp.where(index < length, v, 0.0)


class Scatter:
    def __init__(self, mesh, shards, buf, recvs, send, recv):
        self.bits = bit_list(mesh)
        self.n = len(self.bits)
        self.orders = scatter_orders(mesh)
        self.first = self.orders[0][0]
        assert all(order[0] == self.first for order in self.orders)
        self.mine = my_bits(self.bits)
        self.shards, self.buf, self.recvs = shards, buf, recvs
        self.send, self.recv = send, recv
        rows = shards.shape[-2]
        one, two = (int(rows * f) // 8 * 8 for f in (0.36, 0.71))
        self.spans = [(0, one), (one, two - one), (two, rows - two)]

    def copy(self, colour, k):
        order, mine, n = self.orders[colour], self.mine, self.n
        done, now = order[:k], order[k]
        at = (pl.ds(*self.spans[colour]),)
        index = tuple(
            1 - mine[i] if i == now else mine[i] if i in done else slice(None) for i in range(n)
        )
        if k == 0:
            src = self.shards.at[index + at]
        else:
            src = self.buf.at[tuple(v for i, v in enumerate(index) if i != self.first) + at]
        return pltpu.make_async_remote_copy(
            src_ref=src,
            dst_ref=self.recvs[k].at[(slice(None),) * (n - 1 - k) + at],
            send_sem=self.send.at[colour, k],
            recv_sem=self.recv.at[colour, k],
            device_id=partner(*self.bits[now]),
            device_id_type=MESH,
        )

    def load(self, sem):
        index = tuple(self.mine[i] if i == self.first else slice(None) for i in range(self.n))
        return pltpu.make_async_copy(self.shards.at[index], self.buf, sem)

    def advance(self, colour, k):
        self.copy(colour, k).wait()
        order, n = self.orders[colour], self.n
        free = [i for i in range(n) if i not in order[: k + 1]]
        at = (pl.ds(*self.spans[colour]),)

        def add(d, carry):
            sub = tuple((d >> (len(free) - 1 - i)) & 1 for i in range(len(free)))
            index = tuple(
                sub[free.index(i)] if i in free else self.mine[i]
                for i in range(n)
                if i != self.first
            )
            self.buf[index + at] = self.buf[index + at] + self.recvs[k][sub + at]
            return carry

        lax.fori_loop(0, 1 << len(free), add, 0)
        if k + 1 < n:
            self.copy(colour, k + 1).start()

    def result(self):
        return self.buf[tuple(v for i, v in enumerate(self.mine) if i != self.first)]


def scatter_plan(n):
    if n == 5:
        return {8: [(0, 1), (1, 1), (2, 1)], 13: [(0, 2), (1, 2)], 15: [(2, 2)], 17: [(0, 3), (1, 3), (2, 3)]}
    return {}


def stencil_bwd_kernel(
    mesh, chunks, cells, height_ref, mix_ref, gconv_ref,
    cols, edge, corners, table, trowh, wd, extra, w1, shards,
    tail_ref, part_ref, gm_ref,
    g_scr, m_scr, k_scr, t_scr, e_scr, colh, rowh, cornh, buf, *rest,
):
    n = len(bit_list(mesh))
    recvs, (send, recv, hsend, hrecv, load_sem, out_sem) = rest[:n], rest[n:]
    scatter = Scatter(mesh, shards, buf, recvs, send, recv)
    step = pl.program_id(0)
    rows = mix_ref.shape[1]
    width = chunks * cells
    height = height_ref[0]
    plan = scatter_plan(n)

    @pl.when(step == 0)
    def _():
        scatter.load(load_sem).start()
        greet(scatter.bits, True)
        start_halo(halo_copies(cols, edge, corners, colh, rowh, cornh, hsend, hrecv))
        for colour in range(3):
            scatter.copy(colour, 0).start()
        hrow = iota((rows, 16), 0)
        for t in range(TAPS):
            l = t // 5
            own = table[t * rows : (t + 1) * rows, :]
            if l == 0:
                own = jnp.concatenate([own[1:], own[:1]], 0)
                own = jnp.where(hrow == height - 1, trowh[1, t : t + 1, :], own)
            if l == 2:
                own = jnp.concatenate([trowh[0, t : t + 1, :], own[: rows - 1]], 0)
            t_scr[t * rows : (t + 1) * rows, :] = own
        k_scr[...] = jnp.dot(
            t_scr[...], wd[...], preferred_element_type=F32, precision=HIGHEST
        ).reshape(k_scr.shape)
        e_scr[...] = jnp.zeros_like(e_scr)

    @pl.when(step < chunks)
    def _():
        def cell(j, carry):
            v = gconv_ref[j]
            mixed = mix_ref[j].astype(F32)
            at = (step * cells + j + REACH) * SLOTS
            for q in range(CB):
                lanes = slice(q * LANES, (q + 1) * LANES)
                g_scr[q, pl.ds(at + 1, rows), :] = v[:, lanes]
                m_scr[q, step * cells + j] = mixed[:, lanes]
            return carry

        lax.fori_loop(0, cells, cell, 0, unroll=2)

    @pl.when(step == chunks)
    def _():
        scatter.load(load_sem).wait()
        for colour in range(3):
            scatter.advance(colour, 0)
        wait_halo(halo_copies(cols, edge, corners, colh, rowh, cornh, hsend, hrecv))
        lat, _, nlat, *_ = neighbours()
        keep = ((lat > 0).astype(F32), (lat < nlat - 1).astype(F32))

        def put(column, top, low, fresh=None):
            at = column * SLOTS
            here = iota((rows, LANES), 0) == height
            for q in range(CB):
                lanes = slice(q * LANES, (q + 1) * LANES)
                body = pl.ds(at + 1, rows)
                old = g_scr[q, body, :] if fresh is None else fresh[:, lanes]
                g_scr[q, body, :] = jnp.where(here, low[:, lanes], old)
                g_scr[q, pl.ds(at, 1), :] = top[:, lanes]
                g_scr[q, pl.ds(at + rows + 1, 1), :] = low[:, lanes]

        def beside(ref):
            return [jnp.where(keep[r] > 0, ref(r).astype(F32), 0.0) for r in range(2)]

        for side in range(2):
            top, low = beside(lambda r: cornh[r, side])
            for i in range(REACH):
                column = i if side == 0 else width + REACH + i
                put(column, top[i : i + 1], low[i : i + 1], colh[side, i].astype(F32))

        def strip(c, carry):
            tops, lows = beside(lambda r: rowh[c, r])
            for i in range(cells):
                put(c * cells + i + REACH, tops[i : i + 1], lows[i : i + 1])
            return carry

        lax.fori_loop(0, chunks, strip, 0)
        for q in range(CB):
            lanes = slice(q * LANES, (q + 1) * LANES)
            for hb in range(rows // 8):
                at = slice(8 * hb, 8 * hb + 8)

                def cell(i, carry):
                    j = i * REUSE
                    mixed = [m_scr[q, j + u, at, :] for u in range(REUSE)]
                    total = [None] * REUSE
                    for l in range(3):
                        near = [
                            g_scr[q, pl.ds((j + u) * SLOTS + 8 * hb + 2 - l, 8), :]
                            for u in range(REUSE + 2 * REACH)
                        ]
                        for w in range(5):
                            t = 5 * l + w
                            tap = k_scr[t, at, lanes]
                            views = near[2 * REACH - w : 2 * REACH - w + REUSE]
                            terms = [tap * v for v in views]
                            total = [a if b is None else a + b for a, b in zip(terms, total)]
                            sums = [m * v for m, v in zip(mixed, views)]
                            while len(sums) > 1:
                                sums = [
                                    sums[k] + sums[k + 1] if k + 1 < len(sums) else sums[k]
                                    for k in range(0, len(sums), 2)
                                ]
                            e_scr[t, at, lanes] = e_scr[t, at, lanes] + sums[0]
                    for u in range(REUSE):
                        m_scr[q, j + u, at, :] = total[u]
                    return carry

                lax.fori_loop(0, width // REUSE, cell, 0)
                for colour, k in plan.get(q * (rows // 8) + hb, []):
                    scatter.advance(colour, k)
            pltpu.make_async_copy(m_scr.at[q], gm_ref.at[q], out_sem.at[q]).start()

        tail_ref[...] = jnp.zeros_like(tail_ref)
        add_vector(tail_ref, OFF_B1, as_blocks(extra[NOISE : NOISE + 1, :], FF))
        add_vector(tail_ref, OFF_B2, as_blocks(extra[NOISE + 1 : NOISE + 2, :], C))
        disco = lax.dot_general(
            t_scr[...], e_scr[...].reshape(TAPS * rows, CP), (((0,), (0,)), ((), ())),
            preferred_element_type=F32, precision=HIGHEST,
        )
        for k in range(K):
            add_vector(tail_ref, OFF_DISCO + k * C, as_blocks(disco[k : k + 1, :], C))
        ng = extra[0:NOISE, :]
        hi = ng.astype(BF16)
        mid = (ng - hi.astype(F32)).astype(BF16)
        lo = (ng - hi.astype(F32) - mid.astype(F32)).astype(BF16)
        parts = [dot(p, w1[...], ((1,), (1,))) for p in (hi, mid, lo)]
        gn = parts[0] + parts[1] + parts[2]
        for k in range(NOISE):
            add_vector(tail_ref, OFF_NOISE + k * C, as_blocks(gn[k : k + 1, :], C))
        taken = {e for events in plan.values() for e in events}
        for k in range(1, n):
            for colour in range(3):
                if (colour, k) not in taken:
                    scatter.advance(colour, k)
        part_ref[...] = scatter.result()
        for q in range(CB):
            pltpu.make_async_copy(m_scr.at[q], gm_ref.at[q], out_sem.at[q]).wait()


def stencil_bwd(
    mesh, height, mixed, gconv, cols, edge, corners, table, trowh, wd, extra, w1, shards,
    tail_rows, chunks,
):
    width, rows, _ = mixed.shape
    cells = width // chunks
    shard_rows = shards.shape[-2]
    n = len(bit_list(mesh))
    first = lambda i: jnp.where(i < chunks, i, chunks - 1)
    sd = jax.ShapeDtypeStruct
    by_first = lambda c: pl.BlockSpec((cells, rows, c), lambda i: (first(i), 0, 0))
    return pl.pallas_call(
        partial(stencil_bwd_kernel, mesh, chunks, cells),
        name="stencil_bwd",
        grid=(chunks + 1,),
        out_shape=(
            sd((tail_rows, LANES), F32),
            sd((shard_rows, LANES), F32),
            sd((CB, width, rows, LANES), F32),
        ),
        in_specs=[pl.BlockSpec(memory_space=pltpu.SMEM), by_first(CP), by_first(CP)]
        + [vmem_spec()] * 8
        + [any_spec()],
        out_specs=(vmem_spec(), vmem_spec(), any_spec()),
        scratch_shapes=[
            pltpu.VMEM((CB, (width + 2 * REACH) * SLOTS, LANES), F32),
            pltpu.VMEM((CB, width, rows, LANES), F32),
            pltpu.VMEM((TAPS, rows, CP), F32),
            pltpu.VMEM((TAPS * rows, 16), F32),
            pltpu.VMEM((TAPS, rows, CP), F32),
            pltpu.VMEM(cols.shape, BF16),
            pltpu.VMEM(edge.shape, BF16),
            pltpu.VMEM(corners.shape, BF16),
            pltpu.VMEM((2,) * (n - 1) + (shard_rows, LANES), F32),
        ]
        + [pltpu.VMEM((2,) * (n - 1 - k) + (shard_rows, LANES), F32) for k in range(n)]
        + [
            pltpu.SemaphoreType.DMA((3, n)),
            pltpu.SemaphoreType.DMA((3, n)),
            pltpu.SemaphoreType.DMA((8,)),
            pltpu.SemaphoreType.DMA((8,)),
            pltpu.SemaphoreType.DMA,
            pltpu.SemaphoreType.DMA((CB,)),
        ],
        compiler_params=params(
            dimension_semantics=("arbitrary",), collective_id=1, has_side_effects=True
        ),
    )(height, mixed, gconv, cols, edge, corners, table, trowh, wd, extra, w1, shards)


def norm_bwd_kernel(
    height_ref, gm_ref, x_ref, mean_ref, inv_ref, g_ref, gain, tail_in, out_ref, tail_ref, gg_scr
):
    step = pl.program_id(0)
    cells, rows, _ = x_ref.shape
    gvec = gain[2:3, :C]
    live = iota((rows, C), 0) < height_ref[0]

    @pl.when(step == 0)
    def _():
        gg_scr[...] = jnp.zeros_like(gg_scr)

    def cell(j, total):
        inv = inv_ref[j][:, :1]
        normed = (x_ref[j].astype(F32) - mean_ref[j][:, :1]) * inv
        gm = jnp.concatenate([gm_ref[q, j] for q in range(CB)], 1)[:, :C]
        gm = jnp.where(live, gm, 0.0)
        total = total + gm * normed
        v = gm * gvec
        mean = jnp.mean(v, -1, keepdims=True)
        mean_n = jnp.mean(v * normed, -1, keepdims=True)
        up = jnp.where(live, g_ref[j].astype(F32), 0.0)
        out_ref[j] = inv * (v - mean - normed * mean_n) + up
        return total

    gg_scr[:, :C] = lax.fori_loop(0, cells, cell, gg_scr[:, :C], unroll=2)

    @pl.when(step == pl.num_programs(0) - 1)
    def _():
        tail_ref[...] = tail_in[...]
        add_vector(tail_ref, OFF_GAIN, as_blocks(jnp.sum(gg_scr[...], 0, keepdims=True), C))


def norm_bwd(height, gm, x, mean, inv, g, small, tail, chunks):
    width, rows, _ = x.shape
    cells = width // chunks
    sd = jax.ShapeDtypeStruct
    block = lambda c: pl.BlockSpec((cells, rows, c), lambda i: (i, 0, 0))
    return pl.pallas_call(
        norm_bwd_kernel,
        name="norm_bwd",
        grid=(chunks,),
        out_shape=(sd((width, rows, C), F32), sd(tail.shape, F32)),
        in_specs=[
            pl.BlockSpec(memory_space=pltpu.SMEM),
            pl.BlockSpec((CB, cells, rows, LANES), lambda i: (0, i, 0, 0)),
            block(C),
            block(LANES),
            block(LANES),
            block(C),
            vmem_spec(),
            vmem_spec(),
        ],
        out_specs=(block(C), vmem_spec()),
        scratch_shapes=[pltpu.VMEM((rows, CP), F32)],
        compiler_params=params(dimension_semantics=("arbitrary",)),
    )(height, gm, x, mean, inv, g, small, tail)


def tail_kernel(mesh, part_ref, tail_ref, grad_ref, scale_ref, got, msg, full, place, send, recv):
    nlat, nlon = mesh.shape["lat"], mesh.shape["lon"]
    n = nlat * nlon
    lat, lon = lax.axis_index("lat"), lax.axis_index("lon")
    me = lat * nlon + lon
    piece = tail_ref.shape[1]
    shard_rows = part_ref.shape[0]
    barrier = pltpu.get_barrier_semaphore()

    def others(body):
        def step(i, carry):
            body(lax.rem(me + i, n))
            return carry

        lax.fori_loop(1, n, step, 0)

    def hello(d):
        pl.semaphore_signal(
            barrier, inc=1, device_id=(d // nlon, lax.rem(d, nlon)), device_id_type=MESH
        )

    others(hello)
    pl.semaphore_wait(barrier, n - 1)

    def scatter_piece(d):
        pltpu.make_async_remote_copy(
            src_ref=tail_ref.at[d],
            dst_ref=got.at[me],
            send_sem=send.at[0],
            recv_sem=recv.at[0],
            device_id=(d // nlon, lax.rem(d, nlon)),
            device_id_type=MESH,
        ).start()

    def wait_all(buffer, k):
        pltpu.make_async_remote_copy(
            src_ref=buffer.at[pl.ds(0, n - 1)],
            dst_ref=buffer.at[pl.ds(0, n - 1)],
            send_sem=send.at[k],
            recv_sem=recv.at[k],
            device_id=(lat, lon),
            device_id_type=MESH,
        ).wait()

    others(scatter_piece)
    got[me] = tail_ref[me]
    square = jnp.sum(part_ref[...] * part_ref[...])
    wait_all(got, 0)

    total = lax.fori_loop(
        1, n, lambda i, acc: acc + got[lax.rem(i, n)], got[0]
    )
    square = square + jnp.sum(total * total)
    msg[0:piece, :] = total
    msg[piece : piece + 1, :] = jnp.broadcast_to(square, (1, LANES))

    def share(d):
        pltpu.make_async_remote_copy(
            src_ref=msg,
            dst_ref=full.at[me],
            send_sem=send.at[1],
            recv_sem=recv.at[1],
            device_id=(d // nlon, lax.rem(d, nlon)),
            device_id_type=MESH,
        ).start()

    others(share)
    full[me] = msg[...]
    place[...] = jnp.zeros_like(place)
    wait_all(full, 1)

    def take(d, acc):
        place[pl.ds(shard_rows + d * piece, piece), :] = full[d, 0:piece, :]
        return acc + full[d, piece : piece + 1, :]

    squares = lax.fori_loop(0, n, take, jnp.zeros((1, LANES), F32))
    start = jnp.clip(me * shard_rows - TAIL_ROW + shard_rows, 0, shard_rows + n * piece)
    grad_ref[...] = part_ref[...] + place[pl.ds(start, shard_rows), :]
    scale_ref[...] = jnp.broadcast_to(jnp.sqrt(squares), scale_ref.shape)


def finish(mesh, part, tail):
    n, piece, _ = tail.shape
    shard_rows = part.shape[0]
    sd = jax.ShapeDtypeStruct
    return pl.pallas_call(
        partial(tail_kernel, mesh),
        name="small_gradients",
        out_shape=(sd(part.shape, F32), sd((8, LANES), F32)),
        in_specs=[vmem_spec()] * 2,
        out_specs=(vmem_spec(),) * 2,
        scratch_shapes=[
            pltpu.VMEM((n, piece, LANES), F32),
            pltpu.VMEM((piece + 1, LANES), F32),
            pltpu.VMEM((n, piece + 1, LANES), F32),
            pltpu.VMEM((2 * shard_rows + n * piece + 8, LANES), F32),
            pltpu.SemaphoreType.DMA((2,)),
            pltpu.SemaphoreType.DMA((2,)),
        ],
        compiler_params=params(collective_id=3, has_side_effects=True),
    )(part, tail)


def stencil_table(support_vals, support_lon):
    rows = support_vals.shape[0]
    vals = support_vals.reshape(rows, S // 3, 3, K)
    offsets = jnp.arange(-REACH, REACH + 1)
    hit = support_lon.reshape(rows, S // 3, 3)[:, :, :, None] == offsets
    picked = jnp.where(hit[:, :, :, :, None], vals[:, :, :, None, :], 0.0)
    return jnp.transpose(jnp.sum(picked, 1), (1, 2, 0, 3))


def flat_table(table):
    t = table.reshape(-1, K)
    return jnp.pad(t, ((0, 0), (0, 16 - K)))


def local(
    mesh, block_in, noise, cotangent, band_heights, support_lon, support_vals,
    master, moment_one, moment_two, average, step_count,
):
    rows, width, _ = block_in.shape
    devices = mesh.shape["lat"] * mesh.shape["lon"]
    shard = master.shape[0]
    shard_rows = shard // LANES
    assert shard_rows * LANES == shard
    flat_rows = shard_rows * devices
    chunks = 6
    cells = width // chunks
    height = lax.dynamic_slice_in_dim(band_heights, lax.axis_index("lat"), 1, 0)
    x = jnp.transpose(block_in, (1, 0, 2))
    g = jnp.transpose(cotangent, (1, 0, 2))

    table = flat_table(stencil_table(support_vals, support_lon))
    planes = table.reshape(TAPS, rows, 16)
    trow = jnp.stack([planes[:, 0], lax.dynamic_index_in_dim(planes, height[0] - 1, 1, keepdims=False)])
    trow = jnp.pad(trow, ((0, 0), (0, 1), (0, 0)))
    share = master.astype(BF16).reshape(shard_rows, LANES)
    edge = jnp.stack([x[:, 0], lax.dynamic_index_in_dim(x, height[0] - 1, 1, keepdims=False)], 1)
    cols = jnp.stack([x[:REACH], x[width - REACH :]])
    corners = jnp.stack([edge[:REACH], edge[width - REACH :]], 0)
    corners = jnp.transpose(corners, (2, 0, 1, 3))
    edge = jnp.transpose(edge.reshape(chunks, cells, 2, C), (0, 2, 1, 3))
    aug = jnp.concatenate(
        [
            jnp.zeros((width, rows, 1), BF16),
            jnp.transpose(noise, (2, 1, 0)),
            jnp.ones((width, rows, 1), BF16),
            jnp.zeros((width, rows, LANES - NOISE - 2), BF16),
        ],
        2,
    )
    conv, mean, inv, mixed, w1, w2, wd, small, trowh = stencil_fwd(
        mesh, height, x, share, cols, edge, corners, trow, table, aug, chunks
    )
    shards = (2,) * len(bit_list(mesh)) + (shard_rows, LANES)
    out, gconv, grow, gcol, gcorn, packed, extra = mlp(
        height, conv, g, x, w1, w2, small, shards, chunks
    )
    piece = -(-(flat_rows - TAIL_ROW) // devices)
    tail, part, gm = stencil_bwd(
        mesh, height, mixed, gconv, gcol, grow, gcorn, table, trowh, wd, extra, w1, packed,
        devices * piece, chunks,
    )
    grad_in, tail = norm_bwd(height, gm, x, mean, inv, g, small, tail, chunks)
    grad, norm = finish(mesh, part, tail.reshape(devices, piece, LANES))
    grad_part = grad.reshape(shard)
    grad_norm = norm[0, :1]
    factor = 0.01 / jnp.maximum(grad_norm, 0.01)
    clipped = grad_part * factor
    new_one = 0.9 * moment_one + 0.1 * clipped
    new_two = 0.999 * moment_two + 0.001 * clipped * clipped
    step_float = step_count[0].astype(F32)
    fix_one = 1.0 - jnp.power(jnp.float32(0.9), step_float)
    fix_two = 1.0 - jnp.power(jnp.float32(0.999), step_float)
    update = new_one / fix_one / (jnp.sqrt(new_two / fix_two) + 1e-08) + 0.1 * master
    new_master = master - 0.02 * update
    new_avg = 0.9 * average + 0.1 * new_master
    return (
        jnp.transpose(out, (1, 0, 2)),
        jnp.transpose(grad_in, (1, 0, 2)),
        grad_part,
        grad_norm,
        new_master,
        new_one,
        new_two,
        new_avg,
        new_master.astype(BF16),
    )


def solution(mesh):
    flat = P(("lat", "lon"))
    field = P("lat", "lon", None)
    return jax.shard_map(
        partial(local, mesh),
        mesh=mesh,
        in_specs=(
            field, P(None, "lat", "lon"), field, P(), P("lat", None), P("lat", None, None),
            flat, flat, flat, flat, P(),
        ),
        out_specs=(field, field, flat, P(), flat, flat, flat, flat, flat),
        check_vma=False,
    )
```

```python
from functools import partial
import math

import jax
import jax.numpy as jnp
from jax import lax
from jax.experimental import pallas as pl
from jax.experimental.pallas import tpu as pltpu
from jax.sharding import PartitionSpec as P

C = 641
FF = 1282
NOISE = 8
K = 9
S = 12
REACH = 2
LANES = 128
CB = 6
CP = CB * LANES
FB = 11
FP = FB * LANES
TAPS = 15
MESH = pl.DeviceIdType.MESH
HIGHEST = lax.Precision.HIGHEST
F32 = jnp.float32
BF16 = jnp.bfloat16
VMEM_LIMIT = 60 * 1024 * 1024
SLOTS = 28
REUSE = 10
ROW_TWO = (C * FF) // LANES
LANE_TWO = (C * FF) % LANES
TAIL_ROW = (2 * C * FF) // LANES
OFF_B1 = 2 * C * FF
OFF_B2 = OFF_B1 + FF
OFF_GAIN = OFF_B2 + C
OFF_DISCO = OFF_GAIN + C
OFF_NOISE = OFF_DISCO + K * C
END_FLAT = OFF_NOISE + NOISE * C


def params(**kw):
    return pltpu.CompilerParams(vmem_limit_bytes=VMEM_LIMIT, **kw)


def any_spec():
    return pl.BlockSpec(memory_space=pl.ANY)


def vmem_spec():
    return pl.BlockSpec(memory_space=pltpu.VMEM)


def iota(shape, dim):
    return lax.broadcasted_iota(jnp.int32, shape, dim)


def bit_list(mesh):
    bits = []
    for axis in ("lat", "lon"):
        count = int(math.log2(mesh.shape[axis]))
        assert 1 << count == mesh.shape[axis]
        bits += [(axis, b) for b in reversed(range(count))]
    return bits


def my_bits(bits):
    ids = {"lat": lax.axis_index("lat"), "lon": lax.axis_index("lon")}
    return [(ids[a] >> b) & 1 for a, b in bits]


def partner(axis, bit):
    lat, lon = lax.axis_index("lat"), lax.axis_index("lon")
    if axis == "lat":
        return (lat ^ (1 << bit), lon)
    return (lat, lon ^ (1 << bit))


def stage_orders(mesh):
    bits = bit_list(mesh)
    n = len(bits)
    if (mesh.shape["lat"], mesh.shape["lon"]) == (8, 4):
        return [[0, 1, 2, 3, 4], [0, 1, 3, 2, 4]]
    order = list(range(n))
    return [order, order]


def scatter_orders(mesh):
    n = len(bit_list(mesh))
    if (mesh.shape["lat"], mesh.shape["lon"]) == (8, 4):
        return [[4, 3, 2, 1, 0], [4, 2, 3, 1, 0], [4, 1, 0, 3, 2]]
    return [list(reversed(range(n)))] * 3


def rotl_rows(v, first, unit):
    index = (iota((8, LANES), 1) + first + unit * iota((8, LANES), 0)) % LANES
    return jnp.take_along_axis(v, index, axis=1)


def row_vector(flat_ref, offset, length):
    blocks = -(-length // LANES)
    row, shift = divmod(offset, LANES)
    near = flat_ref[row : row + blocks, :]
    if shift:
        far = flat_ref[row + 1 : row + 1 + blocks, :]
        lane = iota((blocks, LANES), 1)
        near = pltpu.roll(jnp.where(lane >= shift, near, far), LANES - shift, 1)
    index = iota((blocks, LANES), 0) * LANES + iota((blocks, LANES), 1)
    return jnp.where(index < length, near, 0.0)


def put_row(ref, row, value):
    for q in range(value.shape[0]):
        ref[row : row + 1, q * LANES : (q + 1) * LANES] = value[q : q + 1, :].astype(ref.dtype)


def unpack_weights(flat, w1, w2):
    lane = iota((8, LANES), 1)
    row = iota((8, LANES), 0)

    def rows_one(base, first):
        near = [flat[pl.ds(base + q, 8, stride=10), :] for q in range(FB + 1)]
        out = [
            rotl_rows(jnp.where(lane >= first + 2 * row, near[q], near[q + 1]), first, 2)
            for q in range(FB)
        ]
        out[-1] = jnp.where(lane < FF - (FB - 1) * LANES, out[-1], 0.0)
        return out

    def body_one(b, carry):
        for k in range(0, 8, 2):
            pair = [rows_one(641 * b + 80 * (k + h), 16 * (k + h)) for h in range(2)]
            at = pl.ds(pl.multiple_of(64 * b + 8 * k, 16), 16)
            for q in range(FB):
                v = jnp.concatenate([pair[0][q], pair[1][q]], 0)
                w1[at, q * LANES : (q + 1) * LANES] = v.astype(BF16)
        return carry

    last = C - 1
    lax.fori_loop(0, last // 64, body_one, 0)
    zero = jnp.zeros((8, LANES), F32)
    for q, v in enumerate(rows_one(641 * (last // 64), 0)):
        v = jnp.concatenate([jnp.where(row == 0, v, 0.0), zero], 0)
        w1[last : last + 16, q * LANES : (q + 1) * LANES] = v.astype(BF16)
    w1[last + 16 :, :] = jnp.zeros((CP - last - 16, FP), BF16)

    def rows_two(base, first):
        count = CB + 2 if first + 7 >= LANES else CB + 1
        near = [flat[pl.ds(base + q, 8, stride=5), :] for q in range(count)]
        out = []
        for q in range(CB):
            v = jnp.where(lane >= first + row, near[q], near[q + 1])
            if first + 7 >= LANES:
                v = jnp.where(lane < first + row - LANES, near[q + 2], v)
            out.append(rotl_rows(v, first, 1))
        out[-1] = jnp.where(lane < C - (CB - 1) * LANES, out[-1], 0.0)
        return out

    def body_two(b, carry):
        for k in range(0, 16, 2):
            pair = [
                rows_two(ROW_TWO + 641 * b + 40 * (k + h), LANE_TWO + 8 * (k + h))
                for h in range(2)
            ]
            at = pl.ds(pl.multiple_of(128 * b + 8 * k, 16), 16)
            for q in range(CB):
                v = jnp.concatenate([pair[0][q], pair[1][q]], 0)
                w2[at, q * LANES : (q + 1) * LANES] = v.astype(BF16)
        return carry

    full = FF // LANES
    lax.fori_loop(0, full, body_two, 0)
    for q, v in enumerate(rows_two(ROW_TWO + 641 * full, LANE_TWO)):
        v = jnp.concatenate([jnp.where(row < FF - full * LANES, v, 0.0), zero], 0)
        w2[full * LANES : full * LANES + 16, q * LANES : (q + 1) * LANES] = v.astype(BF16)
    w2[full * LANES + 16 :, :] = jnp.zeros((FP - full * LANES - 16, CP), BF16)


def unpack_small(flat, base, wn, wd, small, wnf):
    vector = lambda offset, length: row_vector(flat, offset - base * LANES, length)
    small[...] = jnp.zeros_like(small)
    put_row(small, 0, vector(OFF_B1, FF))
    put_row(small, 1, vector(OFF_B2, C))
    put_row(small, 2, vector(OFF_GAIN, C))
    wd[...] = jnp.zeros_like(wd)
    wnf[...] = jnp.zeros_like(wnf)
    for k in range(K):
        put_row(wd, k, vector(OFF_DISCO + k * C, C))
    for k in range(NOISE):
        put_row(wnf, 1 + k, vector(OFF_NOISE + k * C, C))
    wn[...] = wnf[...].astype(BF16)


def neighbours():
    lat, lon = lax.axis_index("lat"), lax.axis_index("lon")
    nlat, nlon = lax.axis_size("lat"), lax.axis_size("lon")
    return lat, lon, nlat, nlon, lax.rem(lon + 1, nlon), lax.rem(lon + nlon - 1, nlon)


def halo_copies(cols, rows, corners, colh, rowh, cornh, send, recv, trow=None, trowh=None):
    lat, lon, nlat, nlon, east, west = neighbours()
    out = []

    def add(src, dst, target, k, sends, gets):
        out.append(
            (
                sends,
                gets,
                pltpu.make_async_remote_copy(
                    src_ref=src,
                    dst_ref=dst,
                    send_sem=send.at[k],
                    recv_sem=recv.at[k],
                    device_id=target,
                    device_id_type=MESH,
                ),
            )
        )

    has_up, has_down = lat > 0, lat < nlat - 1
    up, down = lat - 1, lat + 1
    add(rows.at[:, 0], rowh.at[:, 1], (up, lon), 2, has_up, has_down)
    add(rows.at[:, 1], rowh.at[:, 0], (down, lon), 3, has_down, has_up)
    add(cols.at[0], colh.at[1], (lat, west), 0, None, None)
    add(cols.at[1], colh.at[0], (lat, east), 1, None, None)
    add(corners.at[0, 0], cornh.at[1, 1], (up, west), 4, has_up, has_down)
    add(corners.at[0, 1], cornh.at[1, 0], (up, east), 5, has_up, has_down)
    add(corners.at[1, 0], cornh.at[0, 1], (down, west), 6, has_down, has_up)
    add(corners.at[1, 1], cornh.at[0, 0], (down, east), 7, has_down, has_up)
    if trow is not None:
        add(trow.at[0], trowh.at[1], (up, lon), 8, has_up, has_down)
        add(trow.at[1], trowh.at[0], (down, lon), 9, has_down, has_up)
    return out


def start_halo(copies):
    for sends, _, copy in copies:
        if sends is None:
            copy.start()
        else:
            pl.when(sends)(copy.start)


def wait_halo(copies):
    for sends, gets, copy in copies:
        if sends is None:
            copy.wait()
        else:
            pl.when(sends)(copy.wait_send)
            pl.when(gets)(copy.wait_recv)


def for_others(mesh, body):
    nlat, nlon = mesh.shape["lat"], mesh.shape["lon"]
    lat, lon = lax.axis_index("lat"), lax.axis_index("lon")
    beside = [(lon + b) & (nlon - 1) for b in range(nlon)]
    for x in beside[1:]:
        body((lat, x), lat * nlon + x)

    def row(a, carry):
        y = (lat + a) & (nlat - 1)
        for x in beside:
            body((y, x), y * nlon + x)
        return carry

    lax.fori_loop(1, nlat, row, 0)


def greet_all(mesh):
    barrier = pltpu.get_barrier_semaphore()

    def hello(target, d):
        pl.semaphore_signal(barrier, inc=1, device_id=target, device_id_type=MESH)

    for_others(mesh, hello)
    pl.semaphore_wait(barrier, mesh.shape["lat"] * mesh.shape["lon"] - 1)


def greet(bits, halo):
    barrier = pltpu.get_barrier_semaphore()
    lat, lon, nlat, nlon, east, west = neighbours()

    def hello(target):
        pl.semaphore_signal(barrier, inc=1, device_id=target, device_id_type=MESH)

    count = 0
    for axis, bit in bits:
        hello(partner(axis, bit))
        count += 1
    if halo:
        for target in ((lat, east), (lat, west)):
            hello(target)
            count += 1
        for side, cond in ((lat - 1, lat > 0), (lat + 1, lat < nlat - 1)):

            @pl.when(cond)
            def _(side=side):
                for x in (lon, east, west):
                    hello((side, x))

    if halo:
        count = count + 3 * (lat > 0).astype(jnp.int32) + 3 * (lat < nlat - 1).astype(jnp.int32)
    pl.semaphore_wait(barrier, count)


class Gather:
    def __init__(self, mesh, share, buf, early, send, recv, bsend, brecv):
        self.bits = bit_list(mesh)
        self.n = len(self.bits)
        self.orders = stage_orders(mesh)
        self.mine = my_bits(self.bits)
        self.share, self.buf, self.early = share, buf, early
        self.send, self.recv, self.bsend, self.brecv = send, recv, bsend, brecv
        rows = share.shape[0]
        cut = (rows * 2 // 3 + 15) // 16 * 16
        self.spans = [(0, cut), (cut, rows - cut)]
        self.roots, self.start = early_shards(1 << self.n, rows)

    def own(self, sem):
        return pltpu.make_async_copy(self.share, self.buf.at[tuple(self.mine)], sem)

    def copy(self, colour, k):
        order = self.orders[colour]
        index = tuple(
            slice(None) if i in order[:k] else self.mine[i] for i in range(self.n)
        ) + (pl.ds(*self.spans[colour]),)
        return pltpu.make_async_remote_copy(
            src_ref=self.buf.at[index],
            dst_ref=self.buf.at[index],
            send_sem=self.send.at[colour, k],
            recv_sem=self.recv.at[colour, k],
            device_id=partner(*self.bits[order[k]]),
            device_id_type=MESH,
        )

    def advance(self, k):
        for colour in range(2):
            self.copy(colour, k).wait()
            if k + 1 < self.n:
                self.copy(colour, k + 1).start()

    def same(self, root, indices):
        cond = True
        for i in indices:
            cond = jnp.logical_and(cond, self.mine[i] == ((root >> (self.n - 1 - i)) & 1))
        return cond

    def early_own(self, sem):
        for r, root in enumerate(self.roots):

            @pl.when(self.same(root, range(self.n)))
            def _(r=r):
                rows = self.share.shape[0] - self.start
                copy = pltpu.make_async_copy(
                    self.share.at[pl.ds(self.start, rows)], self.early.at[r], sem
                )
                copy.start()
                copy.wait()

    def early_copies(self, k):
        order = self.orders[0]
        for r, root in enumerate(self.roots):
            sends = self.same(root, order[k:])
            now = order[k]
            other = self.mine[now] != ((root >> (self.n - 1 - now)) & 1)
            gets = jnp.logical_and(other, self.same(root, order[k + 1 :]))
            yield sends, gets, pltpu.make_async_remote_copy(
                src_ref=self.early.at[r],
                dst_ref=self.early.at[r],
                send_sem=self.bsend.at[r, k],
                recv_sem=self.brecv.at[r, k],
                device_id=partner(*self.bits[now]),
                device_id_type=MESH,
            )

    def early_start(self, k):
        for sends, _, copy in self.early_copies(k):
            pl.when(sends)(copy.start)

    def early_wait(self, k):
        for sends, gets, copy in self.early_copies(k):
            pl.when(sends)(copy.wait_send)
            pl.when(gets)(copy.wait_recv)


def early_shards(devices, shard_rows):
    roots = list(range(TAIL_ROW // shard_rows, (END_FLAT - 1) // LANES // shard_rows + 1))
    start = (TAIL_ROW - roots[0] * shard_rows) // 16 * 16 if len(roots) == 1 else 0
    return roots, start


def gather_plan(n):
    if n == 5:
        return {0: (0, -1), 1: (1, -1), 2: (2, 8), 3: (4, 14)}
    return {}


def norm_parts(x):
    mean = jnp.mean(x, -1, keepdims=True)
    center = x - mean
    var = jnp.mean(center * center, -1, keepdims=True)
    return center, lax.rsqrt(var + 1e-05)


def rounded(v):
    return v.astype(BF16).astype(F32)


def stencil_fwd_kernel(
    mesh, chunks, cells, height_ref, x_ref, share, cols, edge, corners, trow, table, aug,
    out_ref, mix_hbm, w1, w2, wd, small, trowh,
    m_scr, k_scr, nt_scr, mix_scr, wnf, wn, colh, rowh, cornh, trh, buf, early, flat, eflat,
    send, recv, bsend, brecv, hsend, hrecv, own_sem, mix_sem,
):
    gather = Gather(mesh, share, buf, early, send, recv, bsend, brecv)
    n = gather.n
    plan = gather_plan(n)
    step = pl.program_id(0)
    rows = x_ref.shape[1]
    width = chunks * cells
    height = height_ref[0]
    shard_rows = share.shape[0]
    halos = lambda: halo_copies(cols, edge, corners, colh, rowh, cornh, hsend, hrecv, trow, trh)
    mix_copy = lambda: pltpu.make_async_copy(mix_scr, mix_hbm, mix_sem)

    @pl.when(step == 0)
    def _():
        gather.own(own_sem).start()
        gather.early_own(mix_sem)
        gather.own(own_sem).wait()
        greet(gather.bits, True)
        gather.early_start(0)
        for colour in range(2):
            gather.copy(colour, 0).start()
        start_halo(halos())

    for k in range(n):

        @pl.when(step == min(k + 1, chunks))
        def _(k=k):
            gather.early_wait(k)
            if k + 1 < n:
                gather.early_start(k + 1)

    @pl.when(step < chunks)
    def _():
        def cell(j, carry):
            x = x_ref[j].astype(F32)
            mean = jnp.mean(x, -1, keepdims=True)
            center = x - mean
            inv = lax.rsqrt(jnp.mean(center * center, -1, keepdims=True) + 1e-05)
            normed = center * inv
            at = pl.ds((step * cells + j + REACH) * SLOTS + 1, rows)
            for g in range(CB):
                lo, hi = g * LANES, min((g + 1) * LANES, C)
                m_scr[g, at, : hi - lo] = normed[:, lo:hi]
            return carry

        lax.fori_loop(0, cells, cell, 0, unroll=10)

    @pl.when(step == chunks)
    def _():
        if 0 in plan:
            gather.advance(0)
        lat, _, nlat, *_ = neighbours()
        wait_halo(halos())
        keep = (lat > 0, lat < nlat - 1)
        for r in range(2):
            trowh[r] = jnp.where(keep[r], trh[r], 0.0)

        base = gather.roots[0] * shard_rows + gather.start
        count = shard_rows - gather.start
        eflat[...] = jnp.zeros_like(eflat)
        for r in range(len(gather.roots)):
            eflat[r * count : (r + 1) * count, :] = early[r].astype(F32)
        unpack_small(eflat, base, wn, wd, small, wnf)
        k_scr[...] = jnp.dot(
            table[...], wd[...], preferred_element_type=F32, precision=HIGHEST
        ).reshape(k_scr.shape)
        gvec = small[2:3, :C]

        def mix(v):
            center, inv = norm_parts(v.astype(F32))
            return rounded(center * inv * gvec)

        def beside(ref):
            return [jnp.where(keep[r], mix(ref(r)), 0.0) for r in range(2)]

        def put(column, top, low, fresh=None):
            at = column * SLOTS
            hrow = iota((rows, LANES), 0)
            for q in range(CB):
                lo, hi = q * LANES, min((q + 1) * LANES, C)
                body = pl.ds(at + 1, rows)
                wide = slice(0, hi - lo)
                if fresh is None:
                    v = rounded(m_scr[q, body, wide] * gvec[:, lo:hi])
                    v = jnp.where(hrow[:, wide] < height, v, 0.0)
                    mix_scr[column - REACH, :, lo:hi] = v.astype(BF16)
                else:
                    v = jnp.where(hrow[:, wide] < height, fresh[:, lo:hi], 0.0)
                m_scr[q, body, wide] = jnp.where(hrow[:, wide] == height, low[:, lo:hi], v)
                m_scr[q, pl.ds(at, 1), wide] = top[:, lo:hi]
                m_scr[q, pl.ds(at + rows + 1, 1), wide] = low[:, lo:hi]

        lanes = slice((CB - 1) * LANES, CB * LANES)
        mix_scr[:, :, lanes] = jnp.zeros((width, rows, LANES), BF16)
        for side in range(2):
            top, low = beside(lambda r: cornh[r, side])
            for i in range(REACH):
                column = i if side == 0 else width + REACH + i
                put(column, top[i : i + 1], low[i : i + 1], mix(colh[side, i]))

        def strip(c, carry):
            tops, lows = beside(lambda r: rowh[c, r])
            for i in range(cells):
                put(c * cells + i + REACH, tops[i : i + 1], lows[i : i + 1])
            return carry

        lax.fori_loop(0, chunks, strip, 0)
        mix_copy().start()

    for k, (at, loop) in plan.items():
        if k > 0 and loop < 0:

            @pl.when(step == chunks + at)
            def _(k=k):
                gather.advance(k)

    @pl.when(step >= chunks)
    def _():
        first = (step - chunks) * cells
        nt_scr[...] = jnp.dot(
            aug[...].reshape(cells * rows, LANES), wn[...], preferred_element_type=F32
        )
        lane = iota((8, LANES), 1)
        for g in range(CB):
            lanes = slice(g * LANES, (g + 1) * LANES)
            for hb in range(rows // 8):
                at = slice(8 * hb, 8 * hb + 8)

                def cell(i, carry):
                    j = i * REUSE
                    acc = [nt_scr[pl.ds((j + u) * rows + 8 * hb, 8), lanes] for u in range(REUSE)]
                    for l in range(3):
                        near = [
                            m_scr[g, pl.ds((first + j + u) * SLOTS + 8 * hb + l, 8), :]
                            for u in range(REUSE + 2 * REACH)
                        ]
                        for w in range(5):
                            tap = k_scr[5 * l + w, at, lanes]
                            acc = [a + tap * near[u + w] for u, a in enumerate(acc)]
                    for u in range(REUSE):
                        v = acc[u]
                        if g == CB - 1:
                            v = jnp.where(lane == 0, v, aug[j + u, at, :].astype(F32))
                        out_ref[j + u, at, lanes] = v.astype(BF16)
                    return carry

                lax.fori_loop(0, cells // REUSE, cell, 0)
                for k, (past, loop) in plan.items():
                    if loop == g * (rows // 8) + hb:

                        @pl.when(step == chunks + past)
                        def _(k=k):
                            gather.advance(k)

    @pl.when(step == 2 * chunks - 1)
    def _():
        for k in range(n):
            if k not in plan:
                gather.advance(k)
        total = 1 << n

        def widen(d, carry):
            index = tuple((d >> (n - 1 - i)) & 1 for i in range(n))
            flat[pl.ds(d * shard_rows, shard_rows), :] = buf[index].astype(F32)
            return carry

        lax.fori_loop(0, total, widen, 0)
        flat[total * shard_rows :, :] = jnp.zeros((flat.shape[0] - total * shard_rows, LANES), F32)
        unpack_weights(flat, w1, w2)
        mix_copy().wait()


def stencil_fwd(mesh, height, x, share, cols, edge, corners, trow, table, aug, chunks):
    width, rows, _ = x.shape
    cells = width // chunks
    assert cells % REUSE == 0
    n = len(bit_list(mesh))
    shard_rows = share.shape[0]
    total = shard_rows << n
    roots, start = early_shards(1 << n, shard_rows)
    count = shard_rows - start
    first = lambda i: jnp.where(i < chunks, i, chunks - 1)
    second = lambda i: jnp.where(i < chunks, 0, i - chunks)
    sd = jax.ShapeDtypeStruct
    by_first = lambda c: pl.BlockSpec((cells, rows, c), lambda i: (first(i), 0, 0))
    by_second = lambda c: pl.BlockSpec((cells, rows, c), lambda i: (second(i), 0, 0))
    dma = pltpu.SemaphoreType.DMA
    return pl.pallas_call(
        partial(stencil_fwd_kernel, mesh, chunks, cells),
        name="stencil_fwd",
        grid=(2 * chunks,),
        out_shape=(
            sd((width, rows, CP), BF16),
            sd((width, rows, CP), BF16),
            sd((CP, FP), BF16),
            sd((FP, CP), BF16),
            sd((16, CP), F32),
            sd((8, FP), F32),
            sd(trow.shape, F32),
        ),
        in_specs=[pl.BlockSpec(memory_space=pltpu.SMEM), by_first(C)]
        + [vmem_spec()] * 6
        + [by_second(LANES)],
        out_specs=(by_second(CP), any_spec())
        + (vmem_spec(),) * 5,
        scratch_shapes=[
            pltpu.VMEM((CB, (width + 2 * REACH) * SLOTS, LANES), F32),
            pltpu.VMEM((TAPS, rows, CP), F32),
            pltpu.VMEM((cells * rows, CP), F32),
            pltpu.VMEM((width, rows, CP), BF16),
            pltpu.VMEM((LANES, CP), F32),
            pltpu.VMEM((LANES, CP), BF16),
            pltpu.VMEM(cols.shape, BF16),
            pltpu.VMEM(edge.shape, BF16),
            pltpu.VMEM(corners.shape, BF16),
            pltpu.VMEM(trow.shape, F32),
            pltpu.VMEM((2,) * n + (shard_rows, LANES), BF16),
            pltpu.VMEM((len(roots), count, LANES), BF16),
            pltpu.VMEM((total + 96, LANES), F32),
            pltpu.VMEM((len(roots) * count + 16, LANES), F32),
            dma((2, n)),
            dma((2, n)),
            dma((len(roots), n)),
            dma((len(roots), n)),
            dma((10,)),
            dma((10,)),
            dma,
            dma,
        ],
        compiler_params=params(
            dimension_semantics=("arbitrary",), collective_id=0, has_side_effects=True
        ),
    )(height, x, share, cols, edge, corners, trow, table, aug)


def pack_weights(one, two, flat):
    lane = iota((8, LANES), 1)
    row = iota((8, LANES), 0)
    flat[...] = jnp.zeros_like(flat)

    def turned(v, first, unit):
        return pltpu.roll(v, first, 1, stride=unit, stride_axis=0)

    def main(ref, at, first, unit, out, base, step, count):
        keep = lane >= first + unit * row
        before = jnp.zeros((8, LANES), F32)
        for q in range(count):
            now = turned(ref[q, at, :], first, unit)
            flat[pl.ds(base + q, 8, stride=step), :] = jnp.where(keep, now, before)
            before = now

    def rest(ref, at, first, unit, count, width, mask=None):
        s = first + unit * row
        before = turned(ref[count - 1, at, :], first, unit)
        now = turned(ref[count, at, :], first, unit)
        v = jnp.where(lane < s, before, jnp.where(lane < s + width, now, 0.0))
        return v if mask is None else jnp.where(mask, v, 0.0)

    shift = 8 - LANE_TWO
    base_two = ROW_TWO - 5 * LANE_TWO
    full = FF // LANES
    extra = C - (CB - 1) * LANES

    def two_main(b, carry):
        for k in range(16):
            at = pl.ds(128 * b + 8 * k + shift, 8)
            main(two, at, 8 * k, 1, flat, base_two + 641 * b + 40 * k, 5, CB - 1)
        return carry

    lax.fori_loop(0, full, two_main, 0)
    end = slice(128 * full + shift, 128 * full + shift + 8)
    mask = row < FF - full * LANES + LANE_TWO
    before = jnp.zeros((8, LANES), F32)
    for q in range(CB - 1):
        now = jnp.where(mask, turned(two[q, end, :], 0, 1), 0.0)
        at = pl.ds(base_two + 641 * full + q, 8, stride=5)
        flat[at, :] = jnp.where(lane >= row, now, before)
        before = now

    def one_main(b, carry):
        for k in range(8):
            at = pl.ds(pl.multiple_of(64 * b + 8 * k, 8), 8)
            main(one, at, 16 * k, 2, flat, 641 * b + 80 * k, 10, FB - 1)
        return carry

    last = C - 1
    assert last % 64 == 0
    lax.fori_loop(0, last // 64, one_main, 0)
    row_last = 641 * (last // 64)
    for q in range(FB - 1):
        flat[row_last + q : row_last + q + 1, :] = one[q, last : last + 1, :]

    def add_all(places, values):
        olds = [flat[at, :] for at in places]
        for at, old, v in zip(places, olds, values):
            flat[at, :] = old + v

    def one_rest(b, carry):
        values = [
            rest(one, pl.ds(pl.multiple_of(64 * b + 8 * k, 8), 8), 16 * k, 2, FB - 1, FF - (FB - 1) * LANES)
            for k in range(8)
        ]
        add_all([pl.ds(641 * b + 80 * k + FB - 1, 8, stride=10) for k in range(8)], values)
        return carry

    lax.fori_loop(0, last // 64, one_rest, 0)
    lane1 = iota((1, LANES), 1)
    v = jnp.where(lane1 < FF - (FB - 1) * LANES, one[FB - 1, last : last + 1, :], 0.0)
    add_all([slice(row_last + FB - 1, row_last + FB)], [v])

    def two_rest(b, carry):
        values = [
            rest(two, pl.ds(128 * b + 8 * k + shift, 8), 8 * k, 1, CB - 1, extra) for k in range(16)
        ]
        places = [pl.ds(base_two + 641 * b + 40 * k + CB - 1, 8, stride=5) for k in range(16)]
        add_all(places, values)
        return carry

    lax.fori_loop(0, full, two_rest, 0)
    add_all(
        [pl.ds(base_two + 641 * full + CB - 1, 8, stride=5)],
        [rest(two, end, 0, 1, CB - 1, extra, mask)],
    )


GELU_A = math.sqrt(2.0 / math.pi)
GELU_B = 0.044715
WIDE = 256


def dot(a, b, dims=((1,), (0,))):
    return lax.dot_general(a, b, (dims, ((), ())), preferred_element_type=F32)


def mlp_kernel(
    blocks, height_ref, conv_ref, g_ref, x_ref, w1, w2, small,
    out_ref, gconv_ref, rows_ref, cols_ref, corn_ref, shards_ref, extra_ref,
    one, two, g_scr, conv_t, act, gh, flat, w1_rest,
):
    step = pl.program_id(0)
    cells, rows, _ = x_ref.shape
    m = cells * rows
    height = height_ref[0]

    @pl.when(step == 0)
    def _():
        one[...] = jnp.zeros_like(one)
        two[...] = jnp.zeros_like(two)
        g_scr[...] = jnp.zeros_like(g_scr)
        w1_rest[...] = w1[:, FP // WIDE * WIDE :].astype(F32).T[: w1_rest.shape[0]]

    live = (iota((1, rows, 1), 1) < height).astype(F32)
    g_scr[:, :C] = (g_ref[...].astype(F32) * live).reshape(m, C).astype(BF16)
    rows_one = conv_t.shape[0]

    def hidden(start, wide, tail):
        lanes = pl.ds(start, wide)
        h = dot(conv_ref[...].reshape(m, CP), w1[:, lanes]) + small[0:1, lanes]
        ga = dot(g_scr[...], w2[lanes, :], ((1,), (1,)))
        h2 = h * h
        t = jnp.tanh(h * (GELU_A + (GELU_A * GELU_B) * h2))
        cdf = 0.5 * t + 0.5
        value = (h * cdf).astype(BF16)
        slope = cdf + h * (0.5 - 0.5 * (t * t)) * (GELU_A + (3 * GELU_A * GELU_B) * h2)
        if tail:
            ones = iota((m, wide), 1) == FF - (FB - 1) * LANES
            value = jnp.where(ones, jnp.ones_like(value), value)
        act[:, lanes] = value
        gh[:, lanes] = (ga * slope).astype(BF16)

    def turn(i, count):
        part = conv_ref[:, :, pl.ds(i * LANES, LANES)].reshape(m, LANES)
        conv_t[pl.ds(i * LANES, count), :] = part.T[:count]

    full = FP // WIDE
    assert full == CB - 1
    for f in range(full):
        turn(f, LANES)
        hidden(f * WIDE, WIDE, False)
    turn(CB - 1, rows_one - (CB - 1) * LANES)
    hidden(full * WIDE, FP % WIDE, True)

    main = full * WIDE
    spare = [
        (act[:, main + i : main + i + 1].astype(F32), gh[:, main + i : main + i + 1].astype(F32))
        for i in range(FF - main)
    ]
    for n in range(CP // WIDE):
        lanes = slice(n * WIDE, (n + 1) * WIDE)
        end = min((n + 1) * WIDE, C)
        part = slice(n * WIDE, end)
        branch = dot(act[:, :main], w2[:main, lanes])
        gc = dot(gh[:, :main], w1[lanes, :main], ((1,), (1,)))
        for i, (a, b) in enumerate(spare):
            branch = branch + a * w2[main : main + 16, lanes].astype(F32)[i : i + 1]
            gc = gc + b * w1_rest[i : i + 1, lanes]
        v = x_ref[:, :, part].astype(F32).reshape(m, -1) + branch[:, : end - n * WIDE] + small[1:2, part]
        out_ref[:, :, part] = (v.reshape(cells, rows, -1) * live).astype(BF16)
        for i in range(WIDE // LANES):
            gconv_ref[n * (WIDE // LANES) + i] = gc[:, i * LANES : (i + 1) * LANES]

    def weights(start, wide):
        lanes = pl.ds(start, wide)
        r1 = dot(conv_t[...], gh[:, lanes])
        r2 = dot(act[:, lanes], g_scr[...], ((0,), (0,)))
        for i in range(wide // LANES):
            one[start // LANES + i] += r1[:, i * LANES : (i + 1) * LANES]
        for q in range(CB):
            two[q, pl.ds(start + 8, wide), :] += r2[:, q * LANES : (q + 1) * LANES]

    def third(f, carry):
        weights(pl.multiple_of(f * WIDE, WIDE), WIDE)
        return carry

    lax.fori_loop(0, FP // WIDE, third, 0)
    weights(FP // WIDE * WIDE, FP % WIDE)

    whole, left = divmod(cells, 8)
    for r, slot in ((0, 0), (1, height - 1)):
        for q in range(CB):
            lanes = slice(q * LANES, (q + 1) * LANES)
            pick = lambda c: gconv_ref[q, pl.ds(slot + c * rows, 8, stride=rows), :]
            v = [pick(8 * i) for i in range(whole)]
            if left:
                v.append(pltpu.roll(pick(cells - 8), left, 0))
            v = jnp.concatenate(v, 0).astype(BF16)
            rows_ref[0, r, :, lanes] = v
            for side, at, first in ((0, 0, 0), (1, blocks - 1, cells - REACH)):

                @pl.when(step == at)
                def _(side=side, first=first, v=v, lanes=lanes, r=r):
                    corn_ref[r, side, :, lanes] = v[first : first + REACH]

    for side, at, first in ((0, 0, 0), (1, blocks - 1, cells - REACH)):

        @pl.when(step == at)
        def _(side=side, first=first):
            for i in range(REACH):
                base = (first + i) * rows
                for q in range(CB):
                    lanes = slice(q * LANES, (q + 1) * LANES)
                    cols_ref[side, i, :, lanes] = gconv_ref[q, base : base + rows, :].astype(BF16)

    @pl.when(step == blocks - 1)
    def _():
        extra_ref[...] = jnp.zeros_like(extra_ref)
        for q in range(FB):
            extra_ref[0 : NOISE + 1, q * LANES : (q + 1) * LANES] = one[q, C : C + NOISE + 1, :]
        for q in range(CB):
            lanes = slice(q * LANES, (q + 1) * LANES)
            extra_ref[NOISE + 1 : NOISE + 2, lanes] = two[q, FF + 8 : FF + 9, :]
        pack_weights(one, two, flat)
        bits = len(shards_ref.shape) - 2
        shard_rows = shards_ref.shape[-2]

        def store(d, carry):
            index = tuple((d >> (bits - 1 - i)) & 1 for i in range(bits))
            shards_ref[index] = flat[pl.ds(d * shard_rows, shard_rows), :]
            return carry

        lax.fori_loop(0, 1 << bits, store, 0)


def mlp(height, conv, g, x, w1, w2, small, shards, blocks):
    width, rows, _ = x.shape
    cells = width // blocks
    m = cells * rows
    sd = jax.ShapeDtypeStruct
    block = lambda c: pl.BlockSpec((cells, rows, c), lambda i: (i, 0, 0))
    rows_one = -(-(C + NOISE + 1) // 16) * 16
    flops = 12 * width * rows * C * FF
    return pl.pallas_call(
        partial(mlp_kernel, blocks),
        name="mlp",
        grid=(blocks,),
        out_shape=(
            sd((width, rows, C), BF16),
            sd((CB, width * rows, LANES), F32),
            sd((blocks, 2, -(-cells // 8) * 8, CP), BF16),
            sd((2, REACH, rows, CP), BF16),
            sd((2, 2, REACH, CP), BF16),
            sd(shards, F32),
            sd((16, FP), F32),
        ),
        in_specs=[
            pl.BlockSpec(memory_space=pltpu.SMEM),
            block(CP),
            block(C),
            block(C),
            vmem_spec(),
            vmem_spec(),
            vmem_spec(),
        ],
        out_specs=(
            block(C),
            pl.BlockSpec((CB, m, LANES), lambda i: (0, i, 0)),
            pl.BlockSpec((1, 2, -(-cells // 8) * 8, CP), lambda i: (i, 0, 0, 0)),
            vmem_spec(),
            vmem_spec(),
            vmem_spec(),
            vmem_spec(),
        ),
        scratch_shapes=[
            pltpu.VMEM((FB, rows_one, LANES), F32),
            pltpu.VMEM((CB, FP + 16, LANES), F32),
            pltpu.VMEM((m, CP), BF16),
            pltpu.VMEM((rows_one, m), BF16),
            pltpu.VMEM((m, FP), BF16),
            pltpu.VMEM((m, FP), BF16),
            pltpu.VMEM((math.prod(shards[:-1]), LANES), F32),
            pltpu.VMEM((8, CP), F32),
        ],
        compiler_params=params(dimension_semantics=("arbitrary",)),
        cost_estimate=pl.CostEstimate(flops=flops, bytes_accessed=50_000_000, transcendentals=0),
    )(height, conv, g, x, w1, w2, small)


def add_vector(tail, offset, value):
    row, shift = divmod(offset - TAIL_ROW * LANES, LANES)
    blocks = value.shape[0]
    lane = iota((blocks + 1, LANES), 1)
    zero = jnp.zeros((1, LANES), F32)
    here = pltpu.roll(jnp.concatenate([value, zero], 0), shift, 1) if shift else jnp.concatenate([value, zero], 0)
    back = jnp.concatenate([zero, here[:blocks]], 0)
    at = slice(row, row + blocks + 1)
    tail[at, :] = tail[at, :] + jnp.where(lane >= shift, here, back if shift else here)


def as_blocks(value, length):
    blocks = -(-length // LANES)
    v = jnp.concatenate([value[:, q * LANES : (q + 1) * LANES] for q in range(blocks)], 0)
    index = iota((blocks, LANES), 0) * LANES + iota((blocks, LANES), 1)
    return jnp.where(index < length, v, 0.0)


class Scatter:
    def __init__(self, mesh, shards, buf, recvs, send, recv):
        self.bits = bit_list(mesh)
        self.n = len(self.bits)
        self.orders = scatter_orders(mesh)
        self.first = self.orders[0][0]
        assert all(order[0] == self.first for order in self.orders)
        self.mine = my_bits(self.bits)
        self.shards, self.buf, self.recvs = shards, buf, recvs
        self.send, self.recv = send, recv
        rows = shards.shape[-2]
        one, two = (int(rows * f) // 8 * 8 for f in (0.36, 0.71))
        self.spans = [(0, one), (one, two - one), (two, rows - two)]

    def copy(self, colour, k):
        order, mine, n = self.orders[colour], self.mine, self.n
        done, now = order[:k], order[k]
        at = (pl.ds(*self.spans[colour]),)
        index = tuple(
            1 - mine[i] if i == now else mine[i] if i in done else slice(None) for i in range(n)
        )
        if k == 0:
            src = self.shards.at[index + at]
        else:
            src = self.buf.at[tuple(v for i, v in enumerate(index) if i != self.first) + at]
        return pltpu.make_async_remote_copy(
            src_ref=src,
            dst_ref=self.recvs[k].at[(slice(None),) * (n - 1 - k) + at],
            send_sem=self.send.at[colour, k],
            recv_sem=self.recv.at[colour, k],
            device_id=partner(*self.bits[now]),
            device_id_type=MESH,
        )

    def load(self, sem):
        index = tuple(self.mine[i] if i == self.first else slice(None) for i in range(self.n))
        return pltpu.make_async_copy(self.shards.at[index], self.buf, sem)

    def advance(self, colour, k):
        self.copy(colour, k).wait()
        order, n = self.orders[colour], self.n
        free = [i for i in range(n) if i not in order[: k + 1]]
        at = (pl.ds(*self.spans[colour]),)

        def add(d, carry):
            sub = tuple((d >> (len(free) - 1 - i)) & 1 for i in range(len(free)))
            index = tuple(
                sub[free.index(i)] if i in free else self.mine[i]
                for i in range(n)
                if i != self.first
            )
            self.buf[index + at] = self.buf[index + at] + self.recvs[k][sub + at]
            return carry

        lax.fori_loop(0, 1 << len(free), add, 0)
        if k + 1 < n:
            self.copy(colour, k + 1).start()

    def result(self):
        return self.buf[tuple(v for i, v in enumerate(self.mine) if i != self.first)]


def scatter_plan(n):
    if n == 5:
        return {
            7: [(0, 1), (1, 1), (2, 1)],
            12: [(0, 2), (1, 2)],
            13: [(2, 2)],
            17: [(0, 3), (1, 3), (2, 3)],
        }
    return {}


class Tail:
    def __init__(self, mesh, pieces, got, msg, full, place, send, recv):
        self.mesh = mesh
        self.n = mesh.shape["lat"] * mesh.shape["lon"]
        self.lat, self.lon = lax.axis_index("lat"), lax.axis_index("lon")
        self.me = self.lat * mesh.shape["lon"] + self.lon
        self.pieces, self.got, self.msg, self.full, self.place = pieces, got, msg, full, place
        self.send, self.recv = send, recv

    def others(self, source, target, k):
        def send(device, d):
            pltpu.make_async_remote_copy(
                src_ref=source(d),
                dst_ref=target.at[self.me],
                send_sem=self.send.at[k],
                recv_sem=self.recv.at[k],
                device_id=device,
                device_id_type=MESH,
            ).start()

        for_others(self.mesh, send)

    def wait_all(self, buffer, k):
        pltpu.make_async_remote_copy(
            src_ref=buffer.at[pl.ds(0, self.n - 1)],
            dst_ref=buffer.at[pl.ds(0, self.n - 1)],
            send_sem=self.send.at[k],
            recv_sem=self.recv.at[k],
            device_id=(self.lat, self.lon),
            device_id_type=MESH,
        ).wait()

    def scatter(self, flat):
        piece = self.pieces.shape[1]

        def split(d, carry):
            self.pieces[d] = flat[pl.ds(d * piece, piece), :]
            return carry

        lax.fori_loop(0, self.n, split, 0)
        self.others(lambda d: self.pieces.at[d], self.got, 0)
        self.got[self.me] = self.pieces[self.me]
        self.place[...] = jnp.zeros_like(self.place)

    def finish(self, part, grad_ref, norm_ref):
        n, piece = self.n, self.pieces.shape[1]
        shard_rows = part.shape[0]
        square = jnp.sum(part * part)
        self.wait_all(self.got, 0)
        total = lax.fori_loop(1, n, lambda i, acc: acc + self.got[i], self.got[0])
        square = square + jnp.sum(total * total)
        self.msg[0:piece, :] = total
        self.msg[piece : piece + 1, :] = jnp.broadcast_to(square, (1, LANES))
        self.others(lambda d: self.msg, self.full, 1)
        self.full[self.me] = self.msg[...]
        self.wait_all(self.full, 1)

        def take(d, acc):
            self.place[pl.ds(shard_rows + d * piece, piece), :] = self.full[d, 0:piece, :]
            return acc + self.full[d, piece : piece + 1, :]

        squares = lax.fori_loop(0, n, take, jnp.zeros((1, LANES), F32))
        start = jnp.clip(self.me * shard_rows - TAIL_ROW + shard_rows, 0, shard_rows + n * piece)
        grad_ref[...] = part + self.place[pl.ds(start, shard_rows), :]
        norm_ref[...] = jnp.broadcast_to(jnp.sqrt(squares), norm_ref.shape)


def backward_kernel(
    mesh, chunks, cells, strip_cells, height_ref, mix_ref, gconv_ref, x_hbm, g_hbm,
    cols, edge, corners, table, trowh, wd, gain, extra, w1, shards,
    out_ref, grad_ref, norm_ref,
    x_scr, up_scr, st_scr, g_scr, m_scr, k_scr, t_scr, e_scr, gg_scr, tail_scr, colh, rowh, cornh,
    pieces, got, msg, full, place, buf, *rest,
):
    n = len(bit_list(mesh))
    recvs, (send, recv, hsend, hrecv, tsend, trecv, load_sem) = rest[:n], rest[n:]
    scatter = Scatter(mesh, shards, buf, recvs, send, recv)
    tail = Tail(mesh, pieces, got, msg, full, place, tsend, trecv)
    step = pl.program_id(0)
    width, rows, _ = mix_ref.shape
    height = height_ref[0]
    plan = scatter_plan(n)
    gvec = gain[2:3, :C]
    halos = lambda: halo_copies(cols, edge, corners, colh, rowh, cornh, hsend, hrecv)
    load_x = lambda: pltpu.make_async_copy(x_hbm, x_scr, load_sem.at[1])
    load_up = lambda: pltpu.make_async_copy(g_hbm, up_scr, load_sem.at[2])

    @pl.when(step == 0)
    def _():
        load_x().start()
        greet_all(mesh)
        start_halo(halos())
        for colour in range(3):
            scatter.copy(colour, 0).start()
        scatter.load(load_sem.at[0]).start()
        load_up().start()
        hrow = iota((rows, 16), 0)
        for t in range(TAPS):
            l = t // 5
            own = table[t * rows : (t + 1) * rows, :]
            if l == 0:
                own = jnp.concatenate([own[1:], own[:1]], 0)
                own = jnp.where(hrow == height - 1, trowh[1, t : t + 1, :], own)
            if l == 2:
                own = jnp.concatenate([trowh[0, t : t + 1, :], own[: rows - 1]], 0)
            t_scr[t * rows : (t + 1) * rows, :] = own
        kernel = jnp.dot(t_scr[...], wd[...], preferred_element_type=F32, precision=HIGHEST)
        for q in range(CB):
            k_scr[q] = kernel[:, q * LANES : (q + 1) * LANES].reshape(k_scr.shape[1:])
        e_scr[...] = jnp.zeros_like(e_scr)
        gg_scr[...] = jnp.zeros_like(gg_scr)
        load_x().wait()
        first_lane = iota((rows, LANES), 1) == 0

        def stats(j, carry):
            x = x_scr[j].astype(F32)
            mean = jnp.mean(x, -1, keepdims=True)
            center = x - mean
            inv = lax.rsqrt(jnp.mean(center * center, -1, keepdims=True) + 1e-05)
            st_scr[j] = jnp.where(first_lane, mean, inv)
            return carry

        lax.fori_loop(0, width, stats, 0, unroll=10)

    @pl.when(step == 1)
    def _():
        wait_halo(halos())
        scatter.load(load_sem.at[0]).wait()
        for colour in range(3):
            scatter.advance(colour, 0)

    @pl.when((step >= 1) & (step <= CB))
    def _():
        q = step - 1
        lanes = pl.ds(pl.multiple_of(q * LANES, LANES), LANES)
        lat, _, nlat, *_ = neighbours()
        keep = (lat > 0, lat < nlat - 1)
        here = iota((rows, LANES), 0) == height

        def put(column, top, low, v):
            at = column * SLOTS
            g_scr[pl.ds(at + 1, rows), :] = jnp.where(here, low, v)
            g_scr[pl.ds(at, 1), :] = top
            g_scr[pl.ds(at + rows + 1, 1), :] = low

        def beside(ref):
            return [jnp.where(keep[r], ref(r).astype(F32), 0.0) for r in range(2)]

        for side in range(2):
            top, low = beside(lambda r: cornh[r, side, :, lanes])
            for i in range(REACH):
                column = i if side == 0 else width + REACH + i
                put(column, top[i : i + 1], low[i : i + 1], colh[side, i, :, lanes].astype(F32))

        def strip(c, carry):
            tops, lows = beside(lambda r: rowh[c, r, :, lanes])
            for i in range(strip_cells):
                j = c * strip_cells + i
                v = gconv_ref[0, pl.ds(pl.multiple_of(j * rows, 8), rows), :]
                put(j + REACH, tops[i : i + 1], lows[i : i + 1], v)
                m_scr[q, j] = mix_ref[j].astype(F32)
            return carry

        lax.fori_loop(0, edge.shape[0], strip, 0)
        for hb in range(rows // 8):
            at = slice(8 * hb, 8 * hb + 8)

            def cell(i, carry):
                j = i * REUSE
                mixed = [m_scr[q, j + u, at, :] for u in range(REUSE)]
                total = [None] * REUSE
                for l in range(3):
                    near = [
                        g_scr[pl.ds((j + u) * SLOTS + 8 * hb + 2 - l, 8), :]
                        for u in range(REUSE + 2 * REACH)
                    ]
                    for w in range(5):
                        t = 5 * l + w
                        tap = k_scr[q, t, at, :]
                        views = near[2 * REACH - w : 2 * REACH - w + REUSE]
                        terms = [tap * v for v in views]
                        total = [a if b is None else a + b for a, b in zip(terms, total)]
                        sums = [m * v for m, v in zip(mixed, views)]
                        while len(sums) > 1:
                            sums = [
                                sums[k] + sums[k + 1] if k + 1 < len(sums) else sums[k]
                                for k in range(0, len(sums), 2)
                            ]
                        e_scr[q, t, at, :] = e_scr[q, t, at, :] + sums[0]
                for u in range(REUSE):
                    m_scr[q, j + u, at, :] = total[u]
                return carry

            lax.fori_loop(0, width // REUSE, cell, 0)
            for loop, events in plan.items():
                if loop % (rows // 8) == hb:

                    @pl.when(q == loop // (rows // 8))
                    def _(events=events):
                        for colour, k in events:
                            scatter.advance(colour, k)

    @pl.when(step == CB)
    def _():
        load_up().wait()
        tail_scr[...] = jnp.zeros_like(tail_scr)
        add_vector(tail_scr, OFF_B1, as_blocks(extra[NOISE : NOISE + 1, :], FF))
        add_vector(tail_scr, OFF_B2, as_blocks(extra[NOISE + 1 : NOISE + 2, :], C))
        disco = jnp.concatenate(
            [
                lax.dot_general(
                    t_scr[...], e_scr[q].reshape(TAPS * rows, LANES), (((0,), (0,)), ((), ())),
                    preferred_element_type=F32, precision=HIGHEST,
                )
                for q in range(CB)
            ],
            1,
        )
        for k in range(K):
            add_vector(tail_scr, OFF_DISCO + k * C, as_blocks(disco[k : k + 1, :], C))
        ng = extra[0:NOISE, :]
        hi = ng.astype(BF16)
        mid = (ng - hi.astype(F32)).astype(BF16)
        lo = (ng - hi.astype(F32) - mid.astype(F32)).astype(BF16)
        parts = [dot(p, w1[...], ((1,), (1,))) for p in (hi, mid, lo)]
        gn = parts[0] + parts[1] + parts[2]
        for k in range(NOISE):
            add_vector(tail_scr, OFF_NOISE + k * C, as_blocks(gn[k : k + 1, :], C))

    @pl.when(step > CB)
    def _():
        first = (step - CB - 1) * cells
        live = iota((rows, C), 0) < height

        def cell(i, total):
            j = first + i
            st = st_scr[j]
            inv = st[:, 1:2]
            normed = (x_scr[j].astype(F32) - st[:, :1]) * inv
            gm = jnp.concatenate([m_scr[q, j] for q in range(CB)], 1)[:, :C]
            gm = jnp.where(live, gm, 0.0)
            total = total + gm * normed
            v = gm * gvec
            mean = jnp.mean(v, -1, keepdims=True)
            mean_n = jnp.mean(v * normed, -1, keepdims=True)
            up = jnp.where(live, up_scr[j].astype(F32), 0.0)
            out_ref[i] = inv * (v - mean - normed * mean_n) + up
            return total

        gg_scr[:, :C] = lax.fori_loop(0, cells, cell, gg_scr[:, :C], unroll=4)

    @pl.when(step == CB + chunks)
    def _():
        add_vector(tail_scr, OFF_GAIN, as_blocks(jnp.sum(gg_scr[...], 0, keepdims=True), C))
        tail.scatter(tail_scr)
        taken = {e for events in plan.values() for e in events}
        for k in range(1, n):
            for colour in range(3):
                if (colour, k) not in taken:
                    scatter.advance(colour, k)
        tail.finish(scatter.result(), grad_ref, norm_ref)


def backward(
    mesh, height, mixed, gconv, x, g, cols, edge, corners, table, trowh, wd, small, extra,
    w1, shards, piece, chunks,
):
    width, rows, _ = mixed.shape
    cells = width // chunks
    shard_rows = shards.shape[-2]
    n = len(bit_list(mesh))
    devices = 1 << n
    group = lambda i: jnp.clip(i - 1, 0, CB - 1)
    last = lambda i: jnp.where(i <= CB, 0, i - CB - 1)
    sd = jax.ShapeDtypeStruct
    dma = pltpu.SemaphoreType.DMA
    return pl.pallas_call(
        partial(backward_kernel, mesh, chunks, cells, width // edge.shape[0]),
        name="backward",
        grid=(1 + CB + chunks,),
        out_shape=(
            sd((width, rows, C), F32),
            sd((shard_rows, LANES), F32),
            sd((8, LANES), F32),
        ),
        in_specs=[
            pl.BlockSpec(memory_space=pltpu.SMEM),
            pl.BlockSpec((width, rows, LANES), lambda i: (0, 0, group(i))),
            pl.BlockSpec((1, width * rows, LANES), lambda i: (group(i), 0, 0)),
            any_spec(),
            any_spec(),
        ]
        + [vmem_spec()] * 9
        + [any_spec()],
        out_specs=(
            pl.BlockSpec((cells, rows, C), lambda i: (last(i), 0, 0)),
            vmem_spec(),
            vmem_spec(),
        ),
        scratch_shapes=[
            pltpu.VMEM(x.shape, BF16),
            pltpu.VMEM(x.shape, BF16),
            pltpu.VMEM((width, rows, LANES), F32),
            pltpu.VMEM(((width + 2 * REACH) * SLOTS, LANES), F32),
            pltpu.VMEM((CB, width, rows, LANES), F32),
            pltpu.VMEM((CB, TAPS, rows, LANES), F32),
            pltpu.VMEM((TAPS * rows, 16), F32),
            pltpu.VMEM((CB, TAPS, rows, LANES), F32),
            pltpu.VMEM((rows, CP), F32),
            pltpu.VMEM((devices * piece, LANES), F32),
            pltpu.VMEM(cols.shape, BF16),
            pltpu.VMEM(edge.shape, BF16),
            pltpu.VMEM(corners.shape, BF16),
            pltpu.VMEM((devices, piece, LANES), F32),
            pltpu.VMEM((devices, piece, LANES), F32),
            pltpu.VMEM((piece + 1, LANES), F32),
            pltpu.VMEM((devices, piece + 1, LANES), F32),
            pltpu.VMEM((2 * shard_rows + devices * piece + 8, LANES), F32),
            pltpu.VMEM((2,) * (n - 1) + (shard_rows, LANES), F32),
        ]
        + [pltpu.VMEM((2,) * (n - 1 - k) + (shard_rows, LANES), F32) for k in range(n)]
        + [dma((3, n)), dma((3, n)), dma((8,)), dma((8,)), dma((2,)), dma((2,)), dma((3,))],
        compiler_params=params(
            dimension_semantics=("arbitrary",), collective_id=1, has_side_effects=True
        ),
    )(
        height, mixed, gconv, x, g, cols, edge, corners, table, trowh, wd, small, extra, w1, shards,
    )


def stencil_table(support_vals, support_lon):
    rows = support_vals.shape[0]
    vals = support_vals.reshape(rows, S // 3, 3, K)
    offsets = jnp.arange(-REACH, REACH + 1)
    hit = support_lon.reshape(rows, S // 3, 3)[:, :, :, None] == offsets
    picked = jnp.where(hit[:, :, :, :, None], vals[:, :, :, None, :], 0.0)
    return jnp.transpose(jnp.sum(picked, 1), (1, 2, 0, 3))


def flat_table(table):
    t = table.reshape(-1, K)
    return jnp.pad(t, ((0, 0), (0, 16 - K)))


def local(
    mesh, block_in, noise, cotangent, band_heights, support_lon, support_vals,
    master, moment_one, moment_two, average, step_count,
):
    rows, width, _ = block_in.shape
    devices = mesh.shape["lat"] * mesh.shape["lon"]
    shard = master.shape[0]
    shard_rows = shard // LANES
    assert shard_rows * LANES == shard
    flat_rows = shard_rows * devices
    chunks = 6
    cells = width // chunks
    height = lax.dynamic_slice_in_dim(band_heights, lax.axis_index("lat"), 1, 0)
    x = jnp.transpose(block_in, (1, 0, 2))
    g = jnp.transpose(cotangent, (1, 0, 2))

    table = flat_table(stencil_table(support_vals, support_lon))
    planes = table.reshape(TAPS, rows, 16)
    trow = jnp.stack([planes[:, 0], lax.dynamic_index_in_dim(planes, height[0] - 1, 1, keepdims=False)])
    trow = jnp.pad(trow, ((0, 0), (0, 1), (0, 0)))
    share = master.astype(BF16).reshape(shard_rows, LANES)
    edge = jnp.stack([x[:, 0], lax.dynamic_index_in_dim(x, height[0] - 1, 1, keepdims=False)], 1)
    cols = jnp.stack([x[:REACH], x[width - REACH :]])
    corners = jnp.stack([edge[:REACH], edge[width - REACH :]], 0)
    corners = jnp.transpose(corners, (2, 0, 1, 3))
    edge = jnp.transpose(edge.reshape(chunks, cells, 2, C), (0, 2, 1, 3))
    aug = jnp.concatenate(
        [
            jnp.zeros((width, rows, 1), BF16),
            jnp.transpose(noise, (2, 1, 0)),
            jnp.ones((width, rows, 1), BF16),
            jnp.zeros((width, rows, LANES - NOISE - 2), BF16),
        ],
        2,
    )
    conv, mixed, w1, w2, wd, small, trowh = stencil_fwd(
        mesh, height, x, share, cols, edge, corners, trow, table, aug, chunks
    )
    shards = (2,) * len(bit_list(mesh)) + (shard_rows, LANES)
    out, gconv, grow, gcol, gcorn, packed, extra = mlp(
        height, conv, g, x, w1, w2, small, shards, chunks
    )
    piece = -(-(flat_rows - TAIL_ROW) // devices)
    grad_in, grad, norm = backward(
        mesh, height, mixed, gconv, x, g, gcol, grow, gcorn, table, trowh, wd, small,
        extra, w1, packed, piece, 9,
    )
    grad_part = grad.reshape(shard)
    grad_norm = norm[0, :1]
    factor = 0.01 / jnp.maximum(grad_norm, 0.01)
    clipped = grad_part * factor
    new_one = 0.9 * moment_one + 0.1 * clipped
    new_two = 0.999 * moment_two + 0.001 * clipped * clipped
    step_float = step_count[0].astype(F32)
    fix_one = 1.0 - jnp.power(jnp.float32(0.9), step_float)
    fix_two = 1.0 - jnp.power(jnp.float32(0.999), step_float)
    update = new_one / fix_one / (jnp.sqrt(new_two / fix_two) + 1e-08) + 0.1 * master
    new_master = master - 0.02 * update
    new_avg = 0.9 * average + 0.1 * new_master
    return (
        jnp.transpose(out, (1, 0, 2)),
        jnp.transpose(grad_in, (1, 0, 2)),
        grad_part,
        grad_norm,
        new_master,
        new_one,
        new_two,
        new_avg,
        new_master.astype(BF16),
    )


def solution(mesh):
    flat = P(("lat", "lon"))
    field = P("lat", "lon", None)
    return jax.shard_map(
        partial(local, mesh),
        mesh=mesh,
        in_specs=(
            field, P(None, "lat", "lon"), field, P(), P("lat", None), P("lat", None, None),
            flat, flat, flat, flat, P(),
        ),
        out_specs=(field, field, flat, P(), flat, flat, flat, flat, flat),
        check_vma=False,
    )
```

```python
from functools import partial
import math

import jax
import jax.numpy as jnp
from jax import lax
from jax.experimental import pallas as pl
from jax.experimental.pallas import tpu as pltpu
from jax.sharding import PartitionSpec as P

C = 641
FF = 1282
NOISE = 8
K = 9
S = 12
REACH = 2
LANES = 128
CB = 6
CP = CB * LANES
FB = 11
FP = FB * LANES
TAPS = 15
MESH = pl.DeviceIdType.MESH
HIGHEST = lax.Precision.HIGHEST
F32 = jnp.float32
BF16 = jnp.bfloat16
VMEM_LIMIT = 60 * 1024 * 1024
SLOTS = 28
REUSE = 10
ROW_TWO = (C * FF) // LANES
LANE_TWO = (C * FF) % LANES
TAIL_ROW = (2 * C * FF) // LANES
OFF_B1 = 2 * C * FF
OFF_B2 = OFF_B1 + FF
OFF_GAIN = OFF_B2 + C
OFF_DISCO = OFF_GAIN + C
OFF_NOISE = OFF_DISCO + K * C
END_FLAT = OFF_NOISE + NOISE * C


def params(**kw):
    return pltpu.CompilerParams(vmem_limit_bytes=VMEM_LIMIT, **kw)


def any_spec():
    return pl.BlockSpec(memory_space=pl.ANY)


def vmem_spec():
    return pl.BlockSpec(memory_space=pltpu.VMEM)


def iota(shape, dim):
    return lax.broadcasted_iota(jnp.int32, shape, dim)


def bit_list(mesh):
    bits = []
    for axis in ("lat", "lon"):
        count = int(math.log2(mesh.shape[axis]))
        assert 1 << count == mesh.shape[axis]
        bits += [(axis, b) for b in reversed(range(count))]
    return bits


def my_bits(bits):
    ids = {"lat": lax.axis_index("lat"), "lon": lax.axis_index("lon")}
    return [(ids[a] >> b) & 1 for a, b in bits]


def partner(axis, bit):
    lat, lon = lax.axis_index("lat"), lax.axis_index("lon")
    if axis == "lat":
        return (lat ^ (1 << bit), lon)
    return (lat, lon ^ (1 << bit))


def stage_orders(mesh):
    bits = bit_list(mesh)
    n = len(bits)
    if (mesh.shape["lat"], mesh.shape["lon"]) == (8, 4):
        return [[0, 1, 2, 3, 4], [0, 1, 3, 2, 4]]
    order = list(range(n))
    return [order, order]


def scatter_orders(mesh):
    n = len(bit_list(mesh))
    if (mesh.shape["lat"], mesh.shape["lon"]) == (8, 4):
        return [[4, 3, 2, 1, 0], [4, 2, 3, 1, 0], [4, 1, 0, 3, 2]]
    return [list(reversed(range(n)))] * 3


def rotl_rows(v, first, unit):
    index = (iota((8, LANES), 1) + first + unit * iota((8, LANES), 0)) % LANES
    return jnp.take_along_axis(v, index, axis=1)


def row_vector(flat_ref, offset, length):
    blocks = -(-length // LANES)
    row, shift = divmod(offset, LANES)
    near = flat_ref[row : row + blocks, :]
    if shift:
        far = flat_ref[row + 1 : row + 1 + blocks, :]
        lane = iota((blocks, LANES), 1)
        near = pltpu.roll(jnp.where(lane >= shift, near, far), LANES - shift, 1)
    index = iota((blocks, LANES), 0) * LANES + iota((blocks, LANES), 1)
    return jnp.where(index < length, near, 0.0)


def put_row(ref, row, value):
    for q in range(value.shape[0]):
        ref[row : row + 1, q * LANES : (q + 1) * LANES] = value[q : q + 1, :].astype(ref.dtype)


def unpack_weights(flat, w1, w2):
    lane = iota((8, LANES), 1)
    row = iota((8, LANES), 0)

    def rows_one(base, first):
        near = [flat[pl.ds(base + q, 8, stride=10), :] for q in range(FB + 1)]
        out = [
            rotl_rows(jnp.where(lane >= first + 2 * row, near[q], near[q + 1]), first, 2)
            for q in range(FB)
        ]
        out[-1] = jnp.where(lane < FF - (FB - 1) * LANES, out[-1], 0.0)
        return out

    def body_one(b, carry):
        for k in range(0, 8, 2):
            pair = [rows_one(641 * b + 80 * (k + h), 16 * (k + h)) for h in range(2)]
            at = pl.ds(pl.multiple_of(64 * b + 8 * k, 16), 16)
            for q in range(FB):
                v = jnp.concatenate([pair[0][q], pair[1][q]], 0)
                w1[at, q * LANES : (q + 1) * LANES] = v.astype(BF16)
        return carry

    last = C - 1
    lax.fori_loop(0, last // 64, body_one, 0)
    zero = jnp.zeros((8, LANES), F32)
    for q, v in enumerate(rows_one(641 * (last // 64), 0)):
        v = jnp.concatenate([jnp.where(row == 0, v, 0.0), zero], 0)
        w1[last : last + 16, q * LANES : (q + 1) * LANES] = v.astype(BF16)
    w1[last + 16 :, :] = jnp.zeros((CP - last - 16, FP), BF16)

    def rows_two(base, first):
        count = CB + 2 if first + 7 >= LANES else CB + 1
        near = [flat[pl.ds(base + q, 8, stride=5), :] for q in range(count)]
        out = []
        for q in range(CB):
            v = jnp.where(lane >= first + row, near[q], near[q + 1])
            if first + 7 >= LANES:
                v = jnp.where(lane < first + row - LANES, near[q + 2], v)
            out.append(rotl_rows(v, first, 1))
        out[-1] = jnp.where(lane < C - (CB - 1) * LANES, out[-1], 0.0)
        return out

    def body_two(b, carry):
        for k in range(0, 16, 2):
            pair = [
                rows_two(ROW_TWO + 641 * b + 40 * (k + h), LANE_TWO + 8 * (k + h))
                for h in range(2)
            ]
            at = pl.ds(pl.multiple_of(128 * b + 8 * k, 16), 16)
            for q in range(CB):
                v = jnp.concatenate([pair[0][q], pair[1][q]], 0)
                w2[at, q * LANES : (q + 1) * LANES] = v.astype(BF16)
        return carry

    full = FF // LANES
    lax.fori_loop(0, full, body_two, 0)
    for q, v in enumerate(rows_two(ROW_TWO + 641 * full, LANE_TWO)):
        v = jnp.concatenate([jnp.where(row < FF - full * LANES, v, 0.0), zero], 0)
        w2[full * LANES : full * LANES + 16, q * LANES : (q + 1) * LANES] = v.astype(BF16)
    w2[full * LANES + 16 :, :] = jnp.zeros((FP - full * LANES - 16, CP), BF16)


def unpack_small(flat, base, wn, wd, small, wnf):
    vector = lambda offset, length: row_vector(flat, offset - base * LANES, length)
    small[...] = jnp.zeros_like(small)
    put_row(small, 0, vector(OFF_B1, FF))
    put_row(small, 1, vector(OFF_B2, C))
    put_row(small, 2, vector(OFF_GAIN, C))
    wd[...] = jnp.zeros_like(wd)
    wnf[...] = jnp.zeros_like(wnf)
    for k in range(K):
        put_row(wd, k, vector(OFF_DISCO + k * C, C))
    for k in range(NOISE):
        put_row(wnf, 1 + k, vector(OFF_NOISE + k * C, C))
    wn[...] = wnf[...].astype(BF16)


def neighbours():
    lat, lon = lax.axis_index("lat"), lax.axis_index("lon")
    nlat, nlon = lax.axis_size("lat"), lax.axis_size("lon")
    return lat, lon, nlat, nlon, lax.rem(lon + 1, nlon), lax.rem(lon + nlon - 1, nlon)


def halo_copies(cols, rows, corners, colh, rowh, cornh, send, recv, trow=None, trowh=None):
    lat, lon, nlat, nlon, east, west = neighbours()
    out = []

    def add(src, dst, target, k, sends, gets):
        out.append(
            (
                sends,
                gets,
                pltpu.make_async_remote_copy(
                    src_ref=src,
                    dst_ref=dst,
                    send_sem=send.at[k],
                    recv_sem=recv.at[k],
                    device_id=target,
                    device_id_type=MESH,
                ),
            )
        )

    has_up, has_down = lat > 0, lat < nlat - 1
    up, down = lat - 1, lat + 1
    add(rows.at[:, 0], rowh.at[:, 1], (up, lon), 2, has_up, has_down)
    add(rows.at[:, 1], rowh.at[:, 0], (down, lon), 3, has_down, has_up)
    add(cols.at[0], colh.at[1], (lat, west), 0, None, None)
    add(cols.at[1], colh.at[0], (lat, east), 1, None, None)
    add(corners.at[0, 0], cornh.at[1, 1], (up, west), 4, has_up, has_down)
    add(corners.at[0, 1], cornh.at[1, 0], (up, east), 5, has_up, has_down)
    add(corners.at[1, 0], cornh.at[0, 1], (down, west), 6, has_down, has_up)
    add(corners.at[1, 1], cornh.at[0, 0], (down, east), 7, has_down, has_up)
    if trow is not None:
        add(trow.at[0], trowh.at[1], (up, lon), 8, has_up, has_down)
        add(trow.at[1], trowh.at[0], (down, lon), 9, has_down, has_up)
    return out


def start_halo(copies):
    for sends, _, copy in copies:
        if sends is None:
            copy.start()
        else:
            pl.when(sends)(copy.start)


def wait_halo(copies):
    for sends, gets, copy in copies:
        if sends is None:
            copy.wait()
        else:
            pl.when(sends)(copy.wait_send)
            pl.when(gets)(copy.wait_recv)


def for_others(mesh, body):
    nlat, nlon = mesh.shape["lat"], mesh.shape["lon"]
    lat, lon = lax.axis_index("lat"), lax.axis_index("lon")
    beside = [(lon + b) & (nlon - 1) for b in range(nlon)]
    for x in beside[1:]:
        body((lat, x), lat * nlon + x)

    def row(a, carry):
        y = (lat + a) & (nlat - 1)
        for x in beside:
            body((y, x), y * nlon + x)
        return carry

    lax.fori_loop(1, nlat, row, 0)


def greet_all(mesh):
    barrier = pltpu.get_barrier_semaphore()

    def hello(target, d):
        pl.semaphore_signal(barrier, inc=1, device_id=target, device_id_type=MESH)

    for_others(mesh, hello)
    pl.semaphore_wait(barrier, mesh.shape["lat"] * mesh.shape["lon"] - 1)


def greet(bits, halo):
    barrier = pltpu.get_barrier_semaphore()
    lat, lon, nlat, nlon, east, west = neighbours()

    def hello(target):
        pl.semaphore_signal(barrier, inc=1, device_id=target, device_id_type=MESH)

    count = 0
    for axis, bit in bits:
        hello(partner(axis, bit))
        count += 1
    if halo:
        for target in ((lat, east), (lat, west)):
            hello(target)
            count += 1
        for side, cond in ((lat - 1, lat > 0), (lat + 1, lat < nlat - 1)):

            @pl.when(cond)
            def _(side=side):
                for x in (lon, east, west):
                    hello((side, x))

    if halo:
        count = count + 3 * (lat > 0).astype(jnp.int32) + 3 * (lat < nlat - 1).astype(jnp.int32)
    pl.semaphore_wait(barrier, count)


class Gather:
    def __init__(self, mesh, share, buf, early, send, recv, bsend, brecv):
        self.bits = bit_list(mesh)
        self.n = len(self.bits)
        self.orders = stage_orders(mesh)
        self.mine = my_bits(self.bits)
        self.share, self.buf, self.early = share, buf, early
        self.send, self.recv, self.bsend, self.brecv = send, recv, bsend, brecv
        rows = share.shape[0]
        cut = (rows * 2 // 3 + 15) // 16 * 16
        self.spans = [(0, cut), (cut, rows - cut)]
        self.roots, self.start = early_shards(1 << self.n, rows)

    def own(self, sem):
        return pltpu.make_async_copy(self.share, self.buf.at[tuple(self.mine)], sem)

    def copy(self, colour, k):
        order = self.orders[colour]
        index = tuple(
            slice(None) if i in order[:k] else self.mine[i] for i in range(self.n)
        ) + (pl.ds(*self.spans[colour]),)
        return pltpu.make_async_remote_copy(
            src_ref=self.buf.at[index],
            dst_ref=self.buf.at[index],
            send_sem=self.send.at[colour, k],
            recv_sem=self.recv.at[colour, k],
            device_id=partner(*self.bits[order[k]]),
            device_id_type=MESH,
        )

    def advance(self, k):
        for colour in range(2):
            self.copy(colour, k).wait()
            if k + 1 < self.n:
                self.copy(colour, k + 1).start()

    def same(self, root, indices):
        cond = True
        for i in indices:
            cond = jnp.logical_and(cond, self.mine[i] == ((root >> (self.n - 1 - i)) & 1))
        return cond

    def early_own(self, sem):
        for r, root in enumerate(self.roots):

            @pl.when(self.same(root, range(self.n)))
            def _(r=r):
                rows = self.share.shape[0] - self.start
                copy = pltpu.make_async_copy(
                    self.share.at[pl.ds(self.start, rows)], self.early.at[r], sem
                )
                copy.start()
                copy.wait()

    def early_copies(self, k):
        order = self.orders[0]
        for r, root in enumerate(self.roots):
            sends = self.same(root, order[k:])
            now = order[k]
            other = self.mine[now] != ((root >> (self.n - 1 - now)) & 1)
            gets = jnp.logical_and(other, self.same(root, order[k + 1 :]))
            yield sends, gets, pltpu.make_async_remote_copy(
                src_ref=self.early.at[r],
                dst_ref=self.early.at[r],
                send_sem=self.bsend.at[r, k],
                recv_sem=self.brecv.at[r, k],
                device_id=partner(*self.bits[now]),
                device_id_type=MESH,
            )

    def early_start(self, k):
        for sends, _, copy in self.early_copies(k):
            pl.when(sends)(copy.start)

    def early_wait(self, k):
        for sends, gets, copy in self.early_copies(k):
            pl.when(sends)(copy.wait_send)
            pl.when(gets)(copy.wait_recv)


def early_shards(devices, shard_rows):
    roots = list(range(TAIL_ROW // shard_rows, (END_FLAT - 1) // LANES // shard_rows + 1))
    start = (TAIL_ROW - roots[0] * shard_rows) // 16 * 16 if len(roots) == 1 else 0
    return roots, start


def gather_plan(n):
    if n == 5:
        return {0: (0, -1), 1: (1, -1), 2: (2, 8), 3: (4, 14)}
    return {}


def norm_parts(x):
    mean = jnp.mean(x, -1, keepdims=True)
    center = x - mean
    var = jnp.mean(center * center, -1, keepdims=True)
    return center, lax.rsqrt(var + 1e-05)


def rounded(v):
    return v.astype(BF16).astype(F32)


def stencil_fwd_kernel(
    mesh, chunks, cells, height_ref, x_ref, share, cols, edge, corners, trow, table, aug,
    out_ref, mix_hbm, w1, w2, wd, small, trowh,
    m_scr, k_scr, nt_scr, mix_scr, wnf, wn, colh, rowh, cornh, trh, buf, early, flat, eflat,
    send, recv, bsend, brecv, hsend, hrecv, own_sem, mix_sem,
):
    gather = Gather(mesh, share, buf, early, send, recv, bsend, brecv)
    n = gather.n
    plan = gather_plan(n)
    step = pl.program_id(0)
    rows = x_ref.shape[1]
    width = chunks * cells
    height = height_ref[0]
    shard_rows = share.shape[0]
    halos = lambda: halo_copies(cols, edge, corners, colh, rowh, cornh, hsend, hrecv, trow, trh)
    mix_copy = lambda: pltpu.make_async_copy(mix_scr, mix_hbm, mix_sem)

    @pl.when(step == 0)
    def _():
        gather.own(own_sem).start()
        gather.early_own(mix_sem)
        gather.own(own_sem).wait()
        greet(gather.bits, True)
        gather.early_start(0)
        for colour in range(2):
            gather.copy(colour, 0).start()
        start_halo(halos())

    for k in range(n):

        @pl.when(step == min(k + 1, chunks))
        def _(k=k):
            gather.early_wait(k)
            if k + 1 < n:
                gather.early_start(k + 1)

    @pl.when(step < chunks)
    def _():
        def cell(j, carry):
            x = x_ref[j].astype(F32)
            mean = jnp.mean(x, -1, keepdims=True)
            center = x - mean
            inv = lax.rsqrt(jnp.mean(center * center, -1, keepdims=True) + 1e-05)
            normed = center * inv
            at = pl.ds((step * cells + j + REACH) * SLOTS + 1, rows)
            for g in range(CB):
                lo, hi = g * LANES, min((g + 1) * LANES, C)
                m_scr[g, at, : hi - lo] = normed[:, lo:hi]
            return carry

        lax.fori_loop(0, cells, cell, 0, unroll=10)

    @pl.when(step == chunks)
    def _():
        base = gather.roots[0] * shard_rows + gather.start
        count = shard_rows - gather.start
        eflat[...] = jnp.zeros_like(eflat)
        for r in range(len(gather.roots)):
            eflat[r * count : (r + 1) * count, :] = early[r].astype(F32)
        unpack_small(eflat, base, wn, wd, small, wnf)
        if 0 in plan:
            gather.advance(0)
        k_scr[...] = jnp.dot(
            table[...], wd[...], preferred_element_type=F32, precision=HIGHEST
        ).reshape(k_scr.shape)
        gvec = small[2:3, :C]
        groups = [(q, q * LANES, min((q + 1) * LANES, C)) for q in range(CB)]
        hrow = iota((rows, LANES), 0)
        lanes = slice((CB - 1) * LANES, CB * LANES)
        mix_scr[:, :, lanes] = jnp.zeros((width, rows, LANES), BF16)

        def scale(i, carry):
            for u in range(REUSE):
                column = i * REUSE + u
                body = pl.ds((column + REACH) * SLOTS + 1, rows)
                for q, lo, hi in groups:
                    wide = slice(0, hi - lo)
                    v = rounded(m_scr[q, body, wide] * gvec[:, lo:hi])
                    v = jnp.where(hrow[:, wide] < height, v, 0.0)
                    mix_scr[column, :, lo:hi] = v.astype(BF16)
                    m_scr[q, body, wide] = v
            return carry

        lax.fori_loop(0, width // REUSE, scale, 0)
        mix_copy().start()
        lat, _, nlat, *_ = neighbours()
        wait_halo(halos())
        keep = (lat > 0, lat < nlat - 1)
        for r in range(2):
            trowh[r] = jnp.where(keep[r], trh[r], 0.0)

        def mix(v):
            center, inv = norm_parts(v.astype(F32))
            return rounded(center * inv * gvec)

        def beside(ref):
            return [jnp.where(keep[r], mix(ref(r)), 0.0) for r in range(2)]

        def put(column, top, low, fresh=None):
            at = column * SLOTS
            for q, lo, hi in groups:
                body = pl.ds(at + 1, rows)
                wide = slice(0, hi - lo)
                if fresh is None:
                    v = m_scr[q, body, wide]
                else:
                    v = jnp.where(hrow[:, wide] < height, fresh[:, lo:hi], 0.0)
                m_scr[q, body, wide] = jnp.where(hrow[:, wide] == height, low[:, lo:hi], v)
                m_scr[q, pl.ds(at, 1), wide] = top[:, lo:hi]
                m_scr[q, pl.ds(at + rows + 1, 1), wide] = low[:, lo:hi]

        for side in range(2):
            top, low = beside(lambda r: cornh[r, side])
            for i in range(REACH):
                column = i if side == 0 else width + REACH + i
                put(column, top[i : i + 1], low[i : i + 1], mix(colh[side, i]))

        def strip(c, carry):
            tops, lows = beside(lambda r: rowh[c, r])
            for i in range(cells):
                put(c * cells + i + REACH, tops[i : i + 1], lows[i : i + 1])
            return carry

        lax.fori_loop(0, chunks, strip, 0)

    for k, (at, loop) in plan.items():
        if k > 0 and loop < 0:

            @pl.when(step == chunks + at)
            def _(k=k):
                gather.advance(k)

    @pl.when(step >= chunks)
    def _():
        first = (step - chunks) * cells
        nt_scr[...] = jnp.dot(
            aug[...].reshape(cells * rows, LANES), wn[...], preferred_element_type=F32
        )
        lane = iota((8, LANES), 1)
        for g in range(CB):
            lanes = slice(g * LANES, (g + 1) * LANES)
            for hb in range(rows // 8):
                at = slice(8 * hb, 8 * hb + 8)

                def cell(i, carry):
                    j = i * REUSE
                    acc = [nt_scr[pl.ds((j + u) * rows + 8 * hb, 8), lanes] for u in range(REUSE)]
                    for l in range(3):
                        near = [
                            m_scr[g, pl.ds((first + j + u) * SLOTS + 8 * hb + l, 8), :]
                            for u in range(REUSE + 2 * REACH)
                        ]
                        for w in range(5):
                            tap = k_scr[5 * l + w, at, lanes]
                            acc = [a + tap * near[u + w] for u, a in enumerate(acc)]
                    for u in range(REUSE):
                        v = acc[u]
                        if g == CB - 1:
                            v = jnp.where(lane == 0, v, aug[j + u, at, :].astype(F32))
                        out_ref[j + u, at, lanes] = v.astype(BF16)
                    return carry

                lax.fori_loop(0, cells // REUSE, cell, 0)
                for k, (past, loop) in plan.items():
                    if loop == g * (rows // 8) + hb:

                        @pl.when(step == chunks + past)
                        def _(k=k):
                            gather.advance(k)

    @pl.when(step == 2 * chunks - 1)
    def _():
        for k in range(n):
            if k not in plan:
                gather.advance(k)
        total = 1 << n

        def widen(d, carry):
            index = tuple((d >> (n - 1 - i)) & 1 for i in range(n))
            flat[pl.ds(d * shard_rows, shard_rows), :] = buf[index].astype(F32)
            return carry

        lax.fori_loop(0, total, widen, 0)
        flat[total * shard_rows :, :] = jnp.zeros((flat.shape[0] - total * shard_rows, LANES), F32)
        unpack_weights(flat, w1, w2)
        mix_copy().wait()


def stencil_fwd(mesh, height, x, share, cols, edge, corners, trow, table, aug, chunks):
    width, rows, _ = x.shape
    cells = width // chunks
    assert cells % REUSE == 0
    n = len(bit_list(mesh))
    shard_rows = share.shape[0]
    total = shard_rows << n
    roots, start = early_shards(1 << n, shard_rows)
    count = shard_rows - start
    first = lambda i: jnp.where(i < chunks, i, chunks - 1)
    second = lambda i: jnp.where(i < chunks, 0, i - chunks)
    sd = jax.ShapeDtypeStruct
    by_first = lambda c: pl.BlockSpec((cells, rows, c), lambda i: (first(i), 0, 0))
    by_second = lambda c: pl.BlockSpec((cells, rows, c), lambda i: (second(i), 0, 0))
    dma = pltpu.SemaphoreType.DMA
    return pl.pallas_call(
        partial(stencil_fwd_kernel, mesh, chunks, cells),
        name="stencil_fwd",
        grid=(2 * chunks,),
        out_shape=(
            sd((width, rows, CP), BF16),
            sd((width, rows, CP), BF16),
            sd((CP, FP), BF16),
            sd((FP, CP), BF16),
            sd((16, CP), F32),
            sd((8, FP), F32),
            sd(trow.shape, F32),
        ),
        in_specs=[pl.BlockSpec(memory_space=pltpu.SMEM), by_first(C)]
        + [vmem_spec()] * 6
        + [by_second(LANES)],
        out_specs=(by_second(CP), any_spec())
        + (vmem_spec(),) * 5,
        scratch_shapes=[
            pltpu.VMEM((CB, (width + 2 * REACH) * SLOTS, LANES), F32),
            pltpu.VMEM((TAPS, rows, CP), F32),
            pltpu.VMEM((cells * rows, CP), F32),
            pltpu.VMEM((width, rows, CP), BF16),
            pltpu.VMEM((LANES, CP), F32),
            pltpu.VMEM((LANES, CP), BF16),
            pltpu.VMEM(cols.shape, BF16),
            pltpu.VMEM(edge.shape, BF16),
            pltpu.VMEM(corners.shape, BF16),
            pltpu.VMEM(trow.shape, F32),
            pltpu.VMEM((2,) * n + (shard_rows, LANES), BF16),
            pltpu.VMEM((len(roots), count, LANES), BF16),
            pltpu.VMEM((total + 96, LANES), F32),
            pltpu.VMEM((len(roots) * count + 16, LANES), F32),
            dma((2, n)),
            dma((2, n)),
            dma((len(roots), n)),
            dma((len(roots), n)),
            dma((10,)),
            dma((10,)),
            dma,
            dma,
        ],
        compiler_params=params(
            dimension_semantics=("arbitrary",), collective_id=0, has_side_effects=True
        ),
    )(height, x, share, cols, edge, corners, trow, table, aug)


def pack_weights(one, two, flat):
    lane = iota((8, LANES), 1)
    row = iota((8, LANES), 0)
    flat[...] = jnp.zeros_like(flat)

    def turned(v, first, unit):
        return pltpu.roll(v, first, 1, stride=unit, stride_axis=0)

    def main(ref, at, first, unit, out, base, step, count):
        keep = lane >= first + unit * row
        before = jnp.zeros((8, LANES), F32)
        for q in range(count):
            now = turned(ref[q, at, :], first, unit)
            flat[pl.ds(base + q, 8, stride=step), :] = jnp.where(keep, now, before)
            before = now

    def rest(ref, at, first, unit, count, width, mask=None):
        s = first + unit * row
        before = turned(ref[count - 1, at, :], first, unit)
        now = turned(ref[count, at, :], first, unit)
        v = jnp.where(lane < s, before, jnp.where(lane < s + width, now, 0.0))
        return v if mask is None else jnp.where(mask, v, 0.0)

    shift = 8 - LANE_TWO
    base_two = ROW_TWO - 5 * LANE_TWO
    full = FF // LANES
    extra = C - (CB - 1) * LANES

    def two_main(b, carry):
        for k in range(16):
            at = pl.ds(128 * b + 8 * k + shift, 8)
            main(two, at, 8 * k, 1, flat, base_two + 641 * b + 40 * k, 5, CB - 1)
        return carry

    lax.fori_loop(0, full, two_main, 0)
    end = slice(128 * full + shift, 128 * full + shift + 8)
    mask = row < FF - full * LANES + LANE_TWO
    before = jnp.zeros((8, LANES), F32)
    for q in range(CB - 1):
        now = jnp.where(mask, turned(two[q, end, :], 0, 1), 0.0)
        at = pl.ds(base_two + 641 * full + q, 8, stride=5)
        flat[at, :] = jnp.where(lane >= row, now, before)
        before = now

    def one_main(b, carry):
        for k in range(8):
            at = pl.ds(pl.multiple_of(64 * b + 8 * k, 8), 8)
            main(one, at, 16 * k, 2, flat, 641 * b + 80 * k, 10, FB - 1)
        return carry

    last = C - 1
    assert last % 64 == 0
    lax.fori_loop(0, last // 64, one_main, 0)
    row_last = 641 * (last // 64)
    for q in range(FB - 1):
        flat[row_last + q : row_last + q + 1, :] = one[q, last : last + 1, :]

    def add_all(places, values):
        olds = [flat[at, :] for at in places]
        for at, old, v in zip(places, olds, values):
            flat[at, :] = old + v

    def one_rest(b, carry):
        values = [
            rest(one, pl.ds(pl.multiple_of(64 * b + 8 * k, 8), 8), 16 * k, 2, FB - 1, FF - (FB - 1) * LANES)
            for k in range(8)
        ]
        add_all([pl.ds(641 * b + 80 * k + FB - 1, 8, stride=10) for k in range(8)], values)
        return carry

    lax.fori_loop(0, last // 64, one_rest, 0)
    lane1 = iota((1, LANES), 1)
    v = jnp.where(lane1 < FF - (FB - 1) * LANES, one[FB - 1, last : last + 1, :], 0.0)
    add_all([slice(row_last + FB - 1, row_last + FB)], [v])

    def two_rest(b, carry):
        values = [
            rest(two, pl.ds(128 * b + 8 * k + shift, 8), 8 * k, 1, CB - 1, extra) for k in range(16)
        ]
        places = [pl.ds(base_two + 641 * b + 40 * k + CB - 1, 8, stride=5) for k in range(16)]
        add_all(places, values)
        return carry

    lax.fori_loop(0, full, two_rest, 0)
    add_all(
        [pl.ds(base_two + 641 * full + CB - 1, 8, stride=5)],
        [rest(two, end, 0, 1, CB - 1, extra, mask)],
    )


GELU_A = math.sqrt(2.0 / math.pi)
GELU_B = 0.044715
WIDE = 256


def dot(a, b, dims=((1,), (0,))):
    return lax.dot_general(a, b, (dims, ((), ())), preferred_element_type=F32)


def mlp_kernel(
    blocks, height_ref, conv_ref, g_ref, x_ref, w1, w2, small,
    out_ref, gconv_ref, rows_ref, cols_ref, corn_ref, shards_ref, extra_ref,
    one, two, g_scr, conv_t, act, gh, flat, w1_rest,
):
    step = pl.program_id(0)
    cells, rows, _ = x_ref.shape
    m = cells * rows
    height = height_ref[0]

    @pl.when(step == 0)
    def _():
        one[...] = jnp.zeros_like(one)
        two[...] = jnp.zeros_like(two)
        g_scr[...] = jnp.zeros_like(g_scr)
        w1_rest[...] = w1[:, FP // WIDE * WIDE :].astype(F32).T[: w1_rest.shape[0]]

    live = (iota((1, rows, 1), 1) < height).astype(F32)
    g_scr[:, :C] = (g_ref[...].astype(F32) * live).reshape(m, C).astype(BF16)
    rows_one = conv_t.shape[0]

    def hidden(start, wide, tail):
        lanes = pl.ds(start, wide)
        h = dot(conv_ref[...].reshape(m, CP), w1[:, lanes]) + small[0:1, lanes]
        ga = dot(g_scr[...], w2[lanes, :], ((1,), (1,)))
        h2 = h * h
        t = jnp.tanh(h * (GELU_A + (GELU_A * GELU_B) * h2))
        cdf = 0.5 * t + 0.5
        value = (h * cdf).astype(BF16)
        slope = cdf + h * (0.5 - 0.5 * (t * t)) * (GELU_A + (3 * GELU_A * GELU_B) * h2)
        if tail:
            ones = iota((m, wide), 1) == FF - (FB - 1) * LANES
            value = jnp.where(ones, jnp.ones_like(value), value)
        act[:, lanes] = value
        gh[:, lanes] = (ga * slope).astype(BF16)

    def turn(i, count):
        part = conv_ref[:, :, pl.ds(i * LANES, LANES)].reshape(m, LANES)
        conv_t[pl.ds(i * LANES, count), :] = part.T[:count]

    full = FP // WIDE
    assert full == CB - 1
    for f in range(full):
        turn(f, LANES)
        hidden(f * WIDE, WIDE, False)
    turn(CB - 1, rows_one - (CB - 1) * LANES)
    hidden(full * WIDE, FP % WIDE, True)

    main = full * WIDE
    spare = [
        (act[:, main + i : main + i + 1].astype(F32), gh[:, main + i : main + i + 1].astype(F32))
        for i in range(FF - main)
    ]
    for n in range(CP // WIDE):
        lanes = slice(n * WIDE, (n + 1) * WIDE)
        end = min((n + 1) * WIDE, C)
        part = slice(n * WIDE, end)
        branch = dot(act[:, :main], w2[:main, lanes])
        gc = dot(gh[:, :main], w1[lanes, :main], ((1,), (1,)))
        for i, (a, b) in enumerate(spare):
            branch = branch + a * w2[main : main + 16, lanes].astype(F32)[i : i + 1]
            gc = gc + b * w1_rest[i : i + 1, lanes]
        v = x_ref[:, :, part].astype(F32).reshape(m, -1) + branch[:, : end - n * WIDE] + small[1:2, part]
        out_ref[:, :, part] = (v.reshape(cells, rows, -1) * live).astype(BF16)
        for i in range(WIDE // LANES):
            gconv_ref[n * (WIDE // LANES) + i] = gc[:, i * LANES : (i + 1) * LANES]

    def weights(start, wide):
        lanes = pl.ds(start, wide)
        r1 = dot(conv_t[...], gh[:, lanes])
        r2 = dot(act[:, lanes], g_scr[...], ((0,), (0,)))
        for i in range(wide // LANES):
            one[start // LANES + i] += r1[:, i * LANES : (i + 1) * LANES]
        for q in range(CB):
            two[q, pl.ds(start + 8, wide), :] += r2[:, q * LANES : (q + 1) * LANES]

    def third(f, carry):
        weights(pl.multiple_of(f * WIDE, WIDE), WIDE)
        return carry

    lax.fori_loop(0, FP // WIDE, third, 0)
    weights(FP // WIDE * WIDE, FP % WIDE)

    whole, left = divmod(cells, 8)
    for r, slot in ((0, 0), (1, height - 1)):
        for q in range(CB):
            lanes = slice(q * LANES, (q + 1) * LANES)
            pick = lambda c: gconv_ref[q, pl.ds(slot + c * rows, 8, stride=rows), :]
            v = [pick(8 * i) for i in range(whole)]
            if left:
                v.append(pltpu.roll(pick(cells - 8), left, 0))
            v = jnp.concatenate(v, 0).astype(BF16)
            rows_ref[0, r, :, lanes] = v
            for side, at, first in ((0, 0, 0), (1, blocks - 1, cells - REACH)):

                @pl.when(step == at)
                def _(side=side, first=first, v=v, lanes=lanes, r=r):
                    corn_ref[r, side, :, lanes] = v[first : first + REACH]

    for side, at, first in ((0, 0, 0), (1, blocks - 1, cells - REACH)):

        @pl.when(step == at)
        def _(side=side, first=first):
            for i in range(REACH):
                base = (first + i) * rows
                for q in range(CB):
                    lanes = slice(q * LANES, (q + 1) * LANES)
                    cols_ref[side, i, :, lanes] = gconv_ref[q, base : base + rows, :].astype(BF16)

    @pl.when(step == blocks - 1)
    def _():
        extra_ref[...] = jnp.zeros_like(extra_ref)
        for q in range(FB):
            extra_ref[0 : NOISE + 1, q * LANES : (q + 1) * LANES] = one[q, C : C + NOISE + 1, :]
        for q in range(CB):
            lanes = slice(q * LANES, (q + 1) * LANES)
            extra_ref[NOISE + 1 : NOISE + 2, lanes] = two[q, FF + 8 : FF + 9, :]
        pack_weights(one, two, flat)
        bits = len(shards_ref.shape) - 2
        shard_rows = shards_ref.shape[-2]

        def store(d, carry):
            index = tuple((d >> (bits - 1 - i)) & 1 for i in range(bits))
            shards_ref[index] = flat[pl.ds(d * shard_rows, shard_rows), :]
            return carry

        lax.fori_loop(0, 1 << bits, store, 0)


def mlp(height, conv, g, x, w1, w2, small, shards, blocks):
    width, rows, _ = x.shape
    cells = width // blocks
    m = cells * rows
    sd = jax.ShapeDtypeStruct
    block = lambda c: pl.BlockSpec((cells, rows, c), lambda i: (i, 0, 0))
    rows_one = -(-(C + NOISE + 1) // 16) * 16
    flops = 12 * width * rows * C * FF
    return pl.pallas_call(
        partial(mlp_kernel, blocks),
        name="mlp",
        grid=(blocks,),
        out_shape=(
            sd((width, rows, C), BF16),
            sd((CB, width * rows, LANES), F32),
            sd((blocks, 2, -(-cells // 8) * 8, CP), BF16),
            sd((2, REACH, rows, CP), BF16),
            sd((2, 2, REACH, CP), BF16),
            sd(shards, F32),
            sd((16, FP), F32),
        ),
        in_specs=[
            pl.BlockSpec(memory_space=pltpu.SMEM),
            block(CP),
            block(C),
            block(C),
            vmem_spec(),
            vmem_spec(),
            vmem_spec(),
        ],
        out_specs=(
            block(C),
            pl.BlockSpec((CB, m, LANES), lambda i: (0, i, 0)),
            pl.BlockSpec((1, 2, -(-cells // 8) * 8, CP), lambda i: (i, 0, 0, 0)),
            vmem_spec(),
            vmem_spec(),
            vmem_spec(),
            vmem_spec(),
        ),
        scratch_shapes=[
            pltpu.VMEM((FB, rows_one, LANES), F32),
            pltpu.VMEM((CB, FP + 16, LANES), F32),
            pltpu.VMEM((m, CP), BF16),
            pltpu.VMEM((rows_one, m), BF16),
            pltpu.VMEM((m, FP), BF16),
            pltpu.VMEM((m, FP), BF16),
            pltpu.VMEM((math.prod(shards[:-1]), LANES), F32),
            pltpu.VMEM((8, CP), F32),
        ],
        compiler_params=params(dimension_semantics=("arbitrary",)),
        cost_estimate=pl.CostEstimate(flops=flops, bytes_accessed=50_000_000, transcendentals=0),
    )(height, conv, g, x, w1, w2, small)


def add_vector(tail, offset, value):
    row, shift = divmod(offset - TAIL_ROW * LANES, LANES)
    blocks = value.shape[0]
    lane = iota((blocks + 1, LANES), 1)
    zero = jnp.zeros((1, LANES), F32)
    here = pltpu.roll(jnp.concatenate([value, zero], 0), shift, 1) if shift else jnp.concatenate([value, zero], 0)
    back = jnp.concatenate([zero, here[:blocks]], 0)
    at = slice(row, row + blocks + 1)
    tail[at, :] = tail[at, :] + jnp.where(lane >= shift, here, back if shift else here)


def as_blocks(value, length):
    blocks = -(-length // LANES)
    v = jnp.concatenate([value[:, q * LANES : (q + 1) * LANES] for q in range(blocks)], 0)
    index = iota((blocks, LANES), 0) * LANES + iota((blocks, LANES), 1)
    return jnp.where(index < length, v, 0.0)


class Scatter:
    def __init__(self, mesh, shards, buf, recvs, send, recv):
        self.bits = bit_list(mesh)
        self.n = len(self.bits)
        self.orders = scatter_orders(mesh)
        self.first = self.orders[0][0]
        assert all(order[0] == self.first for order in self.orders)
        self.mine = my_bits(self.bits)
        self.shards, self.buf, self.recvs = shards, buf, recvs
        self.send, self.recv = send, recv
        rows = shards.shape[-2]
        one, two = (int(rows * f) // 8 * 8 for f in (0.36, 0.71))
        self.spans = [(0, one), (one, two - one), (two, rows - two)]

    def copy(self, colour, k):
        order, mine, n = self.orders[colour], self.mine, self.n
        done, now = order[:k], order[k]
        at = (pl.ds(*self.spans[colour]),)
        index = tuple(
            1 - mine[i] if i == now else mine[i] if i in done else slice(None) for i in range(n)
        )
        if k == 0:
            src = self.shards.at[index + at]
        else:
            src = self.buf.at[tuple(v for i, v in enumerate(index) if i != self.first) + at]
        return pltpu.make_async_remote_copy(
            src_ref=src,
            dst_ref=self.recvs[k].at[(slice(None),) * (n - 1 - k) + at],
            send_sem=self.send.at[colour, k],
            recv_sem=self.recv.at[colour, k],
            device_id=partner(*self.bits[now]),
            device_id_type=MESH,
        )

    def load(self, sem):
        index = tuple(self.mine[i] if i == self.first else slice(None) for i in range(self.n))
        return pltpu.make_async_copy(self.shards.at[index], self.buf, sem)

    def advance(self, colour, k):
        self.copy(colour, k).wait()
        order, n = self.orders[colour], self.n
        free = [i for i in range(n) if i not in order[: k + 1]]
        at = (pl.ds(*self.spans[colour]),)

        def add(d, carry):
            sub = tuple((d >> (len(free) - 1 - i)) & 1 for i in range(len(free)))
            index = tuple(
                sub[free.index(i)] if i in free else self.mine[i]
                for i in range(n)
                if i != self.first
            )
            self.buf[index + at] = self.buf[index + at] + self.recvs[k][sub + at]
            return carry

        lax.fori_loop(0, 1 << len(free), add, 0)
        if k + 1 < n:
            self.copy(colour, k + 1).start()

    def result(self):
        return self.buf[tuple(v for i, v in enumerate(self.mine) if i != self.first)]


def scatter_plan(n):
    if n == 5:
        return {
            7: [(0, 1), (1, 1), (2, 1)],
            12: [(0, 2), (1, 2)],
            13: [(2, 2)],
            17: [(0, 3), (1, 3), (2, 3)],
        }
    return {}


class Tail:
    def __init__(self, mesh, pieces, got, msg, full, place, send, recv):
        self.mesh = mesh
        self.n = mesh.shape["lat"] * mesh.shape["lon"]
        self.lat, self.lon = lax.axis_index("lat"), lax.axis_index("lon")
        self.me = self.lat * mesh.shape["lon"] + self.lon
        self.pieces, self.got, self.msg, self.full, self.place = pieces, got, msg, full, place
        self.send, self.recv = send, recv

    def others(self, source, target, k):
        def send(device, d):
            pltpu.make_async_remote_copy(
                src_ref=source(d),
                dst_ref=target.at[self.me],
                send_sem=self.send.at[k],
                recv_sem=self.recv.at[k],
                device_id=device,
                device_id_type=MESH,
            ).start()

        for_others(self.mesh, send)

    def wait_all(self, buffer, k):
        pltpu.make_async_remote_copy(
            src_ref=buffer.at[pl.ds(0, self.n - 1)],
            dst_ref=buffer.at[pl.ds(0, self.n - 1)],
            send_sem=self.send.at[k],
            recv_sem=self.recv.at[k],
            device_id=(self.lat, self.lon),
            device_id_type=MESH,
        ).wait()

    def scatter(self, flat):
        piece = self.pieces.shape[1]

        def split(d, carry):
            self.pieces[d] = flat[pl.ds(d * piece, piece), :]
            return carry

        lax.fori_loop(0, self.n, split, 0)
        self.others(lambda d: self.pieces.at[d], self.got, 0)
        self.got[self.me] = self.pieces[self.me]
        self.place[...] = jnp.zeros_like(self.place)

    def finish(self, part, own_gain, grad_ref, norm_ref):
        n, piece = self.n, self.pieces.shape[1]
        shard_rows = part.shape[0]
        square = jnp.sum(part * part)
        self.wait_all(self.got, 0)
        total = lax.fori_loop(1, n, lambda i, acc: acc + self.got[i], self.got[0])
        square = square + jnp.sum(total * total)
        self.msg[0:piece, :] = total
        self.msg[piece : piece + 1, :] = jnp.broadcast_to(square, (1, LANES))
        self.msg[piece + 1 :, :] = own_gain
        self.others(lambda d: self.msg, self.full, 1)
        self.full[self.me] = self.msg[...]
        self.wait_all(self.full, 1)

        def take(d, acc):
            self.place[pl.ds(shard_rows + d * piece, piece), :] = self.full[d, 0:piece, :]
            return acc + self.full[d, piece:, :]

        sums = lax.fori_loop(0, n, take, jnp.zeros((1 + CB, LANES), F32))
        gain = sums[1:]
        add_vector(self.place, OFF_GAIN + shard_rows * LANES, gain)
        squares = sums[:1] + jnp.sum(gain * gain)
        start = jnp.clip(self.me * shard_rows - TAIL_ROW + shard_rows, 0, shard_rows + n * piece)
        grad_ref[...] = part + self.place[pl.ds(start, shard_rows), :]
        norm_ref[...] = jnp.broadcast_to(jnp.sqrt(squares), norm_ref.shape)


def backward_kernel(
    mesh, chunks, cells, strip_cells, height_ref, mix_ref, gconv_ref, x_hbm, g_hbm,
    cols, edge, corners, table, trowh, wd, gain, extra, w1, shards,
    out_ref, grad_ref, norm_ref,
    x_scr, up_scr, st_scr, g_scr, m_scr, k_scr, t_scr, e_scr, gg_scr, tail_scr, colh, rowh, cornh,
    pieces, got, msg, full, place, buf, *rest,
):
    n = len(bit_list(mesh))
    recvs, (send, recv, hsend, hrecv, tsend, trecv, load_sem) = rest[:n], rest[n:]
    scatter = Scatter(mesh, shards, buf, recvs, send, recv)
    tail = Tail(mesh, pieces, got, msg, full, place, tsend, trecv)
    step = pl.program_id(0)
    width, rows, _ = mix_ref.shape
    height = height_ref[0]
    plan = scatter_plan(n)
    gvec = gain[2:3, :C]
    halos = lambda: halo_copies(cols, edge, corners, colh, rowh, cornh, hsend, hrecv)
    load_x = lambda: pltpu.make_async_copy(x_hbm, x_scr, load_sem.at[1])
    load_up = lambda: pltpu.make_async_copy(g_hbm, up_scr, load_sem.at[2])

    @pl.when(step == 0)
    def _():
        load_x().start()
        greet_all(mesh)
        start_halo(halos())
        for colour in range(3):
            scatter.copy(colour, 0).start()
        scatter.load(load_sem.at[0]).start()
        load_up().start()
        hrow = iota((rows, 16), 0)
        for t in range(TAPS):
            l = t // 5
            own = table[t * rows : (t + 1) * rows, :]
            if l == 0:
                own = jnp.concatenate([own[1:], own[:1]], 0)
                own = jnp.where(hrow == height - 1, trowh[1, t : t + 1, :], own)
            if l == 2:
                own = jnp.concatenate([trowh[0, t : t + 1, :], own[: rows - 1]], 0)
            t_scr[t * rows : (t + 1) * rows, :] = own
        kernel = jnp.dot(t_scr[...], wd[...], preferred_element_type=F32, precision=HIGHEST)
        for q in range(CB):
            k_scr[q] = kernel[:, q * LANES : (q + 1) * LANES].reshape(k_scr.shape[1:])
        e_scr[...] = jnp.zeros_like(e_scr)
        gg_scr[...] = jnp.zeros_like(gg_scr)
        load_x().wait()
        first_lane = iota((rows, LANES), 1) == 0

        def stats(j, carry):
            x = x_scr[j].astype(F32)
            mean = jnp.mean(x, -1, keepdims=True)
            center = x - mean
            inv = lax.rsqrt(jnp.mean(center * center, -1, keepdims=True) + 1e-05)
            st_scr[j] = jnp.where(first_lane, mean, inv)
            return carry

        lax.fori_loop(0, width, stats, 0, unroll=10)
        tail_scr[...] = jnp.zeros_like(tail_scr)
        add_vector(tail_scr, OFF_B1, as_blocks(extra[NOISE : NOISE + 1, :], FF))
        add_vector(tail_scr, OFF_B2, as_blocks(extra[NOISE + 1 : NOISE + 2, :], C))
        ng = extra[0:NOISE, :]
        hi = ng.astype(BF16)
        mid = (ng - hi.astype(F32)).astype(BF16)
        lo = (ng - hi.astype(F32) - mid.astype(F32)).astype(BF16)
        parts = [dot(p, w1[...], ((1,), (1,))) for p in (hi, mid, lo)]
        gn = parts[0] + parts[1] + parts[2]
        for k in range(NOISE):
            add_vector(tail_scr, OFF_NOISE + k * C, as_blocks(gn[k : k + 1, :], C))

    @pl.when(step == 1)
    def _():
        wait_halo(halos())
        scatter.load(load_sem.at[0]).wait()
        for colour in range(3):
            scatter.advance(colour, 0)

    @pl.when((step >= 1) & (step <= CB))
    def _():
        q = step - 1
        lanes = pl.ds(pl.multiple_of(q * LANES, LANES), LANES)
        lat, _, nlat, *_ = neighbours()
        keep = (lat > 0, lat < nlat - 1)
        here = iota((rows, LANES), 0) == height

        def put(column, top, low, v):
            at = column * SLOTS
            g_scr[pl.ds(at + 1, rows), :] = jnp.where(here, low, v)
            g_scr[pl.ds(at, 1), :] = top
            g_scr[pl.ds(at + rows + 1, 1), :] = low

        def beside(ref):
            return [jnp.where(keep[r], ref(r).astype(F32), 0.0) for r in range(2)]

        for side in range(2):
            top, low = beside(lambda r: cornh[r, side, :, lanes])
            for i in range(REACH):
                column = i if side == 0 else width + REACH + i
                put(column, top[i : i + 1], low[i : i + 1], colh[side, i, :, lanes].astype(F32))

        def strip(c, carry):
            tops, lows = beside(lambda r: rowh[c, r, :, lanes])
            for i in range(strip_cells):
                j = c * strip_cells + i
                v = gconv_ref[0, pl.ds(pl.multiple_of(j * rows, 8), rows), :]
                put(j + REACH, tops[i : i + 1], lows[i : i + 1], v)
                m_scr[q, j] = mix_ref[j].astype(F32)
            return carry

        lax.fori_loop(0, edge.shape[0], strip, 0)
        for hb in range(rows // 8):
            at = slice(8 * hb, 8 * hb + 8)

            def cell(i, carry):
                j = i * REUSE
                mixed = [m_scr[q, j + u, at, :] for u in range(REUSE)]
                total = [None] * REUSE
                for l in range(3):
                    near = [
                        g_scr[pl.ds((j + u) * SLOTS + 8 * hb + 2 - l, 8), :]
                        for u in range(REUSE + 2 * REACH)
                    ]
                    for w in range(5):
                        t = 5 * l + w
                        tap = k_scr[q, t, at, :]
                        views = near[2 * REACH - w : 2 * REACH - w + REUSE]
                        terms = [tap * v for v in views]
                        total = [a if b is None else a + b for a, b in zip(terms, total)]
                        sums = [m * v for m, v in zip(mixed, views)]
                        while len(sums) > 1:
                            sums = [
                                sums[k] + sums[k + 1] if k + 1 < len(sums) else sums[k]
                                for k in range(0, len(sums), 2)
                            ]
                        e_scr[q, t, at, :] = e_scr[q, t, at, :] + sums[0]
                for u in range(REUSE):
                    m_scr[q, j + u, at, :] = total[u]
                return carry

            lax.fori_loop(0, width // REUSE, cell, 0)
            for loop, events in plan.items():
                if loop % (rows // 8) == hb:

                    @pl.when(q == loop // (rows // 8))
                    def _(events=events):
                        for colour, k in events:
                            scatter.advance(colour, k)

    @pl.when(step == CB)
    def _():
        load_up().wait()
        disco = jnp.concatenate(
            [
                lax.dot_general(
                    t_scr[...], e_scr[q].reshape(TAPS * rows, LANES), (((0,), (0,)), ((), ())),
                    preferred_element_type=F32, precision=HIGHEST,
                )
                for q in range(CB)
            ],
            1,
        )
        for k in range(K):
            add_vector(tail_scr, OFF_DISCO + k * C, as_blocks(disco[k : k + 1, :], C))
        tail.scatter(tail_scr)

    @pl.when(step > CB)
    def _():
        first = (step - CB - 1) * cells
        live = iota((rows, C), 0) < height

        def cell(i, total):
            j = first + i
            st = st_scr[j]
            inv = st[:, 1:2]
            normed = (x_scr[j].astype(F32) - st[:, :1]) * inv
            gm = jnp.concatenate([m_scr[q, j] for q in range(CB)], 1)[:, :C]
            gm = jnp.where(live, gm, 0.0)
            total = total + gm * normed
            v = gm * gvec
            mean = jnp.mean(v, -1, keepdims=True)
            mean_n = jnp.mean(v * normed, -1, keepdims=True)
            up = jnp.where(live, up_scr[j].astype(F32), 0.0)
            out_ref[i] = inv * (v - mean - normed * mean_n) + up
            return total

        gg_scr[:, :C] = lax.fori_loop(0, cells, cell, gg_scr[:, :C], unroll=4)

    @pl.when(step == CB + chunks)
    def _():
        own_gain = as_blocks(jnp.sum(gg_scr[...], 0, keepdims=True), C)
        taken = {e for events in plan.values() for e in events}
        for k in range(1, n):
            for colour in range(3):
                if (colour, k) not in taken:
                    scatter.advance(colour, k)
        tail.finish(scatter.result(), own_gain, grad_ref, norm_ref)


def backward(
    mesh, height, mixed, gconv, x, g, cols, edge, corners, table, trowh, wd, small, extra,
    w1, shards, piece, chunks,
):
    width, rows, _ = mixed.shape
    cells = width // chunks
    shard_rows = shards.shape[-2]
    n = len(bit_list(mesh))
    devices = 1 << n
    group = lambda i: jnp.clip(i - 1, 0, CB - 1)
    last = lambda i: jnp.where(i <= CB, 0, i - CB - 1)
    sd = jax.ShapeDtypeStruct
    dma = pltpu.SemaphoreType.DMA
    return pl.pallas_call(
        partial(backward_kernel, mesh, chunks, cells, width // edge.shape[0]),
        name="backward",
        grid=(1 + CB + chunks,),
        out_shape=(
            sd((width, rows, C), F32),
            sd((shard_rows, LANES), F32),
            sd((8, LANES), F32),
        ),
        in_specs=[
            pl.BlockSpec(memory_space=pltpu.SMEM),
            pl.BlockSpec((width, rows, LANES), lambda i: (0, 0, group(i))),
            pl.BlockSpec((1, width * rows, LANES), lambda i: (group(i), 0, 0)),
            any_spec(),
            any_spec(),
        ]
        + [vmem_spec()] * 9
        + [any_spec()],
        out_specs=(
            pl.BlockSpec((cells, rows, C), lambda i: (last(i), 0, 0)),
            vmem_spec(),
            vmem_spec(),
        ),
        scratch_shapes=[
            pltpu.VMEM(x.shape, BF16),
            pltpu.VMEM(x.shape, BF16),
            pltpu.VMEM((width, rows, LANES), F32),
            pltpu.VMEM(((width + 2 * REACH) * SLOTS, LANES), F32),
            pltpu.VMEM((CB, width, rows, LANES), F32),
            pltpu.VMEM((CB, TAPS, rows, LANES), F32),
            pltpu.VMEM((TAPS * rows, 16), F32),
            pltpu.VMEM((CB, TAPS, rows, LANES), F32),
            pltpu.VMEM((rows, CP), F32),
            pltpu.VMEM((devices * piece, LANES), F32),
            pltpu.VMEM(cols.shape, BF16),
            pltpu.VMEM(edge.shape, BF16),
            pltpu.VMEM(corners.shape, BF16),
            pltpu.VMEM((devices, piece, LANES), F32),
            pltpu.VMEM((devices, piece, LANES), F32),
            pltpu.VMEM((piece + 1 + CB, LANES), F32),
            pltpu.VMEM((devices, piece + 1 + CB, LANES), F32),
            pltpu.VMEM((2 * shard_rows + devices * piece + 8, LANES), F32),
            pltpu.VMEM((2,) * (n - 1) + (shard_rows, LANES), F32),
        ]
        + [pltpu.VMEM((2,) * (n - 1 - k) + (shard_rows, LANES), F32) for k in range(n)]
        + [dma((3, n)), dma((3, n)), dma((8,)), dma((8,)), dma((2,)), dma((2,)), dma((3,))],
        compiler_params=params(
            dimension_semantics=("arbitrary",), collective_id=1, has_side_effects=True
        ),
    )(
        height, mixed, gconv, x, g, cols, edge, corners, table, trowh, wd, small, extra, w1, shards,
    )


def stencil_table(support_vals, support_lon):
    rows = support_vals.shape[0]
    vals = support_vals.reshape(rows, S // 3, 3, K)
    offsets = jnp.arange(-REACH, REACH + 1)
    hit = support_lon.reshape(rows, S // 3, 3)[:, :, :, None] == offsets
    picked = jnp.where(hit[:, :, :, :, None], vals[:, :, :, None, :], 0.0)
    return jnp.transpose(jnp.sum(picked, 1), (1, 2, 0, 3))


def flat_table(table):
    t = table.reshape(-1, K)
    return jnp.pad(t, ((0, 0), (0, 16 - K)))


def local(
    mesh, block_in, noise, cotangent, band_heights, support_lon, support_vals,
    master, moment_one, moment_two, average, step_count,
):
    rows, width, _ = block_in.shape
    devices = mesh.shape["lat"] * mesh.shape["lon"]
    shard = master.shape[0]
    shard_rows = shard // LANES
    assert shard_rows * LANES == shard
    flat_rows = shard_rows * devices
    chunks = 6
    cells = width // chunks
    height = lax.dynamic_slice_in_dim(band_heights, lax.axis_index("lat"), 1, 0)
    x = jnp.transpose(block_in, (1, 0, 2))
    g = jnp.transpose(cotangent, (1, 0, 2))

    table = flat_table(stencil_table(support_vals, support_lon))
    planes = table.reshape(TAPS, rows, 16)
    trow = jnp.stack([planes[:, 0], lax.dynamic_index_in_dim(planes, height[0] - 1, 1, keepdims=False)])
    trow = jnp.pad(trow, ((0, 0), (0, 1), (0, 0)))
    share = master.astype(BF16).reshape(shard_rows, LANES)
    edge = jnp.stack([x[:, 0], lax.dynamic_index_in_dim(x, height[0] - 1, 1, keepdims=False)], 1)
    cols = jnp.stack([x[:REACH], x[width - REACH :]])
    corners = jnp.stack([edge[:REACH], edge[width - REACH :]], 0)
    corners = jnp.transpose(corners, (2, 0, 1, 3))
    edge = jnp.transpose(edge.reshape(chunks, cells, 2, C), (0, 2, 1, 3))
    aug = jnp.concatenate(
        [
            jnp.zeros((width, rows, 1), BF16),
            jnp.transpose(noise, (2, 1, 0)),
            jnp.ones((width, rows, 1), BF16),
            jnp.zeros((width, rows, LANES - NOISE - 2), BF16),
        ],
        2,
    )
    conv, mixed, w1, w2, wd, small, trowh = stencil_fwd(
        mesh, height, x, share, cols, edge, corners, trow, table, aug, chunks
    )
    shards = (2,) * len(bit_list(mesh)) + (shard_rows, LANES)
    out, gconv, grow, gcol, gcorn, packed, extra = mlp(
        height, conv, g, x, w1, w2, small, shards, chunks
    )
    piece = -(-(flat_rows - TAIL_ROW) // devices)
    grad_in, grad, norm = backward(
        mesh, height, mixed, gconv, x, g, gcol, grow, gcorn, table, trowh, wd, small,
        extra, w1, packed, piece, 9,
    )
    grad_part = grad.reshape(shard)
    grad_norm = norm[0, :1]
    factor = 0.01 / jnp.maximum(grad_norm, 0.01)
    clipped = grad_part * factor
    new_one = 0.9 * moment_one + 0.1 * clipped
    new_two = 0.999 * moment_two + 0.001 * clipped * clipped
    step_float = step_count[0].astype(F32)
    fix_one = 1.0 - jnp.power(jnp.float32(0.9), step_float)
    fix_two = 1.0 - jnp.power(jnp.float32(0.999), step_float)
    update = new_one / fix_one / (jnp.sqrt(new_two / fix_two) + 1e-08) + 0.1 * master
    new_master = master - 0.02 * update
    new_avg = 0.9 * average + 0.1 * new_master
    return (
        jnp.transpose(out, (1, 0, 2)),
        jnp.transpose(grad_in, (1, 0, 2)),
        grad_part,
        grad_norm,
        new_master,
        new_one,
        new_two,
        new_avg,
        new_master.astype(BF16),
    )


def solution(mesh):
    flat = P(("lat", "lon"))
    field = P("lat", "lon", None)
    return jax.shard_map(
        partial(local, mesh),
        mesh=mesh,
        in_specs=(
            field, P(None, "lat", "lon"), field, P(), P("lat", None), P("lat", None, None),
            flat, flat, flat, flat, P(),
        ),
        out_specs=(field, field, flat, P(), flat, flat, flat, flat, flat),
        check_vma=False,
    )
```

```python
from functools import partial
import math

import jax
import jax.numpy as jnp
from jax import lax
from jax.experimental import pallas as pl
from jax.experimental.pallas import tpu as pltpu
from jax.sharding import PartitionSpec as P

C = 641
FF = 1282
NOISE = 8
K = 9
S = 12
REACH = 2
LANES = 128
CB = 6
CP = CB * LANES
FB = 11
FP = FB * LANES
TAPS = 15
MESH = pl.DeviceIdType.MESH
HIGHEST = lax.Precision.HIGHEST
F32 = jnp.float32
BF16 = jnp.bfloat16
VMEM_LIMIT = 60 * 1024 * 1024
SLOTS = 28
REUSE = 10
ROW_TWO = (C * FF) // LANES
LANE_TWO = (C * FF) % LANES
TAIL_ROW = (2 * C * FF) // LANES
OFF_B1 = 2 * C * FF
OFF_B2 = OFF_B1 + FF
OFF_GAIN = OFF_B2 + C
OFF_DISCO = OFF_GAIN + C
OFF_NOISE = OFF_DISCO + K * C
END_FLAT = OFF_NOISE + NOISE * C


def params(**kw):
    return pltpu.CompilerParams(vmem_limit_bytes=VMEM_LIMIT, **kw)


def any_spec():
    return pl.BlockSpec(memory_space=pl.ANY)


def vmem_spec():
    return pl.BlockSpec(memory_space=pltpu.VMEM)


def iota(shape, dim):
    return lax.broadcasted_iota(jnp.int32, shape, dim)


def bit_list(mesh):
    bits = []
    for axis in ("lat", "lon"):
        count = int(math.log2(mesh.shape[axis]))
        assert 1 << count == mesh.shape[axis]
        bits += [(axis, b) for b in reversed(range(count))]
    return bits


def my_bits(bits):
    ids = {"lat": lax.axis_index("lat"), "lon": lax.axis_index("lon")}
    return [(ids[a] >> b) & 1 for a, b in bits]


def partner(axis, bit):
    lat, lon = lax.axis_index("lat"), lax.axis_index("lon")
    if axis == "lat":
        return (lat ^ (1 << bit), lon)
    return (lat, lon ^ (1 << bit))


def stage_orders(mesh):
    bits = bit_list(mesh)
    n = len(bits)
    if (mesh.shape["lat"], mesh.shape["lon"]) == (8, 4):
        return [[0, 1, 2, 3, 4], [0, 1, 3, 2, 4]]
    order = list(range(n))
    return [order, order]


def scatter_orders(mesh):
    n = len(bit_list(mesh))
    if (mesh.shape["lat"], mesh.shape["lon"]) == (8, 4):
        return [[4, 3, 2, 1, 0], [4, 2, 3, 1, 0], [4, 1, 0, 3, 2]]
    return [list(reversed(range(n)))] * 3


def rotl_rows(v, first, unit):
    index = (iota((8, LANES), 1) + first + unit * iota((8, LANES), 0)) % LANES
    return jnp.take_along_axis(v, index, axis=1)


def row_vector(flat_ref, offset, length):
    blocks = -(-length // LANES)
    row, shift = divmod(offset, LANES)
    near = flat_ref[row : row + blocks, :]
    if shift:
        far = flat_ref[row + 1 : row + 1 + blocks, :]
        lane = iota((blocks, LANES), 1)
        near = pltpu.roll(jnp.where(lane >= shift, near, far), LANES - shift, 1)
    index = iota((blocks, LANES), 0) * LANES + iota((blocks, LANES), 1)
    return jnp.where(index < length, near, 0.0)


def put_row(ref, row, value):
    for q in range(value.shape[0]):
        ref[row : row + 1, q * LANES : (q + 1) * LANES] = value[q : q + 1, :].astype(ref.dtype)


def unpack_weights(flat, w1, w2):
    lane = iota((8, LANES), 1)
    row = iota((8, LANES), 0)

    def rows_one(base, first):
        near = [flat[pl.ds(base + q, 8, stride=10), :] for q in range(FB + 1)]
        out = [
            rotl_rows(jnp.where(lane >= first + 2 * row, near[q], near[q + 1]), first, 2)
            for q in range(FB)
        ]
        out[-1] = jnp.where(lane < FF - (FB - 1) * LANES, out[-1], 0.0)
        return out

    def body_one(b, carry):
        for k in range(0, 8, 2):
            pair = [rows_one(641 * b + 80 * (k + h), 16 * (k + h)) for h in range(2)]
            at = pl.ds(pl.multiple_of(64 * b + 8 * k, 16), 16)
            for q in range(FB):
                v = jnp.concatenate([pair[0][q], pair[1][q]], 0)
                w1[at, q * LANES : (q + 1) * LANES] = v.astype(BF16)
        return carry

    last = C - 1
    lax.fori_loop(0, last // 64, body_one, 0)
    zero = jnp.zeros((8, LANES), F32)
    for q, v in enumerate(rows_one(641 * (last // 64), 0)):
        v = jnp.concatenate([jnp.where(row == 0, v, 0.0), zero], 0)
        w1[last : last + 16, q * LANES : (q + 1) * LANES] = v.astype(BF16)
    w1[last + 16 :, :] = jnp.zeros((CP - last - 16, FP), BF16)

    def rows_two(base, first):
        count = CB + 2 if first + 7 >= LANES else CB + 1
        near = [flat[pl.ds(base + q, 8, stride=5), :] for q in range(count)]
        out = []
        for q in range(CB):
            v = jnp.where(lane >= first + row, near[q], near[q + 1])
            if first + 7 >= LANES:
                v = jnp.where(lane < first + row - LANES, near[q + 2], v)
            out.append(rotl_rows(v, first, 1))
        out[-1] = jnp.where(lane < C - (CB - 1) * LANES, out[-1], 0.0)
        return out

    def body_two(b, carry):
        for k in range(0, 16, 2):
            pair = [
                rows_two(ROW_TWO + 641 * b + 40 * (k + h), LANE_TWO + 8 * (k + h))
                for h in range(2)
            ]
            at = pl.ds(pl.multiple_of(128 * b + 8 * k, 16), 16)
            for q in range(CB):
                v = jnp.concatenate([pair[0][q], pair[1][q]], 0)
                w2[at, q * LANES : (q + 1) * LANES] = v.astype(BF16)
        return carry

    full = FF // LANES
    lax.fori_loop(0, full, body_two, 0)
    for q, v in enumerate(rows_two(ROW_TWO + 641 * full, LANE_TWO)):
        v = jnp.concatenate([jnp.where(row < FF - full * LANES, v, 0.0), zero], 0)
        w2[full * LANES : full * LANES + 16, q * LANES : (q + 1) * LANES] = v.astype(BF16)
    w2[full * LANES + 16 :, :] = jnp.zeros((FP - full * LANES - 16, CP), BF16)


def unpack_small(flat, base, wn, wd, small, wnf):
    vector = lambda offset, length: row_vector(flat, offset - base * LANES, length)
    small[...] = jnp.zeros_like(small)
    put_row(small, 0, vector(OFF_B1, FF))
    put_row(small, 1, vector(OFF_B2, C))
    put_row(small, 2, vector(OFF_GAIN, C))
    wd[...] = jnp.zeros_like(wd)
    wnf[...] = jnp.zeros_like(wnf)
    for k in range(K):
        put_row(wd, k, vector(OFF_DISCO + k * C, C))
    for k in range(NOISE):
        put_row(wnf, 1 + k, vector(OFF_NOISE + k * C, C))
    wn[...] = wnf[...].astype(BF16)


def neighbours():
    lat, lon = lax.axis_index("lat"), lax.axis_index("lon")
    nlat, nlon = lax.axis_size("lat"), lax.axis_size("lon")
    return lat, lon, nlat, nlon, lax.rem(lon + 1, nlon), lax.rem(lon + nlon - 1, nlon)


def halo_copies(cols, rows, corners, colh, rowh, cornh, send, recv, trow=None, trowh=None):
    lat, lon, nlat, nlon, east, west = neighbours()
    out = []

    def add(src, dst, target, k, sends, gets):
        out.append(
            (
                sends,
                gets,
                pltpu.make_async_remote_copy(
                    src_ref=src,
                    dst_ref=dst,
                    send_sem=send.at[k],
                    recv_sem=recv.at[k],
                    device_id=target,
                    device_id_type=MESH,
                ),
            )
        )

    has_up, has_down = lat > 0, lat < nlat - 1
    up, down = lat - 1, lat + 1
    add(rows.at[:, 0], rowh.at[:, 1], (up, lon), 2, has_up, has_down)
    add(rows.at[:, 1], rowh.at[:, 0], (down, lon), 3, has_down, has_up)
    add(cols.at[0], colh.at[1], (lat, west), 0, None, None)
    add(cols.at[1], colh.at[0], (lat, east), 1, None, None)
    add(corners.at[0, 0], cornh.at[1, 1], (up, west), 4, has_up, has_down)
    add(corners.at[0, 1], cornh.at[1, 0], (up, east), 5, has_up, has_down)
    add(corners.at[1, 0], cornh.at[0, 1], (down, west), 6, has_down, has_up)
    add(corners.at[1, 1], cornh.at[0, 0], (down, east), 7, has_down, has_up)
    if trow is not None:
        add(trow.at[0], trowh.at[1], (up, lon), 8, has_up, has_down)
        add(trow.at[1], trowh.at[0], (down, lon), 9, has_down, has_up)
    return out


def start_halo(copies):
    for sends, _, copy in copies:
        if sends is None:
            copy.start()
        else:
            pl.when(sends)(copy.start)


def wait_halo(copies):
    for sends, gets, copy in copies:
        if sends is None:
            copy.wait()
        else:
            pl.when(sends)(copy.wait_send)
            pl.when(gets)(copy.wait_recv)


def for_others(mesh, body):
    nlat, nlon = mesh.shape["lat"], mesh.shape["lon"]
    lat, lon = lax.axis_index("lat"), lax.axis_index("lon")
    beside = [(lon + b) & (nlon - 1) for b in range(nlon)]
    for x in beside[1:]:
        body((lat, x), lat * nlon + x)

    def row(a, carry):
        y = (lat + a) & (nlat - 1)
        for x in beside:
            body((y, x), y * nlon + x)
        return carry

    lax.fori_loop(1, nlat, row, 0)


def greet_all(mesh):
    barrier = pltpu.get_barrier_semaphore()

    def hello(target, d):
        pl.semaphore_signal(barrier, inc=1, device_id=target, device_id_type=MESH)

    for_others(mesh, hello)
    pl.semaphore_wait(barrier, mesh.shape["lat"] * mesh.shape["lon"] - 1)


def greet(bits, halo):
    barrier = pltpu.get_barrier_semaphore()
    lat, lon, nlat, nlon, east, west = neighbours()

    def hello(target):
        pl.semaphore_signal(barrier, inc=1, device_id=target, device_id_type=MESH)

    count = 0
    for axis, bit in bits:
        hello(partner(axis, bit))
        count += 1
    if halo:
        for target in ((lat, east), (lat, west)):
            hello(target)
            count += 1
        for side, cond in ((lat - 1, lat > 0), (lat + 1, lat < nlat - 1)):

            @pl.when(cond)
            def _(side=side):
                for x in (lon, east, west):
                    hello((side, x))

    if halo:
        count = count + 3 * (lat > 0).astype(jnp.int32) + 3 * (lat < nlat - 1).astype(jnp.int32)
    pl.semaphore_wait(barrier, count)


class Gather:
    def __init__(self, mesh, share, buf, early, send, recv, bsend, brecv):
        self.bits = bit_list(mesh)
        self.n = len(self.bits)
        self.orders = stage_orders(mesh)
        self.mine = my_bits(self.bits)
        self.share, self.buf, self.early = share, buf, early
        self.send, self.recv, self.bsend, self.brecv = send, recv, bsend, brecv
        rows = share.shape[0]
        cut = (rows // 2 + 15) // 16 * 16
        self.spans = [(0, cut), (cut, rows - cut)]
        self.roots, self.start = early_shards(1 << self.n, rows)

    def own(self, sem):
        return pltpu.make_async_copy(self.share, self.buf.at[tuple(self.mine)], sem)

    def copy(self, colour, k):
        order = self.orders[colour]
        index = tuple(
            slice(None) if i in order[:k] else self.mine[i] for i in range(self.n)
        ) + (pl.ds(*self.spans[colour]),)
        return pltpu.make_async_remote_copy(
            src_ref=self.buf.at[index],
            dst_ref=self.buf.at[index],
            send_sem=self.send.at[colour, k],
            recv_sem=self.recv.at[colour, k],
            device_id=partner(*self.bits[order[k]]),
            device_id_type=MESH,
        )

    def advance(self, k):
        for colour in range(2):
            self.copy(colour, k).wait()
            if k + 1 < self.n:
                self.copy(colour, k + 1).start()

    def same(self, root, indices):
        cond = True
        for i in indices:
            cond = jnp.logical_and(cond, self.mine[i] == ((root >> (self.n - 1 - i)) & 1))
        return cond

    def early_own(self, sem):
        for r, root in enumerate(self.roots):

            @pl.when(self.same(root, range(self.n)))
            def _(r=r):
                rows = self.share.shape[0] - self.start
                copy = pltpu.make_async_copy(
                    self.share.at[pl.ds(self.start, rows)], self.early.at[r], sem
                )
                copy.start()
                copy.wait()

    def early_copies(self, k):
        order = self.orders[0]
        for r, root in enumerate(self.roots):
            sends = self.same(root, order[k:])
            now = order[k]
            other = self.mine[now] != ((root >> (self.n - 1 - now)) & 1)
            gets = jnp.logical_and(other, self.same(root, order[k + 1 :]))
            yield sends, gets, pltpu.make_async_remote_copy(
                src_ref=self.early.at[r],
                dst_ref=self.early.at[r],
                send_sem=self.bsend.at[r, k],
                recv_sem=self.brecv.at[r, k],
                device_id=partner(*self.bits[now]),
                device_id_type=MESH,
            )

    def early_start(self, k):
        for sends, _, copy in self.early_copies(k):
            pl.when(sends)(copy.start)

    def early_wait(self, k):
        for sends, gets, copy in self.early_copies(k):
            pl.when(sends)(copy.wait_send)
            pl.when(gets)(copy.wait_recv)


def early_shards(devices, shard_rows):
    roots = list(range(TAIL_ROW // shard_rows, (END_FLAT - 1) // LANES // shard_rows + 1))
    start = (TAIL_ROW - roots[0] * shard_rows) // 16 * 16 if len(roots) == 1 else 0
    return roots, start


def gather_plan(n):
    if n == 5:
        return {0: (0, -1), 1: (1, -1), 2: (2, 8), 3: (4, 14)}
    return {}


def norm_parts(x):
    mean = jnp.mean(x, -1, keepdims=True)
    center = x - mean
    var = jnp.mean(center * center, -1, keepdims=True)
    return center, lax.rsqrt(var + 1e-05)


def rounded(v):
    return v.astype(BF16).astype(F32)


def stencil_fwd_kernel(
    mesh, chunks, cells, height_ref, x_ref, share, cols, edge, corners, trow, table, aug,
    out_ref, mix_hbm, w1, w2, wd, small, trowh,
    m_scr, k_scr, nt_scr, mix_scr, wnf, wn, colh, rowh, cornh, trh, buf, early, flat, eflat,
    send, recv, bsend, brecv, hsend, hrecv, own_sem, mix_sem,
):
    gather = Gather(mesh, share, buf, early, send, recv, bsend, brecv)
    n = gather.n
    plan = gather_plan(n)
    step = pl.program_id(0)
    rows = x_ref.shape[1]
    width = chunks * cells
    height = height_ref[0]
    shard_rows = share.shape[0]
    halos = lambda: halo_copies(cols, edge, corners, colh, rowh, cornh, hsend, hrecv, trow, trh)
    mix_copy = lambda: pltpu.make_async_copy(mix_scr, mix_hbm, mix_sem)

    @pl.when(step == 0)
    def _():
        gather.own(own_sem).start()
        gather.early_own(mix_sem)
        gather.own(own_sem).wait()
        greet(gather.bits, True)
        gather.early_start(0)
        for colour in range(2):
            gather.copy(colour, 0).start()
        start_halo(halos())

    for k in range(n):

        @pl.when(step == min(k + 1, chunks))
        def _(k=k):
            gather.early_wait(k)
            if k + 1 < n:
                gather.early_start(k + 1)

    @pl.when(step < chunks)
    def _():
        def cell(j, carry):
            x = x_ref[j].astype(F32)
            mean = jnp.mean(x, -1, keepdims=True)
            center = x - mean
            inv = lax.rsqrt(jnp.mean(center * center, -1, keepdims=True) + 1e-05)
            normed = center * inv
            at = pl.ds((step * cells + j + REACH) * SLOTS + 1, rows)
            for g in range(CB):
                lo, hi = g * LANES, min((g + 1) * LANES, C)
                m_scr[g, at, : hi - lo] = normed[:, lo:hi]
            return carry

        lax.fori_loop(0, cells, cell, 0, unroll=10)

    @pl.when(step == chunks)
    def _():
        base = gather.roots[0] * shard_rows + gather.start
        count = shard_rows - gather.start
        eflat[...] = jnp.zeros_like(eflat)
        for r in range(len(gather.roots)):
            eflat[r * count : (r + 1) * count, :] = early[r].astype(F32)
        unpack_small(eflat, base, wn, wd, small, wnf)
        if 0 in plan:
            gather.advance(0)
        k_scr[...] = jnp.dot(
            table[...], wd[...], preferred_element_type=F32, precision=HIGHEST
        ).reshape(k_scr.shape)
        gvec = small[2:3, :C]
        groups = [(q, q * LANES, min((q + 1) * LANES, C)) for q in range(CB)]
        hrow = iota((rows, LANES), 0)
        lanes = slice((CB - 1) * LANES, CB * LANES)
        mix_scr[:, :, lanes] = jnp.zeros((width, rows, LANES), BF16)

        def scale(i, carry):
            for u in range(REUSE):
                column = i * REUSE + u
                body = pl.ds((column + REACH) * SLOTS + 1, rows)
                for q, lo, hi in groups:
                    wide = slice(0, hi - lo)
                    v = rounded(m_scr[q, body, wide] * gvec[:, lo:hi])
                    v = jnp.where(hrow[:, wide] < height, v, 0.0)
                    mix_scr[column, :, lo:hi] = v.astype(BF16)
                    m_scr[q, body, wide] = v
            return carry

        lax.fori_loop(0, width // REUSE, scale, 0)
        mix_copy().start()
        lat, _, nlat, *_ = neighbours()
        wait_halo(halos())
        keep = (lat > 0, lat < nlat - 1)
        for r in range(2):
            trowh[r] = jnp.where(keep[r], trh[r], 0.0)

        def mix(v):
            center, inv = norm_parts(v.astype(F32))
            return rounded(center * inv * gvec)

        def beside(ref):
            return [jnp.where(keep[r], mix(ref(r)), 0.0) for r in range(2)]

        def put(column, top, low, fresh=None):
            at = column * SLOTS
            for q, lo, hi in groups:
                body = pl.ds(at + 1, rows)
                wide = slice(0, hi - lo)
                if fresh is None:
                    v = m_scr[q, body, wide]
                else:
                    v = jnp.where(hrow[:, wide] < height, fresh[:, lo:hi], 0.0)
                m_scr[q, body, wide] = jnp.where(hrow[:, wide] == height, low[:, lo:hi], v)
                m_scr[q, pl.ds(at, 1), wide] = top[:, lo:hi]
                m_scr[q, pl.ds(at + rows + 1, 1), wide] = low[:, lo:hi]

        for side in range(2):
            top, low = beside(lambda r: cornh[r, side])
            for i in range(REACH):
                column = i if side == 0 else width + REACH + i
                put(column, top[i : i + 1], low[i : i + 1], mix(colh[side, i]))

        def strip(c, carry):
            tops, lows = beside(lambda r: rowh[c, r])
            for i in range(cells):
                put(c * cells + i + REACH, tops[i : i + 1], lows[i : i + 1])
            return carry

        lax.fori_loop(0, chunks, strip, 0)

    for k, (at, loop) in plan.items():
        if k > 0 and loop < 0:

            @pl.when(step == chunks + at)
            def _(k=k):
                gather.advance(k)

    @pl.when(step >= chunks)
    def _():
        first = (step - chunks) * cells
        nt_scr[...] = jnp.dot(
            aug[...].reshape(cells * rows, LANES), wn[...], preferred_element_type=F32
        )
        lane = iota((8, LANES), 1)
        for g in range(CB):
            lanes = slice(g * LANES, (g + 1) * LANES)
            for hb in range(rows // 8):
                at = slice(8 * hb, 8 * hb + 8)

                def cell(i, carry):
                    j = i * REUSE
                    acc = [nt_scr[pl.ds((j + u) * rows + 8 * hb, 8), lanes] for u in range(REUSE)]
                    for l in range(3):
                        near = [
                            m_scr[g, pl.ds((first + j + u) * SLOTS + 8 * hb + l, 8), :]
                            for u in range(REUSE + 2 * REACH)
                        ]
                        for w in range(5):
                            tap = k_scr[5 * l + w, at, lanes]
                            acc = [a + tap * near[u + w] for u, a in enumerate(acc)]
                    for u in range(REUSE):
                        v = acc[u]
                        if g == CB - 1:
                            v = jnp.where(lane == 0, v, aug[j + u, at, :].astype(F32))
                        out_ref[j + u, at, lanes] = v.astype(BF16)
                    return carry

                lax.fori_loop(0, cells // REUSE, cell, 0)
                for k, (past, loop) in plan.items():
                    if loop == g * (rows // 8) + hb:

                        @pl.when(step == chunks + past)
                        def _(k=k):
                            gather.advance(k)

    @pl.when(step == 2 * chunks - 1)
    def _():
        for k in range(n):
            if k not in plan:
                gather.advance(k)
        total = 1 << n

        def widen(d, carry):
            index = tuple((d >> (n - 1 - i)) & 1 for i in range(n))
            flat[pl.ds(d * shard_rows, shard_rows), :] = buf[index].astype(F32)
            return carry

        lax.fori_loop(0, total, widen, 0)
        flat[total * shard_rows :, :] = jnp.zeros((flat.shape[0] - total * shard_rows, LANES), F32)
        unpack_weights(flat, w1, w2)
        mix_copy().wait()


def stencil_fwd(mesh, height, x, share, cols, edge, corners, trow, table, aug, chunks):
    width, rows, _ = x.shape
    cells = width // chunks
    assert cells % REUSE == 0
    n = len(bit_list(mesh))
    shard_rows = share.shape[0]
    total = shard_rows << n
    roots, start = early_shards(1 << n, shard_rows)
    count = shard_rows - start
    first = lambda i: jnp.where(i < chunks, i, chunks - 1)
    second = lambda i: jnp.where(i < chunks, 0, i - chunks)
    sd = jax.ShapeDtypeStruct
    by_first = lambda c: pl.BlockSpec((cells, rows, c), lambda i: (first(i), 0, 0))
    by_second = lambda c: pl.BlockSpec((cells, rows, c), lambda i: (second(i), 0, 0))
    dma = pltpu.SemaphoreType.DMA
    return pl.pallas_call(
        partial(stencil_fwd_kernel, mesh, chunks, cells),
        name="stencil_fwd",
        grid=(2 * chunks,),
        out_shape=(
            sd((width, rows, CP), BF16),
            sd((width, rows, CP), BF16),
            sd((CP, FP), BF16),
            sd((FP, CP), BF16),
            sd((16, CP), F32),
            sd((8, FP), F32),
            sd(trow.shape, F32),
        ),
        in_specs=[pl.BlockSpec(memory_space=pltpu.SMEM), by_first(C)]
        + [vmem_spec()] * 6
        + [by_second(LANES)],
        out_specs=(by_second(CP), any_spec())
        + (vmem_spec(),) * 5,
        scratch_shapes=[
            pltpu.VMEM((CB, (width + 2 * REACH) * SLOTS, LANES), F32),
            pltpu.VMEM((TAPS, rows, CP), F32),
            pltpu.VMEM((cells * rows, CP), F32),
            pltpu.VMEM((width, rows, CP), BF16),
            pltpu.VMEM((LANES, CP), F32),
            pltpu.VMEM((LANES, CP), BF16),
            pltpu.VMEM(cols.shape, BF16),
            pltpu.VMEM(edge.shape, BF16),
            pltpu.VMEM(corners.shape, BF16),
            pltpu.VMEM(trow.shape, F32),
            pltpu.VMEM((2,) * n + (shard_rows, LANES), BF16),
            pltpu.VMEM((len(roots), count, LANES), BF16),
            pltpu.VMEM((total + 96, LANES), F32),
            pltpu.VMEM((len(roots) * count + 16, LANES), F32),
            dma((2, n)),
            dma((2, n)),
            dma((len(roots), n)),
            dma((len(roots), n)),
            dma((10,)),
            dma((10,)),
            dma,
            dma,
        ],
        compiler_params=params(
            dimension_semantics=("arbitrary",), collective_id=0, has_side_effects=True
        ),
    )(height, x, share, cols, edge, corners, trow, table, aug)


def pack_weights(one, two, flat):
    lane = iota((8, LANES), 1)
    row = iota((8, LANES), 0)
    flat[...] = jnp.zeros_like(flat)

    def turned(v, first, unit):
        return pltpu.roll(v, first, 1, stride=unit, stride_axis=0)

    def main(ref, at, first, unit, out, base, step, count):
        keep = lane >= first + unit * row
        before = jnp.zeros((8, LANES), F32)
        for q in range(count):
            now = turned(ref[q, at, :], first, unit)
            flat[pl.ds(base + q, 8, stride=step), :] = jnp.where(keep, now, before)
            before = now

    def rest(ref, at, first, unit, count, width, mask=None):
        s = first + unit * row
        before = turned(ref[count - 1, at, :], first, unit)
        now = turned(ref[count, at, :], first, unit)
        v = jnp.where(lane < s, before, jnp.where(lane < s + width, now, 0.0))
        return v if mask is None else jnp.where(mask, v, 0.0)

    shift = 8 - LANE_TWO
    base_two = ROW_TWO - 5 * LANE_TWO
    full = FF // LANES
    extra = C - (CB - 1) * LANES

    def two_main(b, carry):
        for k in range(16):
            at = pl.ds(128 * b + 8 * k + shift, 8)
            main(two, at, 8 * k, 1, flat, base_two + 641 * b + 40 * k, 5, CB - 1)
        return carry

    lax.fori_loop(0, full, two_main, 0)
    end = slice(128 * full + shift, 128 * full + shift + 8)
    mask = row < FF - full * LANES + LANE_TWO
    before = jnp.zeros((8, LANES), F32)
    for q in range(CB - 1):
        now = jnp.where(mask, turned(two[q, end, :], 0, 1), 0.0)
        at = pl.ds(base_two + 641 * full + q, 8, stride=5)
        flat[at, :] = jnp.where(lane >= row, now, before)
        before = now

    def one_main(b, carry):
        for k in range(8):
            at = pl.ds(pl.multiple_of(64 * b + 8 * k, 8), 8)
            main(one, at, 16 * k, 2, flat, 641 * b + 80 * k, 10, FB - 1)
        return carry

    last = C - 1
    assert last % 64 == 0
    lax.fori_loop(0, last // 64, one_main, 0)
    row_last = 641 * (last // 64)
    for q in range(FB - 1):
        flat[row_last + q : row_last + q + 1, :] = one[q, last : last + 1, :]

    def add_all(places, values):
        olds = [flat[at, :] for at in places]
        for at, old, v in zip(places, olds, values):
            flat[at, :] = old + v

    def one_rest(b, carry):
        values = [
            rest(one, pl.ds(pl.multiple_of(64 * b + 8 * k, 8), 8), 16 * k, 2, FB - 1, FF - (FB - 1) * LANES)
            for k in range(8)
        ]
        add_all([pl.ds(641 * b + 80 * k + FB - 1, 8, stride=10) for k in range(8)], values)
        return carry

    lax.fori_loop(0, last // 64, one_rest, 0)
    lane1 = iota((1, LANES), 1)
    v = jnp.where(lane1 < FF - (FB - 1) * LANES, one[FB - 1, last : last + 1, :], 0.0)
    add_all([slice(row_last + FB - 1, row_last + FB)], [v])

    def two_rest(b, carry):
        values = [
            rest(two, pl.ds(128 * b + 8 * k + shift, 8), 8 * k, 1, CB - 1, extra) for k in range(16)
        ]
        places = [pl.ds(base_two + 641 * b + 40 * k + CB - 1, 8, stride=5) for k in range(16)]
        add_all(places, values)
        return carry

    lax.fori_loop(0, full, two_rest, 0)
    add_all(
        [pl.ds(base_two + 641 * full + CB - 1, 8, stride=5)],
        [rest(two, end, 0, 1, CB - 1, extra, mask)],
    )


GELU_A = math.sqrt(2.0 / math.pi)
GELU_B = 0.044715
WIDE = 256


def dot(a, b, dims=((1,), (0,))):
    return lax.dot_general(a, b, (dims, ((), ())), preferred_element_type=F32)


def mlp_kernel(
    blocks, height_ref, conv_ref, g_ref, x_ref, w1, w2, small,
    out_ref, gconv_ref, rows_ref, cols_ref, corn_ref, shards_ref, extra_ref,
    one, two, g_scr, conv_t, act, gh, flat, w1_rest,
):
    step = pl.program_id(0)
    cells, rows, _ = x_ref.shape
    m = cells * rows
    height = height_ref[0]

    @pl.when(step == 0)
    def _():
        one[...] = jnp.zeros_like(one)
        two[...] = jnp.zeros_like(two)
        g_scr[...] = jnp.zeros_like(g_scr)
        w1_rest[...] = w1[:, FP // WIDE * WIDE :].astype(F32).T[: w1_rest.shape[0]]

    live = (iota((1, rows, 1), 1) < height).astype(F32)
    g_scr[:, :C] = (g_ref[...].astype(F32) * live).reshape(m, C).astype(BF16)
    rows_one = conv_t.shape[0]

    def hidden(start, wide, tail):
        lanes = pl.ds(start, wide)
        h = dot(conv_ref[...].reshape(m, CP), w1[:, lanes]) + small[0:1, lanes]
        ga = dot(g_scr[...], w2[lanes, :], ((1,), (1,)))
        h2 = h * h
        t = jnp.tanh(h * (GELU_A + (GELU_A * GELU_B) * h2))
        cdf = 0.5 * t + 0.5
        value = (h * cdf).astype(BF16)
        slope = cdf + h * (0.5 - 0.5 * (t * t)) * (GELU_A + (3 * GELU_A * GELU_B) * h2)
        if tail:
            ones = iota((m, wide), 1) == FF - (FB - 1) * LANES
            value = jnp.where(ones, jnp.ones_like(value), value)
        act[:, lanes] = value
        gh[:, lanes] = (ga * slope).astype(BF16)

    def turn(i, count):
        part = conv_ref[:, :, pl.ds(i * LANES, LANES)].reshape(m, LANES)
        conv_t[pl.ds(i * LANES, count), :] = part.T[:count]

    full = FP // WIDE
    assert full == CB - 1
    for f in range(full):
        turn(f, LANES)
        hidden(f * WIDE, WIDE, False)
    turn(CB - 1, rows_one - (CB - 1) * LANES)
    hidden(full * WIDE, FP % WIDE, True)

    main = full * WIDE
    spare = [
        (act[:, main + i : main + i + 1].astype(F32), gh[:, main + i : main + i + 1].astype(F32))
        for i in range(FF - main)
    ]
    for n in range(CP // WIDE):
        lanes = slice(n * WIDE, (n + 1) * WIDE)
        end = min((n + 1) * WIDE, C)
        part = slice(n * WIDE, end)
        branch = dot(act[:, :main], w2[:main, lanes])
        gc = dot(gh[:, :main], w1[lanes, :main], ((1,), (1,)))
        for i, (a, b) in enumerate(spare):
            branch = branch + a * w2[main : main + 16, lanes].astype(F32)[i : i + 1]
            gc = gc + b * w1_rest[i : i + 1, lanes]
        v = x_ref[:, :, part].astype(F32).reshape(m, -1) + branch[:, : end - n * WIDE] + small[1:2, part]
        out_ref[:, :, part] = (v.reshape(cells, rows, -1) * live).astype(BF16)
        for i in range(WIDE // LANES):
            gconv_ref[n * (WIDE // LANES) + i] = gc[:, i * LANES : (i + 1) * LANES]

    def weights(start, wide):
        lanes = pl.ds(start, wide)
        r1 = dot(conv_t[...], gh[:, lanes])
        r2 = dot(act[:, lanes], g_scr[...], ((0,), (0,)))
        for i in range(wide // LANES):
            one[start // LANES + i] += r1[:, i * LANES : (i + 1) * LANES]
        for q in range(CB):
            two[q, pl.ds(start + 8, wide), :] += r2[:, q * LANES : (q + 1) * LANES]

    def third(f, carry):
        weights(pl.multiple_of(f * WIDE, WIDE), WIDE)
        return carry

    lax.fori_loop(0, FP // WIDE, third, 0)
    spare_lanes = pl.ds(main, LANES)
    r1 = dot(conv_t[...], gh[:, spare_lanes])
    r2 = dot(act[:, main : main + 16], g_scr[...], ((0,), (0,)))
    one[FB - 1] += r1
    for q in range(CB):
        two[q, main + 8 : main + 24, :] += r2[:, q * LANES : (q + 1) * LANES]

    whole, left = divmod(cells, 8)
    for r, slot in ((0, 0), (1, height - 1)):
        for q in range(CB):
            lanes = slice(q * LANES, (q + 1) * LANES)
            pick = lambda c: gconv_ref[q, pl.ds(slot + c * rows, 8, stride=rows), :]
            v = [pick(8 * i) for i in range(whole)]
            if left:
                v.append(pltpu.roll(pick(cells - 8), left, 0))
            v = jnp.concatenate(v, 0).astype(BF16)
            rows_ref[0, r, :, lanes] = v
            for side, at, first in ((0, 0, 0), (1, blocks - 1, cells - REACH)):

                @pl.when(step == at)
                def _(side=side, first=first, v=v, lanes=lanes, r=r):
                    corn_ref[r, side, :, lanes] = v[first : first + REACH]

    for side, at, first in ((0, 0, 0), (1, blocks - 1, cells - REACH)):

        @pl.when(step == at)
        def _(side=side, first=first):
            for i in range(REACH):
                base = (first + i) * rows
                for q in range(CB):
                    lanes = slice(q * LANES, (q + 1) * LANES)
                    cols_ref[side, i, :, lanes] = gconv_ref[q, base : base + rows, :].astype(BF16)

    @pl.when(step == blocks - 1)
    def _():
        extra_ref[...] = jnp.zeros_like(extra_ref)
        for q in range(FB):
            extra_ref[0 : NOISE + 1, q * LANES : (q + 1) * LANES] = one[q, C : C + NOISE + 1, :]
        for q in range(CB):
            lanes = slice(q * LANES, (q + 1) * LANES)
            extra_ref[NOISE + 1 : NOISE + 2, lanes] = two[q, FF + 8 : FF + 9, :]
        pack_weights(one, two, flat)
        bits = len(shards_ref.shape) - 2
        shard_rows = shards_ref.shape[-2]

        def store(d, carry):
            index = tuple((d >> (bits - 1 - i)) & 1 for i in range(bits))
            shards_ref[index] = flat[pl.ds(d * shard_rows, shard_rows), :]
            return carry

        lax.fori_loop(0, 1 << bits, store, 0)


def mlp(height, conv, g, x, w1, w2, small, shards, blocks):
    width, rows, _ = x.shape
    cells = width // blocks
    m = cells * rows
    sd = jax.ShapeDtypeStruct
    block = lambda c: pl.BlockSpec((cells, rows, c), lambda i: (i, 0, 0))
    rows_one = -(-(C + NOISE + 1) // 16) * 16
    flops = 12 * width * rows * C * FF
    return pl.pallas_call(
        partial(mlp_kernel, blocks),
        name="mlp",
        grid=(blocks,),
        out_shape=(
            sd((width, rows, C), BF16),
            sd((CB, width * rows, LANES), F32),
            sd((blocks, 2, -(-cells // 8) * 8, CP), BF16),
            sd((2, REACH, rows, CP), BF16),
            sd((2, 2, REACH, CP), BF16),
            sd(shards, F32),
            sd((16, FP), F32),
        ),
        in_specs=[
            pl.BlockSpec(memory_space=pltpu.SMEM),
            block(CP),
            block(C),
            block(C),
            vmem_spec(),
            vmem_spec(),
            vmem_spec(),
        ],
        out_specs=(
            block(C),
            pl.BlockSpec((CB, m, LANES), lambda i: (0, i, 0)),
            pl.BlockSpec((1, 2, -(-cells // 8) * 8, CP), lambda i: (i, 0, 0, 0)),
            vmem_spec(),
            vmem_spec(),
            vmem_spec(),
            vmem_spec(),
        ),
        scratch_shapes=[
            pltpu.VMEM((FB, rows_one, LANES), F32),
            pltpu.VMEM((CB, FP + 16, LANES), F32),
            pltpu.VMEM((m, CP), BF16),
            pltpu.VMEM((rows_one, m), BF16),
            pltpu.VMEM((m, FP), BF16),
            pltpu.VMEM((m, FP), BF16),
            pltpu.VMEM((math.prod(shards[:-1]), LANES), F32),
            pltpu.VMEM((8, CP), F32),
        ],
        compiler_params=params(dimension_semantics=("arbitrary",)),
        cost_estimate=pl.CostEstimate(flops=flops, bytes_accessed=50_000_000, transcendentals=0),
    )(height, conv, g, x, w1, w2, small)


def add_vector(tail, offset, value):
    row, shift = divmod(offset - TAIL_ROW * LANES, LANES)
    blocks = value.shape[0]
    lane = iota((blocks + 1, LANES), 1)
    zero = jnp.zeros((1, LANES), F32)
    here = pltpu.roll(jnp.concatenate([value, zero], 0), shift, 1) if shift else jnp.concatenate([value, zero], 0)
    back = jnp.concatenate([zero, here[:blocks]], 0)
    at = slice(row, row + blocks + 1)
    tail[at, :] = tail[at, :] + jnp.where(lane >= shift, here, back if shift else here)


def as_blocks(value, length):
    blocks = -(-length // LANES)
    v = jnp.concatenate([value[:, q * LANES : (q + 1) * LANES] for q in range(blocks)], 0)
    index = iota((blocks, LANES), 0) * LANES + iota((blocks, LANES), 1)
    return jnp.where(index < length, v, 0.0)


class Scatter:
    def __init__(self, mesh, shards, buf, recvs, send, recv):
        self.bits = bit_list(mesh)
        self.n = len(self.bits)
        self.orders = scatter_orders(mesh)
        self.first = self.orders[0][0]
        assert all(order[0] == self.first for order in self.orders)
        self.mine = my_bits(self.bits)
        self.shards, self.buf, self.recvs = shards, buf, recvs
        self.send, self.recv = send, recv
        rows = shards.shape[-2]
        one, two = (int(rows * f) // 8 * 8 for f in (0.36, 0.71))
        self.spans = [(0, one), (one, two - one), (two, rows - two)]

    def copy(self, colour, k):
        order, mine, n = self.orders[colour], self.mine, self.n
        done, now = order[:k], order[k]
        at = (pl.ds(*self.spans[colour]),)
        index = tuple(
            1 - mine[i] if i == now else mine[i] if i in done else slice(None) for i in range(n)
        )
        if k == 0:
            src = self.shards.at[index + at]
        else:
            src = self.buf.at[tuple(v for i, v in enumerate(index) if i != self.first) + at]
        return pltpu.make_async_remote_copy(
            src_ref=src,
            dst_ref=self.recvs[k].at[(slice(None),) * (n - 1 - k) + at],
            send_sem=self.send.at[colour, k],
            recv_sem=self.recv.at[colour, k],
            device_id=partner(*self.bits[now]),
            device_id_type=MESH,
        )

    def load(self, sem):
        index = tuple(self.mine[i] if i == self.first else slice(None) for i in range(self.n))
        return pltpu.make_async_copy(self.shards.at[index], self.buf, sem)

    def advance(self, colour, k):
        self.copy(colour, k).wait()
        order, n = self.orders[colour], self.n
        free = [i for i in range(n) if i not in order[: k + 1]]
        at = (pl.ds(*self.spans[colour]),)

        def add(d, carry):
            sub = tuple((d >> (len(free) - 1 - i)) & 1 for i in range(len(free)))
            index = tuple(
                sub[free.index(i)] if i in free else self.mine[i]
                for i in range(n)
                if i != self.first
            )
            self.buf[index + at] = self.buf[index + at] + self.recvs[k][sub + at]
            return carry

        lax.fori_loop(0, 1 << len(free), add, 0)
        if k + 1 < n:
            self.copy(colour, k + 1).start()

    def result(self):
        return self.buf[tuple(v for i, v in enumerate(self.mine) if i != self.first)]


def scatter_plan(n):
    if n == 5:
        return {
            7: [(0, 1), (1, 1), (2, 1)],
            12: [(0, 2), (1, 2)],
            13: [(2, 2)],
            17: [(0, 3), (1, 3), (2, 3)],
        }
    return {}


class Tail:
    def __init__(self, mesh, pieces, got, msg, full, place, send, recv):
        self.mesh = mesh
        self.n = mesh.shape["lat"] * mesh.shape["lon"]
        self.lat, self.lon = lax.axis_index("lat"), lax.axis_index("lon")
        self.me = self.lat * mesh.shape["lon"] + self.lon
        self.pieces, self.got, self.msg, self.full, self.place = pieces, got, msg, full, place
        self.send, self.recv = send, recv

    def others(self, source, target, k):
        def send(device, d):
            pltpu.make_async_remote_copy(
                src_ref=source(d),
                dst_ref=target.at[self.me],
                send_sem=self.send.at[k],
                recv_sem=self.recv.at[k],
                device_id=device,
                device_id_type=MESH,
            ).start()

        for_others(self.mesh, send)

    def wait_all(self, buffer, k):
        pltpu.make_async_remote_copy(
            src_ref=buffer.at[pl.ds(0, self.n - 1)],
            dst_ref=buffer.at[pl.ds(0, self.n - 1)],
            send_sem=self.send.at[k],
            recv_sem=self.recv.at[k],
            device_id=(self.lat, self.lon),
            device_id_type=MESH,
        ).wait()

    def scatter(self, flat):
        piece = self.pieces.shape[1]

        def split(d, carry):
            self.pieces[d] = flat[pl.ds(d * piece, piece), :]
            return carry

        lax.fori_loop(0, self.n, split, 0)
        self.others(lambda d: self.pieces.at[d], self.got, 0)
        self.got[self.me] = self.pieces[self.me]
        self.place[...] = jnp.zeros_like(self.place)

    def finish(self, part, own_gain, grad_ref, norm_ref):
        n, piece = self.n, self.pieces.shape[1]
        shard_rows = part.shape[0]
        square = jnp.sum(part * part)
        self.wait_all(self.got, 0)
        total = lax.fori_loop(1, n, lambda i, acc: acc + self.got[i], self.got[0])
        square = square + jnp.sum(total * total)
        self.msg[0:piece, :] = total
        self.msg[piece : piece + 1, :] = jnp.broadcast_to(square, (1, LANES))
        self.msg[piece + 1 :, :] = own_gain
        self.others(lambda d: self.msg, self.full, 1)
        self.full[self.me] = self.msg[...]
        self.wait_all(self.full, 1)

        def take(d, acc):
            self.place[pl.ds(shard_rows + d * piece, piece), :] = self.full[d, 0:piece, :]
            return acc + self.full[d, piece:, :]

        sums = lax.fori_loop(0, n, take, jnp.zeros((1 + CB, LANES), F32))
        gain = sums[1:]
        add_vector(self.place, OFF_GAIN + shard_rows * LANES, gain)
        squares = sums[:1] + jnp.sum(gain * gain)
        start = jnp.clip(self.me * shard_rows - TAIL_ROW + shard_rows, 0, shard_rows + n * piece)
        grad_ref[...] = part + self.place[pl.ds(start, shard_rows), :]
        norm_ref[...] = jnp.broadcast_to(jnp.sqrt(squares), norm_ref.shape)


def backward_kernel(
    mesh, chunks, cells, strip_cells, height_ref, mix_ref, gconv_ref, x_hbm, g_hbm,
    cols, edge, corners, table, trowh, wd, gain, extra, w1, shards,
    out_ref, grad_ref, norm_ref,
    x_scr, up_scr, st_scr, g_scr, m_scr, k_scr, t_scr, e_scr, gg_scr, tail_scr, colh, rowh, cornh,
    pieces, got, msg, full, place, buf, *rest,
):
    n = len(bit_list(mesh))
    recvs, (send, recv, hsend, hrecv, tsend, trecv, load_sem) = rest[:n], rest[n:]
    scatter = Scatter(mesh, shards, buf, recvs, send, recv)
    tail = Tail(mesh, pieces, got, msg, full, place, tsend, trecv)
    step = pl.program_id(0)
    width, rows, _ = mix_ref.shape
    height = height_ref[0]
    plan = scatter_plan(n)
    gvec = gain[2:3, :C]
    halos = lambda: halo_copies(cols, edge, corners, colh, rowh, cornh, hsend, hrecv)
    load_x = lambda: pltpu.make_async_copy(x_hbm, x_scr, load_sem.at[1])
    load_up = lambda: pltpu.make_async_copy(g_hbm, up_scr, load_sem.at[2])

    @pl.when(step == 0)
    def _():
        load_x().start()
        greet_all(mesh)
        start_halo(halos())
        for colour in range(3):
            scatter.copy(colour, 0).start()
        scatter.load(load_sem.at[0]).start()
        load_up().start()
        hrow = iota((rows, 16), 0)
        for t in range(TAPS):
            l = t // 5
            own = table[t * rows : (t + 1) * rows, :]
            if l == 0:
                own = jnp.concatenate([own[1:], own[:1]], 0)
                own = jnp.where(hrow == height - 1, trowh[1, t : t + 1, :], own)
            if l == 2:
                own = jnp.concatenate([trowh[0, t : t + 1, :], own[: rows - 1]], 0)
            t_scr[t * rows : (t + 1) * rows, :] = own
        kernel = jnp.dot(t_scr[...], wd[...], preferred_element_type=F32, precision=HIGHEST)
        for q in range(CB):
            k_scr[q] = kernel[:, q * LANES : (q + 1) * LANES].reshape(k_scr.shape[1:])
        e_scr[...] = jnp.zeros_like(e_scr)
        gg_scr[...] = jnp.zeros_like(gg_scr)
        load_x().wait()
        first_lane = iota((rows, LANES), 1) == 0

        def stats(j, carry):
            x = x_scr[j].astype(F32)
            mean = jnp.mean(x, -1, keepdims=True)
            center = x - mean
            inv = lax.rsqrt(jnp.mean(center * center, -1, keepdims=True) + 1e-05)
            st_scr[j] = jnp.where(first_lane, mean, inv)
            return carry

        lax.fori_loop(0, width, stats, 0, unroll=10)
        tail_scr[...] = jnp.zeros_like(tail_scr)
        add_vector(tail_scr, OFF_B1, as_blocks(extra[NOISE : NOISE + 1, :], FF))
        add_vector(tail_scr, OFF_B2, as_blocks(extra[NOISE + 1 : NOISE + 2, :], C))
        ng = extra[0:NOISE, :]
        hi = ng.astype(BF16)
        mid = (ng - hi.astype(F32)).astype(BF16)
        lo = (ng - hi.astype(F32) - mid.astype(F32)).astype(BF16)
        parts = [dot(p, w1[...], ((1,), (1,))) for p in (hi, mid, lo)]
        gn = parts[0] + parts[1] + parts[2]
        for k in range(NOISE):
            add_vector(tail_scr, OFF_NOISE + k * C, as_blocks(gn[k : k + 1, :], C))

    @pl.when(step == 1)
    def _():
        wait_halo(halos())
        scatter.load(load_sem.at[0]).wait()
        for colour in range(3):
            scatter.advance(colour, 0)

    @pl.when((step >= 1) & (step <= CB))
    def _():
        q = step - 1
        lanes = pl.ds(pl.multiple_of(q * LANES, LANES), LANES)
        lat, _, nlat, *_ = neighbours()
        keep = (lat > 0, lat < nlat - 1)
        here = iota((rows, LANES), 0) == height

        def put(column, top, low, v):
            at = column * SLOTS
            g_scr[pl.ds(at + 1, rows), :] = jnp.where(here, low, v)
            g_scr[pl.ds(at, 1), :] = top
            g_scr[pl.ds(at + rows + 1, 1), :] = low

        def beside(ref):
            return [jnp.where(keep[r], ref(r).astype(F32), 0.0) for r in range(2)]

        for side in range(2):
            top, low = beside(lambda r: cornh[r, side, :, lanes])
            for i in range(REACH):
                column = i if side == 0 else width + REACH + i
                put(column, top[i : i + 1], low[i : i + 1], colh[side, i, :, lanes].astype(F32))

        def strip(c, carry):
            tops, lows = beside(lambda r: rowh[c, r, :, lanes])
            for i in range(strip_cells):
                j = c * strip_cells + i
                v = gconv_ref[0, pl.ds(pl.multiple_of(j * rows, 8), rows), :]
                put(j + REACH, tops[i : i + 1], lows[i : i + 1], v)
                m_scr[q, j] = mix_ref[j].astype(F32)
            return carry

        lax.fori_loop(0, edge.shape[0], strip, 0)
        for hb in range(rows // 8):
            at = slice(8 * hb, 8 * hb + 8)

            def cell(i, carry):
                j = i * REUSE
                mixed = [m_scr[q, j + u, at, :] for u in range(REUSE)]
                total = [None] * REUSE
                for l in range(3):
                    near = [
                        g_scr[pl.ds((j + u) * SLOTS + 8 * hb + 2 - l, 8), :]
                        for u in range(REUSE + 2 * REACH)
                    ]
                    for w in range(5):
                        t = 5 * l + w
                        tap = k_scr[q, t, at, :]
                        views = near[2 * REACH - w : 2 * REACH - w + REUSE]
                        terms = [tap * v for v in views]
                        total = [a if b is None else a + b for a, b in zip(terms, total)]
                        sums = [m * v for m, v in zip(mixed, views)]
                        while len(sums) > 1:
                            sums = [
                                sums[k] + sums[k + 1] if k + 1 < len(sums) else sums[k]
                                for k in range(0, len(sums), 2)
                            ]
                        e_scr[q, t, at, :] = e_scr[q, t, at, :] + sums[0]
                for u in range(REUSE):
                    m_scr[q, j + u, at, :] = total[u]
                return carry

            lax.fori_loop(0, width // REUSE, cell, 0)
            for loop, events in plan.items():
                if loop % (rows // 8) == hb:

                    @pl.when(q == loop // (rows // 8))
                    def _(events=events):
                        for colour, k in events:
                            scatter.advance(colour, k)

    @pl.when(step == CB)
    def _():
        load_up().wait()
        disco = jnp.concatenate(
            [
                lax.dot_general(
                    t_scr[...], e_scr[q].reshape(TAPS * rows, LANES), (((0,), (0,)), ((), ())),
                    preferred_element_type=F32, precision=HIGHEST,
                )
                for q in range(CB)
            ],
            1,
        )
        for k in range(K):
            add_vector(tail_scr, OFF_DISCO + k * C, as_blocks(disco[k : k + 1, :], C))
        tail.scatter(tail_scr)

    @pl.when(step > CB)
    def _():
        first = (step - CB - 1) * cells
        live = iota((rows, C), 0) < height

        def cell(i, total):
            j = first + i
            st = st_scr[j]
            inv = st[:, 1:2]
            normed = (x_scr[j].astype(F32) - st[:, :1]) * inv
            gm = jnp.concatenate([m_scr[q, j] for q in range(CB)], 1)[:, :C]
            gm = jnp.where(live, gm, 0.0)
            total = total + gm * normed
            v = gm * gvec
            mean = jnp.mean(v, -1, keepdims=True)
            mean_n = jnp.mean(v * normed, -1, keepdims=True)
            up = jnp.where(live, up_scr[j].astype(F32), 0.0)
            out_ref[i] = inv * (v - mean - normed * mean_n) + up
            return total

        gg_scr[:, :C] = lax.fori_loop(0, cells, cell, gg_scr[:, :C], unroll=4)

    @pl.when(step == CB + chunks)
    def _():
        own_gain = as_blocks(jnp.sum(gg_scr[...], 0, keepdims=True), C)
        taken = {e for events in plan.values() for e in events}
        for k in range(1, n):
            for colour in range(3):
                if (colour, k) not in taken:
                    scatter.advance(colour, k)
        tail.finish(scatter.result(), own_gain, grad_ref, norm_ref)


def backward(
    mesh, height, mixed, gconv, x, g, cols, edge, corners, table, trowh, wd, small, extra,
    w1, shards, piece, chunks,
):
    width, rows, _ = mixed.shape
    cells = width // chunks
    shard_rows = shards.shape[-2]
    n = len(bit_list(mesh))
    devices = 1 << n
    group = lambda i: jnp.clip(i - 1, 0, CB - 1)
    last = lambda i: jnp.where(i <= CB, 0, i - CB - 1)
    sd = jax.ShapeDtypeStruct
    dma = pltpu.SemaphoreType.DMA
    return pl.pallas_call(
        partial(backward_kernel, mesh, chunks, cells, width // edge.shape[0]),
        name="backward",
        grid=(1 + CB + chunks,),
        out_shape=(
            sd((width, rows, C), F32),
            sd((shard_rows, LANES), F32),
            sd((8, LANES), F32),
        ),
        in_specs=[
            pl.BlockSpec(memory_space=pltpu.SMEM),
            pl.BlockSpec((width, rows, LANES), lambda i: (0, 0, group(i))),
            pl.BlockSpec((1, width * rows, LANES), lambda i: (group(i), 0, 0)),
            any_spec(),
            any_spec(),
        ]
        + [vmem_spec()] * 9
        + [any_spec()],
        out_specs=(
            pl.BlockSpec((cells, rows, C), lambda i: (last(i), 0, 0)),
            vmem_spec(),
            vmem_spec(),
        ),
        scratch_shapes=[
            pltpu.VMEM(x.shape, BF16),
            pltpu.VMEM(x.shape, BF16),
            pltpu.VMEM((width, rows, LANES), F32),
            pltpu.VMEM(((width + 2 * REACH) * SLOTS, LANES), F32),
            pltpu.VMEM((CB, width, rows, LANES), F32),
            pltpu.VMEM((CB, TAPS, rows, LANES), F32),
            pltpu.VMEM((TAPS * rows, 16), F32),
            pltpu.VMEM((CB, TAPS, rows, LANES), F32),
            pltpu.VMEM((rows, CP), F32),
            pltpu.VMEM((devices * piece, LANES), F32),
            pltpu.VMEM(cols.shape, BF16),
            pltpu.VMEM(edge.shape, BF16),
            pltpu.VMEM(corners.shape, BF16),
            pltpu.VMEM((devices, piece, LANES), F32),
            pltpu.VMEM((devices, piece, LANES), F32),
            pltpu.VMEM((piece + 1 + CB, LANES), F32),
            pltpu.VMEM((devices, piece + 1 + CB, LANES), F32),
            pltpu.VMEM((2 * shard_rows + devices * piece + 8, LANES), F32),
            pltpu.VMEM((2,) * (n - 1) + (shard_rows, LANES), F32),
        ]
        + [pltpu.VMEM((2,) * (n - 1 - k) + (shard_rows, LANES), F32) for k in range(n)]
        + [dma((3, n)), dma((3, n)), dma((8,)), dma((8,)), dma((2,)), dma((2,)), dma((3,))],
        compiler_params=params(
            dimension_semantics=("arbitrary",), collective_id=1, has_side_effects=True
        ),
    )(
        height, mixed, gconv, x, g, cols, edge, corners, table, trowh, wd, small, extra, w1, shards,
    )


def stencil_table(support_vals, support_lon):
    rows = support_vals.shape[0]
    vals = support_vals.reshape(rows, S // 3, 3, K)
    offsets = jnp.arange(-REACH, REACH + 1)
    hit = support_lon.reshape(rows, S // 3, 3)[:, :, :, None] == offsets
    picked = jnp.where(hit[:, :, :, :, None], vals[:, :, :, None, :], 0.0)
    return jnp.transpose(jnp.sum(picked, 1), (1, 2, 0, 3))


def flat_table(table):
    t = table.reshape(-1, K)
    return jnp.pad(t, ((0, 0), (0, 16 - K)))


def local(
    mesh, block_in, noise, cotangent, band_heights, support_lon, support_vals,
    master, moment_one, moment_two, average, step_count,
):
    rows, width, _ = block_in.shape
    devices = mesh.shape["lat"] * mesh.shape["lon"]
    shard = master.shape[0]
    shard_rows = shard // LANES
    assert shard_rows * LANES == shard
    flat_rows = shard_rows * devices
    chunks = 6
    cells = width // chunks
    height = lax.dynamic_slice_in_dim(band_heights, lax.axis_index("lat"), 1, 0)
    x = jnp.transpose(block_in, (1, 0, 2))
    g = jnp.transpose(cotangent, (1, 0, 2))

    table = flat_table(stencil_table(support_vals, support_lon))
    planes = table.reshape(TAPS, rows, 16)
    trow = jnp.stack([planes[:, 0], lax.dynamic_index_in_dim(planes, height[0] - 1, 1, keepdims=False)])
    trow = jnp.pad(trow, ((0, 0), (0, 1), (0, 0)))
    share = master.astype(BF16).reshape(shard_rows, LANES)
    edge = jnp.stack([x[:, 0], lax.dynamic_index_in_dim(x, height[0] - 1, 1, keepdims=False)], 1)
    cols = jnp.stack([x[:REACH], x[width - REACH :]])
    corners = jnp.stack([edge[:REACH], edge[width - REACH :]], 0)
    corners = jnp.transpose(corners, (2, 0, 1, 3))
    edge = jnp.transpose(edge.reshape(chunks, cells, 2, C), (0, 2, 1, 3))
    aug = jnp.concatenate(
        [
            jnp.zeros((width, rows, 1), BF16),
            jnp.transpose(noise, (2, 1, 0)),
            jnp.ones((width, rows, 1), BF16),
            jnp.zeros((width, rows, LANES - NOISE - 2), BF16),
        ],
        2,
    )
    conv, mixed, w1, w2, wd, small, trowh = stencil_fwd(
        mesh, height, x, share, cols, edge, corners, trow, table, aug, chunks
    )
    shards = (2,) * len(bit_list(mesh)) + (shard_rows, LANES)
    out, gconv, grow, gcol, gcorn, packed, extra = mlp(
        height, conv, g, x, w1, w2, small, shards, chunks
    )
    piece = -(-(flat_rows - TAIL_ROW) // devices)
    grad_in, grad, norm = backward(
        mesh, height, mixed, gconv, x, g, gcol, grow, gcorn, table, trowh, wd, small,
        extra, w1, packed, piece, 9,
    )
    grad_part = grad.reshape(shard)
    grad_norm = norm[0, :1]
    factor = 0.01 / jnp.maximum(grad_norm, 0.01)
    clipped = grad_part * factor
    new_one = 0.9 * moment_one + 0.1 * clipped
    new_two = 0.999 * moment_two + 0.001 * clipped * clipped
    step_float = step_count[0].astype(F32)
    fix_one = 1.0 - jnp.power(jnp.float32(0.9), step_float)
    fix_two = 1.0 - jnp.power(jnp.float32(0.999), step_float)
    update = new_one / fix_one / (jnp.sqrt(new_two / fix_two) + 1e-08) + 0.1 * master
    new_master = master - 0.02 * update
    new_avg = 0.9 * average + 0.1 * new_master
    return (
        jnp.transpose(out, (1, 0, 2)),
        jnp.transpose(grad_in, (1, 0, 2)),
        grad_part,
        grad_norm,
        new_master,
        new_one,
        new_two,
        new_avg,
        new_master.astype(BF16),
    )


def solution(mesh):
    flat = P(("lat", "lon"))
    field = P("lat", "lon", None)
    return jax.shard_map(
        partial(local, mesh),
        mesh=mesh,
        in_specs=(
            field, P(None, "lat", "lon"), field, P(), P("lat", None), P("lat", None, None),
            flat, flat, flat, flat, P(),
        ),
        out_specs=(field, field, flat, P(), flat, flat, flat, flat, flat),
        check_vma=False,
    )
```
